32 devices in a mesh: expert: 4 (over z), context: 8 (over y, x, core).
Axes of the slice: x: 2, y: 2, z: 4, core: 2. Of those that a mesh axis runs over, the one named last changes fastest.
Arguments:
- hidden_in: bfloat16 [4, 3072, 768], P('expert', 'context'), may hold values from -6 to 6
- prior_logits: float32 [4, 3072, 12], P('expert', 'context'), may hold values from -6 to 6
- routes: int32 [4, 3072, 2], P('expert', 'context'), may hold values from 0 to 11, all different within a row; in each aligned block of 384 rows (0 to 383, 384 to 767, ..., all dimensions but the last counted through in order) at most 96 rows name the same one
- block_ids: int32 [4, 3072], P('expert', 'context'), may hold values from 0 to 23, never falling along the last dimension, each value on 1 to 256 neighbouring positions
- grad_out: bfloat16 [4, 3072, 768], P('expert', 'context'), may hold values from -6 to 6
- attn_gain: float32 [768], replicated, may hold values from 0.25 to 1.75
- query_weight: bfloat16 [768, 768], P('context'), may hold values from -0.21875 to 0.21875
- key_weight: bfloat16 [768, 768], P('context'), may hold values from -0.21875 to 0.21875
- value_weight: bfloat16 [768, 768], P('context'), may hold values from -0.21875 to 0.21875
- output_weight: bfloat16 [768, 768], P('context'), may hold values from -0.875 to 0.875
- moe_gain: float32 [768], replicated, may hold values from 0.25 to 1.75
- router_weight: float32 [768, 12], replicated, may hold values from -0.109375 to 0.109375
- prior_weight: float32 [12, 12], replicated, may hold values from -0.875 to 0.875
- const_mix: float32 [2, 2, 768], replicated, may hold values from -0.21875 to 0.21875
- const_vector: float32 [2, 768], replicated, may hold values from -6 to 6
- gate_weight: bfloat16 [8, 768, 2048], P('expert', 'context'), may hold values from -0.21875 to 0.21875
- up_weight: bfloat16 [8, 768, 2048], P('expert', 'context'), may hold values from -0.21875 to 0.21875
- down_weight: bfloat16 [8, 2048, 768], P('expert', 'context'), may hold values from -1 to 1
Outputs:
- layer_out: bfloat16 [4, 3072, 768], P('expert', 'context')
- grad_input: float32 [4, 3072, 768], P('expert', 'context')
- grad_prior: float32 [4, 3072, 12], P('expert', 'context')
- grad_attn_gain: float32 [768], P('context')
- grad_query: float32 [768, 768], P('context')
- grad_key: float32 [768, 768], P('context')
- grad_value: float32 [768, 768], P('context')
- grad_output_weight: float32 [768, 768], P('context')
- grad_moe_gain: float32 [768], P('context')
- grad_router: float32 [768, 12], P('context')
- grad_prior_weight: float32 [12, 12], replicated
- grad_const_mix: float32 [2, 2, 768], P(None, None, 'context')
- grad_const_vector: float32 [2, 768], P(None, 'context')
- grad_gate: float32 [8, 768, 2048], P('expert', 'context')
- grad_up: float32 [8, 768, 2048], P('expert', 'context')
- grad_down: float32 [8, 2048, 768], P('expert', 'context')
The draws below stay inside these ranges and needn't reach their ends.
Inputs may be any that keep to these rules, and one draw needn't show every extreme that they name: `routes`: each token names two different experts; experts 0 to 7 are feed-forward, 8 the zero expert, 9 the copy expert, the rest constant experts. Among the 384 positions of one device (aligned blocks of 384 positions of a sequence), no expert is named by more than 96 tokens, and in some block one is named by exactly 96. `block_ids`: along a sequence the block id never falls; each id covers 1 to 256 consecutive positions, and some id covers exactly 256.
All inputs are finite; a program needn't handle non-finite values.
Results may differ from the reference program's by a relative error of at most 0.017.
Values may be sent and summed in bfloat16 or wider, within the bound.
A program may use at most 384 MiB of HBM per device.

```python
import math
import jax
import jax.numpy as jnp
import numpy as np
from jax import lax

D = 768
HEADS = 12
HEAD_DIM = 64
H = 2048
FFN_E = 8
NCONST = 2
BLOCK = 256
TOK_DEV = 384
NEXP = 12
CAP = 96
SEQS = 4
SEQLEN = 3072
N_CONTEXT = 8


def shard_levels(key, shape, pieces, least, largest):
    gain, own = 1.0, jax.random.fold_in(key, 6)
    for axis_at, blocks in pieces:
        heights = jnp.exp(jax.random.uniform(jax.random.fold_in(own, axis_at), (blocks,), jnp.float32, least / len(pieces), largest / len(pieces)))
        gain = gain * jnp.repeat(heights, shape[axis_at] // blocks).reshape([-1 if axis == axis_at else 1 for axis in range(len(shape))])
    return gain


def split_up(number_of, total, limit, slope):
    loads = [(1 << 20) // math.isqrt(grade ** slope) + 1 for grade in range(2, number_of + 1)]
    surplus, given = total - limit - (number_of - 1), [1] * (number_of - 1)
    while surplus > 0:
        candidates = [i for i in range(number_of - 1) if given[i] < limit]
        whole, budget = sum([loads[i] for i in candidates]), surplus
        for i in candidates:
            extra = min(limit - given[i], max(1, budget * loads[i] // whole), surplus)
            given[i] = given[i] + extra
            surplus = surplus - extra
    return np.array([limit] + given)


def uneven(own_key, number_of, total, most, slope):
    if number_of == 2:
        one = jax.random.randint(own_key, (), max(1, total - most), min(most, total - 1) + 1)
        return jnp.stack([one, total - one])
    tallies = jnp.asarray(split_up(number_of, total, most, slope), jnp.int32)
    couples = (number_of - 1) // 2
    donor, sink = tallies[1:1 + 2 * couples:2], tallies[2:2 + 2 * couples:2]
    room = jnp.minimum(donor - 1, most - sink)
    moved = jax.random.randint(jax.random.fold_in(own_key, 1), (couples,), 0, 1 << 20) % (room + 1)
    tallies = tallies.at[1:1 + 2 * couples:2].set(donor - moved).at[2:2 + 2 * couples:2].set(sink + moved)
    return tallies[jax.random.permutation(jax.random.fold_in(own_key, 2), number_of)]


def shared_out(key, own, number, rows, amount, top, most, skew):
    ranking = jax.random.permutation(key, amount)
    packed, ordinary = shares(amount, rows * top, most, skew, True), shares(amount, rows * top, most, skew, False)
    places = jnp.arange(amount)

    def named(lengths, rotation):
        used = int((lengths > 0).sum())
        fixed = max(1, used // 4)
        shifted = fixed + (places - fixed + rotation * (used - fixed)) % max(1, amount - fixed)
        return jnp.zeros((amount,), jnp.int32).at[ranking[jnp.where(places < fixed, places, shifted)]].set(jnp.asarray(lengths, jnp.int32))

    lengths = jnp.where(number % 4 == 0, named(packed, number // 4), named(ordinary, number - number // 4 - 1))
    mixed = jax.random.permutation(jax.random.fold_in(own, 3), amount)
    source_of, taker = mixed[0:amount // 2 * 2:2], mixed[1:amount // 2 * 2:2]
    room = jnp.minimum(lengths[source_of] - 1, most - lengths[taker]) // 2
    room = jnp.where((source_of == ranking[0]) | (taker == ranking[0]) | (lengths[taker] == 0), 0, jnp.maximum(room, 0))
    shifted = jax.random.randint(jax.random.fold_in(own, 4), (amount // 2,), 0, 1 << 20) % (room + 1)
    lengths = lengths.at[source_of].add(-shifted).at[taker].add(shifted)
    items = jnp.searchsorted(jnp.cumsum(lengths), jnp.arange(rows * top), side="right").astype(jnp.int32)
    grid = items.reshape(top, rows).T
    grid = grid[jax.random.permutation(jax.random.fold_in(own, 1), rows)]
    rotation = jax.random.randint(jax.random.fold_in(own, 2), (rows, 1), 0, top)
    return jnp.take_along_axis(grid, (jnp.arange(top)[None, :] + rotation) % top, axis=1)


def shares(count, total, reach, skew, full):
    loads = [(1 << 20) // math.isqrt(standing ** skew) + 1 for standing in range(1, count + 1)]
    largest = reach if full else min(reach, max(-(-total // count), total * loads[0] // sum(loads)))
    least = 1 if total - largest >= count - 1 else 0
    counts, spare = [largest] + [least] * (count - 1), total - largest - least * (count - 1)
    while spare > 0:
        candidates = [i for i in range(1, count) if counts[i] < largest] or [i for i in range(1, count) if counts[i] < reach]
        mass, left = sum([loads[i] for i in candidates]), spare
        for i in candidates:
            addition = min(reach - counts[i], max(1, left * loads[i] // mass), spare)
            counts[i] = counts[i] + addition
            spare = spare - addition
    return np.array(counts)


def gaussian(rng, dims, scale, limit, cuts=(), kind=jnp.bfloat16):
    gain = shard_levels(rng, dims, cuts, -0.22, 0.18) if cuts else 1.0
    values = jax.random.normal(rng, dims, jnp.float32) * scale * gain
    return jnp.minimum(jnp.maximum(values, -limit), limit).astype(kind)


def setup_inputs(seed: int = 0) -> dict:
    streams_of = jax.random.split(jax.random.key(seed), 19)
    hidden_in = gaussian(streams_of[0], (SEQS, SEQLEN, D), 1.0, 6.0, ((0, 4), (1, 8)))
    prior_logits = gaussian(streams_of[1], (SEQS, SEQLEN, NEXP), 1.0, 6.0, ((0, 4), (1, 8)), jnp.float32)
    routes_keys = jax.random.split(jax.random.fold_in(streams_of[2], 1), SEQS * SEQLEN // TOK_DEV)
    routes_turns = jax.random.permutation(jax.random.fold_in(streams_of[2], 3), SEQS * SEQLEN // TOK_DEV)
    routes = jax.vmap(lambda own, number: shared_out(jax.random.fold_in(streams_of[2], 2), own, number, TOK_DEV, NEXP, 2, CAP, 2))(routes_keys, routes_turns).reshape((SEQS, SEQLEN, 2))
    block_ids = jax.vmap(lambda own: jnp.searchsorted(jnp.cumsum(uneven(own, 2 * SEQLEN // BLOCK, SEQLEN, BLOCK, 1)), jnp.arange(SEQLEN), side="right"))(jax.random.split(streams_of[3], SEQS)).reshape((SEQS, SEQLEN)).astype(jnp.int32)
    grad_out = gaussian(streams_of[4], (SEQS, SEQLEN, D), 1.0, 6.0, ((0, 4), (1, 8)))
    attn_gain = jnp.clip(1.0 + 0.15 * jax.random.normal(streams_of[5], (D,), jnp.float32), 0.25, 1.75)
    query_weight = gaussian(streams_of[6], (D, D), D ** -0.5, 0.21875, ((0, 8),))
    key_weight = gaussian(streams_of[7], (D, D), D ** -0.5, 0.21875, ((0, 8),))
    value_weight = gaussian(streams_of[8], (D, D), D ** -0.5, 0.21875, ((0, 8),))
    output_weight = gaussian(streams_of[9], (D, D), (D // 16) ** -0.5, 0.875, ((0, 8),))
    moe_gain = jnp.clip(1.0 + 0.15 * jax.random.normal(streams_of[10], (D,), jnp.float32), 0.25, 1.75)
    router_weight = gaussian(streams_of[11], (D, NEXP), (4 * D) ** -0.5, 0.109375, (), jnp.float32)
    prior_weight = gaussian(streams_of[12], (NEXP, NEXP), (4 * NEXP) ** -0.5, 0.875, (), jnp.float32)
    const_mix = gaussian(streams_of[13], (NCONST, 2, D), D ** -0.5, 0.21875, (), jnp.float32)
    const_vector = gaussian(streams_of[14], (NCONST, D), 1.0, 6.0, (), jnp.float32)
    gate_weight = gaussian(streams_of[15], (FFN_E, D, H), D ** -0.5, 0.21875, ((0, 4), (1, 8)))
    up_weight = gaussian(streams_of[16], (FFN_E, D, H), D ** -0.5, 0.21875, ((0, 4), (1, 8)))
    down_weight = gaussian(streams_of[17], (FFN_E, H, D), (max(H // 64, 1)) ** -0.5, 1.0, ((0, 4), (1, 8)))
    return {"hidden_in": hidden_in, "prior_logits": prior_logits, "routes": routes, "block_ids": block_ids, "grad_out": grad_out, "attn_gain": attn_gain, "query_weight": query_weight, "key_weight": key_weight, "value_weight": value_weight, "output_weight": output_weight, "moe_gain": moe_gain, "router_weight": router_weight, "prior_weight": prior_weight, "const_mix": const_mix, "const_vector": const_vector, "gate_weight": gate_weight, "up_weight": up_weight, "down_weight": down_weight}


EPS = 1e-06
THETA = 10000.0
HIGH = lax.Precision.HIGHEST

@jax.custom_vjp
def low(v):
    return lax.optimization_barrier(v.astype(jnp.bfloat16)).astype(jnp.float32)

@jax.custom_vjp
def low_back(v):
    return v

def low_keep(v):
    return (low(v), None)

def low_pass(kept, grad):
    return (grad,)

def back_keep(v):
    return (v, None)

def back_low(kept, grad):
    return (low(grad),)
low.defvjp(low_keep, low_pass)
low_back.defvjp(back_keep, back_low)

def matmul(left, right):
    return jnp.dot(left, right, precision=HIGH, preferred_element_type=jnp.float32)

def rope_tables(positions, head_size):
    half = head_size // 2
    freq = jnp.power(THETA, -2.0 * jnp.arange(half, dtype=jnp.float32) / head_size)
    angle = positions.astype(jnp.float32)[:, None] * freq[None, :]
    return (jnp.cos(angle)[:, None, :], jnp.sin(angle)[:, None, :])

def rotate(field, cos_table, sin_table):
    half = field.shape[-1] // 2
    first = field[..., :half]
    second = field[..., half:]
    return jnp.concatenate([first * cos_table - second * sin_table, second * cos_table + first * sin_table], axis=-1)

def forward_seq(params, inputs, prior_rows, route_rows, seq_ids):
    attn_gain, query_weight, key_weight, value_weight, output_weight, moe_gain, router_weight, prior_weight, const_mix, const_vector, gate_weight, up_weight, down_weight = params
    length = inputs.shape[0]
    inv_rms1 = lax.rsqrt(lax.optimization_barrier(jnp.mean(inputs * inputs, axis=1, keepdims=True)) + EPS)
    attn_input = low(inputs * inv_rms1 * attn_gain)
    query_pre = low_back(matmul(attn_input, query_weight))
    key_pre = low_back(matmul(attn_input, key_weight))
    value_low = low(low_back(matmul(attn_input, value_weight)))
    cos_table, sin_table = rope_tables(jnp.arange(length, dtype=jnp.int32), HEAD_DIM)
    query_heads = low(rotate(query_pre.reshape(length, HEADS, HEAD_DIM), cos_table, sin_table))
    key_heads = low(rotate(key_pre.reshape(length, HEADS, HEAD_DIM), cos_table, sin_table))
    value_heads = value_low.reshape(length, HEADS, HEAD_DIM)
    score_scale = HEAD_DIM ** (-0.5)
    blocks = length // TOK_DEV

    def attend(block_args):
        query_block, id_block = block_args
        scores = low_back(jnp.einsum('qhd,khd->hqk', query_block, key_heads, precision=HIGH) * score_scale)
        allowed = seq_ids[None, None, :] <= id_block[None, :, None]
        scores = jnp.where(allowed, scores, -1e+30)
        weights = low(jax.nn.softmax(scores, axis=-1))
        return jnp.einsum('hqk,khd->qhd', weights, value_heads, precision=HIGH)
    mixed = lax.map(jax.checkpoint(attend), (query_heads.reshape(blocks, TOK_DEV, HEADS, HEAD_DIM), seq_ids.reshape(blocks, TOK_DEV)))
    mix_low = low(low_back(mixed.reshape(length, HEADS * HEAD_DIM)))
    after_attn = inputs + low_back(matmul(mix_low, output_weight))
    inv_rms2 = lax.rsqrt(lax.optimization_barrier(jnp.mean(after_attn * after_attn, axis=1, keepdims=True)) + EPS)
    moe_input = after_attn * inv_rms2 * moe_gain
    logits = matmul(moe_input, router_weight) + matmul(prior_rows, prior_weight)
    probs = jax.nn.softmax(logits, axis=-1)
    expert_ids = jnp.arange(logits.shape[1], dtype=jnp.int32)
    route_hits = ((route_rows[:, 0:1] == expert_ids[None, :]) | (route_rows[:, 1:2] == expert_ids[None, :])).astype(jnp.int32)
    gated = probs * route_hits.astype(jnp.float32)
    const_soft = jax.nn.softmax(jnp.einsum('td,cjd->tcj', moe_input, const_mix, precision=HIGH), axis=-1)
    const_out = const_soft[:, :, 0:1] * moe_input[:, None, :] + const_soft[:, :, 1:2] * const_vector[None, :, :]
    moe_total = gated[:, FFN_E + 1:FFN_E + 2] * moe_input + jnp.einsum('tc,tcd->td', gated[:, FFN_E + 2:], const_out, precision=HIGH)
    rows_low = low(moe_input)
    bound = N_CONTEXT * CAP
    for expert in range(FFN_E):
        index = jnp.nonzero(route_hits[:, expert], size=bound, fill_value=0)[0].astype(jnp.int32)
        valid = (jnp.arange(bound, dtype=jnp.int32) < jnp.sum(route_hits[:, expert])).astype(jnp.float32)
        rows = low_back(rows_low[index])
        gate_pre = low_back(matmul(rows, gate_weight[expert]))
        up_pre = low_back(matmul(rows, up_weight[expert]))
        hidden_low = low(low_back(jax.nn.silu(gate_pre) * up_pre))
        out_rows = low(low_back(matmul(hidden_low, down_weight[expert])))
        factor = valid * probs[index, expert]
        moe_total = moe_total + jnp.zeros_like(moe_input).at[index].add(out_rows * factor[:, None])
    return after_attn + moe_total

def reference(hidden_in, prior_logits, routes, block_ids, grad_out, attn_gain, query_weight, key_weight, value_weight, output_weight, moe_gain, router_weight, prior_weight, const_mix, const_vector, gate_weight, up_weight, down_weight):
    params = tuple((item.astype(jnp.float32) for item in (attn_gain, query_weight, key_weight, value_weight, output_weight, moe_gain, router_weight, prior_weight, const_mix, const_vector, gate_weight, up_weight, down_weight)))

    def seq_step(totals, item):
        inputs, prior_rows, route_rows, seq_ids, cotangent = item

        def forward(param_set, input_rows, prior_set):
            return forward_seq(param_set, input_rows, prior_set, route_rows, seq_ids)
        result, pullback = jax.vjp(forward, params, inputs.astype(jnp.float32), prior_rows)
        grad_params, grad_rows, grad_prior_rows = pullback(cotangent.astype(jnp.float32))
        totals = jax.tree.map(lambda left, right: left + right, totals, grad_params)
        return (totals, (result.astype(jnp.bfloat16), grad_rows, grad_prior_rows))
    zeros = jax.tree.map(jnp.zeros_like, params)
    totals, (layer_out, grad_input, grad_prior) = lax.scan(seq_step, zeros, (hidden_in, prior_logits, routes, block_ids, grad_out))
    return (layer_out, grad_input, grad_prior, totals[0], totals[1], totals[2], totals[3], totals[4], totals[5], totals[6], totals[7], totals[8], totals[9], totals[10], totals[11], totals[12])
```

```python
import functools
import math

import jax
import jax.numpy as jnp
from jax import lax
from jax.experimental import pallas as pl
from jax.experimental.pallas import tpu as pltpu
from jax.sharding import PartitionSpec as P

HEADS = 12
FFN_E = 8
CAP = 96
TILE = 256
EXTRA = 16
HIDDEN_TILE = 256

EPS = 1e-06
THETA = 10000.0
NEGATIVE = -1e30
HIGH = lax.Precision.HIGHEST
F32 = jnp.float32
BF16 = jnp.bfloat16


def dot(left, right, left_dim=1, right_dim=0):
    return lax.dot_general(
        left, right, (((left_dim,), (right_dim,)), ((), ())), preferred_element_type=F32
    )


def turn(rows, cos_rows, sin_rows, heads, size, back=False):
    half = size // 2
    parts = []
    for head in range(heads):
        first = rows[head * size : head * size + half]
        second = rows[head * size + half : (head + 1) * size]
        if back:
            parts.append(first * cos_rows + second * sin_rows)
            parts.append(second * cos_rows - first * sin_rows)
        else:
            parts.append(first * cos_rows - second * sin_rows)
            parts.append(second * cos_rows + first * sin_rows)
    return jnp.concatenate(parts, axis=0)


def own_tile(index, ranks):
    rank = lax.rem(lax.axis_index("context"), ranks)
    place = lax.rem(index, 2)
    return (index // 2) * (2 * ranks) + jnp.where(place == 0, rank, 2 * ranks - 1 - rank)


def lanes(start):
    return pl.ds(pl.multiple_of(start * TILE, TILE), TILE)


def attn_forward_kernel(
    heads, size, ranks, scale,
    a_ref, wt_ref, cos_ref, sin_ref, ids_col_ref, ids_row_ref,
    out_ref, out_t_ref, lse_ref, query_t_ref, key_ref, key_t_ref, value_ref,
    value_t_ref, scores_ref, acc_ref,
):
    length = a_ref.shape[0]
    width = heads * size
    tiles = length // TILE
    own_tiles = tiles // ranks
    ext = size + EXTRA
    tail = (lax.broadcasted_iota(jnp.int32, (EXTRA, TILE), 0) == 0).astype(BF16)

    def project(step, carry):
        at = lanes(step)
        both = dot(wt_ref[width:, :], a_ref[at, :], 1, 1)
        key_t = turn(both[:width], cos_ref[:, at], sin_ref[:, at], heads, size)
        key_t_ref[:, at] = key_t.astype(BF16)
        value_t = both[width:]
        for head in range(heads):
            rows = slice(head * size, (head + 1) * size)
            key_ref[head, at, :] = key_t[rows].T.astype(BF16)
            value_ref[head, at, :] = value_t[rows].T.astype(BF16)
            value_t_ref[head * ext : head * ext + size, at] = value_t[rows].astype(BF16)
            value_t_ref[head * ext + size : (head + 1) * ext, at] = tail
        return carry

    lax.fori_loop(0, tiles, project, 0)

    def attend(index, carry):
        tile = own_tile(index, ranks)
        at = lanes(tile)
        query_t = dot(wt_ref[:width, :], a_ref[at, :], 1, 1)
        query_t = turn(query_t, cos_ref[:, at], sin_ref[:, at], heads, size)
        query_t = query_t.astype(BF16) * jnp.asarray(scale, BF16)
        query_t_ref[:, lanes(index)] = query_t
        query_ids = ids_row_ref[:, at]

        def score(step, tops, masked):
            here = lanes(step)
            fresh = []
            if masked:
                allowed = ids_col_ref[here, :] <= query_ids
            for head in range(heads):
                part = dot(key_ref[head, here, :], query_t[head * size : (head + 1) * size])
                if masked:
                    part = jnp.where(allowed, part, NEGATIVE)
                scores_ref[head, here, :] = part
                fresh.append(
                    jnp.maximum(tops[head], jnp.max(part.reshape(TILE // 8, 8, TILE), axis=0))
                )
            return tuple(fresh)

        tops = tuple(jnp.full((8, TILE), NEGATIVE, F32) for _ in range(heads))
        stop = jnp.minimum(tile + 2, tiles)
        tops = lax.fori_loop(0, tile, lambda s, c: score(s, c, False), tops)
        tops = lax.fori_loop(tile, stop, lambda s, c: score(s, c, True), tops)
        peaks = [jnp.max(top, axis=0, keepdims=True) for top in tops]
        acc_ref[...] = jnp.zeros_like(acc_ref)

        def combine(step, carry):
            here = lanes(step)
            for head in range(heads):
                weights = jnp.exp(scores_ref[head, here, :] - peaks[head]).astype(BF16)
                acc_ref[head] += dot(value_t_ref[head * ext : (head + 1) * ext, here], weights)
            return carry

        lax.fori_loop(0, stop, combine, 0)
        parts = []
        for head in range(heads):
            total = acc_ref[head, size : size + 1, :]
            part = acc_ref[head, :size, :] * (1.0 / total)
            lse_ref[head : head + 1, lanes(index)] = peaks[head] + jnp.log(total)
            parts.append(part)
        joined = jnp.concatenate(parts, axis=0)
        out_t_ref[:, lanes(index)] = joined
        out_ref[lanes(index), :] = joined.T.astype(BF16)
        return carry

    lax.fori_loop(0, own_tiles, attend, 0)


def attn_backward_kernel(
    heads, size, ranks, scale,
    grad_ref, a_ref, wt_ref, cos_ref, sin_ref, ids_col_ref, ids_row_ref,
    out_t_ref, lse_ref, query_t_ref, key_ref, key_t_ref, value_ref,
    da_ref, grad_w_ref,
    query_ref, own_grad_ref, dq_ref, dk_ref, dv_ref,
):
    length = a_ref.shape[0]
    width = heads * size
    tiles = length // TILE
    own_tiles = tiles // ranks
    dk_ref[...] = jnp.zeros_like(dk_ref)
    dv_ref[...] = jnp.zeros_like(dv_ref)
    da_ref[...] = jnp.zeros_like(da_ref)
    grad_w_ref[...] = jnp.zeros_like(grad_w_ref)

    def attend(index, carry):
        tile = own_tile(index, ranks)
        at = lanes(tile)
        query_t = query_t_ref[:, lanes(index)]
        grad_rows = grad_ref[lanes(index), :]
        grad_t = grad_rows.astype(F32).T
        query_rows = query_t.astype(F32).T.astype(BF16)
        query_ids = ids_row_ref[:, at]
        deltas, tops, grads_low = [], [], []
        for head in range(heads):
            rows = slice(head * size, (head + 1) * size)
            query_ref[head] = query_rows[:, rows]
            own_grad_ref[head] = grad_rows[:, rows]
            deltas.append(
                jnp.sum(grad_t[rows] * out_t_ref[rows, lanes(index)], axis=0, keepdims=True)
            )
            tops.append(lse_ref[head : head + 1, lanes(index)])
        grad_t_low = grad_t.astype(BF16)
        dq_ref[...] = jnp.zeros_like(dq_ref)

        def chunk(step, carry, masked):
            here = lanes(step)
            if masked:
                allowed = ids_col_ref[here, :] <= query_ids
            for head in range(heads):
                rows = slice(head * size, (head + 1) * size)
                scores = dot(key_ref[head, here, :], query_t[rows]) - tops[head]
                if masked:
                    scores = jnp.where(allowed, scores, NEGATIVE)
                probs = jnp.exp(scores)
                grad_probs = dot(value_ref[head, here, :], grad_t_low[rows])
                grad_scores = (probs * (grad_probs - deltas[head])).astype(BF16)
                dv_ref[head, here, :] += dot(probs.astype(BF16), own_grad_ref[head])
                dk_ref[head, here, :] += dot(grad_scores, query_ref[head])
                dq_ref[rows, :] += dot(key_t_ref[rows, here], grad_scores)
            return carry

        stop = jnp.minimum(tile + 2, tiles)
        lax.fori_loop(0, tile, lambda s, c: chunk(s, c, False), 0)
        lax.fori_loop(tile, stop, lambda s, c: chunk(s, c, True), 0)
        grad_query = turn(
            dq_ref[...] * scale, cos_ref[:, at], sin_ref[:, at], heads, size, back=True
        )
        grad_w_ref[:width, :] += dot(grad_query.astype(BF16), a_ref[at, :])
        da_ref[at, :] = dot(grad_query.T.astype(BF16), wt_ref[:width, :]).astype(BF16)
        return carry

    lax.fori_loop(0, own_tiles, attend, 0)

    def finish(step, carry):
        at = lanes(step)
        key_grad = jnp.concatenate([dk_ref[head, at, :].T for head in range(heads)], axis=0)
        key_grad = turn(key_grad, cos_ref[:, at], sin_ref[:, at], heads, size, back=True)
        value_grad = jnp.concatenate([dv_ref[head, at, :].T for head in range(heads)], axis=0)
        both = jnp.concatenate([key_grad, value_grad], axis=0)
        grad_w_ref[width:, :] += dot(both.astype(BF16), a_ref[at, :])
        total = da_ref[at, :].astype(F32) + dot(both.T.astype(BF16), wt_ref[width:, :])
        da_ref[at, :] = total.astype(BF16)
        return carry

    lax.fori_loop(0, tiles, finish, 0)


def expert_kernel(
    rows_ref, grad_ref, prob_ref, gate_ref, up_ref, down_ref,
    out_ref, grad_rows_ref, dot_ref, grad_gate_ref, grad_up_ref, grad_down_ref,
    rows_t_ref, dye_ref, out_acc_ref, grad_acc_ref,
):
    step = pl.program_id(1)

    @pl.when(step == 0)
    def _():
        rows_t_ref[...] = rows_ref[:, 0].reshape(dye_ref.shape).astype(F32).T.astype(BF16)
        grads = grad_ref[:, 0].reshape(dye_ref.shape).astype(F32)
        dye_ref[...] = (grads * prob_ref[0]).astype(BF16)
        out_acc_ref[...] = jnp.zeros_like(out_acc_ref)
        grad_acc_ref[...] = jnp.zeros_like(grad_acc_ref)

    rows = rows_ref[:, 0].reshape(dye_ref.shape)
    dye = dye_ref[...]
    gate = gate_ref[0]
    up = up_ref[0]
    down = down_ref[0]
    gate_pre = dot(rows, gate)
    up_pre = dot(rows, up)
    sigmoid = jax.nn.sigmoid(gate_pre)
    silu = gate_pre * sigmoid
    hidden = silu * up_pre
    hidden_low = hidden.astype(BF16)
    out_acc_ref[...] += dot(hidden_low, down)
    grad_hidden = dot(dye, down, 1, 1).astype(BF16).astype(F32)
    grad_down_ref[0] = dot(hidden.T.astype(BF16), dye).astype(BF16)
    grad_gate = (grad_hidden * up_pre * sigmoid * (1.0 + gate_pre * (1.0 - sigmoid))).astype(BF16)
    grad_up = (grad_hidden * silu).astype(BF16)
    grad_gate_ref[0] = dot(rows_t_ref[...], grad_gate).astype(BF16)
    grad_up_ref[0] = dot(rows_t_ref[...], grad_up).astype(BF16)
    grad_acc_ref[...] += dot(grad_gate, gate, 1, 1) + dot(grad_up, up, 1, 1)

    @pl.when(step == pl.num_programs(1) - 1)
    def _():
        out_low = out_acc_ref[...].astype(BF16)
        blocks = out_ref.shape[:1] + out_ref.shape[2:]
        out_ref[:, 0] = out_low.reshape(blocks)
        grad_rows_ref[:, 0] = grad_acc_ref[...].astype(BF16).reshape(blocks)
        grads = grad_ref[:, 0].reshape(dye_ref.shape).astype(F32)
        dot_ref[0] = jnp.sum(out_low.astype(F32) * grads, axis=1, keepdims=True)


def vmem(count):
    return [pl.BlockSpec(memory_space=pltpu.VMEM)] * count


def attn_forward(a_full, weights_t, cos_t, sin_t, ids, heads, size, ranks):
    length = a_full.shape[0]
    own = length // ranks
    width = heads * size
    ext = size + EXTRA
    shapes = (
        jax.ShapeDtypeStruct((own, width), BF16),
        jax.ShapeDtypeStruct((width, own), F32),
        jax.ShapeDtypeStruct((heads, own), F32),
        jax.ShapeDtypeStruct((width, own), BF16),
        jax.ShapeDtypeStruct((heads, length, size), BF16),
        jax.ShapeDtypeStruct((width, length), BF16),
        jax.ShapeDtypeStruct((heads, length, size), BF16),
    )
    return pl.pallas_call(
        functools.partial(attn_forward_kernel, heads, size, ranks, size ** (-0.5)),
        out_shape=shapes,
        in_specs=vmem(6),
        out_specs=vmem(7),
        scratch_shapes=[
            pltpu.VMEM((heads * ext, length), BF16),
            pltpu.VMEM((heads, length, TILE), F32),
            pltpu.VMEM((heads, ext, TILE), F32),
        ],
        compiler_params=pltpu.CompilerParams(vmem_limit_bytes=60 << 20),
        cost_estimate=cost(37),
        name="attn_forward",
    )(a_full, weights_t, cos_t, sin_t, ids[:, None], ids[None, :])


def attn_backward(grad_full, a_full, weights_t, cos_t, sin_t, ids, kept, heads, size, ranks):
    length = a_full.shape[0]
    width = heads * size
    shapes = (
        jax.ShapeDtypeStruct(a_full.shape, BF16),
        jax.ShapeDtypeStruct(weights_t.shape, F32),
    )
    return pl.pallas_call(
        functools.partial(attn_backward_kernel, heads, size, ranks, size ** (-0.5)),
        out_shape=shapes,
        in_specs=vmem(13),
        out_specs=vmem(2),
        scratch_shapes=[
            pltpu.VMEM((heads, TILE, size), BF16),
            pltpu.VMEM((heads, TILE, size), BF16),
            pltpu.VMEM((width, TILE), F32),
            pltpu.VMEM((heads, length, size), F32),
            pltpu.VMEM((heads, length, size), F32),
        ],
        compiler_params=pltpu.CompilerParams(vmem_limit_bytes=63 << 20),
        cost_estimate=cost(58),
        name="attn_backward",
    )(grad_full, a_full, weights_t, cos_t, sin_t, ids[:, None], ids[None, :], *kept)


def experts(rows, grads, gates, gate_full, up_full, down_full):
    owners, count, cap, width = rows.shape
    slots = owners * cap
    hidden = gate_full.shape[2]
    per_row = pl.BlockSpec((owners, 1, cap, width), lambda e, t: (0, e, 0, 0))
    column = pl.BlockSpec((1, slots, 1), lambda e, t: (e, 0, 0))
    wide = pl.BlockSpec((1, width, HIDDEN_TILE), lambda e, t: (e, 0, t))
    tall = pl.BlockSpec((1, HIDDEN_TILE, width), lambda e, t: (e, t, 0))
    return pl.pallas_call(
        expert_kernel,
        grid=(count, hidden // HIDDEN_TILE),
        out_shape=(
            jax.ShapeDtypeStruct(rows.shape, BF16),
            jax.ShapeDtypeStruct(rows.shape, BF16),
            jax.ShapeDtypeStruct((count, slots, 1), F32),
            jax.ShapeDtypeStruct(gate_full.shape, BF16),
            jax.ShapeDtypeStruct(up_full.shape, BF16),
            jax.ShapeDtypeStruct(down_full.shape, BF16),
        ),
        in_specs=[per_row, per_row, column, wide, wide, tall],
        out_specs=(per_row, per_row, column, wide, wide, tall),
        scratch_shapes=[
            pltpu.VMEM((width, slots), BF16),
            pltpu.VMEM((slots, width), BF16),
            pltpu.VMEM((slots, width), F32),
            pltpu.VMEM((slots, width), F32),
        ],
        compiler_params=pltpu.CompilerParams(vmem_limit_bytes=60 << 20),
        cost_estimate=cost(37),
        name="experts",
    )(rows, grads, gates, gate_full, up_full, down_full)


def cost(micros):
    return pl.CostEstimate(flops=micros * 1_150_000_000, bytes_accessed=0, transcendentals=0)


def swap_kernel(axis, stride, count, same, *refs):
    total = len(same)
    sources, targets = refs[:total], refs[total : 2 * total]
    local_sem, send_sem, recv_sem = refs[2 * total :]
    place = lax.axis_index(axis)
    mine = lax.rem(place // stride, count)
    barrier = pltpu.get_barrier_semaphore()
    for far in range(1, count):
        peer = lax.rem(mine + far, count)
        pl.semaphore_signal(
            barrier, inc=1, device_id={axis: place + (peer - mine) * stride},
            device_id_type=pl.DeviceIdType.MESH,
        )
    pl.semaphore_wait(barrier, count - 1)
    copies = []
    for item in range(total):
        for far in range(1, count):
            peer = lax.rem(mine + far, count)
            copies.append(
                pltpu.make_async_remote_copy(
                    src_ref=sources[item] if same[item] else sources[item].at[peer],
                    dst_ref=targets[item].at[mine],
                    send_sem=send_sem.at[item, far],
                    recv_sem=recv_sem.at[item, far],
                    device_id={axis: place + (peer - mine) * stride},
                    device_id_type=pl.DeviceIdType.MESH,
                )
            )
            copies[-1].start()
    for item in range(total):
        copies.append(
            pltpu.make_async_copy(
                sources[item] if same[item] else sources[item].at[mine],
                targets[item].at[mine],
                local_sem.at[item],
            )
        )
        copies[-1].start()
    for copy in copies:
        copy.wait()


def swap(arrays, axis, stride, count, number, same=None):
    same = same or (False,) * len(arrays)
    shapes = tuple(
        jax.ShapeDtypeStruct(((count,) if own else ()) + array.shape, array.dtype)
        for array, own in zip(arrays, same)
    )
    return pl.pallas_call(
        functools.partial(swap_kernel, axis, stride, count, same),
        out_shape=shapes,
        in_specs=vmem(len(arrays)),
        out_specs=vmem(len(arrays)),
        scratch_shapes=[
            pltpu.SemaphoreType.DMA((len(arrays),)),
            pltpu.SemaphoreType.DMA((len(arrays), count)),
            pltpu.SemaphoreType.DMA((len(arrays), count)),
        ],
        compiler_params=pltpu.CompilerParams(
            collective_id=number, has_side_effects=True, vmem_limit_bytes=60 << 20
        ),
        name="swap",
    )(*arrays)


def gather_kernel(chips, ranks, split, *refs):
    total = len(split)
    sources, targets = refs[:total], refs[total : 2 * total]
    local_sem, send_sem, recv_sem, pass_sem, land_sem = refs[2 * total :]
    place = lax.axis_index("context")
    chip, core = place // 2, lax.rem(place, 2)
    partner = 2 * chip + 1 - core

    def piece(item, device):
        return sources[item].at[device // ranks] if split[item] else sources[item]

    def remote(source, target, send, recv, device):
        return pltpu.make_async_remote_copy(
            src_ref=source, dst_ref=target, send_sem=send, recv_sem=recv,
            device_id={"context": device}, device_id_type=pl.DeviceIdType.MESH,
        )

    barrier = pltpu.get_barrier_semaphore()
    for far in range(1, chips):
        pl.semaphore_signal(
            barrier, inc=1, device_id={"context": 2 * lax.rem(chip + far, chips) + core},
            device_id_type=pl.DeviceIdType.MESH,
        )
    pl.semaphore_signal(
        barrier, inc=1, device_id={"context": partner}, device_id_type=pl.DeviceIdType.MESH
    )
    pl.semaphore_wait(barrier, chips)
    sent = {}
    for item in range(total):
        for far in range(chips):
            peer = partner if far == 0 else 2 * lax.rem(chip + far, chips) + core
            sent[item, far] = remote(
                piece(item, peer), targets[item].at[place],
                send_sem.at[item, far], recv_sem.at[item, far], peer,
            )
            sent[item, far].start()
    local = []
    for item in range(total):
        local.append(
            pltpu.make_async_copy(
                piece(item, place), targets[item].at[place], local_sem.at[item]
            )
        )
        local[-1].start()
    passed = []
    for item in range(total):
        for far in range(1, chips):
            sent[item, far].wait_recv()
            block = targets[item].at[2 * lax.rem(chip + chips - far, chips) + core]
            passed.append(
                remote(block, block, pass_sem.at[item, far], land_sem.at[item, far], partner)
            )
            passed[-1].start()
    for item in range(total):
        sent[item, 0].wait_recv()
        for far in range(chips):
            sent[item, far].wait_send()
    for copy in local + passed:
        copy.wait()


def gather(arrays, split, context, ranks, number):
    chips = context // 2
    total = len(arrays)
    shapes = tuple(
        jax.ShapeDtypeStruct((context,) + (array.shape[1:] if cut else array.shape), array.dtype)
        for array, cut in zip(arrays, split)
    )
    return pl.pallas_call(
        functools.partial(gather_kernel, chips, ranks, split),
        out_shape=shapes,
        in_specs=vmem(total),
        out_specs=vmem(total),
        scratch_shapes=[pltpu.SemaphoreType.DMA((total,))]
        + [pltpu.SemaphoreType.DMA((total, chips))] * 4,
        compiler_params=pltpu.CompilerParams(
            collective_id=number, has_side_effects=True, vmem_limit_bytes=60 << 20
        ),
        name="gather",
    )(*arrays)


def granule_kernel(ranks, shard_granules, outward, source_ref, target_ref, send_sem, recv_sem):
    place = lax.axis_index("context")
    context = lax.axis_size("context")
    group, rank = place // ranks, lax.rem(place, ranks)
    groups = context // ranks
    owned = context * shard_granules // ranks
    barrier = pltpu.get_barrier_semaphore()
    for far in range(1, context):
        pl.semaphore_signal(
            barrier, inc=1, device_id={"context": lax.rem(place + far, context)},
            device_id_type=pl.DeviceIdType.MESH,
        )
    pl.semaphore_wait(barrier, context - 1)

    def owner_rank(granule):
        spot = lax.rem(granule // 2, 2 * ranks)
        return jnp.minimum(spot, 2 * ranks - 1 - spot)

    def owner_slot(granule):
        tile = granule // 2
        spot = lax.rem(tile, 2 * ranks)
        upper = jnp.where(spot >= ranks, 1, 0)
        return (tile // (2 * ranks) * 2 + upper) * 2 + lax.rem(granule, 2)

    def granule_of(slot):
        return own_tile(slot // 2, ranks) * 2 + lax.rem(slot, 2)

    def remote(source, target, index, device):
        return pltpu.make_async_remote_copy(
            src_ref=source, dst_ref=target, send_sem=send_sem.at[index],
            recv_sem=recv_sem.at[index], device_id={"context": device},
            device_id_type=pl.DeviceIdType.MESH,
        )

    def outgoing(step):
        if outward:
            granule = granule_of(step)
            home = granule // shard_granules
            slot = group * shard_granules + lax.rem(granule, shard_granules)
            return home, source_ref.at[step], slot
        other, spot = step // shard_granules, step % shard_granules
        granule = place * shard_granules + spot
        return other * ranks + owner_rank(granule), source_ref.at[step], owner_slot(granule)

    def incoming(step):
        if outward:
            other, spot = step // shard_granules, step % shard_granules
            return other * ranks + owner_rank(place * shard_granules + spot)
        return granule_of(step) // shard_granules

    for step in range(owned):
        device, source, slot = outgoing(step)

        @pl.when(device == place)
        def _():
            pltpu.make_async_copy(source, target_ref.at[slot], recv_sem.at[slot]).start()

        @pl.when(device != place)
        def _():
            pltpu.make_async_remote_copy(
                src_ref=source, dst_ref=target_ref.at[slot], send_sem=send_sem.at[step],
                recv_sem=recv_sem.at[slot], device_id={"context": device},
                device_id_type=pl.DeviceIdType.MESH,
            ).start()

    for step in range(owned):
        device, source, slot = outgoing(step)

        @pl.when(device != place)
        def _():
            remote(source, target_ref.at[slot], step, device).wait_send()

        sender = incoming(step)

        @pl.when(sender == place)
        def _():
            pltpu.make_async_copy(source_ref.at[0], target_ref.at[step], recv_sem.at[step]).wait()

        @pl.when(sender != place)
        def _():
            remote(source_ref.at[0], target_ref.at[step], step, sender).wait_recv()


def granules(rows, ranks, shard_granules, outward, number):
    owned = rows.shape[0]
    return pl.pallas_call(
        functools.partial(granule_kernel, ranks, shard_granules, outward),
        out_shape=jax.ShapeDtypeStruct(rows.shape, rows.dtype),
        in_specs=vmem(1),
        out_specs=vmem(1)[0],
        scratch_shapes=[
            pltpu.SemaphoreType.DMA((owned,)),
            pltpu.SemaphoreType.DMA((owned,)),
        ],
        compiler_params=pltpu.CompilerParams(
            collective_id=number, has_side_effects=True, vmem_limit_bytes=60 << 20
        ),
        name="granules",
    )(rows)


def exchange(value, axis_name, axis):
    return lax.all_to_all(value, axis_name, split_axis=axis, concat_axis=axis, tiled=True)


def shards(
    hidden_in,
    prior_logits,
    routes,
    block_ids,
    grad_out,
    attn_gain,
    query_weight,
    key_weight,
    value_weight,
    output_weight,
    moe_gain,
    router_weight,
    prior_weight,
    const_mix,
    const_vector,
    gate_weight,
    up_weight,
    down_weight,
):
    token_rows = hidden_in.shape[1]
    model_width = hidden_in.shape[2]
    head_size = model_width // HEADS
    context = lax.axis_size("context")
    owners = lax.axis_size("expert")
    groups = math.gcd(HEADS, context)
    ranks = context // groups
    heads = HEADS // groups
    width = heads * head_size
    length = context * token_rows
    per_owner = gate_weight.shape[0]
    slot_count = per_owner * owners * CAP
    shard_width = model_width // context
    residual = hidden_in[0].astype(F32)
    prior_rows = prior_logits[0]
    route_rows = routes[0]
    cotangent_low = grad_out[0]
    cotangent = cotangent_low.astype(F32)

    inv_rms1 = lax.rsqrt(jnp.mean(residual * residual, axis=1, keepdims=True) + EPS)
    normed_one = residual * inv_rms1
    attn_input = (normed_one * attn_gain).astype(BF16)
    ids_wide = jnp.broadcast_to(block_ids.astype(F32), (8, token_rows))
    stacked = jnp.stack([query_weight, key_weight, value_weight])
    stacked = stacked.reshape(3, shard_width, groups, width)
    pieces = jnp.transpose(stacked, (2, 0, 3, 1)).reshape(groups, 3 * width, shard_width)
    ids_all, w_all, a_all, output_all = gather(
        (ids_wide, pieces, attn_input, output_weight),
        (False, True, False, False), context, ranks, 0,
    )
    a_full = a_all.reshape(length, model_width)
    output_full = output_all.reshape(model_width, model_width)
    ids = ids_all[:, 0, :].reshape(length)
    weights_t = jnp.transpose(w_all, (1, 0, 2)).reshape(3 * width, model_width)
    half = head_size // 2
    freq = jnp.power(THETA, -2.0 * jnp.arange(half, dtype=F32) / head_size)
    angle = freq[:, None] * jnp.arange(length, dtype=jnp.int32).astype(F32)[None, :]
    cos_t, sin_t = jnp.cos(angle), jnp.sin(angle)

    flat_route = route_rows.reshape(-1)
    ffn_hot = (flat_route[:, None] == jnp.arange(FFN_E, dtype=jnp.int32)[None, :]).astype(jnp.int32)
    before = jnp.sum((jnp.cumsum(ffn_hot, axis=0) - ffn_hot) * ffn_hot, axis=1)
    slot_index = jnp.where(
        flat_route < FFN_E,
        flat_route * CAP + before,
        -1,
    ).reshape(token_rows, 2)
    slot_ids = jnp.arange(slot_count, dtype=jnp.int32)[:, None]
    hit_first = slot_ids == slot_index[None, :, 0]
    hit_second = slot_ids == slot_index[None, :, 1]
    pick_first = hit_first.astype(BF16)
    pick_second = hit_second.astype(BF16)
    pick_either = pick_first + pick_second

    blocks = (owners, per_owner, CAP, model_width)

    def pick(rows):
        return jnp.dot(pick_either, rows, preferred_element_type=F32).astype(BF16).reshape(blocks)

    grad_arrived = exchange(pick(cotangent_low), "expert", 0)

    (
        attn_out, out_t, log_total, query_t, key_heads, key_t, value_heads,
    ) = attn_forward(a_full, weights_t, cos_t, sin_t, ids, heads, head_size, ranks)
    kept = (out_t, log_total, query_t, key_heads, key_t, value_heads)
    gate_full = lax.all_gather(gate_weight, "context", axis=1, tiled=True)
    up_full = lax.all_gather(up_weight, "context", axis=1, tiled=True)
    down_full = lax.all_gather(down_weight, "context", axis=1, tiled=True)
    granule = TILE // 2
    shard_granules = token_rows // granule
    out_blocks = granules(
        attn_out.reshape(-1, granule, width), ranks, shard_granules, True, 1
    ).reshape(groups, token_rows, width)
    mix_low = jnp.transpose(out_blocks, (1, 0, 2)).reshape(token_rows, model_width)

    after_attn = residual + jnp.dot(mix_low, output_full, preferred_element_type=F32)
    inv_rms2 = lax.rsqrt(jnp.mean(after_attn * after_attn, axis=1, keepdims=True) + EPS)
    normed_two = after_attn * inv_rms2
    moe_input = normed_two * moe_gain
    narrow = jnp.concatenate(
        [router_weight, jnp.transpose(const_mix.reshape(-1, model_width))], axis=1
    )
    narrow_out = jnp.dot(moe_input, narrow, precision=HIGH, preferred_element_type=F32)
    expert_count = router_weight.shape[1]
    consts = const_mix.shape[0]
    logits = narrow_out[:, :expert_count] + jnp.dot(
        prior_rows, prior_weight, precision=HIGH, preferred_element_type=F32
    )
    probs = jax.nn.softmax(logits, axis=1)
    expert_ids = jnp.arange(expert_count, dtype=jnp.int32)
    first_hot = (route_rows[:, 0:1] == expert_ids[None, :]).astype(F32)
    second_hot = (route_rows[:, 1:2] == expert_ids[None, :]).astype(F32)
    chosen = first_hot + second_hot
    gated = probs * chosen
    first_gate = jnp.sum(probs * first_hot, axis=1, keepdims=True)
    second_gate = jnp.sum(probs * second_hot, axis=1, keepdims=True)
    slot_gate = jnp.sum(
        jnp.where(hit_first, first_gate[None, :, 0], 0.0)
        + jnp.where(hit_second, second_gate[None, :, 0], 0.0),
        axis=1,
    )
    def spread(values):
        values = values.reshape(owners, per_owner, CAP)
        return jnp.pad(values, ((0, 0), (0, 8 - per_owner), (0, 128 - CAP)))

    gates, arrived = swap(
        (spread(slot_gate), pick(moe_input.astype(BF16))), "expert", 1, owners, 2
    )
    gates = jnp.transpose(gates[:, :per_owner, :CAP], (1, 0, 2)).reshape(per_owner, -1, 1)

    expert_out, grad_rows, owner_dot, grad_gate, grad_up, grad_down = experts(
        arrived, grad_arrived, gates, gate_full, up_full, down_full
    )
    share_gate = lax.psum_scatter(grad_gate, "context", scatter_dimension=1, tiled=True)
    share_up = lax.psum_scatter(grad_up, "context", scatter_dimension=1, tiled=True)
    share_down = lax.psum_scatter(grad_down, "context", scatter_dimension=1, tiled=True)

    owner_dot = jnp.transpose(owner_dot.reshape(per_owner, owners, CAP), (1, 0, 2))
    slot_dot, grad_back = swap((spread(owner_dot), grad_rows), "expert", 1, owners, 3)
    slot_dot = slot_dot[:, :per_owner, :CAP].reshape(slot_count)
    grad_back = grad_back.reshape(slot_count, model_width)
    returned = exchange(expert_out, "expert", 0).reshape(slot_count, model_width)

    const_soft = jax.nn.softmax(narrow_out[:, expert_count:].reshape(token_rows, consts, 2), axis=2)
    const_gate = gated[:, FFN_E + 2 :]
    copy_gate = gated[:, FFN_E + 1 : FFN_E + 2]
    const_out = [
        const_soft[:, c, 0:1] * moe_input + const_soft[:, c, 1:2] * const_vector[c][None, :]
        for c in range(consts)
    ]
    local_moe = copy_gate * moe_input
    for c in range(consts):
        local_moe = local_moe + const_gate[:, c : c + 1] * const_out[c]
    grad_moe_ffn = lax.dot_general(
        pick_either, grad_back, (((0,), (0,)), ((), ())), preferred_element_type=F32
    )
    first_dot = jnp.sum(jnp.where(hit_first, slot_dot[:, None], 0.0), axis=0)[:, None]
    second_dot = jnp.sum(jnp.where(hit_second, slot_dot[:, None], 0.0), axis=0)[:, None]
    copy_dot = jnp.sum(cotangent * moe_input, axis=1, keepdims=True)
    const_dot = [jnp.sum(cotangent * const_out[c], axis=1, keepdims=True) for c in range(consts)]
    extra = jnp.concatenate(
        [jnp.zeros((token_rows, FFN_E + 1), F32), copy_dot, *const_dot], axis=1
    )
    grad_probs = first_hot * first_dot + second_hot * second_dot + chosen * extra
    grad_logits = probs * (grad_probs - jnp.sum(probs * grad_probs, axis=1, keepdims=True))
    grad_prior_rows = lax.dot_general(
        grad_logits, prior_weight, (((1,), (1,)), ((), ())),
        precision=HIGH, preferred_element_type=F32,
    )
    vector_dot = jnp.dot(
        cotangent, jnp.transpose(const_vector), precision=HIGH, preferred_element_type=F32
    )
    grad_soft = jnp.stack(
        [const_gate * copy_dot, const_gate * vector_dot], axis=2
    )
    grad_mix = const_soft * (grad_soft - jnp.sum(const_soft * grad_soft, axis=2, keepdims=True))
    narrow_grad = jnp.concatenate([grad_logits, grad_mix.reshape(token_rows, -1)], axis=1)
    local_scale = copy_gate + jnp.sum(const_soft[:, :, 0] * const_gate, axis=1, keepdims=True)
    grad_moe_input = (
        grad_moe_ffn
        + lax.dot_general(
            narrow_grad, narrow, (((1,), (1,)), ((), ())),
            precision=HIGH, preferred_element_type=F32,
        )
        + local_scale * cotangent
    )
    small_moe = lax.dot_general(
        narrow_grad, moe_input, (((0,), (0,)), ((), ())),
        precision=HIGH, preferred_element_type=F32,
    )
    small_vector = lax.dot_general(
        const_soft[:, :, 1] * const_gate, cotangent, (((0,), (0,)), ((), ())),
        precision=HIGH, preferred_element_type=F32,
    )
    grad_prior_local = lax.dot_general(
        prior_rows, grad_logits, (((0,), (0,)), ((), ())),
        precision=HIGH, preferred_element_type=F32,
    )
    small_gain = jnp.sum(grad_moe_input * normed_two, axis=0, keepdims=True)
    prior_values = jnp.pad(
        grad_prior_local.reshape(-1), (0, -(expert_count * expert_count) % shard_width)
    ).reshape(-1, 1, shard_width)
    prior_lines = prior_values.shape[0]
    small = jnp.concatenate([small_moe, small_vector, small_gain], axis=0)
    small_lines = small.shape[0]
    small = jnp.concatenate(
        [
            small.reshape(small_lines, context, shard_width),
            jnp.broadcast_to(prior_values, (prior_lines, context, shard_width)),
        ],
        axis=0,
    )
    small = jnp.pad(small, ((0, -small.shape[0] % 8), (0, 0), (0, 0)))

    grad_normed_two = grad_moe_input * moe_gain
    grad_after = cotangent + inv_rms2 * (
        grad_normed_two - normed_two * jnp.mean(grad_normed_two * normed_two, axis=1, keepdims=True)
    )
    grad_attn_low = grad_after.astype(BF16)
    grad_mix_low = lax.dot_general(
        grad_attn_low, output_full, (((1,), (1,)), ((), ())), preferred_element_type=F32
    ).astype(BF16)
    grad_pieces = jnp.transpose(grad_mix_low.reshape(token_rows, groups, width), (1, 0, 2))
    grad_own = granules(
        grad_pieces.reshape(-1, granule, width), ranks, shard_granules, False, 4
    ).reshape(-1, width)
    grad_output_local = lax.dot_general(
        mix_low, grad_attn_low, (((0,), (0,)), ((), ())), preferred_element_type=F32
    ).astype(BF16)
    output_parts = exchange(
        grad_output_local.reshape(context, shard_width, model_width), "context", 0
    )

    da_part, grad_w = attn_backward(
        grad_own, a_full, weights_t, cos_t, sin_t, ids, kept, heads, head_size, ranks
    )
    chips = context // 2
    core = lax.rem(lax.axis_index("context"), 2)
    both_parts = jnp.concatenate(
        [grad_w.reshape(3 * width, context, shard_width), small], axis=0
    )
    both_lines = both_parts.shape[0]
    both_parts = jnp.transpose(both_parts, (1, 0, 2)).reshape(chips, 2, both_lines, shard_width)
    da_part = da_part.reshape(chips, 2, token_rows, model_width)
    da_twin, both_twin = swap(
        (jnp.swapaxes(da_part, 0, 1), jnp.swapaxes(both_parts, 0, 1)), "context", 1, 2, 5
    )
    da_chip = (da_twin[0].astype(F32) + da_twin[1].astype(F32)).astype(BF16)
    both_chip = both_twin[0] + both_twin[1]
    da_all, both_all = swap((da_chip, both_chip), "context", 2, chips, 6)
    grad_attn_input = jnp.sum(da_all.astype(F32), axis=0)
    grad_normed_one = grad_attn_input * attn_gain
    grad_input = grad_after + inv_rms1 * (
        grad_normed_one - normed_one * jnp.mean(grad_normed_one * normed_one, axis=1, keepdims=True)
    )

    per_group = ranks // 2
    w_blocks = both_all[:, : 3 * width].reshape(groups, per_group, 3, width, shard_width)
    w_blocks = jnp.sum(w_blocks, axis=1)
    w_share = jnp.transpose(w_blocks, (1, 3, 0, 2)).reshape(3, shard_width, model_width)
    output_share = jnp.sum(output_parts.astype(F32), axis=0)
    shares = jnp.concatenate([w_share, output_share[None]], axis=0).reshape(
        4, owners, shard_width // owners, model_width
    )
    shares = jnp.transpose(shares.astype(BF16), (1, 0, 2, 3))
    small_ctx = jnp.sum(both_all[:, 3 * width :], axis=0)
    shares_all, small_all = swap((shares, small_ctx), "expert", 1, owners, 7, (False, True))
    share_sum = jnp.sum(shares_all.astype(F32), axis=0).astype(BF16)
    (sums,) = swap((share_sum,), "expert", 1, owners, 8, (True,))
    sums = jnp.transpose(sums.astype(F32), (1, 0, 2, 3)).reshape(4, shard_width, model_width)
    w_sum, output_sum = sums[:3], sums[3]
    small_own = jnp.sum(small_all, axis=0)
    grad_attn_gain = jnp.sum(
        w_sum[0] * query_weight.astype(F32)
        + w_sum[1] * key_weight.astype(F32)
        + w_sum[2] * value_weight.astype(F32),
        axis=1,
    )
    column = lax.axis_index("context") * shard_width
    grad_attn_gain = grad_attn_gain / lax.dynamic_slice_in_dim(attn_gain, column, shard_width)
    mixes = expert_count + 2 * consts
    grad_prior_weight = small_own[small_lines : small_lines + prior_lines].reshape(-1)
    grad_prior_weight = grad_prior_weight[: expert_count * expert_count].reshape(
        expert_count, expert_count
    )
    layer_out = after_attn + local_moe
    layer_out = layer_out + first_gate * lax.dot_general(
        pick_first, returned, (((0,), (0,)), ((), ())), preferred_element_type=F32
    )
    layer_out = layer_out + second_gate * lax.dot_general(
        pick_second, returned, (((0,), (0,)), ((), ())), preferred_element_type=F32
    )
    return (
        layer_out.astype(BF16)[None],
        grad_input[None],
        grad_prior_rows[None],
        grad_attn_gain,
        w_sum[0],
        w_sum[1],
        w_sum[2],
        output_sum,
        small_own[small_lines - 1],
        jnp.transpose(small_own[:expert_count]),
        grad_prior_weight,
        small_own[expert_count:mixes].reshape(consts, 2, shard_width),
        small_own[mixes : mixes + consts],
        share_gate.astype(F32),
        share_up.astype(F32),
        share_down.astype(F32),
    )


def solution(mesh):
    return jax.shard_map(
        shards,
        mesh=mesh,
        in_specs=(
            P("expert", "context", None),
            P("expert", "context", None),
            P("expert", "context", None),
            P("expert", "context"),
            P("expert", "context", None),
            P(),
            P("context", None),
            P("context", None),
            P("context", None),
            P("context", None),
            P(),
            P(),
            P(),
            P(),
            P(),
            P("expert", "context", None),
            P("expert", "context", None),
            P("expert", "context", None),
        ),
        out_specs=(
            P("expert", "context", None),
            P("expert", "context", None),
            P("expert", "context", None),
            P("context"),
            P("context", None),
            P("context", None),
            P("context", None),
            P("context", None),
            P("context"),
            P("context", None),
            P(),
            P(None, None, "context"),
            P(None, "context"),
            P("expert", "context", None),
            P("expert", "context", None),
            P("expert", "context", None),
        ),
        check_vma=False,
    )
```

```python
import functools
import math

import jax
import jax.numpy as jnp
from jax import lax
from jax.experimental import pallas as pl
from jax.experimental.pallas import tpu as pltpu
from jax.sharding import PartitionSpec as P

HEADS = 12
FFN_E = 8
CAP = 96
TILE = 256
EXTRA = 16
HIDDEN_TILE = 256

EPS = 1e-06
THETA = 10000.0
NEGATIVE = -1e30
HIGH = lax.Precision.HIGHEST
F32 = jnp.float32
BF16 = jnp.bfloat16


def dot(left, right, left_dim=1, right_dim=0):
    return lax.dot_general(
        left, right, (((left_dim,), (right_dim,)), ((), ())), preferred_element_type=F32
    )


def turn(rows, cos_rows, sin_rows, heads, size, back=False):
    half = size // 2
    parts = []
    for head in range(heads):
        first = rows[head * size : head * size + half]
        second = rows[head * size + half : (head + 1) * size]
        if back:
            parts.append(first * cos_rows + second * sin_rows)
            parts.append(second * cos_rows - first * sin_rows)
        else:
            parts.append(first * cos_rows - second * sin_rows)
            parts.append(second * cos_rows + first * sin_rows)
    return jnp.concatenate(parts, axis=0)


def own_tile(index, ranks):
    rank = lax.rem(lax.axis_index("context"), ranks)
    place = lax.rem(index, 2)
    return (index // 2) * (2 * ranks) + jnp.where(place == 0, rank, 2 * ranks - 1 - rank)


def lanes(start):
    return pl.ds(pl.multiple_of(start * TILE, TILE), TILE)


def attn_forward_kernel(
    heads, size, ranks, scale,
    a_ref, wt_ref, cos_ref, sin_ref, ids_col_ref, ids_row_ref,
    out_ref, out_t_ref, lse_ref, query_t_ref, key_ref, key_t_ref, value_ref,
    value_t_ref, scores_ref, acc_ref,
):
    length = a_ref.shape[0]
    width = heads * size
    tiles = length // TILE
    own_tiles = tiles // ranks
    ext = size + EXTRA
    tail = (lax.broadcasted_iota(jnp.int32, (EXTRA, TILE), 0) == 0).astype(BF16)

    def project(step, carry):
        at = lanes(step)
        both = dot(wt_ref[width:, :], a_ref[at, :], 1, 1)
        key_t = turn(both[:width], cos_ref[:, at], sin_ref[:, at], heads, size)
        key_t_ref[:, at] = key_t.astype(BF16)
        value_t = both[width:]
        for head in range(heads):
            rows = slice(head * size, (head + 1) * size)
            key_ref[head, at, :] = key_t[rows].T.astype(BF16)
            value_ref[head, at, :] = value_t[rows].T.astype(BF16)
            value_t_ref[head * ext : head * ext + size, at] = value_t[rows].astype(BF16)
            value_t_ref[head * ext + size : (head + 1) * ext, at] = tail
        return carry

    lax.fori_loop(0, tiles, project, 0)

    def attend(index, carry):
        tile = own_tile(index, ranks)
        at = lanes(tile)
        query_t = dot(wt_ref[:width, :], a_ref[at, :], 1, 1)
        query_t = turn(query_t, cos_ref[:, at], sin_ref[:, at], heads, size)
        query_t = query_t.astype(BF16) * jnp.asarray(scale, BF16)
        query_t_ref[:, lanes(index)] = query_t
        query_ids = ids_row_ref[:, at]

        def score(step, tops, masked):
            here = lanes(step)
            fresh = []
            if masked:
                allowed = ids_col_ref[here, :] <= query_ids
            for head in range(heads):
                part = dot(key_ref[head, here, :], query_t[head * size : (head + 1) * size])
                if masked:
                    part = jnp.where(allowed, part, NEGATIVE)
                scores_ref[head, here, :] = part
                fresh.append(
                    jnp.maximum(tops[head], jnp.max(part.reshape(TILE // 8, 8, TILE), axis=0))
                )
            return tuple(fresh)

        tops = tuple(jnp.full((8, TILE), NEGATIVE, F32) for _ in range(heads))
        stop = jnp.minimum(tile + 2, tiles)
        tops = lax.fori_loop(0, tile, lambda s, c: score(s, c, False), tops)
        tops = lax.fori_loop(tile, stop, lambda s, c: score(s, c, True), tops)
        peaks = [jnp.max(top, axis=0, keepdims=True) for top in tops]
        acc_ref[...] = jnp.zeros_like(acc_ref)

        def combine(step, carry):
            here = lanes(step)
            for head in range(heads):
                weights = jnp.exp(scores_ref[head, here, :] - peaks[head]).astype(BF16)
                acc_ref[head] += dot(value_t_ref[head * ext : (head + 1) * ext, here], weights)
            return carry

        lax.fori_loop(0, stop, combine, 0)
        parts = []
        for head in range(heads):
            total = acc_ref[head, size : size + 1, :]
            part = acc_ref[head, :size, :] * (1.0 / total)
            lse_ref[head : head + 1, lanes(index)] = peaks[head] + jnp.log(total)
            parts.append(part)
        joined = jnp.concatenate(parts, axis=0)
        out_t_ref[:, lanes(index)] = joined
        out_ref[lanes(index), :] = joined.T.astype(BF16)
        return carry

    lax.fori_loop(0, own_tiles, attend, 0)


def attn_backward_kernel(
    heads, size, ranks, scale,
    grad_ref, a_ref, wt_ref, cos_ref, sin_ref, ids_col_ref, ids_row_ref,
    out_t_ref, lse_ref, query_t_ref, key_ref, key_t_ref, value_ref,
    da_ref, pieces_ref,
    query_ref, own_grad_ref, dq_ref, dk_ref, dv_ref, grad_w_ref,
):
    length = a_ref.shape[0]
    width = heads * size
    tiles = length // TILE
    own_tiles = tiles // ranks
    dk_ref[...] = jnp.zeros_like(dk_ref)
    dv_ref[...] = jnp.zeros_like(dv_ref)
    da_ref[...] = jnp.zeros_like(da_ref)
    grad_w_ref[...] = jnp.zeros_like(grad_w_ref)

    def attend(index, carry):
        tile = own_tile(index, ranks)
        at = lanes(tile)
        query_t = query_t_ref[:, lanes(index)]
        grad_rows = grad_ref[lanes(index), :]
        grad_t = grad_rows.astype(F32).T
        query_rows = query_t.astype(F32).T.astype(BF16)
        query_ids = ids_row_ref[:, at]
        deltas, tops, grads_low = [], [], []
        for head in range(heads):
            rows = slice(head * size, (head + 1) * size)
            query_ref[head] = query_rows[:, rows]
            own_grad_ref[head] = grad_rows[:, rows]
            deltas.append(
                jnp.sum(grad_t[rows] * out_t_ref[rows, lanes(index)], axis=0, keepdims=True)
            )
            tops.append(lse_ref[head : head + 1, lanes(index)])
        grad_t_low = grad_t.astype(BF16)
        dq_ref[...] = jnp.zeros_like(dq_ref)

        def chunk(step, carry, masked):
            here = lanes(step)
            if masked:
                allowed = ids_col_ref[here, :] <= query_ids
            for head in range(heads):
                rows = slice(head * size, (head + 1) * size)
                scores = dot(key_ref[head, here, :], query_t[rows]) - tops[head]
                if masked:
                    scores = jnp.where(allowed, scores, NEGATIVE)
                probs = jnp.exp(scores)
                grad_probs = dot(value_ref[head, here, :], grad_t_low[rows])
                grad_scores = (probs * (grad_probs - deltas[head])).astype(BF16)
                dv_ref[head, here, :] += dot(probs.astype(BF16), own_grad_ref[head])
                dk_ref[head, here, :] += dot(grad_scores, query_ref[head])
                dq_ref[rows, :] += dot(key_t_ref[rows, here], grad_scores)
            return carry

        stop = jnp.minimum(tile + 2, tiles)
        lax.fori_loop(0, tile, lambda s, c: chunk(s, c, False), 0)
        lax.fori_loop(tile, stop, lambda s, c: chunk(s, c, True), 0)
        grad_query = turn(
            dq_ref[...] * scale, cos_ref[:, at], sin_ref[:, at], heads, size, back=True
        )
        grad_w_ref[:width, :] += dot(grad_query.astype(BF16), a_ref[at, :])
        da_ref[at, :] = dot(grad_query.T.astype(BF16), wt_ref[:width, :]).astype(BF16)
        return carry

    lax.fori_loop(0, own_tiles, attend, 0)

    def finish(step, carry):
        at = lanes(step)
        key_grad = jnp.concatenate([dk_ref[head, at, :].T for head in range(heads)], axis=0)
        key_grad = turn(key_grad, cos_ref[:, at], sin_ref[:, at], heads, size, back=True)
        value_grad = jnp.concatenate([dv_ref[head, at, :].T for head in range(heads)], axis=0)
        both = jnp.concatenate([key_grad, value_grad], axis=0)
        grad_w_ref[width:, :] += dot(both.astype(BF16), a_ref[at, :])
        total = da_ref[at, :].astype(F32) + dot(both.T.astype(BF16), wt_ref[width:, :])
        da_ref[at, :] = total.astype(BF16)
        return carry

    lax.fori_loop(0, tiles, finish, 0)
    shard = pieces_ref.shape[2]
    for piece in range(pieces_ref.shape[0]):
        pieces_ref[piece] = grad_w_ref[:, piece * shard : (piece + 1) * shard]


def expert_kernel(
    rows_ref, grad_ref, prob_ref, gate_ref, up_ref, down_ref,
    out_ref, grad_rows_ref, dot_ref, grad_gate_ref, grad_up_ref, grad_down_ref,
    rows_t_ref, dye_ref, out_acc_ref, grad_acc_ref,
):
    step = pl.program_id(1)

    @pl.when(step == 0)
    def _():
        rows_t_ref[...] = rows_ref[:, 0].reshape(dye_ref.shape).astype(F32).T.astype(BF16)
        grads = grad_ref[:, 0].reshape(dye_ref.shape).astype(F32)
        dye_ref[...] = (grads * prob_ref[0]).astype(BF16)
        out_acc_ref[...] = jnp.zeros_like(out_acc_ref)
        grad_acc_ref[...] = jnp.zeros_like(grad_acc_ref)

    rows = rows_ref[:, 0].reshape(dye_ref.shape)
    dye = dye_ref[...]
    gate = gate_ref[0]
    up = up_ref[0]
    down = down_ref[0]
    gate_pre = dot(rows, gate)
    up_pre = dot(rows, up)
    sigmoid = jax.nn.sigmoid(gate_pre)
    silu = gate_pre * sigmoid
    hidden = silu * up_pre
    hidden_low = hidden.astype(BF16)
    out_acc_ref[...] += dot(hidden_low, down)
    grad_hidden = dot(dye, down, 1, 1).astype(BF16).astype(F32)
    grad_down_ref[0] = dot(hidden.T.astype(BF16), dye).astype(BF16)
    grad_gate = (grad_hidden * up_pre * sigmoid * (1.0 + gate_pre * (1.0 - sigmoid))).astype(BF16)
    grad_up = (grad_hidden * silu).astype(BF16)
    grad_gate_ref[0] = dot(rows_t_ref[...], grad_gate).astype(BF16)
    grad_up_ref[0] = dot(rows_t_ref[...], grad_up).astype(BF16)
    grad_acc_ref[...] += dot(grad_gate, gate, 1, 1) + dot(grad_up, up, 1, 1)

    @pl.when(step == pl.num_programs(1) - 1)
    def _():
        out_low = out_acc_ref[...].astype(BF16)
        blocks = out_ref.shape[:1] + out_ref.shape[2:]
        out_ref[:, 0] = out_low.reshape(blocks)
        grad_rows_ref[:, 0] = grad_acc_ref[...].astype(BF16).reshape(blocks)
        grads = grad_ref[:, 0].reshape(dye_ref.shape).astype(F32)
        dot_ref[0] = jnp.sum(out_low.astype(F32) * grads, axis=1, keepdims=True)


def vmem(count):
    return [pl.BlockSpec(memory_space=pltpu.VMEM)] * count


def attn_forward(a_full, weights_t, cos_t, sin_t, ids, heads, size, ranks):
    length = a_full.shape[0]
    own = length // ranks
    width = heads * size
    ext = size + EXTRA
    shapes = (
        jax.ShapeDtypeStruct((own, width), BF16),
        jax.ShapeDtypeStruct((width, own), F32),
        jax.ShapeDtypeStruct((heads, own), F32),
        jax.ShapeDtypeStruct((width, own), BF16),
        jax.ShapeDtypeStruct((heads, length, size), BF16),
        jax.ShapeDtypeStruct((width, length), BF16),
        jax.ShapeDtypeStruct((heads, length, size), BF16),
    )
    return pl.pallas_call(
        functools.partial(attn_forward_kernel, heads, size, ranks, size ** (-0.5)),
        out_shape=shapes,
        in_specs=vmem(6),
        out_specs=vmem(7),
        scratch_shapes=[
            pltpu.VMEM((heads * ext, length), BF16),
            pltpu.VMEM((heads, length, TILE), F32),
            pltpu.VMEM((heads, ext, TILE), F32),
        ],
        compiler_params=pltpu.CompilerParams(vmem_limit_bytes=60 << 20),
        cost_estimate=cost(37),
        name="attn_forward",
    )(a_full, weights_t, cos_t, sin_t, ids[:, None], ids[None, :])


def attn_backward(
    grad_full, a_full, weights_t, cos_t, sin_t, ids, kept, heads, size, ranks, context
):
    length = a_full.shape[0]
    width = heads * size
    shapes = (
        jax.ShapeDtypeStruct(a_full.shape, BF16),
        jax.ShapeDtypeStruct((context, weights_t.shape[0], a_full.shape[1] // context), F32),
    )
    return pl.pallas_call(
        functools.partial(attn_backward_kernel, heads, size, ranks, size ** (-0.5)),
        out_shape=shapes,
        in_specs=vmem(13),
        out_specs=vmem(2),
        scratch_shapes=[
            pltpu.VMEM((heads, TILE, size), BF16),
            pltpu.VMEM((heads, TILE, size), BF16),
            pltpu.VMEM((width, TILE), F32),
            pltpu.VMEM((heads, length, size), F32),
            pltpu.VMEM((heads, length, size), F32),
            pltpu.VMEM(weights_t.shape, F32),
        ],
        compiler_params=pltpu.CompilerParams(vmem_limit_bytes=63 << 20),
        cost_estimate=cost(58),
        name="attn_backward",
    )(grad_full, a_full, weights_t, cos_t, sin_t, ids[:, None], ids[None, :], *kept)


def experts(rows, grads, gates, gate_full, up_full, down_full):
    owners, count, cap, width = rows.shape
    slots = owners * cap
    hidden = gate_full.shape[2]
    per_row = pl.BlockSpec((owners, 1, cap, width), lambda e, t: (0, e, 0, 0))
    column = pl.BlockSpec((1, slots, 1), lambda e, t: (e, 0, 0))
    wide = pl.BlockSpec((1, width, HIDDEN_TILE), lambda e, t: (e, 0, t))
    tall = pl.BlockSpec((1, HIDDEN_TILE, width), lambda e, t: (e, t, 0))
    return pl.pallas_call(
        expert_kernel,
        grid=(count, hidden // HIDDEN_TILE),
        out_shape=(
            jax.ShapeDtypeStruct(rows.shape, BF16),
            jax.ShapeDtypeStruct(rows.shape, BF16),
            jax.ShapeDtypeStruct((count, slots, 1), F32),
            jax.ShapeDtypeStruct(gate_full.shape, BF16),
            jax.ShapeDtypeStruct(up_full.shape, BF16),
            jax.ShapeDtypeStruct(down_full.shape, BF16),
        ),
        in_specs=[per_row, per_row, column, wide, wide, tall],
        out_specs=(per_row, per_row, column, wide, wide, tall),
        scratch_shapes=[
            pltpu.VMEM((width, slots), BF16),
            pltpu.VMEM((slots, width), BF16),
            pltpu.VMEM((slots, width), F32),
            pltpu.VMEM((slots, width), F32),
        ],
        compiler_params=pltpu.CompilerParams(vmem_limit_bytes=60 << 20),
        cost_estimate=cost(37),
        name="experts",
    )(rows, grads, gates, gate_full, up_full, down_full)


def cost(micros):
    return pl.CostEstimate(flops=micros * 1_150_000_000, bytes_accessed=0, transcendentals=0)


def swap_kernel(axis, stride, count, same, *refs):
    total = len(same)
    sources, targets = refs[:total], refs[total : 2 * total]
    local_sem, send_sem, recv_sem = refs[2 * total :]
    place = lax.axis_index(axis)
    mine = lax.rem(place // stride, count)
    barrier = pltpu.get_barrier_semaphore()
    for far in range(1, count):
        peer = lax.rem(mine + far, count)
        pl.semaphore_signal(
            barrier, inc=1, device_id={axis: place + (peer - mine) * stride},
            device_id_type=pl.DeviceIdType.MESH,
        )
    pl.semaphore_wait(barrier, count - 1)
    copies = []
    for item in range(total):
        for far in range(1, count):
            peer = lax.rem(mine + far, count)
            copies.append(
                pltpu.make_async_remote_copy(
                    src_ref=sources[item] if same[item] else sources[item].at[peer],
                    dst_ref=targets[item].at[mine],
                    send_sem=send_sem.at[item, far],
                    recv_sem=recv_sem.at[item, far],
                    device_id={axis: place + (peer - mine) * stride},
                    device_id_type=pl.DeviceIdType.MESH,
                )
            )
            copies[-1].start()
    for item in range(total):
        copies.append(
            pltpu.make_async_copy(
                sources[item] if same[item] else sources[item].at[mine],
                targets[item].at[mine],
                local_sem.at[item],
            )
        )
        copies[-1].start()
    for copy in copies:
        copy.wait()


def swap(arrays, axis, stride, count, number, same=None):
    same = same or (False,) * len(arrays)
    shapes = tuple(
        jax.ShapeDtypeStruct(((count,) if own else ()) + array.shape, array.dtype)
        for array, own in zip(arrays, same)
    )
    return pl.pallas_call(
        functools.partial(swap_kernel, axis, stride, count, same),
        out_shape=shapes,
        in_specs=vmem(len(arrays)),
        out_specs=vmem(len(arrays)),
        scratch_shapes=[
            pltpu.SemaphoreType.DMA((len(arrays),)),
            pltpu.SemaphoreType.DMA((len(arrays), count)),
            pltpu.SemaphoreType.DMA((len(arrays), count)),
        ],
        compiler_params=pltpu.CompilerParams(
            collective_id=number, has_side_effects=True, vmem_limit_bytes=60 << 20
        ),
        name="swap",
    )(*arrays)


def gather_kernel(chips, ranks, split, *refs):
    total = len(split)
    sources, targets = refs[:total], refs[total : 2 * total]
    local_sem, send_sem, recv_sem, pass_sem, land_sem = refs[2 * total :]
    place = lax.axis_index("context")
    chip, core = place // 2, lax.rem(place, 2)
    partner = 2 * chip + 1 - core

    def piece(item, device):
        return sources[item].at[device // ranks] if split[item] else sources[item]

    def remote(source, target, send, recv, device):
        return pltpu.make_async_remote_copy(
            src_ref=source, dst_ref=target, send_sem=send, recv_sem=recv,
            device_id={"context": device}, device_id_type=pl.DeviceIdType.MESH,
        )

    barrier = pltpu.get_barrier_semaphore()
    for far in range(1, chips):
        pl.semaphore_signal(
            barrier, inc=1, device_id={"context": 2 * lax.rem(chip + far, chips) + core},
            device_id_type=pl.DeviceIdType.MESH,
        )
    pl.semaphore_signal(
        barrier, inc=1, device_id={"context": partner}, device_id_type=pl.DeviceIdType.MESH
    )
    pl.semaphore_wait(barrier, chips)
    sent = {}
    for item in range(total):
        for far in range(chips):
            peer = partner if far == 0 else 2 * lax.rem(chip + far, chips) + core
            sent[item, far] = remote(
                piece(item, peer), targets[item].at[place],
                send_sem.at[item, far], recv_sem.at[item, far], peer,
            )
            sent[item, far].start()
    local = []
    for item in range(total):
        local.append(
            pltpu.make_async_copy(
                piece(item, place), targets[item].at[place], local_sem.at[item]
            )
        )
        local[-1].start()
    passed = []
    for item in range(total):
        for far in range(1, chips):
            sent[item, far].wait_recv()
            block = targets[item].at[2 * lax.rem(chip + chips - far, chips) + core]
            passed.append(
                remote(block, block, pass_sem.at[item, far], land_sem.at[item, far], partner)
            )
            passed[-1].start()
    for item in range(total):
        sent[item, 0].wait_recv()
        for far in range(chips):
            sent[item, far].wait_send()
    for copy in local + passed:
        copy.wait()


def gather(arrays, split, context, ranks, number):
    chips = context // 2
    total = len(arrays)
    shapes = tuple(
        jax.ShapeDtypeStruct((context,) + (array.shape[1:] if cut else array.shape), array.dtype)
        for array, cut in zip(arrays, split)
    )
    return pl.pallas_call(
        functools.partial(gather_kernel, chips, ranks, split),
        out_shape=shapes,
        in_specs=vmem(total),
        out_specs=vmem(total),
        scratch_shapes=[pltpu.SemaphoreType.DMA((total,))]
        + [pltpu.SemaphoreType.DMA((total, chips))] * 4,
        compiler_params=pltpu.CompilerParams(
            collective_id=number, has_side_effects=True, vmem_limit_bytes=60 << 20
        ),
        name="gather",
    )(*arrays)


def granule_kernel(ranks, shard_granules, outward, source_ref, target_ref, send_sem, recv_sem):
    place = lax.axis_index("context")
    context = lax.axis_size("context")
    group, rank = place // ranks, lax.rem(place, ranks)
    groups = context // ranks
    owned = context * shard_granules // ranks
    barrier = pltpu.get_barrier_semaphore()
    for far in range(1, context):
        pl.semaphore_signal(
            barrier, inc=1, device_id={"context": lax.rem(place + far, context)},
            device_id_type=pl.DeviceIdType.MESH,
        )
    pl.semaphore_wait(barrier, context - 1)

    def owner_rank(granule):
        spot = lax.rem(granule // 2, 2 * ranks)
        return jnp.minimum(spot, 2 * ranks - 1 - spot)

    def owner_slot(granule):
        tile = granule // 2
        spot = lax.rem(tile, 2 * ranks)
        upper = jnp.where(spot >= ranks, 1, 0)
        return (tile // (2 * ranks) * 2 + upper) * 2 + lax.rem(granule, 2)

    def granule_of(slot):
        return own_tile(slot // 2, ranks) * 2 + lax.rem(slot, 2)

    def remote(source, target, index, device):
        return pltpu.make_async_remote_copy(
            src_ref=source, dst_ref=target, send_sem=send_sem.at[index],
            recv_sem=recv_sem.at[index], device_id={"context": device},
            device_id_type=pl.DeviceIdType.MESH,
        )

    def outgoing(step):
        if outward:
            granule = granule_of(step)
            home = granule // shard_granules
            slot = group * shard_granules + lax.rem(granule, shard_granules)
            return home, source_ref.at[step], slot
        other, spot = step // shard_granules, step % shard_granules
        granule = place * shard_granules + spot
        return other * ranks + owner_rank(granule), source_ref.at[step], owner_slot(granule)

    def incoming(step):
        if outward:
            other, spot = step // shard_granules, step % shard_granules
            return other * ranks + owner_rank(place * shard_granules + spot)
        return granule_of(step) // shard_granules

    for step in range(owned):
        device, source, slot = outgoing(step)

        @pl.when(device == place)
        def _():
            pltpu.make_async_copy(source, target_ref.at[slot], recv_sem.at[slot]).start()

        @pl.when(device != place)
        def _():
            pltpu.make_async_remote_copy(
                src_ref=source, dst_ref=target_ref.at[slot], send_sem=send_sem.at[step],
                recv_sem=recv_sem.at[slot], device_id={"context": device},
                device_id_type=pl.DeviceIdType.MESH,
            ).start()

    for step in range(owned):
        device, source, slot = outgoing(step)

        @pl.when(device != place)
        def _():
            remote(source, target_ref.at[slot], step, device).wait_send()

        sender = incoming(step)

        @pl.when(sender == place)
        def _():
            pltpu.make_async_copy(source_ref.at[0], target_ref.at[step], recv_sem.at[step]).wait()

        @pl.when(sender != place)
        def _():
            remote(source_ref.at[0], target_ref.at[step], step, sender).wait_recv()


def granules(rows, ranks, shard_granules, outward, number):
    owned = rows.shape[0]
    return pl.pallas_call(
        functools.partial(granule_kernel, ranks, shard_granules, outward),
        out_shape=jax.ShapeDtypeStruct(rows.shape, rows.dtype),
        in_specs=vmem(1),
        out_specs=vmem(1)[0],
        scratch_shapes=[
            pltpu.SemaphoreType.DMA((owned,)),
            pltpu.SemaphoreType.DMA((owned,)),
        ],
        compiler_params=pltpu.CompilerParams(
            collective_id=number, has_side_effects=True, vmem_limit_bytes=60 << 20
        ),
        name="granules",
    )(rows)


def finish_kernel(
    chips, owners, groups,
    da_ref, pieces_ref, small_ref, output_ref,
    total_ref, sums_ref, small_all_ref,
    da_twin, da_sum, da_in, w_twin, w_sum, w_in, s_twin, s_sum, s_in, s_total,
    stack_ref, shares, shares_in, block_ref,
    pair_send, pair_recv, chip_send, chip_recv, row_send, row_recv,
):
    place = lax.axis_index("context")
    row = lax.axis_index("expert")
    chip, core = place // 2, lax.rem(place, 2)
    partner = 2 * chip + 1 - core
    barrier = pltpu.get_barrier_semaphore()

    def greet(device):
        pl.semaphore_signal(
            barrier, inc=1, device_id=device, device_id_type=pl.DeviceIdType.MESH
        )

    def remote(source, target, send, recv, device):
        return pltpu.make_async_remote_copy(
            src_ref=source, dst_ref=target, send_sem=send, recv_sem=recv,
            device_id=device, device_id_type=pl.DeviceIdType.MESH,
        )

    greet({"context": partner})
    for far in range(1, chips):
        greet({"context": 2 * lax.rem(chip + far, chips) + core})
    for far in range(1, owners):
        greet({"expert": lax.rem(row + far, owners)})
    pl.semaphore_wait(barrier, chips + owners - 1)

    order = list(range(1, chips)) + [0]
    pair = {}
    for item, (source, target) in enumerate(
        ((small_ref, s_twin), (pieces_ref, w_twin), (da_ref, da_twin))
    ):
        for far in order:
            peer = lax.rem(chip + far, chips)
            pair[item, far] = remote(
                source.at[2 * peer + 1 - core], target.at[peer],
                pair_send.at[item, far], pair_recv.at[item, far], {"context": partner},
            )
            pair[item, far].start()

    def across(item, source, target, far):
        peer = lax.rem(chip + far, chips)
        return remote(
            source.at[peer], target.at[chip], chip_send.at[item, far], chip_recv.at[item, far],
            {"context": 2 * peer + core},
        )

    for far in order:
        peer = lax.rem(chip + far, chips)
        mine = 2 * peer + core
        pair[0, far].wait_recv()
        s_sum[peer] = small_ref[mine] + s_twin[peer]
        pair[1, far].wait_recv()
        w_sum[peer] = (pieces_ref[mine] + w_twin[peer]).astype(BF16)
    moved = {}
    for far in range(1, chips):
        moved[0, far] = across(0, s_sum, s_in, far)
        moved[0, far].start()
        moved[1, far] = across(1, w_sum, w_in, far)
        moved[1, far].start()
    last = None
    for far in order:
        peer = lax.rem(chip + far, chips)
        pair[2, far].wait_recv()
        da_sum[peer] = (
            da_ref[2 * peer + core].astype(F32) + da_twin[peer].astype(F32)
        ).astype(BF16)
        if last is not None:
            moved[2, last] = across(2, da_sum, da_in, last)
            moved[2, last].start()
        last = far
    for far in range(1, chips):
        moved[0, far].wait_recv()
        moved[1, far].wait_recv()
    s_in[chip] = s_sum[chip]
    w_in[chip] = w_sum[chip]

    width = w_sum.shape[1] // 3
    shard = w_sum.shape[2]
    per_group = chips // groups
    for group in range(groups):
        total = w_in[group * per_group].astype(F32)
        for other in range(1, per_group):
            total = total + w_in[group * per_group + other].astype(F32)
        for which in range(3):
            stack_ref[which * shard : (which + 1) * shard, group * width : (group + 1) * width] = (
                total[which * width : (which + 1) * width].T
            )
    stack_ref[3 * shard :, :] = output_ref[...]
    lines = shares.shape[1]
    for owner in range(owners):
        shares[owner] = stack_ref[owner * lines : (owner + 1) * lines, :].astype(BF16)
    total = s_in[0]
    for other in range(1, chips):
        total = total + s_in[other]
    s_total[...] = total
    rows = {}
    for far in range(1, owners):
        peer = lax.rem(row + far, owners)
        rows[0, far] = remote(
            shares.at[peer], shares_in.at[row], row_send.at[0, far], row_recv.at[0, far],
            {"expert": peer},
        )
        rows[0, far].start()
        rows[1, far] = remote(
            s_total, small_all_ref.at[row], row_send.at[1, far], row_recv.at[1, far],
            {"expert": peer},
        )
        rows[1, far].start()
    shares_in[row] = shares[row]
    small_all_ref[row] = total
    for far in range(1, owners):
        rows[0, far].wait_recv()
    summed = shares_in[0].astype(F32)
    for other in range(1, owners):
        summed = summed + shares_in[other].astype(F32)
    block_ref[...] = summed.astype(BF16)
    for far in range(1, chips):
        moved[2, far].wait_recv()
    for far in range(1, owners):
        peer = lax.rem(row + far, owners)
        rows[2, far] = remote(
            block_ref, sums_ref.at[row], row_send.at[2, far], row_recv.at[2, far],
            {"expert": peer},
        )
        rows[2, far].start()
    sums_ref[row] = summed.astype(BF16)
    da_in[chip] = da_sum[chip]
    total = da_in[0].astype(F32)
    for other in range(1, chips):
        total = total + da_in[other].astype(F32)
    total_ref[...] = total
    for far in range(1, owners):
        rows[1, far].wait_recv()
        rows[2, far].wait_recv()
    for copy in list(pair.values()) + list(moved.values()) + list(rows.values()):
        copy.wait_send()


def finish(da, pieces, small, output_share, owners, groups, number):
    context, tokens, width = da.shape
    chips = context // 2
    lines, shard = pieces.shape[1:]
    few = small.shape[1]
    stack = 3 * shard + output_share.shape[0]
    block = (stack // owners, width)
    return pl.pallas_call(
        functools.partial(finish_kernel, chips, owners, groups),
        out_shape=(
            jax.ShapeDtypeStruct((tokens, width), F32),
            jax.ShapeDtypeStruct((owners,) + block, BF16),
            jax.ShapeDtypeStruct((owners, few, shard), F32),
        ),
        in_specs=vmem(4),
        out_specs=vmem(3),
        scratch_shapes=[
            pltpu.VMEM((chips, tokens, width), BF16),
            pltpu.VMEM((chips, tokens, width), BF16),
            pltpu.VMEM((chips, tokens, width), BF16),
            pltpu.VMEM((chips, lines, shard), F32),
            pltpu.VMEM((chips, lines, shard), BF16),
            pltpu.VMEM((chips, lines, shard), BF16),
            pltpu.VMEM((chips, few, shard), F32),
            pltpu.VMEM((chips, few, shard), F32),
            pltpu.VMEM((chips, few, shard), F32),
            pltpu.VMEM((few, shard), F32),
            pltpu.VMEM((stack, width), F32),
            pltpu.VMEM((owners,) + block, BF16),
            pltpu.VMEM((owners,) + block, BF16),
            pltpu.VMEM(block, BF16),
            pltpu.SemaphoreType.DMA((3, chips)),
            pltpu.SemaphoreType.DMA((3, chips)),
            pltpu.SemaphoreType.DMA((3, chips)),
            pltpu.SemaphoreType.DMA((3, chips)),
            pltpu.SemaphoreType.DMA((3, owners)),
            pltpu.SemaphoreType.DMA((3, owners)),
        ],
        compiler_params=pltpu.CompilerParams(
            collective_id=number, has_side_effects=True, vmem_limit_bytes=60 << 20
        ),
        name="finish",
    )(da, pieces, small, output_share)


def exchange(value, axis_name, axis):
    return lax.all_to_all(value, axis_name, split_axis=axis, concat_axis=axis, tiled=True)


def shards(
    hidden_in,
    prior_logits,
    routes,
    block_ids,
    grad_out,
    attn_gain,
    query_weight,
    key_weight,
    value_weight,
    output_weight,
    moe_gain,
    router_weight,
    prior_weight,
    const_mix,
    const_vector,
    gate_weight,
    up_weight,
    down_weight,
):
    token_rows = hidden_in.shape[1]
    model_width = hidden_in.shape[2]
    head_size = model_width // HEADS
    context = lax.axis_size("context")
    owners = lax.axis_size("expert")
    groups = math.gcd(HEADS, context)
    ranks = context // groups
    heads = HEADS // groups
    width = heads * head_size
    length = context * token_rows
    per_owner = gate_weight.shape[0]
    slot_count = per_owner * owners * CAP
    shard_width = model_width // context
    residual = hidden_in[0].astype(F32)
    prior_rows = prior_logits[0]
    route_rows = routes[0]
    cotangent_low = grad_out[0]
    cotangent = cotangent_low.astype(F32)

    inv_rms1 = lax.rsqrt(jnp.mean(residual * residual, axis=1, keepdims=True) + EPS)
    normed_one = residual * inv_rms1
    attn_input = (normed_one * attn_gain).astype(BF16)
    ids_wide = jnp.broadcast_to(block_ids.astype(F32), (8, token_rows))
    stacked = jnp.stack([query_weight, key_weight, value_weight])
    stacked = stacked.reshape(3, shard_width, groups, width)
    pieces = jnp.transpose(stacked, (2, 0, 3, 1)).reshape(groups, 3 * width, shard_width)
    ids_all, w_all, a_all, output_all = gather(
        (ids_wide, pieces, attn_input, output_weight),
        (False, True, False, False), context, ranks, 0,
    )
    a_full = a_all.reshape(length, model_width)
    output_full = output_all.reshape(model_width, model_width)
    ids = ids_all[:, 0, :].reshape(length)
    weights_t = jnp.transpose(w_all, (1, 0, 2)).reshape(3 * width, model_width)
    half = head_size // 2
    freq = jnp.power(THETA, -2.0 * jnp.arange(half, dtype=F32) / head_size)
    angle = freq[:, None] * jnp.arange(length, dtype=jnp.int32).astype(F32)[None, :]
    cos_t, sin_t = jnp.cos(angle), jnp.sin(angle)

    flat_route = route_rows.reshape(-1)
    ffn_hot = (flat_route[:, None] == jnp.arange(FFN_E, dtype=jnp.int32)[None, :]).astype(jnp.int32)
    before = jnp.sum((jnp.cumsum(ffn_hot, axis=0) - ffn_hot) * ffn_hot, axis=1)
    slot_index = jnp.where(
        flat_route < FFN_E,
        flat_route * CAP + before,
        -1,
    ).reshape(token_rows, 2)
    slot_ids = jnp.arange(slot_count, dtype=jnp.int32)[:, None]
    hit_first = slot_ids == slot_index[None, :, 0]
    hit_second = slot_ids == slot_index[None, :, 1]
    pick_first = hit_first.astype(BF16)
    pick_second = hit_second.astype(BF16)
    pick_either = pick_first + pick_second

    blocks = (owners, per_owner, CAP, model_width)

    def pick(rows):
        return jnp.dot(pick_either, rows, preferred_element_type=F32).astype(BF16).reshape(blocks)

    cotangent_late, a_full = lax.optimization_barrier((cotangent_low, a_full))
    grad_arrived = exchange(pick(cotangent_late), "expert", 0)

    (
        attn_out, out_t, log_total, query_t, key_heads, key_t, value_heads,
    ) = attn_forward(a_full, weights_t, cos_t, sin_t, ids, heads, head_size, ranks)
    kept = (out_t, log_total, query_t, key_heads, key_t, value_heads)
    gate_full = lax.all_gather(gate_weight, "context", axis=1, tiled=True)
    up_full = lax.all_gather(up_weight, "context", axis=1, tiled=True)
    down_full = lax.all_gather(down_weight, "context", axis=1, tiled=True)
    granule = TILE // 2
    shard_granules = token_rows // granule
    out_blocks = granules(
        attn_out.reshape(-1, granule, width), ranks, shard_granules, True, 1
    ).reshape(groups, token_rows, width)
    mix_low = jnp.transpose(out_blocks, (1, 0, 2)).reshape(token_rows, model_width)

    after_attn = residual + jnp.dot(mix_low, output_full, preferred_element_type=F32)
    inv_rms2 = lax.rsqrt(jnp.mean(after_attn * after_attn, axis=1, keepdims=True) + EPS)
    normed_two = after_attn * inv_rms2
    moe_input = normed_two * moe_gain
    narrow = jnp.concatenate(
        [router_weight, jnp.transpose(const_mix.reshape(-1, model_width))], axis=1
    )
    narrow_out = jnp.dot(moe_input, narrow, precision=HIGH, preferred_element_type=F32)
    expert_count = router_weight.shape[1]
    consts = const_mix.shape[0]
    logits = narrow_out[:, :expert_count] + jnp.dot(
        prior_rows, prior_weight, precision=HIGH, preferred_element_type=F32
    )
    probs = jax.nn.softmax(logits, axis=1)
    expert_ids = jnp.arange(expert_count, dtype=jnp.int32)
    first_hot = (route_rows[:, 0:1] == expert_ids[None, :]).astype(F32)
    second_hot = (route_rows[:, 1:2] == expert_ids[None, :]).astype(F32)
    chosen = first_hot + second_hot
    gated = probs * chosen
    first_gate = jnp.sum(probs * first_hot, axis=1, keepdims=True)
    second_gate = jnp.sum(probs * second_hot, axis=1, keepdims=True)
    slot_gate = jnp.sum(
        jnp.where(hit_first, first_gate[None, :, 0], 0.0)
        + jnp.where(hit_second, second_gate[None, :, 0], 0.0),
        axis=1,
    )
    def spread(values):
        values = values.reshape(owners, per_owner, CAP)
        return jnp.pad(values, ((0, 0), (0, 8 - per_owner), (0, 128 - CAP)))

    gates, arrived = swap(
        (spread(slot_gate), pick(moe_input.astype(BF16))), "expert", 1, owners, 2
    )
    gates = jnp.transpose(gates[:, :per_owner, :CAP], (1, 0, 2)).reshape(per_owner, -1, 1)

    expert_out, grad_rows, owner_dot, grad_gate, grad_up, grad_down = experts(
        arrived, grad_arrived, gates, gate_full, up_full, down_full
    )
    share_gate = lax.psum_scatter(grad_gate, "context", scatter_dimension=1, tiled=True)
    share_up = lax.psum_scatter(grad_up, "context", scatter_dimension=1, tiled=True)
    share_down = lax.psum_scatter(grad_down, "context", scatter_dimension=1, tiled=True)

    owner_dot = jnp.transpose(owner_dot.reshape(per_owner, owners, CAP), (1, 0, 2))
    slot_dot, grad_back = swap((spread(owner_dot), grad_rows), "expert", 1, owners, 3)
    slot_dot = slot_dot[:, :per_owner, :CAP].reshape(slot_count)
    grad_back = grad_back.reshape(slot_count, model_width)
    expert_out, grad_back = lax.optimization_barrier((expert_out, grad_back))
    returned = exchange(expert_out, "expert", 0).reshape(slot_count, model_width)

    const_soft = jax.nn.softmax(narrow_out[:, expert_count:].reshape(token_rows, consts, 2), axis=2)
    const_gate = gated[:, FFN_E + 2 :]
    copy_gate = gated[:, FFN_E + 1 : FFN_E + 2]
    const_out = [
        const_soft[:, c, 0:1] * moe_input + const_soft[:, c, 1:2] * const_vector[c][None, :]
        for c in range(consts)
    ]
    local_moe = copy_gate * moe_input
    for c in range(consts):
        local_moe = local_moe + const_gate[:, c : c + 1] * const_out[c]
    grad_moe_ffn = lax.dot_general(
        pick_either, grad_back, (((0,), (0,)), ((), ())), preferred_element_type=F32
    )
    first_dot = jnp.sum(jnp.where(hit_first, slot_dot[:, None], 0.0), axis=0)[:, None]
    second_dot = jnp.sum(jnp.where(hit_second, slot_dot[:, None], 0.0), axis=0)[:, None]
    copy_dot = jnp.sum(cotangent * moe_input, axis=1, keepdims=True)
    const_dot = [jnp.sum(cotangent * const_out[c], axis=1, keepdims=True) for c in range(consts)]
    extra = jnp.concatenate(
        [jnp.zeros((token_rows, FFN_E + 1), F32), copy_dot, *const_dot], axis=1
    )
    grad_probs = first_hot * first_dot + second_hot * second_dot + chosen * extra
    grad_logits = probs * (grad_probs - jnp.sum(probs * grad_probs, axis=1, keepdims=True))
    grad_prior_rows = lax.dot_general(
        grad_logits, prior_weight, (((1,), (1,)), ((), ())),
        precision=HIGH, preferred_element_type=F32,
    )
    vector_dot = jnp.dot(
        cotangent, jnp.transpose(const_vector), precision=HIGH, preferred_element_type=F32
    )
    grad_soft = jnp.stack(
        [const_gate * copy_dot, const_gate * vector_dot], axis=2
    )
    grad_mix = const_soft * (grad_soft - jnp.sum(const_soft * grad_soft, axis=2, keepdims=True))
    narrow_grad = jnp.concatenate([grad_logits, grad_mix.reshape(token_rows, -1)], axis=1)
    local_scale = copy_gate + jnp.sum(const_soft[:, :, 0] * const_gate, axis=1, keepdims=True)
    grad_moe_input = (
        grad_moe_ffn
        + lax.dot_general(
            narrow_grad, narrow, (((1,), (1,)), ((), ())),
            precision=HIGH, preferred_element_type=F32,
        )
        + local_scale * cotangent
    )
    small_moe = lax.dot_general(
        narrow_grad, moe_input, (((0,), (0,)), ((), ())),
        precision=HIGH, preferred_element_type=F32,
    )
    small_vector = lax.dot_general(
        const_soft[:, :, 1] * const_gate, cotangent, (((0,), (0,)), ((), ())),
        precision=HIGH, preferred_element_type=F32,
    )
    grad_prior_local = lax.dot_general(
        prior_rows, grad_logits, (((0,), (0,)), ((), ())),
        precision=HIGH, preferred_element_type=F32,
    )
    small_gain = jnp.sum(grad_moe_input * normed_two, axis=0, keepdims=True)
    prior_values = jnp.pad(
        grad_prior_local.reshape(-1), (0, -(expert_count * expert_count) % shard_width)
    ).reshape(-1, 1, shard_width)
    prior_lines = prior_values.shape[0]
    small = jnp.concatenate([small_moe, small_vector, small_gain], axis=0)
    small_lines = small.shape[0]
    small = jnp.concatenate(
        [
            small.reshape(small_lines, context, shard_width),
            jnp.broadcast_to(prior_values, (prior_lines, context, shard_width)),
        ],
        axis=0,
    )
    small = jnp.pad(small, ((0, -small.shape[0] % 8), (0, 0), (0, 0)))
    small = jnp.transpose(small, (1, 0, 2))

    grad_normed_two = grad_moe_input * moe_gain
    grad_after = cotangent + inv_rms2 * (
        grad_normed_two - normed_two * jnp.mean(grad_normed_two * normed_two, axis=1, keepdims=True)
    )
    grad_attn_low = grad_after.astype(BF16)
    grad_mix_low = lax.dot_general(
        grad_attn_low, output_full, (((1,), (1,)), ((), ())), preferred_element_type=F32
    ).astype(BF16)
    grad_pieces = jnp.transpose(grad_mix_low.reshape(token_rows, groups, width), (1, 0, 2))
    grad_own = granules(
        grad_pieces.reshape(-1, granule, width), ranks, shard_granules, False, 4
    ).reshape(-1, width)
    grad_output_local = lax.dot_general(
        mix_low, grad_attn_low, (((0,), (0,)), ((), ())), preferred_element_type=F32
    ).astype(BF16)
    output_parts = exchange(
        grad_output_local.reshape(context, shard_width, model_width), "context", 0
    )

    output_share = jnp.sum(output_parts.astype(F32), axis=0)
    da_part, w_pieces = attn_backward(
        grad_own, a_full, weights_t, cos_t, sin_t, ids, kept, heads, head_size, ranks, context
    )
    da_part, returned = lax.optimization_barrier((da_part, returned))
    grad_attn_input, sums, small_all = finish(
        da_part.reshape(context, token_rows, model_width), w_pieces, small, output_share,
        owners, groups, 5,
    )
    grad_normed_one = grad_attn_input * attn_gain
    grad_input = grad_after + inv_rms1 * (
        grad_normed_one - normed_one * jnp.mean(grad_normed_one * normed_one, axis=1, keepdims=True)
    )
    sums = sums.astype(F32).reshape(4, shard_width, model_width)
    w_sum, output_sum = sums[:3], sums[3]
    small_own = jnp.sum(small_all, axis=0)
    grad_attn_gain = jnp.sum(
        w_sum[0] * query_weight.astype(F32)
        + w_sum[1] * key_weight.astype(F32)
        + w_sum[2] * value_weight.astype(F32),
        axis=1,
    )
    column = lax.axis_index("context") * shard_width
    grad_attn_gain = grad_attn_gain / lax.dynamic_slice_in_dim(attn_gain, column, shard_width)
    mixes = expert_count + 2 * consts
    grad_prior_weight = small_own[small_lines : small_lines + prior_lines].reshape(-1)
    grad_prior_weight = grad_prior_weight[: expert_count * expert_count].reshape(
        expert_count, expert_count
    )
    layer_out = after_attn + local_moe
    layer_out = layer_out + first_gate * lax.dot_general(
        pick_first, returned, (((0,), (0,)), ((), ())), preferred_element_type=F32
    )
    layer_out = layer_out + second_gate * lax.dot_general(
        pick_second, returned, (((0,), (0,)), ((), ())), preferred_element_type=F32
    )
    return (
        layer_out.astype(BF16)[None],
        grad_input[None],
        grad_prior_rows[None],
        grad_attn_gain,
        w_sum[0],
        w_sum[1],
        w_sum[2],
        output_sum,
        small_own[small_lines - 1],
        jnp.transpose(small_own[:expert_count]),
        grad_prior_weight,
        small_own[expert_count:mixes].reshape(consts, 2, shard_width),
        small_own[mixes : mixes + consts],
        share_gate.astype(F32),
        share_up.astype(F32),
        share_down.astype(F32),
    )


def solution(mesh):
    return jax.shard_map(
        shards,
        mesh=mesh,
        in_specs=(
            P("expert", "context", None),
            P("expert", "context", None),
            P("expert", "context", None),
            P("expert", "context"),
            P("expert", "context", None),
            P(),
            P("context", None),
            P("context", None),
            P("context", None),
            P("context", None),
            P(),
            P(),
            P(),
            P(),
            P(),
            P("expert", "context", None),
            P("expert", "context", None),
            P("expert", "context", None),
        ),
        out_specs=(
            P("expert", "context", None),
            P("expert", "context", None),
            P("expert", "context", None),
            P("context"),
            P("context", None),
            P("context", None),
            P("context", None),
            P("context", None),
            P("context"),
            P("context", None),
            P(),
            P(None, None, "context"),
            P(None, "context"),
            P("expert", "context", None),
            P("expert", "context", None),
            P("expert", "context", None),
        ),
        check_vma=False,
    )
```

```python
import functools
import math

import jax
import jax.numpy as jnp
from jax import lax
from jax.experimental import pallas as pl
from jax.experimental.pallas import tpu as pltpu
from jax.sharding import PartitionSpec as P

HEADS = 12
FFN_E = 8
CAP = 96
TILE = 256
EXTRA = 16
HIDDEN_TILE = 256

EPS = 1e-06
THETA = 10000.0
NEGATIVE = -1e30
HIGH = lax.Precision.HIGHEST
F32 = jnp.float32
BF16 = jnp.bfloat16


def dot(left, right, left_dim=1, right_dim=0):
    return lax.dot_general(
        left, right, (((left_dim,), (right_dim,)), ((), ())), preferred_element_type=F32
    )


def turn(rows, cos_rows, sin_rows, heads, size, back=False):
    half = size // 2
    parts = []
    for head in range(heads):
        first = rows[head * size : head * size + half]
        second = rows[head * size + half : (head + 1) * size]
        if back:
            parts.append(first * cos_rows + second * sin_rows)
            parts.append(second * cos_rows - first * sin_rows)
        else:
            parts.append(first * cos_rows - second * sin_rows)
            parts.append(second * cos_rows + first * sin_rows)
    return jnp.concatenate(parts, axis=0)


def own_tile(index, ranks):
    rank = lax.rem(lax.axis_index("context"), ranks)
    place = lax.rem(index, 2)
    return (index // 2) * (2 * ranks) + jnp.where(place == 0, rank, 2 * ranks - 1 - rank)


def lanes(start):
    return span(start, TILE)


def span(start, size):
    return pl.ds(pl.multiple_of(start * size, size), size)


def cost(micros):
    return pl.CostEstimate(flops=micros * 1_150_000_000, bytes_accessed=0, transcendentals=0)


def vmem(count):
    return [pl.BlockSpec(memory_space=pltpu.VMEM)] * count


def hbm(count):
    return [pl.BlockSpec(memory_space=pl.ANY)] * count


def params(number=None, limit=60):
    if number is None:
        return pltpu.CompilerParams(vmem_limit_bytes=limit << 20)
    return pltpu.CompilerParams(
        collective_id=number, has_side_effects=True, vmem_limit_bytes=limit << 20
    )


def remote(source, target, send, recv, device):
    return pltpu.make_async_remote_copy(
        src_ref=source, dst_ref=target, send_sem=send, recv_sem=recv,
        device_id=device, device_id_type=pl.DeviceIdType.MESH,
    )


def meet(context, owners):
    place, row = lax.axis_index("context"), lax.axis_index("expert")
    barrier = pltpu.get_barrier_semaphore()
    for far in range(1, context):
        pl.semaphore_signal(
            barrier, inc=1, device_id={"context": lax.rem(place + far, context)},
            device_id_type=pl.DeviceIdType.MESH,
        )
    for far in range(1, owners):
        pl.semaphore_signal(
            barrier, inc=1, device_id={"expert": lax.rem(row + far, owners)},
            device_id_type=pl.DeviceIdType.MESH,
        )
    pl.semaphore_wait(barrier, context + owners - 2)
    return place, row


def attn_forward_kernel(
    dims,
    ids_ref, pieces_ref, input_ref, cos_ref, sin_ref, grads_ref, output_ref, gate_ref, up_ref,
    out_ref, out_t_ref, lse_ref, query_t_ref, key_ref, key_t_ref, value_ref,
    a_ref, ids_all_ref, wt_ref, output_all_ref, wide_ref, grads_all_ref,
    w_all_ref, value_t_ref, scores_ref, acc_ref,
    local_sem, send_sem, recv_sem, pass_sem, land_sem, row_send, row_recv, wide_send, wide_recv,
):
    heads, size, ranks, scale, context, owners, roles = dims
    length = a_ref.shape[0]
    rows = length // context
    shard = output_ref.shape[0]
    half = wide_ref.shape[2]
    width = heads * size
    tiles = length // TILE
    own_tiles = tiles // ranks
    ext = size + EXTRA
    chips = context // 2
    place, row = meet(context, owners)
    chip, core = place // 2, lax.rem(place, 2)
    partner = place + 1 - 2 * core

    def source(item, device):
        return (ids_ref, pieces_ref.at[device // ranks], input_ref, output_ref)[item]

    def target(item, device):
        return (
            ids_all_ref.at[:, span(device, rows)],
            w_all_ref.at[device],
            a_ref.at[span(device, rows), :],
            output_all_ref.at[span(device, shard), :],
        )[item]

    def sends(item, far):
        peer = partner if isinstance(far, int) and far == 0 else None
        if peer is None:
            peer = 2 * lax.rem(chip + far, chips) + core
        return remote(
            source(item, peer), target(item, place), send_sem.at[item, far],
            recv_sem.at[item, far], {"context": peer},
        )

    def passes(item, far):
        block = target(item, 2 * lax.rem(chip + chips - far, chips) + core)
        return remote(
            block, block, pass_sem.at[item, far], land_sem.at[item, far], {"context": partner}
        )

    def keeps(item):
        return pltpu.make_async_copy(
            source(item, place), target(item, place), local_sem.at[item]
        )

    for item in range(4):
        for far in list(range(1, chips)) + [0]:
            sends(item, far).start()
        keeps(item).start()
    to_rows = []
    for far in range(1, owners):
        peer = lax.rem(row + far, owners)
        to_rows.append(
            remote(
                grads_ref.at[peer], grads_all_ref.at[row], row_send.at[far], row_recv.at[far],
                {"expert": peer},
            )
        )
    to_rows.append(
        pltpu.make_async_copy(grads_ref.at[row], grads_all_ref.at[row], local_sem.at[4])
    )
    wide = []
    for which, weight in enumerate((gate_ref, up_ref)):
        spot = wide_ref.at[which, span(place, shard), :]

        def block(device):
            role = device // 2 // (chips // roles)
            return weight.at[role, :, span(lax.rem(device, 2), half)]

        for far in range(1, context):
            peer = lax.rem(place + far, context)
            wide.append(
                remote(
                    block(peer), spot, wide_send.at[which, far], wide_recv.at[which, far],
                    {"context": peer},
                )
            )
        wide.append(pltpu.make_async_copy(block(place), spot, local_sem.at[5 + which]))
    for copy in to_rows + wide:
        copy.start()

    tail = (lax.broadcasted_iota(jnp.int32, (EXTRA, rows), 0) == 0).astype(BF16)
    for item in range(2):
        for far in range(1, chips):
            sends(item, far).wait_recv()
            passes(item, far).start()
        sends(item, 0).wait_recv()
        keeps(item).wait()
        for far in range(1, chips):
            passes(item, far).wait_recv()
    for device in range(context):
        wt_ref[:, device * shard : (device + 1) * shard] = w_all_ref[device]

    def project(step, carry):
        far, second = step // 2, lax.rem(step, 2)
        block = 2 * lax.rem(chip + chips - far, chips) + jnp.where(second == 0, core, 1 - core)

        @pl.when(jnp.logical_and(far == 0, second == 0))
        def _():
            keeps(2).wait()

        @pl.when(jnp.logical_and(far == 0, second == 1))
        def _():
            sends(2, 0).wait_recv()

        @pl.when(jnp.logical_and(far > 0, second == 0))
        def _():
            sends(2, far).wait_recv()
            passes(2, far).start()

        @pl.when(jnp.logical_and(far > 0, second == 1))
        def _():
            passes(2, far).wait_recv()

        at = span(block, rows)
        both = dot(wt_ref[width:, :], a_ref[at, :], 1, 1)
        key_t = turn(both[:width], cos_ref[:, at], sin_ref[:, at], heads, size)
        key_t_ref[:, at] = key_t.astype(BF16)
        value_t = both[width:]
        for head in range(heads):
            here = slice(head * size, (head + 1) * size)
            key_ref[head, at, :] = key_t[here].T.astype(BF16)
            value_ref[head, at, :] = value_t[here].T.astype(BF16)
            value_t_ref[head * ext : head * ext + size, at] = value_t[here].astype(BF16)
            value_t_ref[head * ext + size : (head + 1) * ext, at] = tail
        return carry

    lax.fori_loop(0, 2 * chips, project, 0)

    def attend(index, carry):
        tile = own_tile(index, ranks)
        at = lanes(tile)
        query_t = dot(wt_ref[:width, :], a_ref[at, :], 1, 1)
        query_t = turn(query_t, cos_ref[:, at], sin_ref[:, at], heads, size)
        query_t = query_t.astype(BF16) * jnp.asarray(scale, BF16)
        query_t_ref[:, lanes(index)] = query_t
        query_ids = ids_all_ref[0:1, at]

        def score(step, tops, masked):
            here = lanes(step)
            fresh = []
            if masked:
                allowed = ids_all_ref[:, here].T[:, 0:1] <= query_ids
            for head in range(heads):
                part = dot(key_ref[head, here, :], query_t[head * size : (head + 1) * size])
                if masked:
                    part = jnp.where(allowed, part, NEGATIVE)
                scores_ref[head, here, :] = part
                fresh.append(
                    jnp.maximum(tops[head], jnp.max(part.reshape(TILE // 8, 8, TILE), axis=0))
                )
            return tuple(fresh)

        tops = tuple(jnp.full((8, TILE), NEGATIVE, F32) for _ in range(heads))
        stop = jnp.minimum(tile + 2, tiles)
        tops = lax.fori_loop(0, tile, lambda s, c: score(s, c, False), tops)
        tops = lax.fori_loop(tile, stop, lambda s, c: score(s, c, True), tops)
        peaks = [jnp.max(top, axis=0, keepdims=True) for top in tops]
        acc_ref[...] = jnp.zeros_like(acc_ref)

        def combine(step, carry):
            here = lanes(step)
            for head in range(heads):
                weights = jnp.exp(scores_ref[head, here, :] - peaks[head]).astype(BF16)
                acc_ref[head] += dot(value_t_ref[head * ext : (head + 1) * ext, here], weights)
            return carry

        lax.fori_loop(0, stop, combine, 0)
        parts = []
        for head in range(heads):
            total = acc_ref[head, size : size + 1, :]
            part = acc_ref[head, :size, :] * (1.0 / total)
            lse_ref[head : head + 1, lanes(index)] = peaks[head] + jnp.log(total)
            parts.append(part)
        joined = jnp.concatenate(parts, axis=0)
        out_t_ref[:, lanes(index)] = joined
        out_ref[lanes(index), :] = joined.T.astype(BF16)
        return carry

    lax.fori_loop(0, own_tiles, attend, 0)
    for far in range(1, chips):
        sends(3, far).wait_recv()
        passes(3, far).start()
    sends(3, 0).wait_recv()
    keeps(3).wait()
    for far in range(1, chips):
        passes(3, far).wait_recv()
    for item in range(4):
        sends(item, 0).wait_send()
        for far in range(1, chips):
            sends(item, far).wait_send()
            passes(item, far).wait_send()
    for copy in to_rows + wide:
        copy.wait()


def attn_forward(
    ids, pieces, attn_input, cos_t, sin_t, grads, output_weight, gate_weight, up_weight,
    heads, size, ranks, context, roles, number,
):
    rows, model = attn_input.shape
    owners = grads.shape[0]
    length = rows * context
    own = length // ranks
    width = heads * size
    ext = size + EXTRA
    shard = output_weight.shape[0]
    chips = context // 2
    shapes = (
        jax.ShapeDtypeStruct((own, width), BF16),
        jax.ShapeDtypeStruct((width, own), F32),
        jax.ShapeDtypeStruct((heads, own), F32),
        jax.ShapeDtypeStruct((width, own), BF16),
        jax.ShapeDtypeStruct((heads, length, size), BF16),
        jax.ShapeDtypeStruct((width, length), BF16),
        jax.ShapeDtypeStruct((heads, length, size), BF16),
        jax.ShapeDtypeStruct((length, model), BF16),
        jax.ShapeDtypeStruct((8, length), F32),
        jax.ShapeDtypeStruct((3 * width, model), BF16),
        jax.ShapeDtypeStruct((model, model), BF16),
        jax.ShapeDtypeStruct((2, model, gate_weight.shape[2] // 2), BF16),
        jax.ShapeDtypeStruct(grads.shape, BF16),
    )
    dims = (heads, size, ranks, size ** (-0.5), context, owners, roles)
    return pl.pallas_call(
        functools.partial(attn_forward_kernel, dims),
        out_shape=shapes,
        in_specs=vmem(5) + hbm(4),
        out_specs=vmem(10) + hbm(3),
        scratch_shapes=[
            pltpu.VMEM((context, 3 * width, shard), BF16),
            pltpu.VMEM((heads * ext, length), BF16),
            pltpu.VMEM((heads, length, TILE), F32),
            pltpu.VMEM((heads, ext, TILE), F32),
            pltpu.SemaphoreType.DMA((7,)),
            pltpu.SemaphoreType.DMA((4, chips)),
            pltpu.SemaphoreType.DMA((4, chips)),
            pltpu.SemaphoreType.DMA((4, chips)),
            pltpu.SemaphoreType.DMA((4, chips)),
            pltpu.SemaphoreType.DMA((owners,)),
            pltpu.SemaphoreType.DMA((owners,)),
            pltpu.SemaphoreType.DMA((2, context)),
            pltpu.SemaphoreType.DMA((2, context)),
        ],
        compiler_params=params(number, 62),
        cost_estimate=cost(80),
        name="attn_forward",
    )(ids, pieces, attn_input, cos_t, sin_t, grads, output_weight, gate_weight, up_weight)


def attn_backward_kernel(
    dims,
    grad_ref, a_ref, wt_ref, cos_ref, sin_ref, ids_all_ref,
    out_t_ref, lse_ref, query_t_ref, key_ref, key_t_ref, value_ref,
    wide_ref, down_ref, outs_ref, output_ref,
    da_ref, pieces_ref, wide_in_ref, down_in_ref, outs_in_ref, output_in_ref,
    query_ref, own_grad_ref, dq_ref, dk_ref, dv_ref, grad_w_ref,
    wide_send, wide_recv, down_send, down_recv, output_send, output_recv,
    row_send, row_recv, local_sem,
):
    heads, size, ranks, scale, context, owners, roles = dims
    length = a_ref.shape[0]
    shard = pieces_ref.shape[2]
    width = heads * size
    tiles = length // TILE
    own_tiles = tiles // ranks
    chips = context // 2
    place, row = meet(context, owners)
    chip, core = place // 2, lax.rem(place, 2)
    copies = []
    for far in range(context):
        peer = lax.rem(place + far, context)
        pairs = (
            (wide_ref.at[:, span(peer, shard), :], wide_in_ref, wide_send, wide_recv),
            (output_ref.at[span(peer, shard), :], output_in_ref, output_send, output_recv),
        )
        for item, (source, target, send, recv) in enumerate(pairs):
            if far == 0:
                copies.append(
                    pltpu.make_async_copy(source, target.at[place], local_sem.at[item])
                )
            else:
                copies.append(
                    remote(
                        source, target.at[place], send.at[far], recv.at[far], {"context": peer}
                    )
                )
    for far in range(owners):
        peer = lax.rem(row + far, owners)
        if far == 0:
            copies.append(
                pltpu.make_async_copy(outs_ref.at[row], outs_in_ref.at[row], local_sem.at[2])
            )
        else:
            copies.append(
                remote(
                    outs_ref.at[peer], outs_in_ref.at[row], row_send.at[far], row_recv.at[far],
                    {"expert": peer},
                )
            )
    for copy in copies:
        copy.start()
    down_rows = down_in_ref.shape[1]

    def down_copy(index, here):
        device = core * chips + index
        source = down_ref.at[span(index, down_rows), :]
        spot = down_in_ref.at[chip]
        if here:
            return pltpu.make_async_copy(source, spot, down_recv.at[chip])
        return remote(
            source, spot, down_send.at[index], down_recv.at[chip], {"context": device}
        )

    for index in range(chips):
        here = core * chips + index == place

        @pl.when(here)
        def _():
            down_copy(index, True).start()

        @pl.when(jnp.logical_not(here))
        def _():
            down_copy(index, False).start()

    dk_ref[...] = jnp.zeros_like(dk_ref)
    dv_ref[...] = jnp.zeros_like(dv_ref)
    da_ref[...] = jnp.zeros_like(da_ref)
    grad_w_ref[...] = jnp.zeros_like(grad_w_ref)
    def attend(index, carry):
        tile = own_tile(index, ranks)
        at = lanes(tile)
        query_t = query_t_ref[:, lanes(index)]
        grad_rows = grad_ref[lanes(index), :]
        grad_t = grad_rows.astype(F32).T
        query_rows = query_t.astype(F32).T.astype(BF16)
        query_ids = ids_all_ref[0:1, at]
        deltas, tops, grads_low = [], [], []
        for head in range(heads):
            rows = slice(head * size, (head + 1) * size)
            query_ref[head] = query_rows[:, rows]
            own_grad_ref[head] = grad_rows[:, rows]
            deltas.append(
                jnp.sum(grad_t[rows] * out_t_ref[rows, lanes(index)], axis=0, keepdims=True)
            )
            tops.append(lse_ref[head : head + 1, lanes(index)])
        grad_t_low = grad_t.astype(BF16)
        dq_ref[...] = jnp.zeros_like(dq_ref)

        def chunk(step, carry, masked):
            here = lanes(step)
            if masked:
                allowed = ids_all_ref[:, here].T[:, 0:1] <= query_ids
            for head in range(heads):
                rows = slice(head * size, (head + 1) * size)
                scores = dot(key_ref[head, here, :], query_t[rows]) - tops[head]
                if masked:
                    scores = jnp.where(allowed, scores, NEGATIVE)
                probs = jnp.exp(scores)
                grad_probs = dot(value_ref[head, here, :], grad_t_low[rows])
                grad_scores = (probs * (grad_probs - deltas[head])).astype(BF16)
                dv_ref[head, here, :] += dot(probs.astype(BF16), own_grad_ref[head])
                dk_ref[head, here, :] += dot(grad_scores, query_ref[head])
                dq_ref[rows, :] += dot(key_t_ref[rows, here], grad_scores)
            return carry

        stop = jnp.minimum(tile + 2, tiles)
        lax.fori_loop(0, tile, lambda s, c: chunk(s, c, False), 0)
        lax.fori_loop(tile, stop, lambda s, c: chunk(s, c, True), 0)
        grad_query = turn(
            dq_ref[...] * scale, cos_ref[:, at], sin_ref[:, at], heads, size, back=True
        )
        grad_w_ref[:width, :] += dot(grad_query.astype(BF16), a_ref[at, :])
        da_ref[at, :] = dot(grad_query.T.astype(BF16), wt_ref[:width, :]).astype(BF16)
        return carry

    lax.fori_loop(0, own_tiles, attend, 0)

    def finish(step, carry):
        at = lanes(step)
        key_grad = jnp.concatenate([dk_ref[head, at, :].T for head in range(heads)], axis=0)
        key_grad = turn(key_grad, cos_ref[:, at], sin_ref[:, at], heads, size, back=True)
        value_grad = jnp.concatenate([dv_ref[head, at, :].T for head in range(heads)], axis=0)
        both = jnp.concatenate([key_grad, value_grad], axis=0)
        grad_w_ref[width:, :] += dot(both.astype(BF16), a_ref[at, :])
        total = da_ref[at, :].astype(F32) + dot(both.T.astype(BF16), wt_ref[width:, :])
        da_ref[at, :] = total.astype(BF16)
        return carry

    lax.fori_loop(0, tiles, finish, 0)
    for piece in range(pieces_ref.shape[0]):
        pieces_ref[piece] = grad_w_ref[:, piece * shard : (piece + 1) * shard]
    for copy in copies:
        copy.wait()
    for index in range(chips):
        here = core * chips + index == place
        giver = 2 * index + place // chips

        @pl.when(jnp.logical_not(here))
        def _():
            down_copy(index, False).wait_send()

        land = down_in_ref.at[index]

        @pl.when(giver == place)
        def _():
            pltpu.make_async_copy(
                down_ref.at[span(0, down_rows), :], land, down_recv.at[index]
            ).wait()

        @pl.when(giver != place)
        def _():
            remote(
                down_ref.at[span(0, down_rows), :], land, down_send.at[index],
                down_recv.at[index], {"context": giver},
            ).wait_recv()


def attn_backward(
    grad_own, a_full, weights_t, cos_t, sin_t, ids, kept,
    grad_wide, grad_down, outs, grad_output, heads, size, ranks, context, roles, number,
):
    length, model = a_full.shape
    width = heads * size
    owners = outs.shape[0]
    shard = model // context
    chips = context // 2
    down_rows = grad_down.shape[0] // chips
    shapes = (
        jax.ShapeDtypeStruct(a_full.shape, BF16),
        jax.ShapeDtypeStruct((context, weights_t.shape[0], shard), F32),
        jax.ShapeDtypeStruct((context, 2, shard, grad_wide.shape[2]), BF16),
        jax.ShapeDtypeStruct((chips, down_rows, model), BF16),
        jax.ShapeDtypeStruct(outs.shape, BF16),
        jax.ShapeDtypeStruct((context, shard, model), BF16),
    )
    dims = (heads, size, ranks, size ** (-0.5), context, owners, roles)
    return pl.pallas_call(
        functools.partial(attn_backward_kernel, dims),
        out_shape=shapes,
        in_specs=vmem(12) + hbm(4),
        out_specs=vmem(2) + hbm(4),
        scratch_shapes=[
            pltpu.VMEM((heads, TILE, size), BF16),
            pltpu.VMEM((heads, TILE, size), BF16),
            pltpu.VMEM((width, TILE), F32),
            pltpu.VMEM((heads, length, size), F32),
            pltpu.VMEM((heads, length, size), F32),
            pltpu.VMEM(weights_t.shape, F32),
        ]
        + [pltpu.SemaphoreType.DMA((context,))] * 2
        + [pltpu.SemaphoreType.DMA((chips,))] * 2
        + [pltpu.SemaphoreType.DMA((context,))] * 2
        + [pltpu.SemaphoreType.DMA((owners,))] * 2
        + [pltpu.SemaphoreType.DMA((3,))],
        compiler_params=params(number, 63),
        cost_estimate=cost(60),
        name="attn_backward",
    )(
        grad_own, a_full, weights_t, cos_t, sin_t, ids, *kept,
        grad_wide, grad_down, outs, grad_output,
    )


def expert_kernel(
    rows_ref, grad_ref, prob_ref, wide_ref, down_ref,
    out_ref, grad_rows_ref, dot_ref, grad_wide_ref, grad_down_ref,
    rows_t_ref, dye_ref, out_acc_ref, grad_acc_ref,
):
    step = pl.program_id(0)
    flat = dye_ref.shape

    @pl.when(step == 0)
    def _():
        rows_t_ref[...] = rows_ref[...].reshape(flat).astype(F32).T.astype(BF16)
        grads = grad_ref[...].reshape(flat).astype(F32)
        dye_ref[...] = (grads * prob_ref[...]).astype(BF16)
        out_acc_ref[...] = jnp.zeros_like(out_acc_ref)
        grad_acc_ref[...] = jnp.zeros_like(grad_acc_ref)

    rows = rows_ref[...].reshape(flat)
    dye = dye_ref[...]
    gate, up, down = wide_ref[0], wide_ref[1], down_ref[...]
    gate_pre = dot(rows, gate)
    up_pre = dot(rows, up)
    sigmoid = jax.nn.sigmoid(gate_pre)
    silu = gate_pre * sigmoid
    hidden = silu * up_pre
    out_acc_ref[...] += dot(hidden.astype(BF16), down)
    grad_hidden = dot(dye, down, 1, 1).astype(BF16).astype(F32)
    grad_down_ref[...] = dot(hidden.T.astype(BF16), dye).astype(BF16)
    grad_gate = (grad_hidden * up_pre * sigmoid * (1.0 + gate_pre * (1.0 - sigmoid))).astype(BF16)
    grad_up = (grad_hidden * silu).astype(BF16)
    grad_wide_ref[0] = dot(rows_t_ref[...], grad_gate).astype(BF16)
    grad_wide_ref[1] = dot(rows_t_ref[...], grad_up).astype(BF16)
    grad_acc_ref[...] += dot(grad_gate, gate, 1, 1) + dot(grad_up, up, 1, 1)

    @pl.when(step == pl.num_programs(0) - 1)
    def _():
        out = out_acc_ref[...]
        out_ref[...] = out.astype(BF16).reshape(out_ref.shape)
        grad_rows_ref[...] = grad_acc_ref[...].astype(BF16).reshape(out_ref.shape)
        grads = grad_ref[...].reshape(flat).astype(F32)
        dot_ref[...] = jnp.sum(out * grads, axis=1, keepdims=True)


def experts(rows, grads, gates, wide_full, down_full):
    width = rows.shape[-1]
    slots = rows.size // width
    hidden = wide_full.shape[2]
    per_row = pl.BlockSpec(rows.shape, lambda t: (0,) * rows.ndim)
    column = pl.BlockSpec((slots, 1), lambda t: (0, 0))
    wide = pl.BlockSpec((2, width, HIDDEN_TILE), lambda t: (0, 0, t))
    tall = pl.BlockSpec((HIDDEN_TILE, width), lambda t: (t, 0))
    return pl.pallas_call(
        expert_kernel,
        grid=(hidden // HIDDEN_TILE,),
        out_shape=(
            jax.ShapeDtypeStruct(rows.shape, BF16),
            jax.ShapeDtypeStruct(rows.shape, BF16),
            jax.ShapeDtypeStruct((slots, 1), F32),
            jax.ShapeDtypeStruct(wide_full.shape, BF16),
            jax.ShapeDtypeStruct(down_full.shape, BF16),
        ),
        in_specs=[per_row, per_row, column, wide, tall],
        out_specs=(per_row, per_row, column, wide, tall),
        scratch_shapes=[
            pltpu.VMEM((width, slots), BF16),
            pltpu.VMEM((slots, width), BF16),
            pltpu.VMEM((slots, width), F32),
            pltpu.VMEM((slots, width), F32),
        ],
        compiler_params=params(),
        cost_estimate=cost(37),
        name="experts",
    )(rows, grads, gates, wide_full, down_full)


def dispatch_kernel(
    context, roles,
    gates_ref, rows_ref, grad_ref, down_ref,
    gates_all, rows_all, grad_all, down_all,
    gates_stage, rows_stage,
    local_sem, send_sem, recv_sem, pass_sem, land_sem, twin_sem, come_sem, relay_sem, reach_sem,
    down_send, down_recv,
):
    owners = rows_ref.shape[0]
    chips = context // 2
    place, row = meet(context, owners)
    chip, core = place // 2, lax.rem(place, 2)
    partner = {"context": place + 1 - 2 * core}
    slot = chip // (chips // roles)
    other = (roles - 1) - slot
    twin = {"context": 2 * lax.rem(chip + chips // 2, chips) + core}
    sent, others, local, passed, lent, relayed = {}, {}, [], [], {}, []
    for far in range(1, owners):
        peer = lax.rem(row + far, owners)
        pairs = [
            (gates_ref.at[peer], gates_all.at[slot, core, row]),
            (rows_ref.at[peer, slot], rows_all.at[slot, core, row]),
        ]
        if roles > 1:
            pairs.append((rows_ref.at[peer, other], rows_stage.at[row]))
        for item, (source, target) in enumerate(pairs):
            sent[item, far] = remote(
                source, target, send_sem.at[item, far], recv_sem.at[item, far], {"expert": peer}
            )
            sent[item, far].start()
    own = (
        (gates_ref.at[row], gates_all.at[slot, core, row]),
        (rows_ref.at[row, slot], rows_all.at[slot, core, row]),
        (grad_ref.at[:, slot], grad_all.at[slot, core]),
    )
    for item, (source, target) in enumerate(own):
        local.append(pltpu.make_async_copy(source, target, local_sem.at[item]))
        local[-1].start()
        passed.append(
            remote(source, target, pass_sem.at[item, 0], land_sem.at[item, 0], partner)
        )
        passed[-1].start()
    if roles > 1:
        own = (
            (gates_ref.at[row], gates_all.at[slot, core, row], gates_all.at[other, core, row]),
            (rows_ref.at[row, other], rows_all.at[slot, core, row], rows_all.at[other, core, row]),
            (grad_ref.at[:, other], grad_all.at[slot, core], grad_all.at[other, core]),
        )
        for item, (source, target, arriving) in enumerate(own):
            lent[item, 0] = (
                remote(source, target, twin_sem.at[item, 0], come_sem.at[item, 0], twin), arriving
            )
            lent[item, 0][0].start()

    half = place // chips
    down_rows = down_ref.shape[1]
    spot = down_all.at[span(lax.rem(place, chips), down_rows), :]

    def down_copy(far, here):
        to_chip = lax.rem(chip + far, chips)
        source = down_ref.at[to_chip // (chips // roles)]
        if here:
            return pltpu.make_async_copy(source, spot, down_recv.at[lax.rem(place, chips)])
        return remote(
            source, spot, down_send.at[far], down_recv.at[lax.rem(place, chips)],
            {"context": 2 * to_chip + half},
        )

    for far in range(1, chips):
        down_copy(far, False).start()

    @pl.when(half == core)
    def _():
        down_copy(0, True).start()

    @pl.when(half != core)
    def _():
        down_copy(0, False).start()

    for far in range(1, owners):
        peer = lax.rem(row + owners - far, owners)
        for item in range(2):
            sent[item, far].wait_recv()
            block = (gates_all, rows_all)[item].at[slot, core, peer]
            passed.append(
                remote(block, block, pass_sem.at[item, far], land_sem.at[item, far], partner)
            )
            passed[-1].start()
            if roles > 1:
                if item == 1:
                    sent[2, far].wait_recv()
                source = block if item == 0 else rows_stage.at[peer]
                arriving = (gates_all, rows_all)[item].at[other, core, peer]
                lent[item, far] = (
                    remote(source, block, twin_sem.at[item, far], come_sem.at[item, far], twin),
                    arriving,
                )
                lent[item, far][0].start()
    for (item, far), (copy, arriving) in lent.items():
        copy.wait_recv()
        relayed.append(
            remote(
                arriving, arriving, relay_sem.at[item, far], reach_sem.at[item, far], partner
            )
        )
        relayed[-1].start()
    for copy in sent.values():
        copy.wait_send()
    for copy, arriving in lent.values():
        copy.wait_send()
    for copy in local + passed + relayed:
        copy.wait()
    for far in range(1, chips):
        down_copy(far, False).wait_send()

    @pl.when(half != core)
    def _():
        down_copy(0, False).wait_send()

    for index in range(chips):
        giver = core * chips + index
        land = down_all.at[span(index, down_rows), :]

        @pl.when(giver == place)
        def _():
            pltpu.make_async_copy(down_ref.at[0], land, down_recv.at[index]).wait()

        @pl.when(giver != place)
        def _():
            remote(
                down_ref.at[0], land, down_send.at[0], down_recv.at[index], {"context": giver}
            ).wait_recv()


def dispatch(gates, rows, grads, down_weight, context, roles, number):
    owners, _, cap, width = rows.shape
    chips = context // 2
    down_rows = down_weight.shape[1]
    return pl.pallas_call(
        functools.partial(dispatch_kernel, context, roles),
        out_shape=(
            jax.ShapeDtypeStruct((roles, 2) + gates.shape, gates.dtype),
            jax.ShapeDtypeStruct((roles, 2, owners, cap, width), BF16),
            jax.ShapeDtypeStruct((roles, 2, owners, cap, width), BF16),
            jax.ShapeDtypeStruct((chips * down_rows, width), BF16),
        ),
        in_specs=vmem(3) + hbm(1),
        out_specs=vmem(3) + hbm(1),
        scratch_shapes=[
            pltpu.VMEM(gates.shape, gates.dtype),
            pltpu.VMEM((owners, cap, width), BF16),
            pltpu.SemaphoreType.DMA((3,)),
        ]
        + [pltpu.SemaphoreType.DMA((3, owners))] * 8
        + [pltpu.SemaphoreType.DMA((chips,))] * 2,
        compiler_params=params(number),
        name="dispatch",
    )(gates, rows, grads, down_weight)


def collect_kernel(
    context, roles,
    dots_ref, grad_ref, out_ref, dots_back, grad_back, out_back,
    dots_twin, grad_twin, out_twin, dots_sum, grad_sum, out_sum, dots_relay, grad_relay,
    pair_send, pair_recv, send_sem, recv_sem, lend_sem, come_sem, relay_send, relay_recv,
    out_send, out_recv, out_lend, out_come,
):
    owners = grad_ref.shape[2]
    chips = context // 2
    place, row = meet(context, owners)
    chip, core = place // 2, lax.rem(place, 2)
    partner = {"context": place + 1 - 2 * core}
    slot = chip // (chips // roles)
    other = (roles - 1) - slot
    twin = {"context": 2 * lax.rem(chip + chips // 2, chips) + core}
    order = list(range(1, owners)) + [0]
    turns = (other, slot) if roles > 1 else (slot,)
    pair, sent, lent, relayed, outs, loans = {}, {}, {}, {}, [], []
    items = (
        (dots_ref, dots_twin, dots_sum, dots_relay, dots_back),
        (grad_ref, grad_twin, grad_sum, grad_relay, grad_back),
    )
    for far in order:
        peer = lax.rem(row + far, owners)
        for which, spot in enumerate(turns):
            for item, (source, landing, _, _, _) in enumerate(items):
                pair[item, which, far] = remote(
                    source.at[spot, 1 - core, peer], landing.at[spot, peer],
                    pair_send.at[item, which, far], pair_recv.at[item, which, far], partner,
                )
                pair[item, which, far].start()
    for which, spot in enumerate(turns):
        outs.append(
            remote(
                out_ref.at[spot, 1 - core], out_twin.at[spot],
                out_send.at[which], out_recv.at[which], partner,
            )
        )
        outs[-1].start()

    def leave(which, far):
        peer = lax.rem(row + far, owners)
        spot = turns[which]
        for item, (_, _, total, relay, back) in enumerate(items):
            if roles > 1 and which == 0:
                target = back.at[row, slot] if far == 0 else relay.at[peer]
                lent[item, far] = remote(
                    total.at[spot, peer], target, lend_sem.at[item, far],
                    come_sem.at[item, far], twin,
                )
                lent[item, far].start()
            elif far > 0:
                sent[item, far] = remote(
                    total.at[spot, peer], back.at[row, slot], send_sem.at[item, far],
                    recv_sem.at[item, far], {"expert": peer},
                )
                sent[item, far].start()

    last = None
    for far in order:
        peer = lax.rem(row + far, owners)
        for which, spot in enumerate(turns):
            for item, (source, landing, total, _, _) in enumerate(items):
                pair[item, which, far].wait_recv()
                summed = source[spot, core, peer].astype(F32) + landing[spot, peer].astype(F32)
                total[spot, peer] = summed.astype(total.dtype)
            if last is not None:
                leave(*last)
            last = (which, far)
    dots_back[row, slot] = dots_sum[slot, row]
    grad_back[row, slot] = grad_sum[slot, row]
    leave(*last)
    if roles > 1:
        for far in range(1, owners):
            peer = lax.rem(row + far, owners)
            for item, (_, _, _, relay, back) in enumerate(items):
                lent[item, far].wait_recv()
                relayed[item, far] = remote(
                    relay.at[peer], back.at[row, other], relay_send.at[item, far],
                    relay_recv.at[item, far], {"expert": peer},
                )
                relayed[item, far].start()
    for which, spot in enumerate(turns):
        outs[which].wait_recv()
        for peer in range(owners):
            summed = out_ref[spot, core, peer].astype(F32) + out_twin[spot, peer].astype(F32)
            if roles > 1 and which == 0:
                out_sum[peer] = summed.astype(BF16)
            else:
                out_back[peer, slot] = summed.astype(BF16)
    if roles > 1:
        loans.append(
            remote(out_sum, out_back.at[:, slot], out_lend, out_come, twin)
        )
        loans[-1].start()
        for item in range(2):
            lent[item, 0].wait_recv()
    for copy in list(pair.values()) + outs + list(lent.values()):
        copy.wait_send()
    for copy in list(sent.values()) + list(relayed.values()) + loans:
        copy.wait()


def collect(dots, grads, outs, context, roles, number):
    _, _, owners, cap, width = grads.shape
    home = (owners, roles, cap, width)
    small = (owners, roles) + dots.shape[3:]
    return pl.pallas_call(
        functools.partial(collect_kernel, context, roles),
        out_shape=(
            jax.ShapeDtypeStruct(small, F32),
            jax.ShapeDtypeStruct(home, BF16),
            jax.ShapeDtypeStruct(home, BF16),
        ),
        in_specs=vmem(3),
        out_specs=vmem(3),
        scratch_shapes=[
            pltpu.VMEM((roles, owners) + dots.shape[3:], F32),
            pltpu.VMEM((roles, owners, cap, width), BF16),
            pltpu.VMEM((roles, owners, cap, width), BF16),
            pltpu.VMEM((roles, owners) + dots.shape[3:], F32),
            pltpu.VMEM((roles, owners, cap, width), BF16),
            pltpu.VMEM((owners, cap, width), BF16),
            pltpu.VMEM((owners,) + dots.shape[3:], F32),
            pltpu.VMEM((owners, cap, width), BF16),
            pltpu.SemaphoreType.DMA((2, roles, owners)),
            pltpu.SemaphoreType.DMA((2, roles, owners)),
        ]
        + [pltpu.SemaphoreType.DMA((2, owners))] * 6
        + [pltpu.SemaphoreType.DMA((roles,))] * 2
        + [pltpu.SemaphoreType.DMA] * 2,
        compiler_params=params(number),
        name="collect",
    )(dots, grads, outs)


def granule_kernel(ranks, shard_granules, outward, source_ref, target_ref, send_sem, recv_sem):
    place = lax.axis_index("context")
    context = lax.axis_size("context")
    group, rank = place // ranks, lax.rem(place, ranks)
    groups = context // ranks
    owned = context * shard_granules // ranks
    barrier = pltpu.get_barrier_semaphore()
    for far in range(1, context):
        pl.semaphore_signal(
            barrier, inc=1, device_id={"context": lax.rem(place + far, context)},
            device_id_type=pl.DeviceIdType.MESH,
        )
    pl.semaphore_wait(barrier, context - 1)

    def owner_rank(granule):
        spot = lax.rem(granule // 2, 2 * ranks)
        return jnp.minimum(spot, 2 * ranks - 1 - spot)

    def owner_slot(granule):
        tile = granule // 2
        spot = lax.rem(tile, 2 * ranks)
        upper = jnp.where(spot >= ranks, 1, 0)
        return (tile // (2 * ranks) * 2 + upper) * 2 + lax.rem(granule, 2)

    def granule_of(slot):
        return own_tile(slot // 2, ranks) * 2 + lax.rem(slot, 2)

    def remote(source, target, index, device):
        return pltpu.make_async_remote_copy(
            src_ref=source, dst_ref=target, send_sem=send_sem.at[index],
            recv_sem=recv_sem.at[index], device_id={"context": device},
            device_id_type=pl.DeviceIdType.MESH,
        )

    def outgoing(step):
        if outward:
            granule = granule_of(step)
            home = granule // shard_granules
            slot = group * shard_granules + lax.rem(granule, shard_granules)
            return home, source_ref.at[step], slot
        other, spot = step // shard_granules, step % shard_granules
        granule = place * shard_granules + spot
        return other * ranks + owner_rank(granule), source_ref.at[step], owner_slot(granule)

    def incoming(step):
        if outward:
            other, spot = step // shard_granules, step % shard_granules
            return other * ranks + owner_rank(place * shard_granules + spot)
        return granule_of(step) // shard_granules

    for step in range(owned):
        device, source, slot = outgoing(step)

        @pl.when(device == place)
        def _():
            pltpu.make_async_copy(source, target_ref.at[slot], recv_sem.at[slot]).start()

        @pl.when(device != place)
        def _():
            pltpu.make_async_remote_copy(
                src_ref=source, dst_ref=target_ref.at[slot], send_sem=send_sem.at[step],
                recv_sem=recv_sem.at[slot], device_id={"context": device},
                device_id_type=pl.DeviceIdType.MESH,
            ).start()

    for step in range(owned):
        device, source, slot = outgoing(step)

        @pl.when(device != place)
        def _():
            remote(source, target_ref.at[slot], step, device).wait_send()

        sender = incoming(step)

        @pl.when(sender == place)
        def _():
            pltpu.make_async_copy(source_ref.at[0], target_ref.at[step], recv_sem.at[step]).wait()

        @pl.when(sender != place)
        def _():
            remote(source_ref.at[0], target_ref.at[step], step, sender).wait_recv()


def granules(rows, ranks, shard_granules, outward, number):
    owned = rows.shape[0]
    return pl.pallas_call(
        functools.partial(granule_kernel, ranks, shard_granules, outward),
        out_shape=jax.ShapeDtypeStruct(rows.shape, rows.dtype),
        in_specs=vmem(1),
        out_specs=vmem(1)[0],
        scratch_shapes=[
            pltpu.SemaphoreType.DMA((owned,)),
            pltpu.SemaphoreType.DMA((owned,)),
        ],
        compiler_params=pltpu.CompilerParams(
            collective_id=number, has_side_effects=True, vmem_limit_bytes=60 << 20
        ),
        name="granules",
    )(rows)


def finish_kernel(
    chips, owners, groups,
    da_ref, pieces_ref, small_ref, output_ref,
    total_ref, sums_ref, small_all_ref,
    da_twin, da_sum, da_in, w_twin, w_sum, w_in, s_twin, s_sum, s_in, s_total,
    stack_ref, shares, shares_in, block_ref,
    pair_send, pair_recv, chip_send, chip_recv, row_send, row_recv,
):
    place = lax.axis_index("context")
    row = lax.axis_index("expert")
    chip, core = place // 2, lax.rem(place, 2)
    partner = 2 * chip + 1 - core
    barrier = pltpu.get_barrier_semaphore()

    def greet(device):
        pl.semaphore_signal(
            barrier, inc=1, device_id=device, device_id_type=pl.DeviceIdType.MESH
        )

    greet({"context": partner})
    for far in range(1, chips):
        greet({"context": 2 * lax.rem(chip + far, chips) + core})
    for far in range(1, owners):
        greet({"expert": lax.rem(row + far, owners)})
    pl.semaphore_wait(barrier, chips + owners - 1)

    order = list(range(1, chips)) + [0]
    pair = {}
    for item, (source, target) in enumerate(
        ((small_ref, s_twin), (pieces_ref, w_twin), (da_ref, da_twin))
    ):
        for far in order:
            peer = lax.rem(chip + far, chips)
            pair[item, far] = remote(
                source.at[2 * peer + 1 - core], target.at[peer],
                pair_send.at[item, far], pair_recv.at[item, far], {"context": partner},
            )
            pair[item, far].start()

    def across(item, source, target, far):
        peer = lax.rem(chip + far, chips)
        return remote(
            source.at[peer], target.at[chip], chip_send.at[item, far], chip_recv.at[item, far],
            {"context": 2 * peer + core},
        )

    for far in order:
        peer = lax.rem(chip + far, chips)
        mine = 2 * peer + core
        pair[0, far].wait_recv()
        s_sum[peer] = small_ref[mine] + s_twin[peer]
        pair[1, far].wait_recv()
        w_sum[peer] = (pieces_ref[mine] + w_twin[peer]).astype(BF16)
    moved = {}
    for far in range(1, chips):
        moved[0, far] = across(0, s_sum, s_in, far)
        moved[0, far].start()
        moved[1, far] = across(1, w_sum, w_in, far)
        moved[1, far].start()
    last = None
    for far in order:
        peer = lax.rem(chip + far, chips)
        pair[2, far].wait_recv()
        da_sum[peer] = (
            da_ref[2 * peer + core].astype(F32) + da_twin[peer].astype(F32)
        ).astype(BF16)
        if last is not None:
            moved[2, last] = across(2, da_sum, da_in, last)
            moved[2, last].start()
        last = far
    for far in range(1, chips):
        moved[0, far].wait_recv()
        moved[1, far].wait_recv()
    s_in[chip] = s_sum[chip]
    w_in[chip] = w_sum[chip]

    width = w_sum.shape[1] // 3
    shard = w_sum.shape[2]
    per_group = chips // groups
    for group in range(groups):
        total = w_in[group * per_group].astype(F32)
        for other in range(1, per_group):
            total = total + w_in[group * per_group + other].astype(F32)
        for which in range(3):
            stack_ref[which * shard : (which + 1) * shard, group * width : (group + 1) * width] = (
                total[which * width : (which + 1) * width].T
            )
    total = output_ref[0].astype(F32)
    for other in range(1, output_ref.shape[0]):
        total = total + output_ref[other].astype(F32)
    stack_ref[3 * shard :, :] = total
    lines = shares.shape[1]
    for owner in range(owners):
        shares[owner] = stack_ref[owner * lines : (owner + 1) * lines, :].astype(BF16)
    total = s_in[0]
    for other in range(1, chips):
        total = total + s_in[other]
    s_total[...] = total
    rows = {}
    for far in range(1, owners):
        peer = lax.rem(row + far, owners)
        rows[0, far] = remote(
            shares.at[peer], shares_in.at[row], row_send.at[0, far], row_recv.at[0, far],
            {"expert": peer},
        )
        rows[0, far].start()
        rows[1, far] = remote(
            s_total, small_all_ref.at[row], row_send.at[1, far], row_recv.at[1, far],
            {"expert": peer},
        )
        rows[1, far].start()
    shares_in[row] = shares[row]
    small_all_ref[row] = total
    for far in range(1, owners):
        rows[0, far].wait_recv()
    summed = shares_in[0].astype(F32)
    for other in range(1, owners):
        summed = summed + shares_in[other].astype(F32)
    block_ref[...] = summed.astype(BF16)
    for far in range(1, chips):
        moved[2, far].wait_recv()
    for far in range(1, owners):
        peer = lax.rem(row + far, owners)
        rows[2, far] = remote(
            block_ref, sums_ref.at[row], row_send.at[2, far], row_recv.at[2, far],
            {"expert": peer},
        )
        rows[2, far].start()
    sums_ref[row] = summed.astype(BF16)
    da_in[chip] = da_sum[chip]
    total = da_in[0].astype(F32)
    for other in range(1, chips):
        total = total + da_in[other].astype(F32)
    total_ref[...] = total
    for far in range(1, owners):
        rows[1, far].wait_recv()
        rows[2, far].wait_recv()
    for copy in list(pair.values()) + list(moved.values()) + list(rows.values()):
        copy.wait_send()


def finish(da, pieces, small, output_parts, owners, groups, number):
    context, tokens, width = da.shape
    chips = context // 2
    lines, shard = pieces.shape[1:]
    few = small.shape[1]
    stack = 4 * shard
    block = (stack // owners, width)
    return pl.pallas_call(
        functools.partial(finish_kernel, chips, owners, groups),
        out_shape=(
            jax.ShapeDtypeStruct((tokens, width), F32),
            jax.ShapeDtypeStruct((owners,) + block, BF16),
            jax.ShapeDtypeStruct((owners, few, shard), F32),
        ),
        in_specs=vmem(4),
        out_specs=vmem(3),
        scratch_shapes=[
            pltpu.VMEM((chips, tokens, width), BF16),
            pltpu.VMEM((chips, tokens, width), BF16),
            pltpu.VMEM((chips, tokens, width), BF16),
            pltpu.VMEM((chips, lines, shard), F32),
            pltpu.VMEM((chips, lines, shard), BF16),
            pltpu.VMEM((chips, lines, shard), BF16),
            pltpu.VMEM((chips, few, shard), F32),
            pltpu.VMEM((chips, few, shard), F32),
            pltpu.VMEM((chips, few, shard), F32),
            pltpu.VMEM((few, shard), F32),
            pltpu.VMEM((stack, width), F32),
            pltpu.VMEM((owners,) + block, BF16),
            pltpu.VMEM((owners,) + block, BF16),
            pltpu.VMEM(block, BF16),
            pltpu.SemaphoreType.DMA((3, chips)),
            pltpu.SemaphoreType.DMA((3, chips)),
            pltpu.SemaphoreType.DMA((3, chips)),
            pltpu.SemaphoreType.DMA((3, chips)),
            pltpu.SemaphoreType.DMA((3, owners)),
            pltpu.SemaphoreType.DMA((3, owners)),
        ],
        compiler_params=pltpu.CompilerParams(
            collective_id=number, has_side_effects=True, vmem_limit_bytes=60 << 20
        ),
        name="finish",
    )(da, pieces, small, output_parts)


def shards(
    hidden_in,
    prior_logits,
    routes,
    block_ids,
    grad_out,
    attn_gain,
    query_weight,
    key_weight,
    value_weight,
    output_weight,
    moe_gain,
    router_weight,
    prior_weight,
    const_mix,
    const_vector,
    gate_weight,
    up_weight,
    down_weight,
):
    token_rows = hidden_in.shape[1]
    model_width = hidden_in.shape[2]
    head_size = model_width // HEADS
    context = lax.axis_size("context")
    owners = lax.axis_size("expert")
    groups = math.gcd(HEADS, context)
    ranks = context // groups
    heads = HEADS // groups
    width = heads * head_size
    length = context * token_rows
    per_owner = gate_weight.shape[0]
    slot_count = per_owner * owners * CAP
    shard_width = model_width // context
    roles = per_owner
    residual = hidden_in[0].astype(F32)
    prior_rows = prior_logits[0]
    route_rows = routes[0]
    cotangent_low = grad_out[0]
    cotangent = cotangent_low.astype(F32)

    inv_rms1 = lax.rsqrt(jnp.mean(residual * residual, axis=1, keepdims=True) + EPS)
    normed_one = residual * inv_rms1
    attn_input = (normed_one * attn_gain).astype(BF16)
    ids_wide = jnp.broadcast_to(block_ids.astype(F32), (8, token_rows))
    stacked = jnp.stack([query_weight, key_weight, value_weight])
    stacked = stacked.reshape(3, shard_width, groups, width)
    pieces = jnp.transpose(stacked, (2, 0, 3, 1)).reshape(groups, 3 * width, shard_width)
    half = head_size // 2
    freq = jnp.power(THETA, -2.0 * jnp.arange(half, dtype=F32) / head_size)
    angle = freq[:, None] * jnp.arange(length, dtype=jnp.int32).astype(F32)[None, :]
    cos_t, sin_t = jnp.cos(angle), jnp.sin(angle)

    flat_route = route_rows.reshape(-1)
    ffn_hot = (flat_route[:, None] == jnp.arange(FFN_E, dtype=jnp.int32)[None, :]).astype(jnp.int32)
    before = jnp.sum((jnp.cumsum(ffn_hot, axis=0) - ffn_hot) * ffn_hot, axis=1)
    slot_index = jnp.where(
        flat_route < FFN_E,
        flat_route * CAP + before,
        -1,
    ).reshape(token_rows, 2)
    slot_ids = jnp.arange(slot_count, dtype=jnp.int32)[:, None]
    hit_first = slot_ids == slot_index[None, :, 0]
    hit_second = slot_ids == slot_index[None, :, 1]
    pick_first = hit_first.astype(BF16)
    pick_second = hit_second.astype(BF16)
    pick_either = pick_first + pick_second

    blocks = (owners, per_owner, CAP, model_width)

    def pick(rows):
        return jnp.dot(pick_either, rows, preferred_element_type=F32).astype(BF16).reshape(blocks)

    (
        attn_out, out_t, log_total, query_t, key_heads, key_t, value_heads,
        a_full, ids, weights_t, output_full, wide_full, grad_arrived,
    ) = attn_forward(
        ids_wide, pieces, attn_input, cos_t, sin_t, pick(cotangent_low),
        output_weight, gate_weight, up_weight, heads, head_size, ranks, context, roles, 0,
    )
    kept = (out_t, log_total, query_t, key_heads, key_t, value_heads)
    granule = TILE // 2
    shard_granules = token_rows // granule
    out_blocks = granules(
        attn_out.reshape(-1, granule, width), ranks, shard_granules, True, 1
    ).reshape(groups, token_rows, width)
    mix_low = jnp.transpose(out_blocks, (1, 0, 2)).reshape(token_rows, model_width)

    after_attn = residual + jnp.dot(mix_low, output_full, preferred_element_type=F32)
    inv_rms2 = lax.rsqrt(jnp.mean(after_attn * after_attn, axis=1, keepdims=True) + EPS)
    normed_two = after_attn * inv_rms2
    moe_input = normed_two * moe_gain
    narrow = jnp.concatenate(
        [router_weight, jnp.transpose(const_mix.reshape(-1, model_width))], axis=1
    )
    narrow_out = jnp.dot(moe_input, narrow, precision=HIGH, preferred_element_type=F32)
    expert_count = router_weight.shape[1]
    consts = const_mix.shape[0]
    logits = narrow_out[:, :expert_count] + jnp.dot(
        prior_rows, prior_weight, precision=HIGH, preferred_element_type=F32
    )
    probs = jax.nn.softmax(logits, axis=1)
    expert_ids = jnp.arange(expert_count, dtype=jnp.int32)
    first_hot = (route_rows[:, 0:1] == expert_ids[None, :]).astype(F32)
    second_hot = (route_rows[:, 1:2] == expert_ids[None, :]).astype(F32)
    chosen = first_hot + second_hot
    gated = probs * chosen
    first_gate = jnp.sum(probs * first_hot, axis=1, keepdims=True)
    second_gate = jnp.sum(probs * second_hot, axis=1, keepdims=True)
    slot_gate = jnp.sum(
        jnp.where(hit_first, first_gate[None, :, 0], 0.0)
        + jnp.where(hit_second, second_gate[None, :, 0], 0.0),
        axis=1,
    )
    def spread(values):
        values = values.reshape(owners, per_owner, CAP)
        return jnp.pad(values, ((0, 0), (0, 8 - per_owner), (0, 128 - CAP)))

    gates, arrived, grad_arrived, down_full = dispatch(
        spread(slot_gate), pick(moe_input.astype(BF16)), grad_arrived, down_weight,
        context, roles, 2,
    )
    role = lax.axis_index("context") // 2 // (context // 2 // roles)
    gates = lax.dynamic_index_in_dim(gates, role, 3, keepdims=False)[..., :CAP].reshape(-1, 1)

    expert_out, grad_rows, owner_dot, grad_wide, grad_down = experts(
        arrived, grad_arrived, gates, wide_full, down_full
    )
    owner_dot = jnp.pad(
        owner_dot.reshape(roles, 2, owners, 1, CAP), ((0, 0),) * 3 + ((0, 7), (0, 128 - CAP))
    )
    slot_dot, grad_back, expert_out = collect(
        owner_dot, grad_rows, expert_out, context, roles, 3
    )
    slot_dot = slot_dot[:, :, 0, :CAP].reshape(slot_count)
    grad_back = grad_back.reshape(slot_count, model_width)

    const_soft = jax.nn.softmax(narrow_out[:, expert_count:].reshape(token_rows, consts, 2), axis=2)
    const_gate = gated[:, FFN_E + 2 :]
    copy_gate = gated[:, FFN_E + 1 : FFN_E + 2]
    const_out = [
        const_soft[:, c, 0:1] * moe_input + const_soft[:, c, 1:2] * const_vector[c][None, :]
        for c in range(consts)
    ]
    local_moe = copy_gate * moe_input
    for c in range(consts):
        local_moe = local_moe + const_gate[:, c : c + 1] * const_out[c]
    grad_moe_ffn = lax.dot_general(
        pick_either, grad_back, (((0,), (0,)), ((), ())), preferred_element_type=F32
    )
    first_dot = jnp.sum(jnp.where(hit_first, slot_dot[:, None], 0.0), axis=0)[:, None]
    second_dot = jnp.sum(jnp.where(hit_second, slot_dot[:, None], 0.0), axis=0)[:, None]
    copy_dot = jnp.sum(cotangent * moe_input, axis=1, keepdims=True)
    const_dot = [jnp.sum(cotangent * const_out[c], axis=1, keepdims=True) for c in range(consts)]
    extra = jnp.concatenate(
        [jnp.zeros((token_rows, FFN_E + 1), F32), copy_dot, *const_dot], axis=1
    )
    grad_probs = first_hot * first_dot + second_hot * second_dot + chosen * extra
    grad_logits = probs * (grad_probs - jnp.sum(probs * grad_probs, axis=1, keepdims=True))
    grad_prior_rows = lax.dot_general(
        grad_logits, prior_weight, (((1,), (1,)), ((), ())),
        precision=HIGH, preferred_element_type=F32,
    )
    vector_dot = jnp.dot(
        cotangent, jnp.transpose(const_vector), precision=HIGH, preferred_element_type=F32
    )
    grad_soft = jnp.stack(
        [const_gate * copy_dot, const_gate * vector_dot], axis=2
    )
    grad_mix = const_soft * (grad_soft - jnp.sum(const_soft * grad_soft, axis=2, keepdims=True))
    narrow_grad = jnp.concatenate([grad_logits, grad_mix.reshape(token_rows, -1)], axis=1)
    local_scale = copy_gate + jnp.sum(const_soft[:, :, 0] * const_gate, axis=1, keepdims=True)
    grad_moe_input = (
        grad_moe_ffn
        + lax.dot_general(
            narrow_grad, narrow, (((1,), (1,)), ((), ())),
            precision=HIGH, preferred_element_type=F32,
        )
        + local_scale * cotangent
    )
    small_moe = lax.dot_general(
        narrow_grad, moe_input, (((0,), (0,)), ((), ())),
        precision=HIGH, preferred_element_type=F32,
    )
    small_vector = lax.dot_general(
        const_soft[:, :, 1] * const_gate, cotangent, (((0,), (0,)), ((), ())),
        precision=HIGH, preferred_element_type=F32,
    )
    grad_prior_local = lax.dot_general(
        prior_rows, grad_logits, (((0,), (0,)), ((), ())),
        precision=HIGH, preferred_element_type=F32,
    )
    small_gain = jnp.sum(grad_moe_input * normed_two, axis=0, keepdims=True)
    prior_values = jnp.pad(
        grad_prior_local.reshape(-1), (0, -(expert_count * expert_count) % shard_width)
    ).reshape(-1, 1, shard_width)
    prior_lines = prior_values.shape[0]
    small = jnp.concatenate([small_moe, small_vector, small_gain], axis=0)
    small_lines = small.shape[0]
    small = jnp.concatenate(
        [
            small.reshape(small_lines, context, shard_width),
            jnp.broadcast_to(prior_values, (prior_lines, context, shard_width)),
        ],
        axis=0,
    )
    small = jnp.pad(small, ((0, -small.shape[0] % 8), (0, 0), (0, 0)))
    small = jnp.transpose(small, (1, 0, 2))

    grad_normed_two = grad_moe_input * moe_gain
    grad_after = cotangent + inv_rms2 * (
        grad_normed_two - normed_two * jnp.mean(grad_normed_two * normed_two, axis=1, keepdims=True)
    )
    grad_attn_low = grad_after.astype(BF16)
    grad_mix_low = lax.dot_general(
        grad_attn_low, output_full, (((1,), (1,)), ((), ())), preferred_element_type=F32
    ).astype(BF16)
    grad_pieces = jnp.transpose(grad_mix_low.reshape(token_rows, groups, width), (1, 0, 2))
    grad_own = granules(
        grad_pieces.reshape(-1, granule, width), ranks, shard_granules, False, 4
    ).reshape(-1, width)
    grad_output_local = lax.dot_general(
        mix_low, grad_attn_low, (((0,), (0,)), ((), ())), preferred_element_type=F32
    ).astype(BF16)
    da_part, w_pieces, wide_parts, down_parts, returned, output_parts = attn_backward(
        grad_own, a_full, weights_t, cos_t, sin_t, ids, kept,
        grad_wide, grad_down, expert_out, grad_output_local,
        heads, head_size, ranks, context, roles, 6,
    )
    returned = returned.reshape(slot_count, model_width)
    same = context // 2 // roles
    wide_parts = wide_parts.reshape(roles, same, 2, 2, shard_width, -1)
    wide_sum = jnp.sum(wide_parts.astype(F32), axis=1)
    wide_sum = jnp.transpose(wide_sum, (2, 0, 3, 1, 4)).reshape(2, roles, shard_width, -1)
    down_sum = jnp.sum(
        down_parts.reshape(roles, same, -1, model_width).astype(F32), axis=1
    )
    grad_attn_input, sums, small_all = finish(
        da_part.reshape(context, token_rows, model_width), w_pieces, small, output_parts,
        owners, groups, 5,
    )
    grad_normed_one = grad_attn_input * attn_gain
    grad_input = grad_after + inv_rms1 * (
        grad_normed_one - normed_one * jnp.mean(grad_normed_one * normed_one, axis=1, keepdims=True)
    )
    sums = sums.astype(F32).reshape(4, shard_width, model_width)
    w_sum, output_sum = sums[:3], sums[3]
    small_own = jnp.sum(small_all, axis=0)
    grad_attn_gain = jnp.sum(
        w_sum[0] * query_weight.astype(F32)
        + w_sum[1] * key_weight.astype(F32)
        + w_sum[2] * value_weight.astype(F32),
        axis=1,
    )
    column = lax.axis_index("context") * shard_width
    grad_attn_gain = grad_attn_gain / lax.dynamic_slice_in_dim(attn_gain, column, shard_width)
    mixes = expert_count + 2 * consts
    grad_prior_weight = small_own[small_lines : small_lines + prior_lines].reshape(-1)
    grad_prior_weight = grad_prior_weight[: expert_count * expert_count].reshape(
        expert_count, expert_count
    )
    layer_out = after_attn + local_moe
    layer_out = layer_out + first_gate * lax.dot_general(
        pick_first, returned, (((0,), (0,)), ((), ())), preferred_element_type=F32
    )
    layer_out = layer_out + second_gate * lax.dot_general(
        pick_second, returned, (((0,), (0,)), ((), ())), preferred_element_type=F32
    )
    return (
        layer_out.astype(BF16)[None],
        grad_input[None],
        grad_prior_rows[None],
        grad_attn_gain,
        w_sum[0],
        w_sum[1],
        w_sum[2],
        output_sum,
        small_own[small_lines - 1],
        jnp.transpose(small_own[:expert_count]),
        grad_prior_weight,
        small_own[expert_count:mixes].reshape(consts, 2, shard_width),
        small_own[mixes : mixes + consts],
        wide_sum[0],
        wide_sum[1],
        down_sum,
    )


def solution(mesh):
    return jax.shard_map(
        shards,
        mesh=mesh,
        in_specs=(
            P("expert", "context", None),
            P("expert", "context", None),
            P("expert", "context", None),
            P("expert", "context"),
            P("expert", "context", None),
            P(),
            P("context", None),
            P("context", None),
            P("context", None),
            P("context", None),
            P(),
            P(),
            P(),
            P(),
            P(),
            P("expert", "context", None),
            P("expert", "context", None),
            P("expert", "context", None),
        ),
        out_specs=(
            P("expert", "context", None),
            P("expert", "context", None),
            P("expert", "context", None),
            P("context"),
            P("context", None),
            P("context", None),
            P("context", None),
            P("context", None),
            P("context"),
            P("context", None),
            P(),
            P(None, None, "context"),
            P(None, "context"),
            P("expert", "context", None),
            P("expert", "context", None),
            P("expert", "context", None),
        ),
        check_vma=False,
    )
```

```python
import functools
import math

import jax
import jax.numpy as jnp
from jax import lax
from jax.experimental import pallas as pl
from jax.experimental.pallas import tpu as pltpu
from jax.sharding import PartitionSpec as P

HEADS = 12
FFN_E = 8
CAP = 96
TILE = 256
EXTRA = 16
HIDDEN_TILE = 256

EPS = 1e-06
THETA = 10000.0
NEGATIVE = -1e30
HIGH = lax.Precision.HIGHEST
F32 = jnp.float32
BF16 = jnp.bfloat16


def dot(left, right, left_dim=1, right_dim=0):
    return lax.dot_general(
        left, right, (((left_dim,), (right_dim,)), ((), ())), preferred_element_type=F32
    )


def turn(rows, cos_rows, sin_rows, heads, size, back=False):
    half = size // 2
    parts = []
    for head in range(heads):
        first = rows[head * size : head * size + half]
        second = rows[head * size + half : (head + 1) * size]
        if back:
            parts.append(first * cos_rows + second * sin_rows)
            parts.append(second * cos_rows - first * sin_rows)
        else:
            parts.append(first * cos_rows - second * sin_rows)
            parts.append(second * cos_rows + first * sin_rows)
    return jnp.concatenate(parts, axis=0)


def own_tile(index, ranks):
    rank = lax.rem(lax.axis_index("context"), ranks)
    place = lax.rem(index, 2)
    return (index // 2) * (2 * ranks) + jnp.where(place == 0, rank, 2 * ranks - 1 - rank)


def granule_of(slot, ranks):
    return own_tile(slot // 2, ranks) * 2 + lax.rem(slot, 2)


def owner_rank(granule, ranks):
    spot = lax.rem(granule // 2, 2 * ranks)
    return jnp.minimum(spot, 2 * ranks - 1 - spot)


def owner_slot(granule, ranks):
    tile = granule // 2
    upper = jnp.where(lax.rem(tile, 2 * ranks) >= ranks, 1, 0)
    return (tile // (2 * ranks) * 2 + upper) * 2 + lax.rem(granule, 2)


def here_or_away(device, source, target, send, recv):
    place = lax.axis_index("context")

    @pl.when(device == place)
    def _():
        pltpu.make_async_copy(source, target, recv).start()

    @pl.when(device != place)
    def _():
        remote(source, target, send, recv, {"context": device}).start()


def wait_sent(device, source, target, send, recv):
    @pl.when(device != lax.axis_index("context"))
    def _():
        remote(source, target, send, recv, {"context": device}).wait_send()


def wait_landed(device, source, target, send, recv):
    place = lax.axis_index("context")

    @pl.when(device == place)
    def _():
        pltpu.make_async_copy(source, target, recv).wait()

    @pl.when(device != place)
    def _():
        remote(source, target, send, recv, {"context": device}).wait_recv()


def lanes(start):
    return span(start, TILE)


def span(start, size):
    return pl.ds(pl.multiple_of(start * size, size), size)


def cost(micros):
    return pl.CostEstimate(flops=micros * 1_150_000_000, bytes_accessed=0, transcendentals=0)


def vmem(count):
    return [pl.BlockSpec(memory_space=pltpu.VMEM)] * count


def hbm(count):
    return [pl.BlockSpec(memory_space=pl.ANY)] * count


def params(number=None, limit=60):
    if number is None:
        return pltpu.CompilerParams(vmem_limit_bytes=limit << 20)
    return pltpu.CompilerParams(
        collective_id=number, has_side_effects=True, vmem_limit_bytes=limit << 20
    )


def remote(source, target, send, recv, device):
    return pltpu.make_async_remote_copy(
        src_ref=source, dst_ref=target, send_sem=send, recv_sem=recv,
        device_id=device, device_id_type=pl.DeviceIdType.MESH,
    )


def chip_at(chip, far, chips, square, back=False):
    if square:
        x, y = lax.rem(chip, 2), chip // 2
        x = x + (far % 2) * (1 - 2 * x)
        y = y + (far // 2) * (1 - 2 * y)
        return 2 * y + x
    return lax.rem(chip + (chips - far if back else far), chips)


def meet(context, owners):
    place, row = lax.axis_index("context"), lax.axis_index("expert")
    barrier = pltpu.get_barrier_semaphore()
    for far in range(1, context):
        pl.semaphore_signal(
            barrier, inc=1, device_id={"context": lax.rem(place + far, context)},
            device_id_type=pl.DeviceIdType.MESH,
        )
    for far in range(1, owners):
        pl.semaphore_signal(
            barrier, inc=1, device_id={"expert": lax.rem(row + far, owners)},
            device_id_type=pl.DeviceIdType.MESH,
        )
    pl.semaphore_wait(barrier, context + owners - 2)
    return place, row


def attn_forward_kernel(
    dims,
    ids_ref, pieces_ref, input_ref, cos_ref, sin_ref, grads_ref, output_ref, gate_ref, up_ref,
    out_t_ref, lse_ref, query_t_ref, ids_all_ref, wt_ref,
    key_out, key_t_out, value_out, a_out, mix_ref,
    output_all_ref, wide_ref, grads_all_ref, stage_ref,
    w_all_ref, value_t_ref, scores_ref, acc_ref, key_ref, key_t_ref, value_ref, a_ref, out_ref,
    keep_sem, granule_send, granule_recv,
    local_sem, send_sem, recv_sem, pass_sem, land_sem, half_send, half_recv,
    row_send, row_recv, hop_send, hop_recv, lend_send, lend_recv, wide_send, wide_recv,
):
    heads, size, ranks, scale, context, owners, roles, square = dims
    length = a_ref.shape[0]
    rows = length // context
    shard = output_ref.shape[0]
    half = wide_ref.shape[2]
    width = heads * size
    tiles = length // TILE
    own_tiles = tiles // ranks
    ext = size + EXTRA
    chips = context // 2
    place, row = meet(context, owners)
    chip, core = place // 2, lax.rem(place, 2)
    partner = place + 1 - 2 * core
    slot = chip // (chips // roles)
    other = (roles - 1) - slot
    twin = 2 * lax.rem(chip + chips // 2, chips) + core

    def source(item, device):
        return (ids_ref, pieces_ref.at[device // ranks], input_ref, output_ref)[item]

    def target(item, device):
        return (
            ids_all_ref.at[:, span(device, rows)],
            w_all_ref.at[device],
            a_ref.at[span(device, rows), :],
            output_all_ref.at[span(device, shard), :],
        )[item]

    def from_chip(far):
        return 2 * chip_at(chip, far, chips, square, True) + core

    def sends(item, far):
        if isinstance(far, int) and far == 0:
            peer = partner
        else:
            peer = 2 * chip_at(chip, far, chips, square) + core
        return remote(
            source(item, peer), target(item, place), send_sem.at[item, far],
            recv_sem.at[item, far], {"context": peer},
        )

    def passes(item, far):
        block = target(item, from_chip(far))
        return remote(
            block, block, pass_sem.at[item, far], land_sem.at[item, far], {"context": partner}
        )

    def keeps(item):
        return pltpu.make_async_copy(
            source(item, place), target(item, place), local_sem.at[item]
        )

    def halves(far):
        upper = rows // 2
        start = from_chip(far) * rows + (far - 1) * upper
        block = a_ref.at[pl.ds(pl.multiple_of(start, upper), upper), :]
        return remote(
            block, block, half_send.at[far], half_recv.at[far],
            {"context": 2 * chip_at(chip, 3 - far, chips, square) + core},
        )

    def corner(far):
        upper = rows // 2
        start = from_chip(3) * rows + (far - 1) * upper
        block = a_ref.at[pl.ds(pl.multiple_of(start, upper), upper), :]
        return remote(block, block, half_send.at[far], half_recv.at[far], {"context": partner})

    direct = {item: list(range(1, chips)) for item in range(4)}
    if square:
        direct[2] = [1, 2]
    def begin(item):
        for far in direct[item] + [0]:
            sends(item, far).start()
        keeps(item).start()

    for item in range(3):
        begin(item)
    shard_granules = rows // (TILE // 2)
    group = place // ranks
    owned = out_ref.shape[0]

    def outgoing(step):
        granule = granule_of(step, ranks)
        target_slot = group * shard_granules + lax.rem(granule, shard_granules)
        return (
            granule // shard_granules, out_ref.at[step], mix_ref.at[target_slot],
            granule_send.at[step], granule_recv.at[target_slot],
        )

    def part(device, which):
        return grads_ref.at[device, which]

    to_rows, hops, lends = {}, {}, {}
    for far in range(owners):
        peer = lax.rem(row + far, owners)
        spots = [(slot, grads_all_ref.at[slot, core, row])]
        if roles > 1:
            spots.append((other, stage_ref.at[row]))
        for which, (role, spot) in enumerate(spots):
            if far > 0:
                to_rows[which, far] = remote(
                    part(peer, role), spot, row_send.at[which, far], row_recv.at[which, far],
                    {"expert": peer},
                )
            elif which == 0:
                to_rows[which, far] = pltpu.make_async_copy(part(row, role), spot, local_sem.at[4])
            else:
                lends[0] = remote(
                    part(row, role), grads_all_ref.at[slot, core, row], lend_send.at[0],
                    lend_recv.at[0], {"context": twin},
                )
    for copy in to_rows.values():
        copy.start()

    wide_out, wide_on = [], []
    for which, weight in enumerate((gate_ref, up_ref)):
        spot = wide_ref.at[which, span(place, shard), :]

        def block(device):
            role = device // 2 // (chips // roles)
            return weight.at[role, :, span(lax.rem(device, 2), half)]

        if square:
            peers = [
                (2 * chip_at(chip, far, chips, square) + side, 2 * far + turned)
                for far in (1, 2)
                for turned, side in enumerate((core, 1 - core))
            ] + [(partner, 1)]
        else:
            peers = [(lax.rem(place + far, context), far) for far in range(1, context)]
        for peer, index in peers:
            wide_out.append(
                remote(
                    block(peer), spot, wide_send.at[which, index], wide_recv.at[which, index],
                    {"context": peer},
                )
            )
        wide_out.append(pltpu.make_async_copy(block(place), spot, local_sem.at[5 + which]))
        if square:
            for turned in range(2):
                side = core if turned == 0 else 1 - core
                giver = 2 * chip_at(chip, 2, chips, square) + side
                block_on = wide_ref.at[which, span(giver, shard), :]
                wide_on.append(
                    remote(
                        block_on, block_on, wide_send.at[which, 6 + turned],
                        wide_recv.at[which, 6 + turned],
                        {"context": 2 * chip_at(chip, 1, chips, square) + core},
                    )
                )
    arrives = {}
    if square:
        index = 0
        for which in range(2):
            for far in (1, 2):
                for turned in range(2):
                    arrives[which, far, turned] = wide_out[index]
                    index += 1
            index += 2

    tail = (lax.broadcasted_iota(jnp.int32, (EXTRA, rows), 0) == 0).astype(BF16)
    for item in range(2):
        for far in range(1, chips):
            sends(item, far).wait_recv()
            passes(item, far).start()
        sends(item, 0).wait_recv()
        keeps(item).wait()
        for far in range(1, chips):
            passes(item, far).wait_recv()
    for device in range(context):
        wt_ref[:, device * shard : (device + 1) * shard] = w_all_ref[device]

    def project(step, carry):
        far, second = step // 2, lax.rem(step, 2)
        block = 2 * chip_at(chip, far, chips, square, True) + jnp.where(
            second == 0, core, 1 - core
        )

        @pl.when(jnp.logical_and(far == 0, second == 0))
        def _():
            keeps(2).wait()

        @pl.when(jnp.logical_and(far == 0, second == 1))
        def _():
            sends(2, 0).wait_recv()

        if square:

            @pl.when(jnp.logical_and(far == 1, second == 0))
            def _():
                for near in (1, 2):
                    sends(2, near).wait_recv()
                    halves(near).start()
                    passes(2, near).start()
                begin(3)
                for copy in wide_out:
                    copy.start()

            @pl.when(jnp.logical_and(far == 3, second == 0))
            def _():
                for near in (1, 2):
                    corner(near).wait_recv()
                passes(2, 3).start()

        else:

            @pl.when(jnp.logical_and(far > 0, second == 0))
            def _():
                sends(2, far).wait_recv()
                passes(2, far).start()

        @pl.when(jnp.logical_and(far > 0, second == 1))
        def _():
            passes(2, far).wait_recv()

        at = span(block, rows)
        both = dot(wt_ref[width:, :], a_ref[at, :], 1, 1)
        key_t = turn(both[:width], cos_ref[:, at], sin_ref[:, at], heads, size)
        key_t_ref[:, at] = key_t.astype(BF16)
        value_t = both[width:]
        for head in range(heads):
            here = slice(head * size, (head + 1) * size)
            key_ref[head, at, :] = key_t[here].T.astype(BF16)
            value_ref[head, at, :] = value_t[here].T.astype(BF16)
            value_t_ref[head * ext : head * ext + size, at] = value_t[here].astype(BF16)
            value_t_ref[head * ext + size : (head + 1) * ext, at] = tail
        return carry

    lax.fori_loop(0, 2 * chips, project, 0)
    if not square:
        begin(3)
        for copy in wide_out:
            copy.start()
    stored = [
        pltpu.make_async_copy(source, target, keep_sem.at[index])
        for index, (source, target) in enumerate(
            ((key_ref, key_out), (key_t_ref, key_t_out), (value_ref, value_out), (a_ref, a_out))
        )
    ]
    for copy in stored:
        copy.start()
    if roles > 1:
        lends[0].start()
    for far in range(owners):
        peer = lax.rem(row + owners - far, owners)
        home = grads_all_ref.at[slot, core, peer]
        if far > 0:
            to_rows[0, far].wait_recv()
        else:
            to_rows[0, far].wait()
        hops[far] = remote(
            home, home, hop_send.at[0, far], hop_recv.at[0, far], {"context": partner}
        )
        hops[far].start()
        if roles > 1 and far > 0:
            to_rows[1, far].wait_recv()
            lends[far] = remote(
                stage_ref.at[peer], home, lend_send.at[far], lend_recv.at[far],
                {"context": twin},
            )
            lends[far].start()

    def relays():
        for far in range(1, chips):
            sends(3, far).wait_recv()
            passes(3, far).start()
        for far in lends:
            lends[far].wait_recv()
            afar(far).start()

    def afar(far):
        away = grads_all_ref.at[other, core, lax.rem(row + owners - far, owners)]
        return remote(
            away, away, hop_send.at[1, far], hop_recv.at[1, far], {"context": partner}
        )

    def attend(index, carry):
        @pl.when(index > 0)
        def _():
            for step in range(2):
                here_or_away(*outgoing(2 * index - 2 + step))

        @pl.when(index == own_tiles - 1)
        def _():
            relays()

        if square:

            @pl.when(index == own_tiles // 2)
            def _():
                for which in range(2):
                    for turned in range(2):
                        arrives[which, 2, turned].wait_recv()
                for copy in wide_on:
                    copy.start()

        tile = own_tile(index, ranks)
        at = lanes(tile)
        query_t = dot(wt_ref[:width, :], a_ref[at, :], 1, 1)
        query_t = turn(query_t, cos_ref[:, at], sin_ref[:, at], heads, size)
        query_t = query_t.astype(BF16) * jnp.asarray(scale, BF16)
        query_t_ref[:, lanes(index)] = query_t
        query_ids = ids_all_ref[0:1, at]

        def score(step, tops, masked):
            here = lanes(step)
            fresh = []
            if masked:
                allowed = ids_all_ref[:, here].T[:, 0:1] <= query_ids
            for head in range(heads):
                part = dot(key_ref[head, here, :], query_t[head * size : (head + 1) * size])
                if masked:
                    part = jnp.where(allowed, part, NEGATIVE)
                scores_ref[head, here, :] = part
                fresh.append(
                    jnp.maximum(tops[head], jnp.max(part.reshape(TILE // 8, 8, TILE), axis=0))
                )
            return tuple(fresh)

        tops = tuple(jnp.full((8, TILE), NEGATIVE, F32) for _ in range(heads))
        stop = jnp.minimum(tile + 2, tiles)
        tops = lax.fori_loop(0, tile, lambda s, c: score(s, c, False), tops)
        tops = lax.fori_loop(tile, stop, lambda s, c: score(s, c, True), tops)
        peaks = [jnp.max(top, axis=0, keepdims=True) for top in tops]
        acc_ref[...] = jnp.zeros_like(acc_ref)

        def combine(step, carry):
            here = lanes(step)
            for head in range(heads):
                weights = jnp.exp(scores_ref[head, here, :] - peaks[head]).astype(BF16)
                acc_ref[head] += dot(value_t_ref[head * ext : (head + 1) * ext, here], weights)
            return carry

        lax.fori_loop(0, stop, combine, 0)
        parts = []
        for head in range(heads):
            total = acc_ref[head, size : size + 1, :]
            part = acc_ref[head, :size, :] * (1.0 / total)
            lse_ref[head : head + 1, lanes(index)] = peaks[head] + jnp.log(total)
            parts.append(part)
        joined = jnp.concatenate(parts, axis=0)
        out_t_ref[:, lanes(index)] = joined
        turned_out = joined.T.astype(BF16)
        out_ref[2 * index] = turned_out[: TILE // 2]
        out_ref[2 * index + 1] = turned_out[TILE // 2 :]
        return carry

    lax.fori_loop(0, own_tiles, attend, 0)
    for step in range(2):
        here_or_away(*outgoing(2 * own_tiles - 2 + step))
    sends(3, 0).wait_recv()
    keeps(3).wait()
    for far in range(1, chips):
        passes(3, far).wait_recv()
    for item in range(4):
        for far in direct[item] + [0]:
            sends(item, far).wait_send()
        for far in range(1, chips):
            passes(item, far).wait_send()
    if square:
        for far in (1, 2):
            halves(far).wait_send()
    forwarded = [arrives[which, 2, turned] for which, _, turned in arrives if _ == 2]
    for copy in wide_out:
        if any(copy is one for one in forwarded):
            copy.wait_send()
        else:
            copy.wait()
    for (which, far), copy in to_rows.items():
        if far > 0:
            copy.wait_send()
    for copy in lends.values():
        copy.wait_send()
    for copy in wide_on + list(hops.values()) + [afar(far) for far in lends] + stored:
        copy.wait()

    def settle(step, carry):
        wait_sent(*outgoing(step))
        giver_group, spot = step // shard_granules, lax.rem(step, shard_granules)
        giver = giver_group * ranks + owner_rank(place * shard_granules + spot, ranks)
        wait_landed(
            giver, out_ref.at[0], mix_ref.at[step], granule_send.at[0], granule_recv.at[step]
        )
        return carry

    lax.fori_loop(0, owned, settle, 0)


def attn_forward(
    ids, pieces, attn_input, cos_t, sin_t, grads, output_weight, gate_weight, up_weight,
    heads, size, ranks, context, roles, number,
):
    rows, model = attn_input.shape
    owners = grads.shape[0]
    length = rows * context
    own = length // ranks
    width = heads * size
    ext = size + EXTRA
    shard = output_weight.shape[0]
    chips = context // 2
    granule = TILE // 2
    head_shape = jax.ShapeDtypeStruct((heads, length, size), BF16)
    turned_shape = jax.ShapeDtypeStruct((width, length), BF16)
    a_shape = jax.ShapeDtypeStruct((length, model), BF16)
    own_shape = jax.ShapeDtypeStruct((own // granule, granule, width), BF16)
    shapes = (
        jax.ShapeDtypeStruct((width, own), F32),
        jax.ShapeDtypeStruct((heads, own), F32),
        jax.ShapeDtypeStruct((width, own), BF16),
        jax.ShapeDtypeStruct((8, length), F32),
        jax.ShapeDtypeStruct((3 * width, model), BF16),
        head_shape,
        turned_shape,
        head_shape,
        a_shape,
        own_shape,
        jax.ShapeDtypeStruct((model, model), BF16),
        jax.ShapeDtypeStruct((2, model, gate_weight.shape[2] // 2), BF16),
        jax.ShapeDtypeStruct((roles, 2, owners) + grads.shape[2:], BF16),
        jax.ShapeDtypeStruct((owners,) + grads.shape[2:], BF16),
    )
    square = chips == 4 and roles == 2
    dims = (heads, size, ranks, size ** (-0.5), context, owners, roles, square)
    return pl.pallas_call(
        functools.partial(attn_forward_kernel, dims),
        out_shape=shapes,
        in_specs=vmem(5) + hbm(4),
        out_specs=vmem(5) + hbm(9),
        scratch_shapes=[
            pltpu.VMEM((context, 3 * width, shard), BF16),
            pltpu.VMEM((heads * ext, length), BF16),
            pltpu.VMEM((heads, length, TILE), F32),
            pltpu.VMEM((heads, ext, TILE), F32),
        ]
        + [
            pltpu.VMEM(one.shape, one.dtype)
            for one in (head_shape, turned_shape, head_shape, a_shape, own_shape)
        ]
        + [
            pltpu.SemaphoreType.DMA((4,)),
            pltpu.SemaphoreType.DMA((own // granule,)),
            pltpu.SemaphoreType.DMA((own // granule,)),
            pltpu.SemaphoreType.DMA((7,)),
            pltpu.SemaphoreType.DMA((4, chips)),
            pltpu.SemaphoreType.DMA((4, chips)),
            pltpu.SemaphoreType.DMA((4, chips)),
            pltpu.SemaphoreType.DMA((4, chips)),
            pltpu.SemaphoreType.DMA((3,)),
            pltpu.SemaphoreType.DMA((3,)),
        ]
        + [pltpu.SemaphoreType.DMA((2, owners))] * 4
        + [pltpu.SemaphoreType.DMA((owners,))] * 2
        + [pltpu.SemaphoreType.DMA((2, context))] * 2,
        compiler_params=params(number, 62),
        cost_estimate=cost(80),
        name="attn_forward",
    )(ids, pieces, attn_input, cos_t, sin_t, grads, output_weight, gate_weight, up_weight)


def attn_backward_kernel(
    dims,
    grad_ref, a_ref, wt_ref, cos_ref, sin_ref, ids_all_ref,
    out_t_ref, lse_ref, query_t_ref, key_ref, key_t_ref, value_ref,
    wide_ref, outs_ref, output_ref,
    da_ref, pieces_ref, output_sum_ref, wide_in_ref, outs_in_ref,
    query_ref, own_grad_ref, dq_ref, dk_ref, dv_ref, grad_w_ref,
    landed_ref, output_in_ref, share_ref, shares_ref,
    granule_send, granule_recv, share_send, share_recv,
    wide_send, wide_recv, output_send, output_recv,
    row_send, row_recv, local_sem,
):
    heads, size, ranks, scale, context, owners, roles = dims
    length = a_ref.shape[0]
    shard = pieces_ref.shape[2]
    width = heads * size
    tiles = length // TILE
    own_tiles = tiles // ranks
    chips = context // 2
    place, row = meet(context, owners)
    chip, core = place // 2, lax.rem(place, 2)
    owned = landed_ref.shape[0]
    shard_granules = owned * ranks // context

    def outgoing(step):
        giver = step // shard_granules
        granule = place * shard_granules + lax.rem(step, shard_granules)
        landing = owner_slot(granule, ranks)
        return (
            giver * ranks + owner_rank(granule, ranks), grad_ref.at[step],
            landed_ref.at[landing], granule_send.at[step], granule_recv.at[landing],
        )

    def launch(step, carry):
        here_or_away(*outgoing(step))
        return carry

    lax.fori_loop(0, owned, launch, 0)
    copies, output_copies = [], []
    for item, (grads, target, send, recv) in enumerate(
        (
            (output_ref, output_in_ref, output_send, output_recv),
            (wide_ref, wide_in_ref, wide_send, wide_recv),
        )
    ):
        for far in range(context):
            peer = lax.rem(place + far, context)
            at = span(peer, shard)
            source = grads.at[:, at, :] if item else grads.at[at, :]
            group_copies = copies if item else output_copies
            if far == 0:
                group_copies.append(
                    pltpu.make_async_copy(source, target.at[place], local_sem.at[item])
                )
            else:
                group_copies.append(
                    remote(
                        source, target.at[place], send.at[far], recv.at[far], {"context": peer}
                    )
                )
    for far in range(owners):
        peer = lax.rem(row + far, owners)
        if far == 0:
            copies.append(
                pltpu.make_async_copy(outs_ref.at[row], outs_in_ref.at[row], local_sem.at[2])
            )
        else:
            copies.append(
                remote(
                    outs_ref.at[peer], outs_in_ref.at[row], row_send.at[far], row_recv.at[far],
                    {"expert": peer},
                )
            )
    dk_ref[...] = jnp.zeros_like(dk_ref)
    dv_ref[...] = jnp.zeros_like(dv_ref)
    da_ref[...] = jnp.zeros_like(da_ref)
    grad_w_ref[...] = jnp.zeros_like(grad_w_ref)
    def landed(step, carry):
        giver = granule_of(step, ranks) // shard_granules
        wait_landed(
            giver, grad_ref.at[0], landed_ref.at[step], granule_send.at[0], granule_recv.at[step]
        )
        return carry

    lax.fori_loop(0, owned, landed, 0)
    for copy in output_copies + copies:
        copy.start()

    def share_copy(far):
        return remote(
            share_ref, shares_ref.at[row], share_send.at[far], share_recv.at[far],
            {"expert": lax.rem(row + far, owners)},
        )

    def attend(index, carry):
        tile = own_tile(index, ranks)
        at = lanes(tile)
        query_t = query_t_ref[:, lanes(index)]
        @pl.when(index == own_tiles // 2)
        def _():
            for copy in output_copies:
                copy.wait()
            total = output_in_ref[0].astype(F32)
            for giver in range(1, context):
                total = total + output_in_ref[giver].astype(F32)
            share_ref[...] = total.astype(BF16)

        @pl.when(index == own_tiles // 2 + 1)
        def _():
            for far in range(1, owners):
                share_copy(far).start()

        grad_rows = landed_ref[pl.ds(2 * index, 2)].reshape(TILE, width)
        grad_t = grad_rows.astype(F32).T
        query_rows = query_t.astype(F32).T.astype(BF16)
        query_ids = ids_all_ref[0:1, at]
        deltas, tops, grads_low = [], [], []
        for head in range(heads):
            rows = slice(head * size, (head + 1) * size)
            query_ref[head] = query_rows[:, rows]
            own_grad_ref[head] = grad_rows[:, rows]
            deltas.append(
                jnp.sum(grad_t[rows] * out_t_ref[rows, lanes(index)], axis=0, keepdims=True)
            )
            tops.append(lse_ref[head : head + 1, lanes(index)])
        grad_t_low = grad_t.astype(BF16)
        dq_ref[...] = jnp.zeros_like(dq_ref)

        def chunk(step, carry, masked):
            here = lanes(step)
            if masked:
                allowed = ids_all_ref[:, here].T[:, 0:1] <= query_ids
            for head in range(heads):
                rows = slice(head * size, (head + 1) * size)
                scores = dot(key_ref[head, here, :], query_t[rows]) - tops[head]
                if masked:
                    scores = jnp.where(allowed, scores, NEGATIVE)
                probs = jnp.exp(scores)
                grad_probs = dot(value_ref[head, here, :], grad_t_low[rows])
                grad_scores = (probs * (grad_probs - deltas[head])).astype(BF16)
                dv_ref[head, here, :] += dot(probs.astype(BF16), own_grad_ref[head])
                dk_ref[head, here, :] += dot(grad_scores, query_ref[head])
                dq_ref[rows, :] += dot(key_t_ref[rows, here], grad_scores)
            return carry

        stop = jnp.minimum(tile + 2, tiles)
        lax.fori_loop(0, tile, lambda s, c: chunk(s, c, False), 0)
        lax.fori_loop(tile, stop, lambda s, c: chunk(s, c, True), 0)
        grad_query = turn(
            dq_ref[...] * scale, cos_ref[:, at], sin_ref[:, at], heads, size, back=True
        )
        grad_w_ref[:width, :] += dot(grad_query.astype(BF16), a_ref[at, :])
        da_ref[at, :] = dot(grad_query.T.astype(BF16), wt_ref[:width, :]).astype(BF16)
        return carry

    lax.fori_loop(0, own_tiles, attend, 0)

    def finish(step, carry):
        at = lanes(step)
        key_grad = jnp.concatenate([dk_ref[head, at, :].T for head in range(heads)], axis=0)
        key_grad = turn(key_grad, cos_ref[:, at], sin_ref[:, at], heads, size, back=True)
        value_grad = jnp.concatenate([dv_ref[head, at, :].T for head in range(heads)], axis=0)
        both = jnp.concatenate([key_grad, value_grad], axis=0)
        grad_w_ref[width:, :] += dot(both.astype(BF16), a_ref[at, :])
        total = da_ref[at, :].astype(F32) + dot(both.T.astype(BF16), wt_ref[width:, :])
        da_ref[at, :] = total.astype(BF16)
        return carry

    lax.fori_loop(0, tiles, finish, 0)
    for piece in range(pieces_ref.shape[0]):
        pieces_ref[piece] = grad_w_ref[:, piece * shard : (piece + 1) * shard].astype(BF16)
    for copy in copies:
        copy.wait()
    for far in range(1, owners):
        share_copy(far).wait()
    shares_ref[row] = share_ref[...]
    total = shares_ref[0].astype(F32)
    for giver in range(1, owners):
        total = total + shares_ref[giver].astype(F32)
    output_sum_ref[...] = total

    def settle(step, carry):
        wait_sent(*outgoing(step))
        return carry

    lax.fori_loop(0, owned, settle, 0)


def attn_backward(
    grad_own, a_full, weights_t, cos_t, sin_t, ids, kept,
    grad_wide, outs, grad_output, heads, size, ranks, context, roles, number,
):
    length, model = a_full.shape
    width = heads * size
    owners = outs.shape[0]
    shard = model // context
    shapes = (
        jax.ShapeDtypeStruct(a_full.shape, BF16),
        jax.ShapeDtypeStruct((context, weights_t.shape[0], shard), BF16),
        jax.ShapeDtypeStruct((shard, model), F32),
        jax.ShapeDtypeStruct((context, 2, shard, grad_wide.shape[2]), BF16),
        jax.ShapeDtypeStruct(outs.shape, BF16),
    )
    dims = (heads, size, ranks, size ** (-0.5), context, owners, roles)
    return pl.pallas_call(
        functools.partial(attn_backward_kernel, dims),
        out_shape=shapes,
        in_specs=vmem(12) + hbm(3),
        out_specs=vmem(3) + hbm(2),
        scratch_shapes=[
            pltpu.VMEM((heads, TILE, size), BF16),
            pltpu.VMEM((heads, TILE, size), BF16),
            pltpu.VMEM((width, TILE), F32),
            pltpu.VMEM((heads, length, size), F32),
            pltpu.VMEM((heads, length, size), F32),
            pltpu.VMEM(weights_t.shape, F32),
            pltpu.VMEM(grad_own.shape, BF16),
            pltpu.VMEM((context, shard, model), BF16),
            pltpu.VMEM((shard, model), BF16),
            pltpu.VMEM((owners, shard, model), BF16),
        ]
        + [pltpu.SemaphoreType.DMA((grad_own.shape[0],))] * 2
        + [pltpu.SemaphoreType.DMA((owners,))] * 2
        + [pltpu.SemaphoreType.DMA((context,))] * 4
        + [pltpu.SemaphoreType.DMA((owners,))] * 2
        + [pltpu.SemaphoreType.DMA((3,))],
        compiler_params=params(number, 63),
        cost_estimate=cost(60),
        name="attn_backward",
    )(
        grad_own, a_full, weights_t, cos_t, sin_t, ids, *kept,
        grad_wide, outs, grad_output,
    )


def expert_kernel(
    context, owners,
    rows_ref, grad_ref, prob_ref, wide_hbm, down_hbm,
    out_ref, grad_rows_ref, dot_ref, grad_wide_ref, down_in_ref,
    wide_ref, down_ref, rows_t_ref, dye_ref, out_acc_ref, grad_acc_ref, grad_down_ref,
    load_sem, down_send, down_recv,
):
    flat = dye_ref.shape
    chips = context // 2
    loads = [
        pltpu.make_async_copy(wide_hbm, wide_ref, load_sem.at[0]),
        pltpu.make_async_copy(down_hbm, down_ref, load_sem.at[1]),
    ]
    for copy in loads:
        copy.start()
    place, _ = meet(context, owners)
    chip, core = place // 2, lax.rem(place, 2)
    down_rows = down_in_ref.shape[1]
    per_step = HIDDEN_TILE // down_rows
    tiles = wide_ref.shape[2] // HIDDEN_TILE

    def down_copy(index, here):
        source = grad_down_ref.at[index]
        spot = down_in_ref.at[chip]
        if here:
            return pltpu.make_async_copy(source, spot, down_recv.at[chip])
        return remote(
            source, spot, down_send.at[index], down_recv.at[chip],
            {"context": core * chips + index},
        )

    def start_down(index):
        here = core * chips + index == place

        @pl.when(here)
        def _():
            down_copy(index, True).start()

        @pl.when(jnp.logical_not(here))
        def _():
            down_copy(index, False).start()

    rows_t_ref[...] = rows_ref[...].reshape(flat).astype(F32).T.astype(BF16)
    dye_ref[...] = (grad_ref[...].reshape(flat).astype(F32) * prob_ref[...]).astype(BF16)
    out_acc_ref[...] = jnp.zeros_like(out_acc_ref)
    grad_acc_ref[...] = jnp.zeros_like(grad_acc_ref)
    for copy in loads:
        copy.wait()

    def hidden_tile(step, carry):
        tile = lax.rem(step + (1 - lax.rem(chip, 2)) * (tiles // 2), tiles)
        at = span(tile, HIDDEN_TILE)
        rows = rows_ref[...].reshape(flat)
        dye = dye_ref[...]
        gate, up, down = wide_ref[0, :, at], wide_ref[1, :, at], down_ref[at, :]
        gate_pre = dot(rows, gate)
        up_pre = dot(rows, up)
        sigmoid = jax.nn.sigmoid(gate_pre)
        silu = gate_pre * sigmoid
        hidden = silu * up_pre
        grad_down = dot(hidden.T.astype(BF16), dye).astype(BF16)
        for index in range(per_step):
            grad_down_ref[tile * per_step + index] = grad_down[
                index * down_rows : (index + 1) * down_rows
            ]
        grad_hidden = dot(dye, down, 1, 1).astype(BF16).astype(F32)
        for index in range(per_step):
            start_down(tile * per_step + index)
        out_acc_ref[...] += dot(hidden.astype(BF16), down)
        grad_gate = (
            grad_hidden * up_pre * sigmoid * (1.0 + gate_pre * (1.0 - sigmoid))
        ).astype(BF16)
        grad_up = (grad_hidden * silu).astype(BF16)
        grad_wide_ref[0, :, at] = dot(rows_t_ref[...], grad_gate).astype(BF16)
        grad_wide_ref[1, :, at] = dot(rows_t_ref[...], grad_up).astype(BF16)
        grad_acc_ref[...] += dot(grad_gate, gate, 1, 1) + dot(grad_up, up, 1, 1)
        return carry

    lax.fori_loop(0, tiles, hidden_tile, 0)
    out = out_acc_ref[...]
    out_ref[...] = out.astype(BF16).reshape(out_ref.shape)
    grad_rows_ref[...] = grad_acc_ref[...].astype(BF16).reshape(out_ref.shape)
    grads = grad_ref[...].reshape(flat).astype(F32)
    dot_ref[...] = jnp.sum(out * grads, axis=1, keepdims=True)
    for index in range(chips):
        here = core * chips + index == place
        giver = 2 * index + place // chips
        land = down_in_ref.at[index]

        @pl.when(jnp.logical_not(here))
        def _():
            down_copy(index, False).wait_send()

        @pl.when(giver == place)
        def _():
            pltpu.make_async_copy(grad_down_ref.at[0], land, down_recv.at[index]).wait()

        @pl.when(giver != place)
        def _():
            remote(
                grad_down_ref.at[0], land, down_send.at[index], down_recv.at[index],
                {"context": giver},
            ).wait_recv()


def experts(rows, grads, gates, wide_full, down_full, context, owners, number):
    width = rows.shape[-1]
    slots = rows.size // width
    hidden = wide_full.shape[2]
    blocks = (context // 2, hidden // (context // 2), width)
    return pl.pallas_call(
        functools.partial(expert_kernel, context, owners),
        out_shape=(
            jax.ShapeDtypeStruct(rows.shape, BF16),
            jax.ShapeDtypeStruct(rows.shape, BF16),
            jax.ShapeDtypeStruct((slots, 1), F32),
            jax.ShapeDtypeStruct(wide_full.shape, BF16),
            jax.ShapeDtypeStruct(blocks, BF16),
        ),
        in_specs=vmem(3) + hbm(2),
        out_specs=vmem(4) + hbm(1),
        scratch_shapes=[
            pltpu.VMEM(wide_full.shape, BF16),
            pltpu.VMEM(down_full.shape, BF16),
            pltpu.VMEM((width, slots), BF16),
            pltpu.VMEM((slots, width), BF16),
            pltpu.VMEM((slots, width), F32),
            pltpu.VMEM((slots, width), F32),
            pltpu.VMEM(blocks, BF16),
            pltpu.SemaphoreType.DMA((2,)),
            pltpu.SemaphoreType.DMA((context // 2,)),
            pltpu.SemaphoreType.DMA((context // 2,)),
        ],
        compiler_params=params(number),
        cost_estimate=cost(37),
        name="experts",
    )(rows, grads, gates, wide_full, down_full)


def dispatch_kernel(
    context, roles, square,
    gates_ref, rows_ref, down_ref,
    gates_all, rows_all, down_all,
    rows_stage,
    local_sem, send_sem, recv_sem, pass_sem, land_sem, twin_sem, come_sem, relay_sem, reach_sem,
    down_send, down_recv, down_on,
):
    owners = rows_ref.shape[0]
    chips = context // 2
    place, row = meet(context, owners)
    chip, core = place // 2, lax.rem(place, 2)
    partner = {"context": place + 1 - 2 * core}
    slot = chip // (chips // roles)
    other = (roles - 1) - slot
    twin = {"context": 2 * lax.rem(chip + chips // 2, chips) + core}
    sent, local, passed, lent, relayed = {}, [], [], {}, []
    for far in range(1, owners):
        peer = lax.rem(row + far, owners)
        pairs = [
            (gates_ref.at[peer], gates_all.at[slot, core, row]),
            (rows_ref.at[peer, slot], rows_all.at[slot, core, row]),
        ]
        if roles > 1:
            pairs.append((rows_ref.at[peer, other], rows_stage.at[row]))
        for item, (source, target) in enumerate(pairs):
            sent[item, far] = remote(
                source, target, send_sem.at[item, far], recv_sem.at[item, far], {"expert": peer}
            )
            sent[item, far].start()
    own = (
        (gates_ref.at[row], gates_all.at[slot, core, row]),
        (rows_ref.at[row, slot], rows_all.at[slot, core, row]),
    )
    for item, (source, target) in enumerate(own):
        local.append(pltpu.make_async_copy(source, target, local_sem.at[item]))
        local[-1].start()
        passed.append(
            remote(source, target, pass_sem.at[item, 0], land_sem.at[item, 0], partner)
        )
        passed[-1].start()
    if roles > 1:
        own = (
            (gates_ref.at[row], gates_all.at[slot, core, row], gates_all.at[other, core, row]),
            (rows_ref.at[row, other], rows_all.at[slot, core, row], rows_all.at[other, core, row]),
        )
        for item, (source, target, arriving) in enumerate(own):
            lent[item, 0] = (
                remote(source, target, twin_sem.at[item, 0], come_sem.at[item, 0], twin), arriving
            )
            lent[item, 0][0].start()

    half = place // chips
    down_rows = down_ref.shape[1]
    index = lax.rem(place, chips)
    spot = down_all.at[span(index, down_rows), :]

    def down_copy(far, here):
        to_chip = chip_at(chip, far, chips, square)
        source = down_ref.at[to_chip // (chips // roles)]
        if here:
            return pltpu.make_async_copy(source, spot, down_recv.at[index])
        return remote(
            source, spot, down_send.at[far], down_recv.at[index],
            {"context": 2 * to_chip + half},
        )

    @pl.when(half == core)
    def _():
        down_copy(0, True).start()

    @pl.when(half != core)
    def _():
        down_copy(0, False).start()

    fars = [1, 2] if square else list(range(1, chips))
    for far in fars:
        down_copy(far, False).start()

    def arrival(number):
        land = down_all.at[span(number, down_rows), :]
        giver = core * chips + number

        @pl.when(giver == place)
        def _():
            pltpu.make_async_copy(down_ref.at[0], land, down_recv.at[number]).wait()

        @pl.when(giver != place)
        def _():
            remote(
                down_ref.at[0], land, down_send.at[0], down_recv.at[number], {"context": giver}
            ).wait_recv()

    def onward(number):
        land = down_all.at[span(number, down_rows), :]
        return remote(
            land, land, down_on.at[number], down_recv.at[number],
            {"context": 2 * chip_at(chip, 1, chips, square) + core},
        )

    def from_below(number):
        giver = core * chips + number
        return giver // 2 == chip_at(chip, 2, chips, square)

    for far in range(1, owners):
        peer = lax.rem(row + owners - far, owners)
        for item in range(2):
            sent[item, far].wait_recv()
            block = (gates_all, rows_all)[item].at[slot, core, peer]
            passed.append(
                remote(block, block, pass_sem.at[item, far], land_sem.at[item, far], partner)
            )
            passed[-1].start()
            if roles > 1:
                if item == 1:
                    sent[2, far].wait_recv()
                source = block if item == 0 else rows_stage.at[peer]
                arriving = (gates_all, rows_all)[item].at[other, core, peer]
                lent[item, far] = (
                    remote(source, block, twin_sem.at[item, far], come_sem.at[item, far], twin),
                    arriving,
                )
                lent[item, far][0].start()
        if square and far == 1:
            for number in range(chips):

                @pl.when(from_below(number))
                def _():
                    arrival(number)
                    onward(number).start()

    for (item, far), (copy, arriving) in lent.items():
        copy.wait_recv()
        relayed.append(
            remote(
                arriving, arriving, relay_sem.at[item, far], reach_sem.at[item, far], partner
            )
        )
        relayed[-1].start()
    for copy in sent.values():
        copy.wait_send()
    for copy, arriving in lent.values():
        copy.wait_send()
    for copy in local + passed + relayed:
        copy.wait()
    for far in fars:
        down_copy(far, False).wait_send()

    @pl.when(half != core)
    def _():
        down_copy(0, False).wait_send()

    for number in range(chips):
        if square:

            @pl.when(from_below(number))
            def _():
                onward(number).wait_send()

            @pl.when(jnp.logical_not(from_below(number)))
            def _():
                arrival(number)

        else:
            arrival(number)


def dispatch(gates, rows, down_weight, context, roles, number):
    owners, _, cap, width = rows.shape
    chips = context // 2
    down_rows = down_weight.shape[1]
    square = chips == 4 and roles == 2
    return pl.pallas_call(
        functools.partial(dispatch_kernel, context, roles, square),
        out_shape=(
            jax.ShapeDtypeStruct((roles, 2) + gates.shape, gates.dtype),
            jax.ShapeDtypeStruct((roles, 2, owners, cap, width), BF16),
            jax.ShapeDtypeStruct((chips * down_rows, width), BF16),
        ),
        in_specs=vmem(2) + hbm(1),
        out_specs=vmem(2) + hbm(1),
        scratch_shapes=[
            pltpu.VMEM((owners, cap, width), BF16),
            pltpu.SemaphoreType.DMA((2,)),
        ]
        + [pltpu.SemaphoreType.DMA((3, owners))] * 8
        + [pltpu.SemaphoreType.DMA((chips,))] * 3,
        compiler_params=params(number),
        name="dispatch",
    )(gates, rows, down_weight)


def collect_kernel(
    context, roles,
    dots_ref, grad_ref, out_ref, dots_back, grad_back, out_back,
    dots_twin, grad_twin, out_twin, dots_sum, grad_sum, out_sum, dots_relay, grad_relay,
    pair_send, pair_recv, send_sem, recv_sem, lend_sem, come_sem, relay_send, relay_recv,
    out_send, out_recv, out_lend, out_come,
):
    owners = grad_ref.shape[2]
    chips = context // 2
    place, row = meet(context, owners)
    chip, core = place // 2, lax.rem(place, 2)
    partner = {"context": place + 1 - 2 * core}
    slot = chip // (chips // roles)
    other = (roles - 1) - slot
    twin = {"context": 2 * lax.rem(chip + chips // 2, chips) + core}
    order = list(range(1, owners)) + [0]
    turns = (other, slot) if roles > 1 else (slot,)
    pair, sent, lent, relayed, outs, loans = {}, {}, {}, {}, [], []
    items = (
        (dots_ref, dots_twin, dots_sum, dots_relay, dots_back),
        (grad_ref, grad_twin, grad_sum, grad_relay, grad_back),
    )
    for far in order:
        peer = lax.rem(row + far, owners)
        for which, spot in enumerate(turns):
            for item, (source, landing, _, _, _) in enumerate(items):
                pair[item, which, far] = remote(
                    source.at[spot, 1 - core, peer], landing.at[spot, peer],
                    pair_send.at[item, which, far], pair_recv.at[item, which, far], partner,
                )
                pair[item, which, far].start()
    for which, spot in enumerate(turns):
        outs.append(
            remote(
                out_ref.at[spot, 1 - core], out_twin.at[spot],
                out_send.at[which], out_recv.at[which], partner,
            )
        )
        outs[-1].start()

    def leave(which, far):
        peer = lax.rem(row + far, owners)
        spot = turns[which]
        for item, (_, _, total, relay, back) in enumerate(items):
            if roles > 1 and which == 0:
                target = back.at[row, slot] if far == 0 else relay.at[peer]
                lent[item, far] = remote(
                    total.at[spot, peer], target, lend_sem.at[item, far],
                    come_sem.at[item, far], twin,
                )
                lent[item, far].start()
            elif far > 0:
                sent[item, far] = remote(
                    total.at[spot, peer], back.at[row, slot], send_sem.at[item, far],
                    recv_sem.at[item, far], {"expert": peer},
                )
                sent[item, far].start()

    last = None
    for far in order:
        peer = lax.rem(row + far, owners)
        for which, spot in enumerate(turns):
            for item, (source, landing, total, _, _) in enumerate(items):
                pair[item, which, far].wait_recv()
                summed = source[spot, core, peer].astype(F32) + landing[spot, peer].astype(F32)
                total[spot, peer] = summed.astype(total.dtype)
            if last is not None:
                leave(*last)
            last = (which, far)
    dots_back[row, slot] = dots_sum[slot, row]
    grad_back[row, slot] = grad_sum[slot, row]
    leave(*last)
    if roles > 1:
        for far in range(1, owners):
            peer = lax.rem(row + far, owners)
            for item, (_, _, _, relay, back) in enumerate(items):
                lent[item, far].wait_recv()
                relayed[item, far] = remote(
                    relay.at[peer], back.at[row, other], relay_send.at[item, far],
                    relay_recv.at[item, far], {"expert": peer},
                )
                relayed[item, far].start()
    for which, spot in enumerate(turns):
        outs[which].wait_recv()
        for peer in range(owners):
            summed = out_ref[spot, core, peer].astype(F32) + out_twin[spot, peer].astype(F32)
            if roles > 1 and which == 0:
                out_sum[peer] = summed.astype(BF16)
            else:
                out_back[peer, slot] = summed.astype(BF16)
    if roles > 1:
        loans.append(
            remote(out_sum, out_back.at[:, slot], out_lend, out_come, twin)
        )
        loans[-1].start()
        for item in range(2):
            lent[item, 0].wait_recv()
    for copy in list(pair.values()) + outs + list(lent.values()):
        copy.wait_send()
    for copy in list(sent.values()) + list(relayed.values()) + loans:
        copy.wait()


def collect(dots, grads, outs, context, roles, number):
    _, _, owners, cap, width = grads.shape
    home = (owners, roles, cap, width)
    small = (owners, roles) + dots.shape[3:]
    return pl.pallas_call(
        functools.partial(collect_kernel, context, roles),
        out_shape=(
            jax.ShapeDtypeStruct(small, F32),
            jax.ShapeDtypeStruct(home, BF16),
            jax.ShapeDtypeStruct(home, BF16),
        ),
        in_specs=vmem(3),
        out_specs=vmem(3),
        scratch_shapes=[
            pltpu.VMEM((roles, owners) + dots.shape[3:], F32),
            pltpu.VMEM((roles, owners, cap, width), BF16),
            pltpu.VMEM((roles, owners, cap, width), BF16),
            pltpu.VMEM((roles, owners) + dots.shape[3:], F32),
            pltpu.VMEM((roles, owners, cap, width), BF16),
            pltpu.VMEM((owners, cap, width), BF16),
            pltpu.VMEM((owners,) + dots.shape[3:], F32),
            pltpu.VMEM((owners, cap, width), BF16),
            pltpu.SemaphoreType.DMA((2, roles, owners)),
            pltpu.SemaphoreType.DMA((2, roles, owners)),
        ]
        + [pltpu.SemaphoreType.DMA((2, owners))] * 6
        + [pltpu.SemaphoreType.DMA((roles,))] * 2
        + [pltpu.SemaphoreType.DMA] * 2,
        compiler_params=params(number),
        name="collect",
    )(dots, grads, outs)


def finish_kernel(
    chips, owners, groups,
    da_ref, pieces_ref, small_ref,
    total_ref, sums_ref, small_all_ref,
    da_twin, da_sum, da_in, w_twin, w_sum, w_in, s_twin, s_sum, s_in, s_total,
    stack_ref, shares, shares_in, block_ref,
    pair_send, pair_recv, chip_send, chip_recv, row_send, row_recv,
):
    place = lax.axis_index("context")
    row = lax.axis_index("expert")
    chip, core = place // 2, lax.rem(place, 2)
    partner = 2 * chip + 1 - core
    barrier = pltpu.get_barrier_semaphore()

    def greet(device):
        pl.semaphore_signal(
            barrier, inc=1, device_id=device, device_id_type=pl.DeviceIdType.MESH
        )

    greet({"context": partner})
    for far in range(1, chips):
        greet({"context": 2 * lax.rem(chip + far, chips) + core})
    for far in range(1, owners):
        greet({"expert": lax.rem(row + far, owners)})
    pl.semaphore_wait(barrier, chips + owners - 1)

    order = list(range(1, chips)) + [0]
    pair = {}
    for item, (source, target) in enumerate(
        ((small_ref, s_twin), (pieces_ref, w_twin), (da_ref, da_twin))
    ):
        for far in order:
            peer = lax.rem(chip + far, chips)
            pair[item, far] = remote(
                source.at[2 * peer + 1 - core], target.at[peer],
                pair_send.at[item, far], pair_recv.at[item, far], {"context": partner},
            )
            pair[item, far].start()

    def across(item, source, target, far):
        peer = lax.rem(chip + far, chips)
        return remote(
            source.at[peer], target.at[chip], chip_send.at[item, far], chip_recv.at[item, far],
            {"context": 2 * peer + core},
        )

    for far in order:
        peer = lax.rem(chip + far, chips)
        mine = 2 * peer + core
        pair[0, far].wait_recv()
        s_sum[peer] = small_ref[mine] + s_twin[peer]
        pair[1, far].wait_recv()
        w_sum[peer] = (
            pieces_ref[mine].astype(F32) + w_twin[peer].astype(F32)
        ).astype(BF16)
    moved = {}
    for far in range(1, chips):
        moved[0, far] = across(0, s_sum, s_in, far)
        moved[0, far].start()
        moved[1, far] = across(1, w_sum, w_in, far)
        moved[1, far].start()
    last = None
    for far in order:
        peer = lax.rem(chip + far, chips)
        pair[2, far].wait_recv()
        da_sum[peer] = (
            da_ref[2 * peer + core].astype(F32) + da_twin[peer].astype(F32)
        ).astype(BF16)
        if last is not None:
            moved[2, last] = across(2, da_sum, da_in, last)
            moved[2, last].start()
        last = far
    for far in range(1, chips):
        moved[0, far].wait_recv()
        moved[1, far].wait_recv()
    s_in[chip] = s_sum[chip]
    w_in[chip] = w_sum[chip]

    width = w_sum.shape[1] // 3
    shard = w_sum.shape[2]
    per_group = chips // groups
    for group in range(groups):
        total = w_in[group * per_group].astype(F32)
        for other in range(1, per_group):
            total = total + w_in[group * per_group + other].astype(F32)
        for which in range(3):
            stack_ref[which * shard : (which + 1) * shard, group * width : (group + 1) * width] = (
                total[which * width : (which + 1) * width].T
            )
    lines = shares.shape[1]
    for owner in range(owners):
        shares[owner] = stack_ref[owner * lines : (owner + 1) * lines, :].astype(BF16)
    total = s_in[0]
    for other in range(1, chips):
        total = total + s_in[other]
    s_total[...] = total
    rows = {}
    for far in range(1, owners):
        peer = lax.rem(row + far, owners)
        rows[0, far] = remote(
            shares.at[peer], shares_in.at[row], row_send.at[0, far], row_recv.at[0, far],
            {"expert": peer},
        )
        rows[0, far].start()
        rows[1, far] = remote(
            s_total, small_all_ref.at[row], row_send.at[1, far], row_recv.at[1, far],
            {"expert": peer},
        )
        rows[1, far].start()
    shares_in[row] = shares[row]
    small_all_ref[row] = total
    for far in range(1, owners):
        rows[0, far].wait_recv()
    summed = shares_in[0].astype(F32)
    for other in range(1, owners):
        summed = summed + shares_in[other].astype(F32)
    block_ref[...] = summed.astype(BF16)
    for far in range(1, chips):
        moved[2, far].wait_recv()
    for far in range(1, owners):
        peer = lax.rem(row + far, owners)
        rows[2, far] = remote(
            block_ref, sums_ref.at[row], row_send.at[2, far], row_recv.at[2, far],
            {"expert": peer},
        )
        rows[2, far].start()
    sums_ref[row] = summed.astype(BF16)
    da_in[chip] = da_sum[chip]
    total = da_in[0].astype(F32)
    for other in range(1, chips):
        total = total + da_in[other].astype(F32)
    total_ref[...] = total
    for far in range(1, owners):
        rows[1, far].wait_recv()
        rows[2, far].wait_recv()
    for copy in list(pair.values()) + list(moved.values()) + list(rows.values()):
        copy.wait_send()


def finish(da, pieces, small, owners, groups, number):
    context, tokens, width = da.shape
    chips = context // 2
    lines, shard = pieces.shape[1:]
    few = small.shape[1]
    stack = 3 * shard
    block = (stack // owners, width)
    return pl.pallas_call(
        functools.partial(finish_kernel, chips, owners, groups),
        out_shape=(
            jax.ShapeDtypeStruct((tokens, width), F32),
            jax.ShapeDtypeStruct((owners,) + block, BF16),
            jax.ShapeDtypeStruct((owners, few, shard), F32),
        ),
        in_specs=vmem(3),
        out_specs=vmem(3),
        scratch_shapes=[
            pltpu.VMEM((chips, tokens, width), BF16),
            pltpu.VMEM((chips, tokens, width), BF16),
            pltpu.VMEM((chips, tokens, width), BF16),
            pltpu.VMEM((chips, lines, shard), BF16),
            pltpu.VMEM((chips, lines, shard), BF16),
            pltpu.VMEM((chips, lines, shard), BF16),
            pltpu.VMEM((chips, few, shard), F32),
            pltpu.VMEM((chips, few, shard), F32),
            pltpu.VMEM((chips, few, shard), F32),
            pltpu.VMEM((few, shard), F32),
            pltpu.VMEM((stack, width), F32),
            pltpu.VMEM((owners,) + block, BF16),
            pltpu.VMEM((owners,) + block, BF16),
            pltpu.VMEM(block, BF16),
            pltpu.SemaphoreType.DMA((3, chips)),
            pltpu.SemaphoreType.DMA((3, chips)),
            pltpu.SemaphoreType.DMA((3, chips)),
            pltpu.SemaphoreType.DMA((3, chips)),
            pltpu.SemaphoreType.DMA((3, owners)),
            pltpu.SemaphoreType.DMA((3, owners)),
        ],
        compiler_params=pltpu.CompilerParams(
            collective_id=number, has_side_effects=True, vmem_limit_bytes=60 << 20
        ),
        name="finish",
    )(da, pieces, small)


def shards(
    hidden_in,
    prior_logits,
    routes,
    block_ids,
    grad_out,
    attn_gain,
    query_weight,
    key_weight,
    value_weight,
    output_weight,
    moe_gain,
    router_weight,
    prior_weight,
    const_mix,
    const_vector,
    gate_weight,
    up_weight,
    down_weight,
):
    token_rows = hidden_in.shape[1]
    model_width = hidden_in.shape[2]
    head_size = model_width // HEADS
    context = lax.axis_size("context")
    owners = lax.axis_size("expert")
    groups = math.gcd(HEADS, context)
    ranks = context // groups
    heads = HEADS // groups
    width = heads * head_size
    length = context * token_rows
    per_owner = gate_weight.shape[0]
    slot_count = per_owner * owners * CAP
    shard_width = model_width // context
    roles = per_owner
    residual = hidden_in[0].astype(F32)
    prior_rows = prior_logits[0]
    route_rows = routes[0]
    cotangent_low = grad_out[0]
    cotangent = cotangent_low.astype(F32)

    inv_rms1 = lax.rsqrt(jnp.mean(residual * residual, axis=1, keepdims=True) + EPS)
    normed_one = residual * inv_rms1
    attn_input = (normed_one * attn_gain).astype(BF16)
    ids_wide = jnp.broadcast_to(block_ids.astype(F32), (8, token_rows))
    stacked = jnp.stack([query_weight, key_weight, value_weight])
    stacked = stacked.reshape(3, shard_width, groups, width)
    pieces = jnp.transpose(stacked, (2, 0, 3, 1)).reshape(groups, 3 * width, shard_width)
    half = head_size // 2
    freq = jnp.power(THETA, -2.0 * jnp.arange(half, dtype=F32) / head_size)
    angle = freq[:, None] * jnp.arange(length, dtype=jnp.int32).astype(F32)[None, :]
    cos_t, sin_t = jnp.cos(angle), jnp.sin(angle)

    flat_route = route_rows.reshape(-1)
    ffn_hot = (flat_route[:, None] == jnp.arange(FFN_E, dtype=jnp.int32)[None, :]).astype(jnp.int32)
    before = jnp.sum((jnp.cumsum(ffn_hot, axis=0) - ffn_hot) * ffn_hot, axis=1)
    slot_index = jnp.where(
        flat_route < FFN_E,
        flat_route * CAP + before,
        -1,
    ).reshape(token_rows, 2)
    slot_ids = jnp.arange(slot_count, dtype=jnp.int32)[:, None]
    hit_first = slot_ids == slot_index[None, :, 0]
    hit_second = slot_ids == slot_index[None, :, 1]
    pick_first = hit_first.astype(BF16)
    pick_second = hit_second.astype(BF16)
    pick_either = pick_first + pick_second

    blocks = (owners, per_owner, CAP, model_width)

    def pick(rows):
        return jnp.dot(pick_either, rows, preferred_element_type=F32).astype(BF16).reshape(blocks)

    (
        out_t, log_total, query_t, ids, weights_t, key_heads, key_t, value_heads,
        a_full, mix_granules, output_full, wide_full, grad_arrived, _,
    ) = attn_forward(
        ids_wide, pieces, attn_input, cos_t, sin_t, pick(cotangent_low),
        output_weight, gate_weight, up_weight, heads, head_size, ranks, context, roles, 0,
    )
    kept = (out_t, log_total, query_t, key_heads, key_t, value_heads)
    out_blocks = mix_granules.reshape(groups, token_rows, width)
    mix_low = jnp.transpose(out_blocks, (1, 0, 2)).reshape(token_rows, model_width)

    after_attn = residual + jnp.dot(mix_low, output_full, preferred_element_type=F32)
    inv_rms2 = lax.rsqrt(jnp.mean(after_attn * after_attn, axis=1, keepdims=True) + EPS)
    normed_two = after_attn * inv_rms2
    moe_input = normed_two * moe_gain
    narrow = jnp.concatenate(
        [router_weight, jnp.transpose(const_mix.reshape(-1, model_width))], axis=1
    )
    narrow_out = jnp.dot(moe_input, narrow, precision=HIGH, preferred_element_type=F32)
    expert_count = router_weight.shape[1]
    consts = const_mix.shape[0]
    logits = narrow_out[:, :expert_count] + jnp.dot(
        prior_rows, prior_weight, precision=HIGH, preferred_element_type=F32
    )
    probs = jax.nn.softmax(logits, axis=1)
    expert_ids = jnp.arange(expert_count, dtype=jnp.int32)
    first_hot = (route_rows[:, 0:1] == expert_ids[None, :]).astype(F32)
    second_hot = (route_rows[:, 1:2] == expert_ids[None, :]).astype(F32)
    chosen = first_hot + second_hot
    gated = probs * chosen
    first_gate = jnp.sum(probs * first_hot, axis=1, keepdims=True)
    second_gate = jnp.sum(probs * second_hot, axis=1, keepdims=True)
    slot_gate = jnp.sum(
        jnp.where(hit_first, first_gate[None, :, 0], 0.0)
        + jnp.where(hit_second, second_gate[None, :, 0], 0.0),
        axis=1,
    )
    def spread(values):
        values = values.reshape(owners, per_owner, CAP)
        return jnp.pad(values, ((0, 0), (0, 8 - per_owner), (0, 128 - CAP)))

    gates, arrived, down_full = dispatch(
        spread(slot_gate), pick(moe_input.astype(BF16)), down_weight, context, roles, 2
    )
    role = lax.axis_index("context") // 2 // (context // 2 // roles)
    gates = lax.dynamic_index_in_dim(gates, role, 3, keepdims=False)[..., :CAP].reshape(-1, 1)

    expert_out, grad_rows, owner_dot, grad_wide, down_parts = experts(
        arrived, grad_arrived, gates, wide_full, down_full, context, owners, 7
    )
    owner_dot = jnp.pad(
        owner_dot.reshape(roles, 2, owners, 1, CAP), ((0, 0),) * 3 + ((0, 7), (0, 128 - CAP))
    )
    slot_dot, grad_back, expert_out = collect(
        owner_dot, grad_rows, expert_out, context, roles, 3
    )
    slot_dot = slot_dot[:, :, 0, :CAP].reshape(slot_count)
    grad_back = grad_back.reshape(slot_count, model_width)

    const_soft = jax.nn.softmax(narrow_out[:, expert_count:].reshape(token_rows, consts, 2), axis=2)
    const_gate = gated[:, FFN_E + 2 :]
    copy_gate = gated[:, FFN_E + 1 : FFN_E + 2]
    const_out = [
        const_soft[:, c, 0:1] * moe_input + const_soft[:, c, 1:2] * const_vector[c][None, :]
        for c in range(consts)
    ]
    local_moe = copy_gate * moe_input
    for c in range(consts):
        local_moe = local_moe + const_gate[:, c : c + 1] * const_out[c]
    grad_moe_ffn = lax.dot_general(
        pick_either, grad_back, (((0,), (0,)), ((), ())), preferred_element_type=F32
    )
    first_dot = jnp.sum(jnp.where(hit_first, slot_dot[:, None], 0.0), axis=0)[:, None]
    second_dot = jnp.sum(jnp.where(hit_second, slot_dot[:, None], 0.0), axis=0)[:, None]
    copy_dot = jnp.sum(cotangent * moe_input, axis=1, keepdims=True)
    const_dot = [jnp.sum(cotangent * const_out[c], axis=1, keepdims=True) for c in range(consts)]
    extra = jnp.concatenate(
        [jnp.zeros((token_rows, FFN_E + 1), F32), copy_dot, *const_dot], axis=1
    )
    grad_probs = first_hot * first_dot + second_hot * second_dot + chosen * extra
    grad_logits = probs * (grad_probs - jnp.sum(probs * grad_probs, axis=1, keepdims=True))
    grad_prior_rows = lax.dot_general(
        grad_logits, prior_weight, (((1,), (1,)), ((), ())),
        precision=HIGH, preferred_element_type=F32,
    )
    vector_dot = jnp.dot(
        cotangent, jnp.transpose(const_vector), precision=HIGH, preferred_element_type=F32
    )
    grad_soft = jnp.stack(
        [const_gate * copy_dot, const_gate * vector_dot], axis=2
    )
    grad_mix = const_soft * (grad_soft - jnp.sum(const_soft * grad_soft, axis=2, keepdims=True))
    narrow_grad = jnp.concatenate([grad_logits, grad_mix.reshape(token_rows, -1)], axis=1)
    local_scale = copy_gate + jnp.sum(const_soft[:, :, 0] * const_gate, axis=1, keepdims=True)
    grad_moe_input = (
        grad_moe_ffn
        + lax.dot_general(
            narrow_grad, narrow, (((1,), (1,)), ((), ())),
            precision=HIGH, preferred_element_type=F32,
        )
        + local_scale * cotangent
    )
    small_moe = lax.dot_general(
        narrow_grad, moe_input, (((0,), (0,)), ((), ())),
        precision=HIGH, preferred_element_type=F32,
    )
    small_vector = lax.dot_general(
        const_soft[:, :, 1] * const_gate, cotangent, (((0,), (0,)), ((), ())),
        precision=HIGH, preferred_element_type=F32,
    )
    grad_prior_local = lax.dot_general(
        prior_rows, grad_logits, (((0,), (0,)), ((), ())),
        precision=HIGH, preferred_element_type=F32,
    )
    small_gain = jnp.sum(grad_moe_input * normed_two, axis=0, keepdims=True)
    prior_values = jnp.pad(
        grad_prior_local.reshape(-1), (0, -(expert_count * expert_count) % shard_width)
    ).reshape(-1, 1, shard_width)
    prior_lines = prior_values.shape[0]
    small = jnp.concatenate([small_moe, small_vector, small_gain], axis=0)
    small_lines = small.shape[0]
    small = jnp.concatenate(
        [
            small.reshape(small_lines, context, shard_width),
            jnp.broadcast_to(prior_values, (prior_lines, context, shard_width)),
        ],
        axis=0,
    )
    small = jnp.pad(small, ((0, -small.shape[0] % 8), (0, 0), (0, 0)))
    small = jnp.transpose(small, (1, 0, 2))

    grad_normed_two = grad_moe_input * moe_gain
    grad_after = cotangent + inv_rms2 * (
        grad_normed_two - normed_two * jnp.mean(grad_normed_two * normed_two, axis=1, keepdims=True)
    )
    grad_attn_low = grad_after.astype(BF16)
    grad_mix_low = lax.dot_general(
        grad_attn_low, output_full, (((1,), (1,)), ((), ())), preferred_element_type=F32
    ).astype(BF16)
    grad_pieces = jnp.transpose(grad_mix_low.reshape(token_rows, groups, width), (1, 0, 2))
    grad_own = grad_pieces.reshape(-1, TILE // 2, width)
    grad_output_local = lax.dot_general(
        mix_low, grad_attn_low, (((0,), (0,)), ((), ())), preferred_element_type=F32
    ).astype(BF16)
    da_part, w_pieces, output_sum, wide_parts, returned = attn_backward(
        grad_own, a_full, weights_t, cos_t, sin_t, ids, kept,
        grad_wide, expert_out, grad_output_local,
        heads, head_size, ranks, context, roles, 6,
    )
    returned = returned.reshape(slot_count, model_width)
    same = context // 2 // roles
    wide_parts = wide_parts.reshape(roles, same, 2, 2, shard_width, -1)

    def whole(which):
        total = jnp.sum(wide_parts[:, :, :, which].astype(F32), axis=1)
        return jnp.concatenate([total[:, 0], total[:, 1]], axis=-1)

    down_sum = jnp.sum(
        down_parts.reshape(roles, same, -1, model_width).astype(F32), axis=1
    )
    grad_attn_input, sums, small_all = finish(
        da_part.reshape(context, token_rows, model_width), w_pieces, small,
        owners, groups, 5,
    )
    grad_normed_one = grad_attn_input * attn_gain
    grad_input = grad_after + inv_rms1 * (
        grad_normed_one - normed_one * jnp.mean(grad_normed_one * normed_one, axis=1, keepdims=True)
    )
    w_sum = sums.astype(F32).reshape(3, shard_width, model_width)
    small_own = jnp.sum(small_all, axis=0)
    grad_attn_gain = jnp.sum(
        w_sum[0] * query_weight.astype(F32)
        + w_sum[1] * key_weight.astype(F32)
        + w_sum[2] * value_weight.astype(F32),
        axis=1,
    )
    column = lax.axis_index("context") * shard_width
    grad_attn_gain = grad_attn_gain / lax.dynamic_slice_in_dim(attn_gain, column, shard_width)
    mixes = expert_count + 2 * consts
    grad_prior_weight = small_own[small_lines : small_lines + prior_lines].reshape(-1)
    grad_prior_weight = grad_prior_weight[: expert_count * expert_count].reshape(
        expert_count, expert_count
    )
    layer_out = after_attn + local_moe
    layer_out = layer_out + first_gate * lax.dot_general(
        pick_first, returned, (((0,), (0,)), ((), ())), preferred_element_type=F32
    )
    layer_out = layer_out + second_gate * lax.dot_general(
        pick_second, returned, (((0,), (0,)), ((), ())), preferred_element_type=F32
    )
    return (
        layer_out.astype(BF16)[None],
        grad_input[None],
        grad_prior_rows[None],
        grad_attn_gain,
        w_sum[0],
        w_sum[1],
        w_sum[2],
        output_sum,
        small_own[small_lines - 1],
        jnp.transpose(small_own[:expert_count]),
        grad_prior_weight,
        small_own[expert_count:mixes].reshape(consts, 2, shard_width),
        small_own[mixes : mixes + consts],
        whole(0),
        whole(1),
        down_sum,
    )


def solution(mesh):
    return jax.shard_map(
        shards,
        mesh=mesh,
        in_specs=(
            P("expert", "context", None),
            P("expert", "context", None),
            P("expert", "context", None),
            P("expert", "context"),
            P("expert", "context", None),
            P(),
            P("context", None),
            P("context", None),
            P("context", None),
            P("context", None),
            P(),
            P(),
            P(),
            P(),
            P(),
            P("expert", "context", None),
            P("expert", "context", None),
            P("expert", "context", None),
        ),
        out_specs=(
            P("expert", "context", None),
            P("expert", "context", None),
            P("expert", "context", None),
            P("context"),
            P("context", None),
            P("context", None),
            P("context", None),
            P("context", None),
            P("context"),
            P("context", None),
            P(),
            P(None, None, "context"),
            P(None, "context"),
            P("expert", "context", None),
            P("expert", "context", None),
            P("expert", "context", None),
        ),
        check_vma=False,
    )
```

```python
import functools
import math

import jax
import jax.numpy as jnp
from jax import lax
from jax.experimental import pallas as pl
from jax.experimental.pallas import tpu as pltpu
from jax.sharding import PartitionSpec as P

HEADS = 12
FFN_E = 8
CAP = 96
TILE = 256
EXTRA = 16
HIDDEN_TILE = 256

EPS = 1e-06
THETA = 10000.0
NEGATIVE = -1e30
HIGH = lax.Precision.HIGHEST
F32 = jnp.float32
BF16 = jnp.bfloat16


def dot(left, right, left_dim=1, right_dim=0):
    return lax.dot_general(
        left, right, (((left_dim,), (right_dim,)), ((), ())), preferred_element_type=F32
    )


def turn(rows, cos_rows, sin_rows, heads, size, back=False):
    half = size // 2
    parts = []
    for head in range(heads):
        first = rows[head * size : head * size + half]
        second = rows[head * size + half : (head + 1) * size]
        if back:
            parts.append(first * cos_rows + second * sin_rows)
            parts.append(second * cos_rows - first * sin_rows)
        else:
            parts.append(first * cos_rows - second * sin_rows)
            parts.append(second * cos_rows + first * sin_rows)
    return jnp.concatenate(parts, axis=0)


def own_tile(index, ranks):
    rank = lax.rem(lax.axis_index("context"), ranks)
    place = lax.rem(index, 2)
    return (index // 2) * (2 * ranks) + jnp.where(place == 0, rank, 2 * ranks - 1 - rank)


def granule_of(slot, ranks):
    return own_tile(slot // 2, ranks) * 2 + lax.rem(slot, 2)


def owner_rank(granule, ranks):
    spot = lax.rem(granule // 2, 2 * ranks)
    return jnp.minimum(spot, 2 * ranks - 1 - spot)


def owner_slot(granule, ranks):
    tile = granule // 2
    upper = jnp.where(lax.rem(tile, 2 * ranks) >= ranks, 1, 0)
    return (tile // (2 * ranks) * 2 + upper) * 2 + lax.rem(granule, 2)


def here_or_away(device, source, target, send, recv):
    place = lax.axis_index("context")

    @pl.when(device == place)
    def _():
        pltpu.make_async_copy(source, target, recv).start()

    @pl.when(device != place)
    def _():
        remote(source, target, send, recv, {"context": device}).start()


def wait_sent(device, source, target, send, recv):
    @pl.when(device != lax.axis_index("context"))
    def _():
        remote(source, target, send, recv, {"context": device}).wait_send()


def wait_landed(device, source, target, send, recv):
    place = lax.axis_index("context")

    @pl.when(device == place)
    def _():
        pltpu.make_async_copy(source, target, recv).wait()

    @pl.when(device != place)
    def _():
        remote(source, target, send, recv, {"context": device}).wait_recv()


def lanes(start):
    return span(start, TILE)


def span(start, size):
    return pl.ds(pl.multiple_of(start * size, size), size)


def cost(micros):
    return pl.CostEstimate(flops=micros * 1_150_000_000, bytes_accessed=0, transcendentals=0)


def vmem(count):
    return [pl.BlockSpec(memory_space=pltpu.VMEM)] * count


def hbm(count):
    return [pl.BlockSpec(memory_space=pl.ANY)] * count


def params(number=None, limit=60):
    if number is None:
        return pltpu.CompilerParams(vmem_limit_bytes=limit << 20)
    return pltpu.CompilerParams(
        collective_id=number, has_side_effects=True, vmem_limit_bytes=limit << 20
    )


def remote(source, target, send, recv, device):
    return pltpu.make_async_remote_copy(
        src_ref=source, dst_ref=target, send_sem=send, recv_sem=recv,
        device_id=device, device_id_type=pl.DeviceIdType.MESH,
    )


def chip_at(chip, far, chips, square, back=False):
    if square:
        x, y = lax.rem(chip, 2), chip // 2
        x = x + (far % 2) * (1 - 2 * x)
        y = y + (far // 2) * (1 - 2 * y)
        return 2 * y + x
    return lax.rem(chip + (chips - far if back else far), chips)


def meet(context, owners):
    place, row = lax.axis_index("context"), lax.axis_index("expert")
    barrier = pltpu.get_barrier_semaphore()
    for far in range(1, context):
        pl.semaphore_signal(
            barrier, inc=1, device_id={"context": lax.rem(place + far, context)},
            device_id_type=pl.DeviceIdType.MESH,
        )
    for far in range(1, owners):
        pl.semaphore_signal(
            barrier, inc=1, device_id={"expert": lax.rem(row + far, owners)},
            device_id_type=pl.DeviceIdType.MESH,
        )
    pl.semaphore_wait(barrier, context + owners - 2)
    return place, row


def attn_forward_kernel(
    dims,
    ids_ref, pieces_ref, input_ref, cos_ref, sin_ref, grads_ref, output_ref, gate_ref, up_ref,
    out_t_ref, lse_ref, query_t_ref, ids_all_ref, wt_ref,
    key_out, key_t_out, value_out, a_out, mix_ref,
    output_all_ref, wide_ref, grads_all_ref, stage_ref,
    w_all_ref, value_t_ref, scores_ref, acc_ref, key_ref, key_t_ref, value_ref, a_ref, out_ref,
    keep_sem, granule_send, granule_recv,
    local_sem, send_sem, recv_sem, pass_sem, land_sem, half_send, half_recv,
    row_send, row_recv, hop_send, hop_recv, lend_send, lend_recv, wide_send, wide_recv,
):
    heads, size, ranks, scale, context, owners, roles, square = dims
    length = a_ref.shape[0]
    rows = length // context
    shard = output_ref.shape[0]
    half = wide_ref.shape[2]
    width = heads * size
    tiles = length // TILE
    own_tiles = tiles // ranks
    ext = size + EXTRA
    chips = context // 2
    place, row = meet(context, owners)
    chip, core = place // 2, lax.rem(place, 2)
    partner = place + 1 - 2 * core
    slot = chip // (chips // roles)
    other = (roles - 1) - slot
    twin = 2 * lax.rem(chip + chips // 2, chips) + core

    def source(item, device):
        return (ids_ref, pieces_ref.at[device // ranks], input_ref, output_ref)[item]

    def target(item, device):
        return (
            ids_all_ref.at[:, span(device, rows)],
            w_all_ref.at[device],
            a_ref.at[span(device, rows), :],
            output_all_ref.at[span(device, shard), :],
        )[item]

    def from_chip(far):
        return 2 * chip_at(chip, far, chips, square, True) + core

    def sends(item, far):
        if isinstance(far, int) and far == 0:
            peer = partner
        else:
            peer = 2 * chip_at(chip, far, chips, square) + core
        return remote(
            source(item, peer), target(item, place), send_sem.at[item, far],
            recv_sem.at[item, far], {"context": peer},
        )

    def passes(item, far):
        block = target(item, from_chip(far))
        return remote(
            block, block, pass_sem.at[item, far], land_sem.at[item, far], {"context": partner}
        )

    def keeps(item):
        return pltpu.make_async_copy(
            source(item, place), target(item, place), local_sem.at[item]
        )

    def halves(far):
        upper = rows // 2
        start = from_chip(far) * rows + (far - 1) * upper
        block = a_ref.at[pl.ds(pl.multiple_of(start, upper), upper), :]
        return remote(
            block, block, half_send.at[far], half_recv.at[far],
            {"context": 2 * chip_at(chip, 3 - far, chips, square) + core},
        )

    def corner(far):
        upper = rows // 2
        start = from_chip(3) * rows + (far - 1) * upper
        block = a_ref.at[pl.ds(pl.multiple_of(start, upper), upper), :]
        return remote(block, block, half_send.at[far], half_recv.at[far], {"context": partner})

    direct = {item: list(range(1, chips)) for item in range(4)}
    if square:
        direct[2] = [1, 2]
    def begin(item):
        for far in direct[item] + [0]:
            sends(item, far).start()
        keeps(item).start()

    for item in range(3):
        begin(item)
    shard_granules = rows // (TILE // 2)
    group = place // ranks
    owned = out_ref.shape[0]

    def outgoing(step):
        granule = granule_of(step, ranks)
        target_slot = group * shard_granules + lax.rem(granule, shard_granules)
        return (
            granule // shard_granules, out_ref.at[step], mix_ref.at[target_slot],
            granule_send.at[step], granule_recv.at[target_slot],
        )

    def part(device, which):
        return grads_ref.at[device, which]

    to_rows, hops, lends = {}, {}, {}
    for far in range(owners):
        peer = lax.rem(row + far, owners)
        spots = [(slot, grads_all_ref.at[slot, core, row])]
        if roles > 1:
            spots.append((other, stage_ref.at[row]))
        for which, (role, spot) in enumerate(spots):
            if far > 0:
                to_rows[which, far] = remote(
                    part(peer, role), spot, row_send.at[which, far], row_recv.at[which, far],
                    {"expert": peer},
                )
            elif which == 0:
                to_rows[which, far] = pltpu.make_async_copy(part(row, role), spot, local_sem.at[4])
            else:
                lends[0] = remote(
                    part(row, role), grads_all_ref.at[slot, core, row], lend_send.at[0],
                    lend_recv.at[0], {"context": twin},
                )
    for copy in to_rows.values():
        copy.start()

    wide_out, wide_on = [], []
    for which, weight in enumerate((gate_ref, up_ref)):
        spot = wide_ref.at[which, span(place, shard), :]

        def block(device):
            role = device // 2 // (chips // roles)
            return weight.at[role, :, span(lax.rem(device, 2), half)]

        if square:
            peers = [
                (2 * chip_at(chip, far, chips, square) + side, 2 * far + turned)
                for far in (1, 2)
                for turned, side in enumerate((core, 1 - core))
            ] + [(partner, 1)]
        else:
            peers = [(lax.rem(place + far, context), far) for far in range(1, context)]
        for peer, index in peers:
            wide_out.append(
                remote(
                    block(peer), spot, wide_send.at[which, index], wide_recv.at[which, index],
                    {"context": peer},
                )
            )
        wide_out.append(pltpu.make_async_copy(block(place), spot, local_sem.at[5 + which]))
        if square:
            for turned in range(2):
                side = core if turned == 0 else 1 - core
                giver = 2 * chip_at(chip, 2, chips, square) + side
                block_on = wide_ref.at[which, span(giver, shard), :]
                wide_on.append(
                    remote(
                        block_on, block_on, wide_send.at[which, 6 + turned],
                        wide_recv.at[which, 6 + turned],
                        {"context": 2 * chip_at(chip, 1, chips, square) + core},
                    )
                )
    arrives = {}
    if square:
        index = 0
        for which in range(2):
            for far in (1, 2):
                for turned in range(2):
                    arrives[which, far, turned] = wide_out[index]
                    index += 1
            index += 2

    tail = (lax.broadcasted_iota(jnp.int32, (EXTRA, rows), 0) == 0).astype(BF16)
    for item in range(2):
        for far in range(1, chips):
            sends(item, far).wait_recv()
            passes(item, far).start()
        sends(item, 0).wait_recv()
        keeps(item).wait()
        for far in range(1, chips):
            passes(item, far).wait_recv()
    for device in range(context):
        wt_ref[:, device * shard : (device + 1) * shard] = w_all_ref[device]

    def project(step, carry):
        far, second = step // 2, lax.rem(step, 2)
        block = 2 * chip_at(chip, far, chips, square, True) + jnp.where(
            second == 0, core, 1 - core
        )

        @pl.when(jnp.logical_and(far == 0, second == 0))
        def _():
            keeps(2).wait()

        @pl.when(jnp.logical_and(far == 0, second == 1))
        def _():
            sends(2, 0).wait_recv()

        if square:

            @pl.when(jnp.logical_and(far == 1, second == 0))
            def _():
                for near in (1, 2):
                    sends(2, near).wait_recv()
                    halves(near).start()
                    passes(2, near).start()
                begin(3)
                for copy in wide_out:
                    copy.start()

            @pl.when(jnp.logical_and(far == 3, second == 0))
            def _():
                for near in (1, 2):
                    corner(near).wait_recv()
                passes(2, 3).start()

        else:

            @pl.when(jnp.logical_and(far > 0, second == 0))
            def _():
                sends(2, far).wait_recv()
                passes(2, far).start()

        @pl.when(jnp.logical_and(far > 0, second == 1))
        def _():
            passes(2, far).wait_recv()

        at = span(block, rows)
        both = dot(wt_ref[width:, :], a_ref[at, :], 1, 1)
        key_t = turn(both[:width], cos_ref[:, at], sin_ref[:, at], heads, size)
        key_t_ref[:, at] = key_t.astype(BF16)
        value_t = both[width:]
        for head in range(heads):
            here = slice(head * size, (head + 1) * size)
            key_ref[head, at, :] = key_t[here].T.astype(BF16)
            value_ref[head, at, :] = value_t[here].T.astype(BF16)
            value_t_ref[head * ext : head * ext + size, at] = value_t[here].astype(BF16)
            value_t_ref[head * ext + size : (head + 1) * ext, at] = tail
        return carry

    lax.fori_loop(0, 2 * chips, project, 0)
    if not square:
        begin(3)
        for copy in wide_out:
            copy.start()
    stored = [
        pltpu.make_async_copy(source, target, keep_sem.at[index])
        for index, (source, target) in enumerate(
            ((key_ref, key_out), (key_t_ref, key_t_out), (value_ref, value_out), (a_ref, a_out))
        )
    ]
    for copy in stored:
        copy.start()
    if roles > 1:
        lends[0].start()
    for far in range(owners):
        peer = lax.rem(row + owners - far, owners)
        home = grads_all_ref.at[slot, core, peer]
        if far > 0:
            to_rows[0, far].wait_recv()
        else:
            to_rows[0, far].wait()
        hops[far] = remote(
            home, home, hop_send.at[0, far], hop_recv.at[0, far], {"context": partner}
        )
        hops[far].start()
        if roles > 1 and far > 0:
            to_rows[1, far].wait_recv()
            lends[far] = remote(
                stage_ref.at[peer], home, lend_send.at[far], lend_recv.at[far],
                {"context": twin},
            )
            lends[far].start()

    def relays():
        for far in range(1, chips):
            sends(3, far).wait_recv()
            passes(3, far).start()
        for far in lends:
            lends[far].wait_recv()
            afar(far).start()

    def afar(far):
        away = grads_all_ref.at[other, core, lax.rem(row + owners - far, owners)]
        return remote(
            away, away, hop_send.at[1, far], hop_recv.at[1, far], {"context": partner}
        )

    def attend(index, carry):
        @pl.when(index > 0)
        def _():
            for step in range(2):
                here_or_away(*outgoing(2 * index - 2 + step))

        @pl.when(index == own_tiles - 1)
        def _():
            relays()

        if square:

            @pl.when(index == own_tiles // 2)
            def _():
                for which in range(2):
                    for turned in range(2):
                        arrives[which, 2, turned].wait_recv()
                for copy in wide_on:
                    copy.start()

        tile = own_tile(index, ranks)
        at = lanes(tile)
        query_t = dot(wt_ref[:width, :], a_ref[at, :], 1, 1)
        query_t = turn(query_t, cos_ref[:, at], sin_ref[:, at], heads, size)
        query_t = query_t.astype(BF16) * jnp.asarray(scale, BF16)
        query_t_ref[:, lanes(index)] = query_t
        query_ids = ids_all_ref[0:1, at]

        def score(step, tops, masked):
            here = lanes(step)
            fresh = []
            if masked:
                allowed = ids_all_ref[:, here].T[:, 0:1] <= query_ids
            for head in range(heads):
                part = dot(key_ref[head, here, :], query_t[head * size : (head + 1) * size])
                if masked:
                    part = jnp.where(allowed, part, NEGATIVE)
                scores_ref[head, here, :] = part
                fresh.append(
                    jnp.maximum(tops[head], jnp.max(part.reshape(TILE // 8, 8, TILE), axis=0))
                )
            return tuple(fresh)

        tops = tuple(jnp.full((8, TILE), NEGATIVE, F32) for _ in range(heads))
        stop = jnp.minimum(tile + 2, tiles)
        tops = lax.fori_loop(0, tile, lambda s, c: score(s, c, False), tops)
        tops = lax.fori_loop(tile, stop, lambda s, c: score(s, c, True), tops)
        peaks = [jnp.max(top, axis=0, keepdims=True) for top in tops]
        acc_ref[...] = jnp.zeros_like(acc_ref)

        def combine(step, carry):
            here = lanes(step)
            for head in range(heads):
                weights = jnp.exp(scores_ref[head, here, :] - peaks[head]).astype(BF16)
                acc_ref[head] += dot(value_t_ref[head * ext : (head + 1) * ext, here], weights)
            return carry

        lax.fori_loop(0, stop, combine, 0)
        parts = []
        for head in range(heads):
            total = acc_ref[head, size : size + 1, :]
            part = acc_ref[head, :size, :] * (1.0 / total)
            lse_ref[head : head + 1, lanes(index)] = peaks[head] + jnp.log(total)
            parts.append(part)
        joined = jnp.concatenate(parts, axis=0)
        out_t_ref[:, lanes(index)] = joined
        turned_out = joined.T.astype(BF16)
        out_ref[2 * index] = turned_out[: TILE // 2]
        out_ref[2 * index + 1] = turned_out[TILE // 2 :]
        return carry

    lax.fori_loop(0, own_tiles, attend, 0)
    for step in range(2):
        here_or_away(*outgoing(2 * own_tiles - 2 + step))
    sends(3, 0).wait_recv()
    keeps(3).wait()
    for far in range(1, chips):
        passes(3, far).wait_recv()
    for item in range(4):
        for far in direct[item] + [0]:
            sends(item, far).wait_send()
        for far in range(1, chips):
            passes(item, far).wait_send()
    if square:
        for far in (1, 2):
            halves(far).wait_send()
    forwarded = [arrives[which, 2, turned] for which, _, turned in arrives if _ == 2]
    for copy in wide_out:
        if any(copy is one for one in forwarded):
            copy.wait_send()
        else:
            copy.wait()
    for (which, far), copy in to_rows.items():
        if far > 0:
            copy.wait_send()
    for copy in lends.values():
        copy.wait_send()
    for copy in wide_on + list(hops.values()) + [afar(far) for far in lends] + stored:
        copy.wait()

    def settle(step, carry):
        wait_sent(*outgoing(step))
        giver_group, spot = step // shard_granules, lax.rem(step, shard_granules)
        giver = giver_group * ranks + owner_rank(place * shard_granules + spot, ranks)
        wait_landed(
            giver, out_ref.at[0], mix_ref.at[step], granule_send.at[0], granule_recv.at[step]
        )
        return carry

    lax.fori_loop(0, owned, settle, 0)


def attn_forward(
    ids, pieces, attn_input, cos_t, sin_t, grads, output_weight, gate_weight, up_weight,
    heads, size, ranks, context, roles, number,
):
    rows, model = attn_input.shape
    owners = grads.shape[0]
    length = rows * context
    own = length // ranks
    width = heads * size
    ext = size + EXTRA
    shard = output_weight.shape[0]
    chips = context // 2
    granule = TILE // 2
    head_shape = jax.ShapeDtypeStruct((heads, length, size), BF16)
    turned_shape = jax.ShapeDtypeStruct((width, length), BF16)
    a_shape = jax.ShapeDtypeStruct((length, model), BF16)
    own_shape = jax.ShapeDtypeStruct((own // granule, granule, width), BF16)
    shapes = (
        jax.ShapeDtypeStruct((width, own), F32),
        jax.ShapeDtypeStruct((heads, own), F32),
        jax.ShapeDtypeStruct((width, own), BF16),
        jax.ShapeDtypeStruct((8, length), F32),
        jax.ShapeDtypeStruct((3 * width, model), BF16),
        head_shape,
        turned_shape,
        head_shape,
        a_shape,
        own_shape,
        jax.ShapeDtypeStruct((model, model), BF16),
        jax.ShapeDtypeStruct((2, model, gate_weight.shape[2] // 2), BF16),
        jax.ShapeDtypeStruct((roles, 2, owners) + grads.shape[2:], BF16),
        jax.ShapeDtypeStruct((owners,) + grads.shape[2:], BF16),
    )
    square = chips == 4 and roles == 2
    dims = (heads, size, ranks, size ** (-0.5), context, owners, roles, square)
    return pl.pallas_call(
        functools.partial(attn_forward_kernel, dims),
        out_shape=shapes,
        in_specs=vmem(5) + hbm(4),
        out_specs=vmem(5) + hbm(9),
        scratch_shapes=[
            pltpu.VMEM((context, 3 * width, shard), BF16),
            pltpu.VMEM((heads * ext, length), BF16),
            pltpu.VMEM((heads, length, TILE), F32),
            pltpu.VMEM((heads, ext, TILE), F32),
        ]
        + [
            pltpu.VMEM(one.shape, one.dtype)
            for one in (head_shape, turned_shape, head_shape, a_shape, own_shape)
        ]
        + [
            pltpu.SemaphoreType.DMA((4,)),
            pltpu.SemaphoreType.DMA((own // granule,)),
            pltpu.SemaphoreType.DMA((own // granule,)),
            pltpu.SemaphoreType.DMA((7,)),
            pltpu.SemaphoreType.DMA((4, chips)),
            pltpu.SemaphoreType.DMA((4, chips)),
            pltpu.SemaphoreType.DMA((4, chips)),
            pltpu.SemaphoreType.DMA((4, chips)),
            pltpu.SemaphoreType.DMA((3,)),
            pltpu.SemaphoreType.DMA((3,)),
        ]
        + [pltpu.SemaphoreType.DMA((2, owners))] * 4
        + [pltpu.SemaphoreType.DMA((owners,))] * 2
        + [pltpu.SemaphoreType.DMA((2, context))] * 2,
        compiler_params=params(number, 62),
        cost_estimate=cost(80),
        name="attn_forward",
    )(ids, pieces, attn_input, cos_t, sin_t, grads, output_weight, gate_weight, up_weight)


def attn_backward_kernel(
    dims,
    grad_ref, a_ref, wt_ref, cos_ref, sin_ref, ids_all_ref,
    out_t_ref, lse_ref, query_t_ref, key_ref, key_t_ref, value_ref,
    wide_ref, outs_ref, output_ref,
    da_ref, pieces_ref, output_sum_ref, wide_in_ref, outs_in_ref,
    query_ref, own_grad_ref, dq_ref, dk_ref, dv_ref, grad_w_ref,
    landed_ref, output_in_ref, share_ref, shares_ref,
    granule_send, granule_recv, share_send, share_recv,
    wide_send, wide_recv, output_send, output_recv,
    row_send, row_recv, local_sem,
):
    heads, size, ranks, scale, context, owners, roles = dims
    length = a_ref.shape[0]
    shard = pieces_ref.shape[2]
    width = heads * size
    tiles = length // TILE
    own_tiles = tiles // ranks
    chips = context // 2
    place, row = meet(context, owners)
    chip, core = place // 2, lax.rem(place, 2)
    owned = landed_ref.shape[0]
    shard_granules = owned * ranks // context

    def outgoing(step):
        giver = step // shard_granules
        granule = place * shard_granules + lax.rem(step, shard_granules)
        landing = owner_slot(granule, ranks)
        return (
            giver * ranks + owner_rank(granule, ranks), grad_ref.at[step],
            landed_ref.at[landing], granule_send.at[step], granule_recv.at[landing],
        )

    def launch(step, carry):
        here_or_away(*outgoing(step))
        return carry

    lax.fori_loop(0, owned, launch, 0)
    copies, output_copies = [], []
    for item, (grads, target, send, recv) in enumerate(
        (
            (output_ref, output_in_ref, output_send, output_recv),
            (wide_ref, wide_in_ref, wide_send, wide_recv),
        )
    ):
        for far in range(context):
            peer = lax.rem(place + far, context)
            at = span(peer, shard)
            source = grads.at[:, at, :] if item else grads.at[at, :]
            group_copies = copies if item else output_copies
            if far == 0:
                group_copies.append(
                    pltpu.make_async_copy(source, target.at[place], local_sem.at[item])
                )
            else:
                group_copies.append(
                    remote(
                        source, target.at[place], send.at[far], recv.at[far], {"context": peer}
                    )
                )
    for far in range(owners):
        peer = lax.rem(row + far, owners)
        if far == 0:
            copies.append(
                pltpu.make_async_copy(outs_ref.at[row], outs_in_ref.at[row], local_sem.at[2])
            )
        else:
            copies.append(
                remote(
                    outs_ref.at[peer], outs_in_ref.at[row], row_send.at[far], row_recv.at[far],
                    {"expert": peer},
                )
            )
    dk_ref[...] = jnp.zeros_like(dk_ref)
    dv_ref[...] = jnp.zeros_like(dv_ref)
    da_ref[...] = jnp.zeros_like(da_ref)
    grad_w_ref[...] = jnp.zeros_like(grad_w_ref)
    def landed(step, carry):
        giver = granule_of(step, ranks) // shard_granules
        wait_landed(
            giver, grad_ref.at[0], landed_ref.at[step], granule_send.at[0], granule_recv.at[step]
        )
        return carry

    lax.fori_loop(0, owned, landed, 0)
    for copy in output_copies + copies:
        copy.start()

    def share_copy(far):
        return remote(
            share_ref, shares_ref.at[row], share_send.at[far], share_recv.at[far],
            {"expert": lax.rem(row + far, owners)},
        )

    def attend(index, carry):
        tile = own_tile(index, ranks)
        at = lanes(tile)
        query_t = query_t_ref[:, lanes(index)]
        @pl.when(index == own_tiles // 2)
        def _():
            for copy in output_copies:
                copy.wait()
            total = output_in_ref[0].astype(F32)
            for giver in range(1, context):
                total = total + output_in_ref[giver].astype(F32)
            share_ref[...] = total.astype(BF16)

        @pl.when(index == own_tiles // 2 + 1)
        def _():
            for far in range(1, owners):
                share_copy(far).start()

        grad_rows = landed_ref[pl.ds(2 * index, 2)].reshape(TILE, width)
        grad_t = grad_rows.astype(F32).T
        query_rows = query_t.astype(F32).T.astype(BF16)
        query_ids = ids_all_ref[0:1, at]
        deltas, tops, grads_low = [], [], []
        for head in range(heads):
            rows = slice(head * size, (head + 1) * size)
            query_ref[head] = query_rows[:, rows]
            own_grad_ref[head] = grad_rows[:, rows]
            deltas.append(
                jnp.sum(grad_t[rows] * out_t_ref[rows, lanes(index)], axis=0, keepdims=True)
            )
            tops.append(lse_ref[head : head + 1, lanes(index)])
        grad_t_low = grad_t.astype(BF16)
        dq_ref[...] = jnp.zeros_like(dq_ref)

        def chunk(step, carry, masked):
            here = lanes(step)
            if masked:
                allowed = ids_all_ref[:, here].T[:, 0:1] <= query_ids
            for head in range(heads):
                rows = slice(head * size, (head + 1) * size)
                scores = dot(key_ref[head, here, :], query_t[rows]) - tops[head]
                if masked:
                    scores = jnp.where(allowed, scores, NEGATIVE)
                probs = jnp.exp(scores)
                grad_probs = dot(value_ref[head, here, :], grad_t_low[rows])
                grad_scores = (probs * (grad_probs - deltas[head])).astype(BF16)
                dv_ref[head, here, :] += dot(probs.astype(BF16), own_grad_ref[head])
                dk_ref[head, here, :] += dot(grad_scores, query_ref[head])
                dq_ref[rows, :] += dot(key_t_ref[rows, here], grad_scores)
            return carry

        stop = jnp.minimum(tile + 2, tiles)
        lax.fori_loop(0, tile, lambda s, c: chunk(s, c, False), 0)
        lax.fori_loop(tile, stop, lambda s, c: chunk(s, c, True), 0)
        grad_query = turn(
            dq_ref[...] * scale, cos_ref[:, at], sin_ref[:, at], heads, size, back=True
        )
        grad_w_ref[:width, :] += dot(grad_query.astype(BF16), a_ref[at, :])
        da_ref[at, :] = dot(grad_query.T.astype(BF16), wt_ref[:width, :]).astype(BF16)
        return carry

    lax.fori_loop(0, own_tiles, attend, 0)

    def finish(step, carry):
        at = lanes(step)
        key_grad = jnp.concatenate([dk_ref[head, at, :].T for head in range(heads)], axis=0)
        key_grad = turn(key_grad, cos_ref[:, at], sin_ref[:, at], heads, size, back=True)
        value_grad = jnp.concatenate([dv_ref[head, at, :].T for head in range(heads)], axis=0)
        both = jnp.concatenate([key_grad, value_grad], axis=0)
        grad_w_ref[width:, :] += dot(both.astype(BF16), a_ref[at, :])
        total = da_ref[at, :].astype(F32) + dot(both.T.astype(BF16), wt_ref[width:, :])
        da_ref[at, :] = total.astype(BF16)
        return carry

    lax.fori_loop(0, tiles, finish, 0)
    for piece in range(pieces_ref.shape[0]):
        pieces_ref[piece] = grad_w_ref[:, piece * shard : (piece + 1) * shard].astype(BF16)
    for copy in copies:
        copy.wait()
    for far in range(1, owners):
        share_copy(far).wait()
    shares_ref[row] = share_ref[...]
    total = shares_ref[0].astype(F32)
    for giver in range(1, owners):
        total = total + shares_ref[giver].astype(F32)
    output_sum_ref[...] = total

    def settle(step, carry):
        wait_sent(*outgoing(step))
        return carry

    lax.fori_loop(0, owned, settle, 0)


def attn_backward(
    grad_own, a_full, weights_t, cos_t, sin_t, ids, kept,
    grad_wide, outs, grad_output, heads, size, ranks, context, roles, number,
):
    length, model = a_full.shape
    width = heads * size
    owners = outs.shape[0]
    shard = model // context
    shapes = (
        jax.ShapeDtypeStruct(a_full.shape, BF16),
        jax.ShapeDtypeStruct((context, weights_t.shape[0], shard), BF16),
        jax.ShapeDtypeStruct((shard, model), F32),
        jax.ShapeDtypeStruct((context, 2, shard, grad_wide.shape[2]), BF16),
        jax.ShapeDtypeStruct(outs.shape, BF16),
    )
    dims = (heads, size, ranks, size ** (-0.5), context, owners, roles)
    return pl.pallas_call(
        functools.partial(attn_backward_kernel, dims),
        out_shape=shapes,
        in_specs=vmem(12) + hbm(3),
        out_specs=vmem(3) + hbm(2),
        scratch_shapes=[
            pltpu.VMEM((heads, TILE, size), BF16),
            pltpu.VMEM((heads, TILE, size), BF16),
            pltpu.VMEM((width, TILE), F32),
            pltpu.VMEM((heads, length, size), F32),
            pltpu.VMEM((heads, length, size), F32),
            pltpu.VMEM(weights_t.shape, F32),
            pltpu.VMEM(grad_own.shape, BF16),
            pltpu.VMEM((context, shard, model), BF16),
            pltpu.VMEM((shard, model), BF16),
            pltpu.VMEM((owners, shard, model), BF16),
        ]
        + [pltpu.SemaphoreType.DMA((grad_own.shape[0],))] * 2
        + [pltpu.SemaphoreType.DMA((owners,))] * 2
        + [pltpu.SemaphoreType.DMA((context,))] * 4
        + [pltpu.SemaphoreType.DMA((owners,))] * 2
        + [pltpu.SemaphoreType.DMA((3,))],
        compiler_params=params(number, 63),
        cost_estimate=cost(60),
        name="attn_backward",
    )(
        grad_own, a_full, weights_t, cos_t, sin_t, ids, *kept,
        grad_wide, outs, grad_output,
    )


def moe_kernel(
    context, owners, roles, square,
    gates_ref, rows_ref, grads_hbm, wide_hbm, down_hbm,
    dots_back, grad_back, out_back, grad_wide_out, down_in,
    gates_all, rows_all, rows_stage, grads_ref, wide_ref, down_ref,
    rows_t_ref, dye_ref, out_acc, grad_acc, grad_wide_ref, grad_down_ref,
    dots_ref, grad_low, out_low, dots_twin, grad_twin, out_twin,
    dots_sum, grad_sum, out_sum, dots_relay, grad_relay,
    load_sem, local_sem, send_sem, recv_sem, pass_sem, land_sem, twin_sem, come_sem,
    relay_sem, reach_sem, down_send, down_recv, down_on, back_send, back_recv,
    pair_send, pair_recv, home_send, home_recv, lend_send, lend_recv, on_send, on_recv,
    out_send, out_recv, loan_send, loan_recv,
):
    chips = context // 2
    cap, width = rows_all.shape[1:]
    flat = dye_ref.shape
    loads = [
        pltpu.make_async_copy(source, target, load_sem.at[index])
        for index, (source, target) in enumerate(((grads_hbm, grads_ref), (wide_hbm, wide_ref)))
    ]
    for copy in loads:
        copy.start()
    place, row = meet(context, owners)
    chip, core = place // 2, lax.rem(place, 2)
    partner = {"context": place + 1 - 2 * core}
    slot = chip // (chips // roles)
    other = (roles - 1) - slot
    twin = {"context": 2 * lax.rem(chip + chips // 2, chips) + core}

    def block(spot, side, peer):
        return (spot * 2 + side) * owners + peer

    sent, local, passed, lent, relayed = {}, [], [], {}, []
    for far in range(1, owners):
        peer = lax.rem(row + far, owners)
        pairs = [
            (gates_ref.at[peer], gates_all.at[block(slot, core, row)]),
            (rows_ref.at[peer, slot], rows_all.at[block(slot, core, row)]),
        ]
        if roles > 1:
            pairs.append((rows_ref.at[peer, other], rows_stage.at[row]))
        for item, (source, target) in enumerate(pairs):
            sent[item, far] = remote(
                source, target, send_sem.at[item, far], recv_sem.at[item, far], {"expert": peer}
            )
            sent[item, far].start()
    mine = block(slot, core, row)
    for item, (source, target) in enumerate(
        ((gates_ref.at[row], gates_all.at[mine]), (rows_ref.at[row, slot], rows_all.at[mine]))
    ):
        local.append(pltpu.make_async_copy(source, target, local_sem.at[item]))
        local[-1].start()
        passed.append(
            remote(source, target, pass_sem.at[item, 0], land_sem.at[item, 0], partner)
        )
        passed[-1].start()
    if roles > 1:
        for item, (source, everything) in enumerate(
            ((gates_ref.at[row], gates_all), (rows_ref.at[row, other], rows_all))
        ):
            lent[item, 0] = (
                remote(
                    source, everything.at[mine], twin_sem.at[item, 0], come_sem.at[item, 0], twin
                ),
                everything.at[block(other, core, row)],
            )
            lent[item, 0][0].start()

    half = place // chips
    down_rows = down_hbm.shape[1]
    mark = lax.rem(place, chips)
    spot_down = down_ref.at[span(mark, down_rows), :]

    def down_copy(far, here):
        to_chip = chip_at(chip, far, chips, square)
        source = down_hbm.at[to_chip // (chips // roles)]
        if here:
            return pltpu.make_async_copy(source, spot_down, down_recv.at[mark])
        return remote(
            source, spot_down, down_send.at[far], down_recv.at[mark],
            {"context": 2 * to_chip + half},
        )

    @pl.when(half == core)
    def _():
        down_copy(0, True).start()

    @pl.when(half != core)
    def _():
        down_copy(0, False).start()

    fars = [1, 2] if square else list(range(1, chips))
    for far in fars:
        down_copy(far, False).start()

    def arrival(number):
        wait_landed(
            core * chips + number, down_hbm.at[0], down_ref.at[span(number, down_rows), :],
            down_send.at[0], down_recv.at[number],
        )

    def onward(number):
        land = down_ref.at[span(number, down_rows), :]
        return remote(
            land, land, down_on.at[number], down_recv.at[number],
            {"context": 2 * chip_at(chip, 1, chips, square) + core},
        )

    def from_below(number):
        return (core * chips + number) // 2 == chip_at(chip, 2, chips, square)

    for far in range(1, owners):
        peer = lax.rem(row + owners - far, owners)
        for item, everything in enumerate((gates_all, rows_all)):
            sent[item, far].wait_recv()
            landed = everything.at[block(slot, core, peer)]
            passed.append(
                remote(landed, landed, pass_sem.at[item, far], land_sem.at[item, far], partner)
            )
            passed[-1].start()
            if roles > 1:
                if item == 1:
                    sent[2, far].wait_recv()
                lent[item, far] = (
                    remote(
                        landed if item == 0 else rows_stage.at[peer], landed,
                        twin_sem.at[item, far], come_sem.at[item, far], twin,
                    ),
                    everything.at[block(other, core, peer)],
                )
                lent[item, far][0].start()
        if square and far == 1:
            for number in range(chips):

                @pl.when(from_below(number))
                def _():
                    arrival(number)
                    onward(number).start()

    for (item, far), (copy, arriving) in lent.items():
        copy.wait_recv()
        relayed.append(
            remote(
                arriving, arriving, relay_sem.at[item, far], reach_sem.at[item, far], partner
            )
        )
        relayed[-1].start()
    for number in range(chips):
        if square:

            @pl.when(from_below(number))
            def _():
                onward(number).wait_send()

            @pl.when(jnp.logical_not(from_below(number)))
            def _():
                arrival(number)

        else:
            arrival(number)
    for copy in loads + local:
        copy.wait()
    for copy in passed + relayed:
        copy.wait()

    blocks = roles * 2 * owners
    rows_t_ref[...] = rows_all[...].reshape(flat).astype(F32).T.astype(BF16)
    for number in range(blocks):
        columns = gates_all[number].T[:cap]
        column = columns[:, 0:1]
        if roles > 1:
            column = jnp.where(slot == 0, column, columns[:, 1:2])
        dye_ref[number * cap : (number + 1) * cap, :] = (
            grads_ref[number].astype(F32) * column
        ).astype(BF16)
    out_acc[...] = jnp.zeros_like(out_acc)
    grad_acc[...] = jnp.zeros_like(grad_acc)
    back_rows = down_in.shape[1]
    per_step = HIDDEN_TILE // back_rows
    tiles = wide_ref.shape[2] // HIDDEN_TILE

    def leaving(index):
        return (
            core * chips + index, grad_down_ref.at[index], down_in.at[chip],
            back_send.at[index], back_recv.at[chip],
        )

    def hidden_tile(step, carry):
        tile = lax.rem(step + (1 - lax.rem(chip, 2)) * (tiles // 2), tiles)
        at = span(tile, HIDDEN_TILE)
        rows = rows_all[...].reshape(flat)
        dye = dye_ref[...]
        gate, up, down = wide_ref[0, :, at], wide_ref[1, :, at], down_ref[at, :]
        gate_pre = dot(rows, gate)
        up_pre = dot(rows, up)
        sigmoid = jax.nn.sigmoid(gate_pre)
        silu = gate_pre * sigmoid
        hidden = silu * up_pre
        grad_down = dot(hidden.T.astype(BF16), dye).astype(BF16)
        for index in range(per_step):
            grad_down_ref[tile * per_step + index] = grad_down[
                index * back_rows : (index + 1) * back_rows
            ]
        grad_hidden = dot(dye, down, 1, 1).astype(BF16).astype(F32)
        for index in range(per_step):
            here_or_away(*leaving(tile * per_step + index))
        out_acc[...] += dot(hidden.astype(BF16), down).reshape(out_acc.shape)
        grad_gate = (
            grad_hidden * up_pre * sigmoid * (1.0 + gate_pre * (1.0 - sigmoid))
        ).astype(BF16)
        grad_up = (grad_hidden * silu).astype(BF16)
        grad_wide_ref[0, :, at] = dot(rows_t_ref[...], grad_gate).astype(BF16)
        grad_wide_ref[1, :, at] = dot(rows_t_ref[...], grad_up).astype(BF16)
        total = dot(grad_gate, gate, 1, 1) + dot(grad_up, up, 1, 1)
        grad_acc[...] += total.reshape(grad_acc.shape)
        return carry

    lax.fori_loop(0, tiles, hidden_tile, 0)
    store = pltpu.make_async_copy(grad_wide_ref, grad_wide_out, load_sem.at[2])
    store.start()

    order = list(range(1, owners)) + [0]
    turns = (other, slot) if roles > 1 else (slot,)
    pair, gone, loaned, handed, outs, loans = {}, {}, {}, {}, [], []
    items = (
        (dots_ref, dots_twin, dots_sum, dots_relay, dots_back),
        (grad_low, grad_twin, grad_sum, grad_relay, grad_back),
    )

    def share(which, far):
        spot, peer = turns[which], lax.rem(row + far, owners)
        sources = (dots_ref.at[block(spot, 1 - core, peer)], grad_low.at[spot, peer])
        for item, source in enumerate(sources):
            pair[item, which, far] = remote(
                source, items[item][1].at[spot, peer],
                pair_send.at[item, which, far], pair_recv.at[item, which, far], partner,
            )
            pair[item, which, far].start()

    def line(number):
        product = out_acc[number] * grads_ref[number].astype(F32)
        total = product[:, :128]
        for start in range(128, width, 128):
            total = total + product[:, start : start + 128]
        totals = jnp.sum(total.T, axis=0, keepdims=True)
        dots_ref[number, :, :cap] = jnp.broadcast_to(totals, (8, cap))

    last = None
    for far in order:
        peer = lax.rem(row + far, owners)
        for which, spot in enumerate(turns):
            number = block(spot, 1 - core, peer)
            grad_low[spot, peer] = grad_acc[number].astype(BF16)
            line(number)
            if last is not None:
                share(*last)
            last = (which, far)
    for far in order:
        peer = lax.rem(row + far, owners)
        for spot in turns:
            out_low[spot, peer] = out_acc[block(spot, 1 - core, peer)].astype(BF16)
            line(block(spot, core, peer))
        if far == order[0]:
            share(*last)
    for which, spot in enumerate(turns):
        outs.append(
            remote(
                out_low.at[spot], out_twin.at[spot], out_send.at[which], out_recv.at[which],
                partner,
            )
        )

    def leave(which, far):
        peer = lax.rem(row + far, owners)
        spot = turns[which]
        for item, (_, _, total, relay, back) in enumerate(items):
            if roles > 1 and which == 0:
                target = back.at[row, slot] if far == 0 else relay.at[peer]
                loaned[item, far] = remote(
                    total.at[spot, peer], target, lend_send.at[item, far],
                    lend_recv.at[item, far], twin,
                )
                loaned[item, far].start()
            elif far > 0:
                gone[item, far] = remote(
                    total.at[spot, peer], back.at[row, slot], home_send.at[item, far],
                    home_recv.at[item, far], {"expert": peer},
                )
                gone[item, far].start()

    last = None
    for far in order:
        peer = lax.rem(row + far, owners)
        for which, spot in enumerate(turns):
            number = block(spot, core, peer)
            for item in range(2):
                pair[item, which, far].wait_recv()
            dots_sum[spot, peer] = dots_ref[number] + dots_twin[spot, peer]
            grad_sum[spot, peer] = (
                grad_acc[number] + grad_twin[spot, peer].astype(F32)
            ).astype(BF16)
            if last is not None:
                leave(*last)
            else:
                for copy in outs:
                    copy.start()
            last = (which, far)
    dots_back[row, slot] = dots_sum[slot, row]
    grad_back[row, slot] = grad_sum[slot, row]
    leave(*last)
    if roles > 1:
        for far in range(1, owners):
            peer = lax.rem(row + far, owners)
            for item, (_, _, _, relay, back) in enumerate(items):
                loaned[item, far].wait_recv()
                handed[item, far] = remote(
                    relay.at[peer], back.at[row, other], on_send.at[item, far],
                    on_recv.at[item, far], {"expert": peer},
                )
                handed[item, far].start()
    for which, spot in enumerate(turns):
        outs[which].wait_recv()
        for peer in range(owners):
            summed = out_acc[block(spot, core, peer)] + out_twin[spot, peer].astype(F32)
            if roles > 1 and which == 0:
                out_sum[peer] = summed.astype(BF16)
            else:
                out_back[peer, slot] = summed.astype(BF16)
    if roles > 1:
        loans.append(remote(out_sum, out_back.at[:, slot], loan_send, loan_recv, twin))
        loans[-1].start()
        for item in range(2):
            loaned[item, 0].wait_recv()
    for copy in sent.values():
        copy.wait_send()
    for copy, _ in lent.values():
        copy.wait_send()
    for far in fars:
        down_copy(far, False).wait_send()

    @pl.when(half != core)
    def _():
        down_copy(0, False).wait_send()

    for index in range(chips):
        wait_sent(*leaving(index))
        wait_landed(
            2 * index + place // chips, grad_down_ref.at[0], down_in.at[index],
            back_send.at[index], back_recv.at[index],
        )
    for copy in list(pair.values()) + outs + list(loaned.values()):
        copy.wait_send()
    for copy in list(gone.values()) + list(handed.values()) + loans + [store]:
        copy.wait()


def moe(gates, rows, grads, wide_full, down_weight, context, roles, number):
    owners, _, cap, width = rows.shape
    chips = context // 2
    hidden = wide_full.shape[2]
    blocks = roles * 2 * owners
    slots = blocks * cap
    line = gates.shape[1:]
    square = chips == 4 and roles == 2
    low = (owners, cap, width)
    back = (chips, hidden // chips, width)
    dma = pltpu.SemaphoreType.DMA
    return pl.pallas_call(
        functools.partial(moe_kernel, context, owners, roles, square),
        out_shape=(
            jax.ShapeDtypeStruct((owners, roles) + line, F32),
            jax.ShapeDtypeStruct((owners, roles, cap, width), BF16),
            jax.ShapeDtypeStruct((owners, roles, cap, width), BF16),
            jax.ShapeDtypeStruct(wide_full.shape, BF16),
            jax.ShapeDtypeStruct(back, BF16),
        ),
        in_specs=vmem(2) + hbm(3),
        out_specs=vmem(3) + hbm(2),
        scratch_shapes=[
            pltpu.VMEM((blocks,) + line, F32),
            pltpu.VMEM((blocks, cap, width), BF16),
            pltpu.VMEM(low, BF16),
            pltpu.VMEM((blocks, cap, width), BF16),
            pltpu.VMEM(wide_full.shape, BF16),
            pltpu.VMEM((hidden, width), BF16),
            pltpu.VMEM((width, slots), BF16),
            pltpu.VMEM((slots, width), BF16),
            pltpu.VMEM((blocks, cap, width), F32),
            pltpu.VMEM((blocks, cap, width), F32),
            pltpu.VMEM(wide_full.shape, BF16),
            pltpu.VMEM(back, BF16),
            pltpu.VMEM((blocks,) + line, F32),
            pltpu.VMEM((roles,) + low, BF16),
            pltpu.VMEM((roles,) + low, BF16),
            pltpu.VMEM((roles, owners) + line, F32),
            pltpu.VMEM((roles,) + low, BF16),
            pltpu.VMEM((roles,) + low, BF16),
            pltpu.VMEM((roles, owners) + line, F32),
            pltpu.VMEM((roles,) + low, BF16),
            pltpu.VMEM(low, BF16),
            pltpu.VMEM((owners,) + line, F32),
            pltpu.VMEM(low, BF16),
            dma((3,)),
            dma((2,)),
        ]
        + [dma((3, owners))] * 8
        + [dma((chips,))] * 5
        + [dma((2, roles, owners))] * 2
        + [dma((2, owners))] * 6
        + [dma((roles,))] * 2
        + [dma] * 2,
        compiler_params=params(number, 62),
        cost_estimate=cost(97),
        name="moe",
    )(gates, rows, grads.reshape(blocks, cap, width), wide_full, down_weight)


def finish_kernel(
    chips, owners, groups,
    da_ref, pieces_ref, small_ref,
    total_ref, sums_ref, small_all_ref,
    da_twin, da_sum, da_in, w_twin, w_sum, w_in, s_twin, s_sum, s_in, s_total,
    stack_ref, shares, shares_in, block_ref,
    pair_send, pair_recv, chip_send, chip_recv, row_send, row_recv,
):
    place = lax.axis_index("context")
    row = lax.axis_index("expert")
    chip, core = place // 2, lax.rem(place, 2)
    partner = 2 * chip + 1 - core
    barrier = pltpu.get_barrier_semaphore()

    def greet(device):
        pl.semaphore_signal(
            barrier, inc=1, device_id=device, device_id_type=pl.DeviceIdType.MESH
        )

    greet({"context": partner})
    for far in range(1, chips):
        greet({"context": 2 * lax.rem(chip + far, chips) + core})
    for far in range(1, owners):
        greet({"expert": lax.rem(row + far, owners)})
    pl.semaphore_wait(barrier, chips + owners - 1)

    order = list(range(1, chips)) + [0]
    pair = {}
    for item, (source, target) in enumerate(
        ((small_ref, s_twin), (pieces_ref, w_twin), (da_ref, da_twin))
    ):
        for far in order:
            peer = lax.rem(chip + far, chips)
            pair[item, far] = remote(
                source.at[2 * peer + 1 - core], target.at[peer],
                pair_send.at[item, far], pair_recv.at[item, far], {"context": partner},
            )
            pair[item, far].start()

    def across(item, source, target, far):
        peer = lax.rem(chip + far, chips)
        return remote(
            source.at[peer], target.at[chip], chip_send.at[item, far], chip_recv.at[item, far],
            {"context": 2 * peer + core},
        )

    for far in order:
        peer = lax.rem(chip + far, chips)
        mine = 2 * peer + core
        pair[0, far].wait_recv()
        s_sum[peer] = small_ref[mine] + s_twin[peer]
        pair[1, far].wait_recv()
        w_sum[peer] = (
            pieces_ref[mine].astype(F32) + w_twin[peer].astype(F32)
        ).astype(BF16)
    moved = {}
    for far in range(1, chips):
        moved[0, far] = across(0, s_sum, s_in, far)
        moved[0, far].start()
        moved[1, far] = across(1, w_sum, w_in, far)
        moved[1, far].start()
    last = None
    for far in order:
        peer = lax.rem(chip + far, chips)
        pair[2, far].wait_recv()
        da_sum[peer] = (
            da_ref[2 * peer + core].astype(F32) + da_twin[peer].astype(F32)
        ).astype(BF16)
        if last is not None:
            moved[2, last] = across(2, da_sum, da_in, last)
            moved[2, last].start()
        last = far
    for far in range(1, chips):
        moved[0, far].wait_recv()
        moved[1, far].wait_recv()
    s_in[chip] = s_sum[chip]
    w_in[chip] = w_sum[chip]

    width = w_sum.shape[1] // 3
    shard = w_sum.shape[2]
    per_group = chips // groups
    for group in range(groups):
        total = w_in[group * per_group].astype(F32)
        for other in range(1, per_group):
            total = total + w_in[group * per_group + other].astype(F32)
        for which in range(3):
            stack_ref[which * shard : (which + 1) * shard, group * width : (group + 1) * width] = (
                total[which * width : (which + 1) * width].T
            )
    lines = shares.shape[1]
    for owner in range(owners):
        shares[owner] = stack_ref[owner * lines : (owner + 1) * lines, :].astype(BF16)
    total = s_in[0]
    for other in range(1, chips):
        total = total + s_in[other]
    s_total[...] = total
    rows = {}
    for far in range(1, owners):
        peer = lax.rem(row + far, owners)
        rows[0, far] = remote(
            shares.at[peer], shares_in.at[row], row_send.at[0, far], row_recv.at[0, far],
            {"expert": peer},
        )
        rows[0, far].start()
        rows[1, far] = remote(
            s_total, small_all_ref.at[row], row_send.at[1, far], row_recv.at[1, far],
            {"expert": peer},
        )
        rows[1, far].start()
    shares_in[row] = shares[row]
    small_all_ref[row] = total
    for far in range(1, owners):
        rows[0, far].wait_recv()
    summed = shares_in[0].astype(F32)
    for other in range(1, owners):
        summed = summed + shares_in[other].astype(F32)
    block_ref[...] = summed.astype(BF16)
    for far in range(1, chips):
        moved[2, far].wait_recv()
    for far in range(1, owners):
        peer = lax.rem(row + far, owners)
        rows[2, far] = remote(
            block_ref, sums_ref.at[row], row_send.at[2, far], row_recv.at[2, far],
            {"expert": peer},
        )
        rows[2, far].start()
    sums_ref[row] = summed.astype(BF16)
    da_in[chip] = da_sum[chip]
    total = da_in[0].astype(F32)
    for other in range(1, chips):
        total = total + da_in[other].astype(F32)
    total_ref[...] = total
    for far in range(1, owners):
        rows[1, far].wait_recv()
        rows[2, far].wait_recv()
    for copy in list(pair.values()) + list(moved.values()) + list(rows.values()):
        copy.wait_send()


def finish(da, pieces, small, owners, groups, number):
    context, tokens, width = da.shape
    chips = context // 2
    lines, shard = pieces.shape[1:]
    few = small.shape[1]
    stack = 3 * shard
    block = (stack // owners, width)
    return pl.pallas_call(
        functools.partial(finish_kernel, chips, owners, groups),
        out_shape=(
            jax.ShapeDtypeStruct((tokens, width), F32),
            jax.ShapeDtypeStruct((owners,) + block, BF16),
            jax.ShapeDtypeStruct((owners, few, shard), F32),
        ),
        in_specs=vmem(3),
        out_specs=vmem(3),
        scratch_shapes=[
            pltpu.VMEM((chips, tokens, width), BF16),
            pltpu.VMEM((chips, tokens, width), BF16),
            pltpu.VMEM((chips, tokens, width), BF16),
            pltpu.VMEM((chips, lines, shard), BF16),
            pltpu.VMEM((chips, lines, shard), BF16),
            pltpu.VMEM((chips, lines, shard), BF16),
            pltpu.VMEM((chips, few, shard), F32),
            pltpu.VMEM((chips, few, shard), F32),
            pltpu.VMEM((chips, few, shard), F32),
            pltpu.VMEM((few, shard), F32),
            pltpu.VMEM((stack, width), F32),
            pltpu.VMEM((owners,) + block, BF16),
            pltpu.VMEM((owners,) + block, BF16),
            pltpu.VMEM(block, BF16),
            pltpu.SemaphoreType.DMA((3, chips)),
            pltpu.SemaphoreType.DMA((3, chips)),
            pltpu.SemaphoreType.DMA((3, chips)),
            pltpu.SemaphoreType.DMA((3, chips)),
            pltpu.SemaphoreType.DMA((3, owners)),
            pltpu.SemaphoreType.DMA((3, owners)),
        ],
        compiler_params=pltpu.CompilerParams(
            collective_id=number, has_side_effects=True, vmem_limit_bytes=60 << 20
        ),
        name="finish",
    )(da, pieces, small)


def shards(
    hidden_in,
    prior_logits,
    routes,
    block_ids,
    grad_out,
    attn_gain,
    query_weight,
    key_weight,
    value_weight,
    output_weight,
    moe_gain,
    router_weight,
    prior_weight,
    const_mix,
    const_vector,
    gate_weight,
    up_weight,
    down_weight,
):
    token_rows = hidden_in.shape[1]
    model_width = hidden_in.shape[2]
    head_size = model_width // HEADS
    context = lax.axis_size("context")
    owners = lax.axis_size("expert")
    groups = math.gcd(HEADS, context)
    ranks = context // groups
    heads = HEADS // groups
    width = heads * head_size
    length = context * token_rows
    per_owner = gate_weight.shape[0]
    slot_count = per_owner * owners * CAP
    shard_width = model_width // context
    roles = per_owner
    residual = hidden_in[0].astype(F32)
    prior_rows = prior_logits[0]
    route_rows = routes[0]
    cotangent_low = grad_out[0]
    cotangent = cotangent_low.astype(F32)

    inv_rms1 = lax.rsqrt(jnp.mean(residual * residual, axis=1, keepdims=True) + EPS)
    normed_one = residual * inv_rms1
    attn_input = (normed_one * attn_gain).astype(BF16)
    ids_wide = jnp.broadcast_to(block_ids.astype(F32), (8, token_rows))
    stacked = jnp.stack([query_weight, key_weight, value_weight])
    stacked = stacked.reshape(3, shard_width, groups, width)
    pieces = jnp.transpose(stacked, (2, 0, 3, 1)).reshape(groups, 3 * width, shard_width)
    half = head_size // 2
    freq = jnp.power(THETA, -2.0 * jnp.arange(half, dtype=F32) / head_size)
    angle = freq[:, None] * jnp.arange(length, dtype=jnp.int32).astype(F32)[None, :]
    cos_t, sin_t = jnp.cos(angle), jnp.sin(angle)

    flat_route = route_rows.reshape(-1)
    ffn_hot = (flat_route[:, None] == jnp.arange(FFN_E, dtype=jnp.int32)[None, :]).astype(jnp.int32)
    before = jnp.sum((jnp.cumsum(ffn_hot, axis=0) - ffn_hot) * ffn_hot, axis=1)
    slot_index = jnp.where(
        flat_route < FFN_E,
        flat_route * CAP + before,
        -1,
    ).reshape(token_rows, 2)
    slot_ids = jnp.arange(slot_count, dtype=jnp.int32)[:, None]
    hit_first = slot_ids == slot_index[None, :, 0]
    hit_second = slot_ids == slot_index[None, :, 1]
    pick_first = hit_first.astype(BF16)
    pick_second = hit_second.astype(BF16)
    pick_either = pick_first + pick_second

    blocks = (owners, per_owner, CAP, model_width)

    def pick(rows):
        return jnp.dot(pick_either, rows, preferred_element_type=F32).astype(BF16).reshape(blocks)

    (
        out_t, log_total, query_t, ids, weights_t, key_heads, key_t, value_heads,
        a_full, mix_granules, output_full, wide_full, grad_arrived, _,
    ) = attn_forward(
        ids_wide, pieces, attn_input, cos_t, sin_t, pick(cotangent_low),
        output_weight, gate_weight, up_weight, heads, head_size, ranks, context, roles, 0,
    )
    kept = (out_t, log_total, query_t, key_heads, key_t, value_heads)
    out_blocks = mix_granules.reshape(groups, token_rows, width)
    mix_low = jnp.transpose(out_blocks, (1, 0, 2)).reshape(token_rows, model_width)

    after_attn = residual + jnp.dot(mix_low, output_full, preferred_element_type=F32)
    inv_rms2 = lax.rsqrt(jnp.mean(after_attn * after_attn, axis=1, keepdims=True) + EPS)
    normed_two = after_attn * inv_rms2
    moe_input = normed_two * moe_gain
    narrow = jnp.concatenate(
        [router_weight, jnp.transpose(const_mix.reshape(-1, model_width))], axis=1
    )
    narrow_out = jnp.dot(moe_input, narrow, precision=HIGH, preferred_element_type=F32)
    expert_count = router_weight.shape[1]
    consts = const_mix.shape[0]
    logits = narrow_out[:, :expert_count] + jnp.dot(
        prior_rows, prior_weight, precision=HIGH, preferred_element_type=F32
    )
    probs = jax.nn.softmax(logits, axis=1)
    expert_ids = jnp.arange(expert_count, dtype=jnp.int32)
    first_hot = (route_rows[:, 0:1] == expert_ids[None, :]).astype(F32)
    second_hot = (route_rows[:, 1:2] == expert_ids[None, :]).astype(F32)
    chosen = first_hot + second_hot
    gated = probs * chosen
    first_gate = jnp.sum(probs * first_hot, axis=1, keepdims=True)
    second_gate = jnp.sum(probs * second_hot, axis=1, keepdims=True)
    slot_gate = jnp.sum(
        jnp.where(hit_first, first_gate[None, :, 0], 0.0)
        + jnp.where(hit_second, second_gate[None, :, 0], 0.0),
        axis=1,
    )
    def spread(values):
        values = values.reshape(owners, per_owner, CAP)
        return jnp.pad(values, ((0, 0), (0, 8 - per_owner), (0, 128 - CAP)))

    slot_dot, grad_back, expert_out, grad_wide, down_parts = moe(
        spread(slot_gate), pick(moe_input.astype(BF16)), grad_arrived, wide_full, down_weight,
        context, roles, 2,
    )
    slot_dot = slot_dot[:, :, 0, :CAP].reshape(slot_count)
    grad_back = grad_back.reshape(slot_count, model_width)

    const_soft = jax.nn.softmax(narrow_out[:, expert_count:].reshape(token_rows, consts, 2), axis=2)
    const_gate = gated[:, FFN_E + 2 :]
    copy_gate = gated[:, FFN_E + 1 : FFN_E + 2]
    const_out = [
        const_soft[:, c, 0:1] * moe_input + const_soft[:, c, 1:2] * const_vector[c][None, :]
        for c in range(consts)
    ]
    local_moe = copy_gate * moe_input
    for c in range(consts):
        local_moe = local_moe + const_gate[:, c : c + 1] * const_out[c]
    grad_moe_ffn = lax.dot_general(
        pick_either, grad_back, (((0,), (0,)), ((), ())), preferred_element_type=F32
    )
    first_dot = jnp.sum(jnp.where(hit_first, slot_dot[:, None], 0.0), axis=0)[:, None]
    second_dot = jnp.sum(jnp.where(hit_second, slot_dot[:, None], 0.0), axis=0)[:, None]
    copy_dot = jnp.sum(cotangent * moe_input, axis=1, keepdims=True)
    const_dot = [jnp.sum(cotangent * const_out[c], axis=1, keepdims=True) for c in range(consts)]
    extra = jnp.concatenate(
        [jnp.zeros((token_rows, FFN_E + 1), F32), copy_dot, *const_dot], axis=1
    )
    grad_probs = first_hot * first_dot + second_hot * second_dot + chosen * extra
    grad_logits = probs * (grad_probs - jnp.sum(probs * grad_probs, axis=1, keepdims=True))
    grad_prior_rows = lax.dot_general(
        grad_logits, prior_weight, (((1,), (1,)), ((), ())),
        precision=HIGH, preferred_element_type=F32,
    )
    vector_dot = jnp.dot(
        cotangent, jnp.transpose(const_vector), precision=HIGH, preferred_element_type=F32
    )
    grad_soft = jnp.stack(
        [const_gate * copy_dot, const_gate * vector_dot], axis=2
    )
    grad_mix = const_soft * (grad_soft - jnp.sum(const_soft * grad_soft, axis=2, keepdims=True))
    narrow_grad = jnp.concatenate([grad_logits, grad_mix.reshape(token_rows, -1)], axis=1)
    local_scale = copy_gate + jnp.sum(const_soft[:, :, 0] * const_gate, axis=1, keepdims=True)
    grad_moe_input = (
        grad_moe_ffn
        + lax.dot_general(
            narrow_grad, narrow, (((1,), (1,)), ((), ())),
            precision=HIGH, preferred_element_type=F32,
        )
        + local_scale * cotangent
    )
    small_moe = lax.dot_general(
        narrow_grad, moe_input, (((0,), (0,)), ((), ())),
        precision=HIGH, preferred_element_type=F32,
    )
    small_vector = lax.dot_general(
        const_soft[:, :, 1] * const_gate, cotangent, (((0,), (0,)), ((), ())),
        precision=HIGH, preferred_element_type=F32,
    )
    grad_prior_local = lax.dot_general(
        prior_rows, grad_logits, (((0,), (0,)), ((), ())),
        precision=HIGH, preferred_element_type=F32,
    )
    small_gain = jnp.sum(grad_moe_input * normed_two, axis=0, keepdims=True)
    prior_values = jnp.pad(
        grad_prior_local.reshape(-1), (0, -(expert_count * expert_count) % shard_width)
    ).reshape(-1, 1, shard_width)
    prior_lines = prior_values.shape[0]
    small = jnp.concatenate([small_moe, small_vector, small_gain], axis=0)
    small_lines = small.shape[0]
    small = jnp.concatenate(
        [
            small.reshape(small_lines, context, shard_width),
            jnp.broadcast_to(prior_values, (prior_lines, context, shard_width)),
        ],
        axis=0,
    )
    small = jnp.pad(small, ((0, -small.shape[0] % 8), (0, 0), (0, 0)))
    small = jnp.transpose(small, (1, 0, 2))

    grad_normed_two = grad_moe_input * moe_gain
    grad_after = cotangent + inv_rms2 * (
        grad_normed_two - normed_two * jnp.mean(grad_normed_two * normed_two, axis=1, keepdims=True)
    )
    grad_attn_low = grad_after.astype(BF16)
    grad_mix_low = lax.dot_general(
        grad_attn_low, output_full, (((1,), (1,)), ((), ())), preferred_element_type=F32
    ).astype(BF16)
    grad_pieces = jnp.transpose(grad_mix_low.reshape(token_rows, groups, width), (1, 0, 2))
    grad_own = grad_pieces.reshape(-1, TILE // 2, width)
    grad_output_local = lax.dot_general(
        mix_low, grad_attn_low, (((0,), (0,)), ((), ())), preferred_element_type=F32
    ).astype(BF16)
    da_part, w_pieces, output_sum, wide_parts, returned = attn_backward(
        grad_own, a_full, weights_t, cos_t, sin_t, ids, kept,
        grad_wide, expert_out, grad_output_local,
        heads, head_size, ranks, context, roles, 6,
    )
    returned = returned.reshape(slot_count, model_width)
    same = context // 2 // roles
    wide_parts = wide_parts.reshape(roles, same, 2, 2, shard_width, -1)

    def whole(which):
        total = jnp.sum(wide_parts[:, :, :, which].astype(F32), axis=1)
        return jnp.concatenate([total[:, 0], total[:, 1]], axis=-1)

    down_sum = jnp.sum(
        down_parts.reshape(roles, same, -1, model_width).astype(F32), axis=1
    )
    grad_attn_input, sums, small_all = finish(
        da_part.reshape(context, token_rows, model_width), w_pieces, small,
        owners, groups, 5,
    )
    grad_normed_one = grad_attn_input * attn_gain
    grad_input = grad_after + inv_rms1 * (
        grad_normed_one - normed_one * jnp.mean(grad_normed_one * normed_one, axis=1, keepdims=True)
    )
    w_sum = sums.astype(F32).reshape(3, shard_width, model_width)
    small_own = jnp.sum(small_all, axis=0)
    grad_attn_gain = jnp.sum(
        w_sum[0] * query_weight.astype(F32)
        + w_sum[1] * key_weight.astype(F32)
        + w_sum[2] * value_weight.astype(F32),
        axis=1,
    )
    column = lax.axis_index("context") * shard_width
    grad_attn_gain = grad_attn_gain / lax.dynamic_slice_in_dim(attn_gain, column, shard_width)
    mixes = expert_count + 2 * consts
    grad_prior_weight = small_own[small_lines : small_lines + prior_lines].reshape(-1)
    grad_prior_weight = grad_prior_weight[: expert_count * expert_count].reshape(
        expert_count, expert_count
    )
    layer_out = after_attn + local_moe
    layer_out = layer_out + first_gate * lax.dot_general(
        pick_first, returned, (((0,), (0,)), ((), ())), preferred_element_type=F32
    )
    layer_out = layer_out + second_gate * lax.dot_general(
        pick_second, returned, (((0,), (0,)), ((), ())), preferred_element_type=F32
    )
    return (
        layer_out.astype(BF16)[None],
        grad_input[None],
        grad_prior_rows[None],
        grad_attn_gain,
        w_sum[0],
        w_sum[1],
        w_sum[2],
        output_sum,
        small_own[small_lines - 1],
        jnp.transpose(small_own[:expert_count]),
        grad_prior_weight,
        small_own[expert_count:mixes].reshape(consts, 2, shard_width),
        small_own[mixes : mixes + consts],
        whole(0),
        whole(1),
        down_sum,
    )


def solution(mesh):
    return jax.shard_map(
        shards,
        mesh=mesh,
        in_specs=(
            P("expert", "context", None),
            P("expert", "context", None),
            P("expert", "context", None),
            P("expert", "context"),
            P("expert", "context", None),
            P(),
            P("context", None),
            P("context", None),
            P("context", None),
            P("context", None),
            P(),
            P(),
            P(),
            P(),
            P(),
            P("expert", "context", None),
            P("expert", "context", None),
            P("expert", "context", None),
        ),
        out_specs=(
            P("expert", "context", None),
            P("expert", "context", None),
            P("expert", "context", None),
            P("context"),
            P("context", None),
            P("context", None),
            P("context", None),
            P("context", None),
            P("context"),
            P("context", None),
            P(),
            P(None, None, "context"),
            P(None, "context"),
            P("expert", "context", None),
            P("expert", "context", None),
            P("expert", "context", None),
        ),
        check_vma=False,
    )
```

```python
import functools
import math

import jax
import jax.numpy as jnp
from jax import lax
from jax.experimental import pallas as pl
from jax.experimental.pallas import tpu as pltpu
from jax.sharding import PartitionSpec as P

HEADS = 12
FFN_E = 8
CAP = 96
TILE = 256
EXTRA = 16
HIDDEN_TILE = 256

EPS = 1e-06
THETA = 10000.0
NEGATIVE = -1e30
HIGH = lax.Precision.HIGHEST
F32 = jnp.float32
BF16 = jnp.bfloat16


def dot(left, right, left_dim=1, right_dim=0):
    return lax.dot_general(
        left, right, (((left_dim,), (right_dim,)), ((), ())), preferred_element_type=F32
    )


def turn(rows, cos_rows, sin_rows, heads, size, back=False):
    half = size // 2
    parts = []
    for head in range(heads):
        first = rows[head * size : head * size + half]
        second = rows[head * size + half : (head + 1) * size]
        if back:
            parts.append(first * cos_rows + second * sin_rows)
            parts.append(second * cos_rows - first * sin_rows)
        else:
            parts.append(first * cos_rows - second * sin_rows)
            parts.append(second * cos_rows + first * sin_rows)
    return jnp.concatenate(parts, axis=0)


def own_tile(index, ranks):
    rank = lax.rem(lax.axis_index("context"), ranks)
    place = lax.rem(index, 2)
    return (index // 2) * (2 * ranks) + jnp.where(place == 0, rank, 2 * ranks - 1 - rank)


def granule_of(slot, ranks):
    return own_tile(slot // 2, ranks) * 2 + lax.rem(slot, 2)


def owner_rank(granule, ranks):
    spot = lax.rem(granule // 2, 2 * ranks)
    return jnp.minimum(spot, 2 * ranks - 1 - spot)


def owner_slot(granule, ranks):
    tile = granule // 2
    upper = jnp.where(lax.rem(tile, 2 * ranks) >= ranks, 1, 0)
    return (tile // (2 * ranks) * 2 + upper) * 2 + lax.rem(granule, 2)


def here_or_away(device, source, target, send, recv):
    place = lax.axis_index("context")

    @pl.when(device == place)
    def _():
        pltpu.make_async_copy(source, target, recv).start()

    @pl.when(device != place)
    def _():
        remote(source, target, send, recv, {"context": device}).start()


def wait_sent(device, source, target, send, recv):
    @pl.when(device != lax.axis_index("context"))
    def _():
        remote(source, target, send, recv, {"context": device}).wait_send()


def wait_landed(device, source, target, send, recv):
    place = lax.axis_index("context")

    @pl.when(device == place)
    def _():
        pltpu.make_async_copy(source, target, recv).wait()

    @pl.when(device != place)
    def _():
        remote(source, target, send, recv, {"context": device}).wait_recv()


def lanes(start):
    return span(start, TILE)


def span(start, size):
    return pl.ds(pl.multiple_of(start * size, size), size)


def cost(micros):
    return pl.CostEstimate(flops=micros * 1_150_000_000, bytes_accessed=0, transcendentals=0)


def vmem(count):
    return [pl.BlockSpec(memory_space=pltpu.VMEM)] * count


def hbm(count):
    return [pl.BlockSpec(memory_space=pl.ANY)] * count


def params(number=None, limit=60):
    if number is None:
        return pltpu.CompilerParams(vmem_limit_bytes=limit << 20)
    return pltpu.CompilerParams(
        collective_id=number, has_side_effects=True, vmem_limit_bytes=limit << 20
    )


def remote(source, target, send, recv, device):
    return pltpu.make_async_remote_copy(
        src_ref=source, dst_ref=target, send_sem=send, recv_sem=recv,
        device_id=device, device_id_type=pl.DeviceIdType.MESH,
    )


def chip_at(chip, far, chips, square, back=False):
    if square:
        x, y = lax.rem(chip, 2), chip // 2
        x = x + (far % 2) * (1 - 2 * x)
        y = y + (far // 2) * (1 - 2 * y)
        return 2 * y + x
    return lax.rem(chip + (chips - far if back else far), chips)


def meet(context, owners):
    place, row = lax.axis_index("context"), lax.axis_index("expert")
    barrier = pltpu.get_barrier_semaphore()
    for far in range(1, context):
        pl.semaphore_signal(
            barrier, inc=1, device_id={"context": lax.rem(place + far, context)},
            device_id_type=pl.DeviceIdType.MESH,
        )
    for far in range(1, owners):
        pl.semaphore_signal(
            barrier, inc=1, device_id={"expert": lax.rem(row + far, owners)},
            device_id_type=pl.DeviceIdType.MESH,
        )
    pl.semaphore_wait(barrier, context + owners - 2)
    return place, row


def attn_forward_kernel(
    dims,
    hidden_ref, gain_ref, own_ids_ref, routes_ref, cotangent_ref, cos_base_ref, sin_base_ref,
    query_w_ref, key_w_ref, value_w_ref, output_ref, gate_ref, up_ref,
    out_t_ref, lse_ref, query_t_ref, ids_all_ref, wt_ref, cos_ref, sin_ref, slots_ref,
    key_out, key_t_out, value_out, a_out, mix_ref,
    output_all_ref, wide_ref, grads_all_ref, stage_ref,
    w_all_ref, value_t_ref, scores_ref, acc_ref, key_ref, key_t_ref, value_ref, a_ref, out_ref,
    ids_ref, pieces_ref, input_ref, grads_ref, keep_sem, granule_send, granule_recv,
    local_sem, send_sem, recv_sem, pass_sem, land_sem, half_send, half_recv,
    row_send, row_recv, hop_send, hop_recv, lend_send, lend_recv, wide_send, wide_recv,
):
    heads, size, ranks, scale, context, owners, roles, square = dims
    length = a_ref.shape[0]
    rows = length // context
    shard = output_ref.shape[0]
    half = wide_ref.shape[2]
    width = heads * size
    tiles = length // TILE
    own_tiles = tiles // ranks
    ext = size + EXTRA
    chips = context // 2
    chunk = 128

    def normalize(step, carry):
        at = span(step, chunk)
        values = hidden_ref[at, :].astype(F32)
        inverse = lax.rsqrt(jnp.mean(values * values, axis=1, keepdims=True) + EPS)
        input_ref[at, :] = (values * inverse * gain_ref[...]).astype(BF16)
        return carry

    lax.fori_loop(0, rows // chunk, normalize, 0)
    ids_ref[...] = jnp.broadcast_to(own_ids_ref[...].astype(F32), ids_ref.shape)
    for which, weight in enumerate((query_w_ref, key_w_ref, value_w_ref)):
        for group in range(context // ranks):
            columns = weight[:, group * width : (group + 1) * width].astype(F32)
            pieces_ref[group, which * width : (which + 1) * width, :] = columns.T.astype(BF16)
    place, row = meet(context, owners)
    chip, core = place // 2, lax.rem(place, 2)
    partner = place + 1 - 2 * core
    slot = chip // (chips // roles)
    other = (roles - 1) - slot
    twin = 2 * lax.rem(chip + chips // 2, chips) + core

    def source(item, device):
        return (ids_ref, pieces_ref.at[device // ranks], input_ref, output_ref)[item]

    def target(item, device):
        return (
            ids_all_ref.at[:, span(device, rows)],
            w_all_ref.at[device],
            a_ref.at[span(device, rows), :],
            output_all_ref.at[span(device, shard), :],
        )[item]

    def from_chip(far):
        return 2 * chip_at(chip, far, chips, square, True) + core

    def sends(item, far):
        if isinstance(far, int) and far == 0:
            peer = partner
        else:
            peer = 2 * chip_at(chip, far, chips, square) + core
        return remote(
            source(item, peer), target(item, place), send_sem.at[item, far],
            recv_sem.at[item, far], {"context": peer},
        )

    def passes(item, far):
        block = target(item, from_chip(far))
        return remote(
            block, block, pass_sem.at[item, far], land_sem.at[item, far], {"context": partner}
        )

    def keeps(item):
        return pltpu.make_async_copy(
            source(item, place), target(item, place), local_sem.at[item]
        )

    def halves(far):
        upper = rows // 2
        start = from_chip(far) * rows + (far - 1) * upper
        block = a_ref.at[pl.ds(pl.multiple_of(start, upper), upper), :]
        return remote(
            block, block, half_send.at[far], half_recv.at[far],
            {"context": 2 * chip_at(chip, 3 - far, chips, square) + core},
        )

    def corner(far):
        upper = rows // 2
        start = from_chip(3) * rows + (far - 1) * upper
        block = a_ref.at[pl.ds(pl.multiple_of(start, upper), upper), :]
        return remote(block, block, half_send.at[far], half_recv.at[far], {"context": partner})

    direct = {item: list(range(1, chips)) for item in range(4)}
    if square:
        direct[2] = [1, 2]
    def begin(item):
        for far in direct[item] + [0]:
            sends(item, far).start()
        keeps(item).start()

    for item in range(3):
        begin(item)

    experts_iota = lax.broadcasted_iota(jnp.int32, (16, rows), 0)
    first_hot = (experts_iota == routes_ref[0:1, :]).astype(F32)
    second_hot = (experts_iota == routes_ref[1:2, :]).astype(F32)
    earlier = lax.broadcasted_iota(jnp.int32, (rows, rows), 0) < lax.broadcasted_iota(
        jnp.int32, (rows, rows), 1
    )
    before = dot((first_hot + second_hot).astype(BF16), earlier.astype(F32).astype(BF16))
    spots = experts_iota.astype(F32) * CAP + before
    slot_lines = []
    for which, hot in enumerate((first_hot, second_hot)):
        found = jnp.sum(hot * spots, axis=0, keepdims=True)
        slot_lines.append(jnp.where(routes_ref[which : which + 1, :] < FFN_E, found, -1.0))
    slots_ref[...] = jnp.concatenate(slot_lines + [jnp.zeros((6, rows), F32)], axis=0)
    per_owner = grads_ref.shape[1] * grads_ref.shape[2]

    def pick_rows(owner, carry):
        places = lax.broadcasted_iota(jnp.int32, (per_owner, rows), 0) + owner * per_owner
        places = places.astype(F32)
        hit = jnp.logical_or(places == slots_ref[0:1, :], places == slots_ref[1:2, :])
        picked = dot(hit.astype(F32).astype(BF16), cotangent_ref[...])
        grads_ref[owner] = picked.astype(BF16).reshape(grads_ref.shape[1:])
        return carry

    lax.fori_loop(0, owners, pick_rows, 0)
    shard_granules = rows // (TILE // 2)
    group = place // ranks
    owned = out_ref.shape[0]

    def outgoing(step):
        granule = granule_of(step, ranks)
        target_slot = group * shard_granules + lax.rem(granule, shard_granules)
        return (
            granule // shard_granules, out_ref.at[step], mix_ref.at[target_slot],
            granule_send.at[step], granule_recv.at[target_slot],
        )

    def part(device, which):
        return grads_ref.at[device, which]

    to_rows, hops, lends = {}, {}, {}
    for far in range(owners):
        peer = lax.rem(row + far, owners)
        spots = [(slot, grads_all_ref.at[slot, core, row])]
        if roles > 1:
            spots.append((other, stage_ref.at[row]))
        for which, (role, spot) in enumerate(spots):
            if far > 0:
                to_rows[which, far] = remote(
                    part(peer, role), spot, row_send.at[which, far], row_recv.at[which, far],
                    {"expert": peer},
                )
            elif which == 0:
                to_rows[which, far] = pltpu.make_async_copy(part(row, role), spot, local_sem.at[4])
            else:
                lends[0] = remote(
                    part(row, role), grads_all_ref.at[slot, core, row], lend_send.at[0],
                    lend_recv.at[0], {"context": twin},
                )
    wide_out, wide_on = [], []
    for which, weight in enumerate((gate_ref, up_ref)):
        spot = wide_ref.at[which, span(place, shard), :]

        def block(device):
            role = device // 2 // (chips // roles)
            return weight.at[role, :, span(lax.rem(device, 2), half)]

        if square:
            peers = [
                (2 * chip_at(chip, far, chips, square) + side, 2 * far + turned)
                for far in (1, 2)
                for turned, side in enumerate((core, 1 - core))
            ] + [(partner, 1)]
        else:
            peers = [(lax.rem(place + far, context), far) for far in range(1, context)]
        for peer, index in peers:
            wide_out.append(
                remote(
                    block(peer), spot, wide_send.at[which, index], wide_recv.at[which, index],
                    {"context": peer},
                )
            )
        wide_out.append(pltpu.make_async_copy(block(place), spot, local_sem.at[5 + which]))
        if square:
            for turned in range(2):
                side = core if turned == 0 else 1 - core
                giver = 2 * chip_at(chip, 2, chips, square) + side
                block_on = wide_ref.at[which, span(giver, shard), :]
                wide_on.append(
                    remote(
                        block_on, block_on, wide_send.at[which, 6 + turned],
                        wide_recv.at[which, 6 + turned],
                        {"context": 2 * chip_at(chip, 1, chips, square) + core},
                    )
                )
    arrives = {}
    if square:
        index = 0
        for which in range(2):
            for far in (1, 2):
                for turned in range(2):
                    arrives[which, far, turned] = wide_out[index]
                    index += 1
            index += 2

    tail = (lax.broadcasted_iota(jnp.int32, (EXTRA, rows), 0) == 0).astype(BF16)
    for item in range(2):
        for far in range(1, chips):
            sends(item, far).wait_recv()
            passes(item, far).start()
        sends(item, 0).wait_recv()
        keeps(item).wait()
        for far in range(1, chips):
            passes(item, far).wait_recv()
    for copy in to_rows.values():
        copy.start()
    for device in range(context):
        wt_ref[:, device * shard : (device + 1) * shard] = w_all_ref[device]

    def project(step, carry):
        far, second = step // 2, lax.rem(step, 2)
        block = 2 * chip_at(chip, far, chips, square, True) + jnp.where(
            second == 0, core, 1 - core
        )

        @pl.when(jnp.logical_and(far == 0, second == 0))
        def _():
            keeps(2).wait()

        @pl.when(jnp.logical_and(far == 0, second == 1))
        def _():
            sends(2, 0).wait_recv()

        if square:

            @pl.when(jnp.logical_and(far == 1, second == 0))
            def _():
                for near in (1, 2):
                    sends(2, near).wait_recv()
                    halves(near).start()
                    passes(2, near).start()
                begin(3)
                for copy in wide_out:
                    copy.start()

            @pl.when(jnp.logical_and(far == 3, second == 0))
            def _():
                for near in (1, 2):
                    corner(near).wait_recv()
                passes(2, 3).start()

        else:

            @pl.when(jnp.logical_and(far > 0, second == 0))
            def _():
                sends(2, far).wait_recv()
                passes(2, far).start()

        @pl.when(jnp.logical_and(far > 0, second == 1))
        def _():
            passes(2, far).wait_recv()

        at = span(block, rows)
        devices = lax.broadcasted_iota(jnp.int32, (size // 2, context), 1) == block
        cos_step = jnp.sum(
            jnp.where(devices, cos_base_ref[:, rows:], 0.0), axis=1, keepdims=True
        )
        sin_step = jnp.sum(
            jnp.where(devices, sin_base_ref[:, rows:], 0.0), axis=1, keepdims=True
        )
        cos_rows, sin_rows = cos_base_ref[:, :rows], sin_base_ref[:, :rows]
        cos_ref[:, at] = cos_step * cos_rows - sin_step * sin_rows
        sin_ref[:, at] = sin_step * cos_rows + cos_step * sin_rows
        both = dot(wt_ref[width:, :], a_ref[at, :], 1, 1)
        key_t = turn(both[:width], cos_ref[:, at], sin_ref[:, at], heads, size)
        key_t_ref[:, at] = key_t.astype(BF16)
        value_t = both[width:]
        for head in range(heads):
            here = slice(head * size, (head + 1) * size)
            key_ref[head, at, :] = key_t[here].T.astype(BF16)
            value_ref[head, at, :] = value_t[here].T.astype(BF16)
            value_t_ref[head * ext : head * ext + size, at] = value_t[here].astype(BF16)
            value_t_ref[head * ext + size : (head + 1) * ext, at] = tail
        return carry

    lax.fori_loop(0, 2 * chips, project, 0)
    if not square:
        begin(3)
        for copy in wide_out:
            copy.start()
    stored = [
        pltpu.make_async_copy(source, target, keep_sem.at[index])
        for index, (source, target) in enumerate(
            ((key_ref, key_out), (key_t_ref, key_t_out), (value_ref, value_out), (a_ref, a_out))
        )
    ]
    for copy in stored:
        copy.start()
    if roles > 1:
        lends[0].start()
    for far in range(owners):
        peer = lax.rem(row + owners - far, owners)
        home = grads_all_ref.at[slot, core, peer]
        if far > 0:
            to_rows[0, far].wait_recv()
        else:
            to_rows[0, far].wait()
        hops[far] = remote(
            home, home, hop_send.at[0, far], hop_recv.at[0, far], {"context": partner}
        )
        hops[far].start()
        if roles > 1 and far > 0:
            to_rows[1, far].wait_recv()
            lends[far] = remote(
                stage_ref.at[peer], home, lend_send.at[far], lend_recv.at[far],
                {"context": twin},
            )
            lends[far].start()

    def relays():
        for far in range(1, chips):
            sends(3, far).wait_recv()
            passes(3, far).start()
        for far in lends:
            lends[far].wait_recv()
            afar(far).start()

    def afar(far):
        away = grads_all_ref.at[other, core, lax.rem(row + owners - far, owners)]
        return remote(
            away, away, hop_send.at[1, far], hop_recv.at[1, far], {"context": partner}
        )

    def attend(index, carry):
        @pl.when(index > 0)
        def _():
            for step in range(2):
                here_or_away(*outgoing(2 * index - 2 + step))

        @pl.when(index == own_tiles - 1)
        def _():
            relays()

        if square:

            @pl.when(index == own_tiles // 2)
            def _():
                for which in range(2):
                    for turned in range(2):
                        arrives[which, 2, turned].wait_recv()
                for copy in wide_on:
                    copy.start()

        tile = own_tile(index, ranks)
        at = lanes(tile)
        query_t = dot(wt_ref[:width, :], a_ref[at, :], 1, 1)
        query_t = turn(query_t, cos_ref[:, at], sin_ref[:, at], heads, size)
        query_t = query_t.astype(BF16) * jnp.asarray(scale, BF16)
        query_t_ref[:, lanes(index)] = query_t
        query_ids = ids_all_ref[0:1, at]

        def score(step, tops, masked):
            here = lanes(step)
            fresh = []
            if masked:
                allowed = ids_all_ref[:, here].T[:, 0:1] <= query_ids
            for head in range(heads):
                part = dot(key_ref[head, here, :], query_t[head * size : (head + 1) * size])
                if masked:
                    part = jnp.where(allowed, part, NEGATIVE)
                scores_ref[head, here, :] = part
                fresh.append(
                    jnp.maximum(tops[head], jnp.max(part.reshape(TILE // 8, 8, TILE), axis=0))
                )
            return tuple(fresh)

        tops = tuple(jnp.full((8, TILE), NEGATIVE, F32) for _ in range(heads))
        stop = jnp.minimum(tile + 2, tiles)
        tops = lax.fori_loop(0, tile, lambda s, c: score(s, c, False), tops)
        tops = lax.fori_loop(tile, stop, lambda s, c: score(s, c, True), tops)
        peaks = [jnp.max(top, axis=0, keepdims=True) for top in tops]
        acc_ref[...] = jnp.zeros_like(acc_ref)

        def combine(step, carry):
            here = lanes(step)
            for head in range(heads):
                weights = jnp.exp(scores_ref[head, here, :] - peaks[head]).astype(BF16)
                acc_ref[head] += dot(value_t_ref[head * ext : (head + 1) * ext, here], weights)
            return carry

        lax.fori_loop(0, stop, combine, 0)
        parts = []
        for head in range(heads):
            total = acc_ref[head, size : size + 1, :]
            part = acc_ref[head, :size, :] * (1.0 / total)
            lse_ref[head : head + 1, lanes(index)] = peaks[head] + jnp.log(total)
            parts.append(part)
        joined = jnp.concatenate(parts, axis=0)
        out_t_ref[:, lanes(index)] = joined
        turned_out = joined.T.astype(BF16)
        out_ref[2 * index] = turned_out[: TILE // 2]
        out_ref[2 * index + 1] = turned_out[TILE // 2 :]
        return carry

    lax.fori_loop(0, own_tiles, attend, 0)
    for step in range(2):
        here_or_away(*outgoing(2 * own_tiles - 2 + step))
    sends(3, 0).wait_recv()
    keeps(3).wait()
    for far in range(1, chips):
        passes(3, far).wait_recv()
    for item in range(4):
        for far in direct[item] + [0]:
            sends(item, far).wait_send()
        for far in range(1, chips):
            passes(item, far).wait_send()
    if square:
        for far in (1, 2):
            halves(far).wait_send()
    forwarded = [arrives[which, 2, turned] for which, _, turned in arrives if _ == 2]
    for copy in wide_out:
        if any(copy is one for one in forwarded):
            copy.wait_send()
        else:
            copy.wait()
    for (which, far), copy in to_rows.items():
        if far > 0:
            copy.wait_send()
    for copy in lends.values():
        copy.wait_send()
    for copy in wide_on + list(hops.values()) + [afar(far) for far in lends] + stored:
        copy.wait()

    def settle(step, carry):
        wait_sent(*outgoing(step))
        giver_group, spot = step // shard_granules, lax.rem(step, shard_granules)
        giver = giver_group * ranks + owner_rank(place * shard_granules + spot, ranks)
        wait_landed(
            giver, out_ref.at[0], mix_ref.at[step], granule_send.at[0], granule_recv.at[step]
        )
        return carry

    lax.fori_loop(0, owned, settle, 0)


def attn_forward(
    hidden, gain, ids, routes, cotangent, cos_base, sin_base,
    query_weight, key_weight, value_weight, output_weight, gate_weight, up_weight,
    heads, size, ranks, context, owners, roles, number,
):
    rows, model = hidden.shape
    length = rows * context
    own = length // ranks
    width = heads * size
    ext = size + EXTRA
    shard = output_weight.shape[0]
    chips = context // 2
    granule = TILE // 2
    head_shape = jax.ShapeDtypeStruct((heads, length, size), BF16)
    turned_shape = jax.ShapeDtypeStruct((width, length), BF16)
    a_shape = jax.ShapeDtypeStruct((length, model), BF16)
    own_shape = jax.ShapeDtypeStruct((own // granule, granule, width), BF16)
    shapes = (
        jax.ShapeDtypeStruct((width, own), F32),
        jax.ShapeDtypeStruct((heads, own), F32),
        jax.ShapeDtypeStruct((width, own), BF16),
        jax.ShapeDtypeStruct((8, length), F32),
        jax.ShapeDtypeStruct((3 * width, model), BF16),
        jax.ShapeDtypeStruct((size // 2, length), F32),
        jax.ShapeDtypeStruct((size // 2, length), F32),
        jax.ShapeDtypeStruct((8, rows), F32),
        head_shape,
        turned_shape,
        head_shape,
        a_shape,
        own_shape,
        jax.ShapeDtypeStruct((model, model), BF16),
        jax.ShapeDtypeStruct((2, model, gate_weight.shape[2] // 2), BF16),
        jax.ShapeDtypeStruct((roles, 2, owners, CAP, model), BF16),
        jax.ShapeDtypeStruct((owners, CAP, model), BF16),
    )
    square = chips == 4 and roles == 2
    dims = (heads, size, ranks, size ** (-0.5), context, owners, roles, square)
    return pl.pallas_call(
        functools.partial(attn_forward_kernel, dims),
        out_shape=shapes,
        in_specs=vmem(10) + hbm(3),
        out_specs=vmem(8) + hbm(9),
        scratch_shapes=[
            pltpu.VMEM((context, 3 * width, shard), BF16),
            pltpu.VMEM((heads * ext, length), BF16),
            pltpu.VMEM((heads, length, TILE), F32),
            pltpu.VMEM((heads, ext, TILE), F32),
        ]
        + [
            pltpu.VMEM(one.shape, one.dtype)
            for one in (head_shape, turned_shape, head_shape, a_shape, own_shape)
        ]
        + [
            pltpu.VMEM((8, rows), F32),
            pltpu.VMEM((context // ranks, 3 * width, shard), BF16),
            pltpu.VMEM((rows, model), BF16),
            pltpu.VMEM((owners, roles, CAP, model), BF16),
        ]
        + [
            pltpu.SemaphoreType.DMA((4,)),
            pltpu.SemaphoreType.DMA((own // granule,)),
            pltpu.SemaphoreType.DMA((own // granule,)),
            pltpu.SemaphoreType.DMA((7,)),
            pltpu.SemaphoreType.DMA((4, chips)),
            pltpu.SemaphoreType.DMA((4, chips)),
            pltpu.SemaphoreType.DMA((4, chips)),
            pltpu.SemaphoreType.DMA((4, chips)),
            pltpu.SemaphoreType.DMA((3,)),
            pltpu.SemaphoreType.DMA((3,)),
        ]
        + [pltpu.SemaphoreType.DMA((2, owners))] * 4
        + [pltpu.SemaphoreType.DMA((owners,))] * 2
        + [pltpu.SemaphoreType.DMA((2, context))] * 2,
        compiler_params=params(number, 62),
        cost_estimate=cost(80),
        name="attn_forward",
    )(
        hidden, gain, ids, routes, cotangent, cos_base, sin_base,
        query_weight, key_weight, value_weight, output_weight, gate_weight, up_weight,
    )


def attn_backward_kernel(
    dims,
    grad_ref, a_ref, wt_ref, cos_ref, sin_ref, ids_all_ref,
    out_t_ref, lse_ref, query_t_ref, key_ref, key_t_ref, value_ref,
    wide_ref, outs_ref, output_ref,
    da_ref, pieces_ref, output_sum_ref, wide_in_ref, outs_in_ref,
    query_ref, own_grad_ref, dq_ref, dk_ref, dv_ref, grad_w_ref,
    landed_ref, output_in_ref, share_ref, shares_ref,
    granule_send, granule_recv, share_send, share_recv,
    wide_send, wide_recv, output_send, output_recv,
    row_send, row_recv, local_sem,
):
    heads, size, ranks, scale, context, owners, roles = dims
    length = a_ref.shape[0]
    shard = pieces_ref.shape[2]
    width = heads * size
    tiles = length // TILE
    own_tiles = tiles // ranks
    chips = context // 2
    place, row = meet(context, owners)
    chip, core = place // 2, lax.rem(place, 2)
    owned = landed_ref.shape[0]
    shard_granules = owned * ranks // context

    def outgoing(step):
        giver = step // shard_granules
        granule = place * shard_granules + lax.rem(step, shard_granules)
        landing = owner_slot(granule, ranks)
        return (
            giver * ranks + owner_rank(granule, ranks), grad_ref.at[step],
            landed_ref.at[landing], granule_send.at[step], granule_recv.at[landing],
        )

    def launch(step, carry):
        here_or_away(*outgoing(step))
        return carry

    lax.fori_loop(0, owned, launch, 0)
    copies, output_copies = [], []
    for item, (grads, target, send, recv) in enumerate(
        (
            (output_ref, output_in_ref, output_send, output_recv),
            (wide_ref, wide_in_ref, wide_send, wide_recv),
        )
    ):
        for far in range(context):
            peer = lax.rem(place + far, context)
            at = span(peer, shard)
            source = grads.at[:, at, :] if item else grads.at[at, :]
            group_copies = copies if item else output_copies
            if far == 0:
                group_copies.append(
                    pltpu.make_async_copy(source, target.at[place], local_sem.at[item])
                )
            else:
                group_copies.append(
                    remote(
                        source, target.at[place], send.at[far], recv.at[far], {"context": peer}
                    )
                )
    for far in range(owners):
        peer = lax.rem(row + far, owners)
        if far == 0:
            copies.append(
                pltpu.make_async_copy(outs_ref.at[row], outs_in_ref.at[row], local_sem.at[2])
            )
        else:
            copies.append(
                remote(
                    outs_ref.at[peer], outs_in_ref.at[row], row_send.at[far], row_recv.at[far],
                    {"expert": peer},
                )
            )
    dk_ref[...] = jnp.zeros_like(dk_ref)
    dv_ref[...] = jnp.zeros_like(dv_ref)
    da_ref[...] = jnp.zeros_like(da_ref)
    grad_w_ref[...] = jnp.zeros_like(grad_w_ref)
    def landed(step, carry):
        giver = granule_of(step, ranks) // shard_granules
        wait_landed(
            giver, grad_ref.at[0], landed_ref.at[step], granule_send.at[0], granule_recv.at[step]
        )
        return carry

    lax.fori_loop(0, owned, landed, 0)
    for copy in output_copies + copies:
        copy.start()

    def share_copy(far):
        return remote(
            share_ref, shares_ref.at[row], share_send.at[far], share_recv.at[far],
            {"expert": lax.rem(row + far, owners)},
        )

    def attend(index, carry):
        tile = own_tile(index, ranks)
        at = lanes(tile)
        query_t = query_t_ref[:, lanes(index)]
        @pl.when(index == own_tiles // 2)
        def _():
            for copy in output_copies:
                copy.wait()
            total = output_in_ref[0].astype(F32)
            for giver in range(1, context):
                total = total + output_in_ref[giver].astype(F32)
            share_ref[...] = total.astype(BF16)

        @pl.when(index == own_tiles // 2 + 1)
        def _():
            for far in range(1, owners):
                share_copy(far).start()

        grad_rows = landed_ref[pl.ds(2 * index, 2)].reshape(TILE, width)
        grad_t = grad_rows.astype(F32).T
        query_rows = query_t.astype(F32).T.astype(BF16)
        query_ids = ids_all_ref[0:1, at]
        deltas, tops, grads_low = [], [], []
        for head in range(heads):
            rows = slice(head * size, (head + 1) * size)
            query_ref[head] = query_rows[:, rows]
            own_grad_ref[head] = grad_rows[:, rows]
            deltas.append(
                jnp.sum(grad_t[rows] * out_t_ref[rows, lanes(index)], axis=0, keepdims=True)
            )
            tops.append(lse_ref[head : head + 1, lanes(index)])
        grad_t_low = grad_t.astype(BF16)
        dq_ref[...] = jnp.zeros_like(dq_ref)

        def chunk(step, carry, masked):
            here = lanes(step)
            if masked:
                allowed = ids_all_ref[:, here].T[:, 0:1] <= query_ids
            for head in range(heads):
                rows = slice(head * size, (head + 1) * size)
                scores = dot(key_ref[head, here, :], query_t[rows]) - tops[head]
                if masked:
                    scores = jnp.where(allowed, scores, NEGATIVE)
                probs = jnp.exp(scores)
                grad_probs = dot(value_ref[head, here, :], grad_t_low[rows])
                grad_scores = (probs * (grad_probs - deltas[head])).astype(BF16)
                dv_ref[head, here, :] += dot(probs.astype(BF16), own_grad_ref[head])
                dk_ref[head, here, :] += dot(grad_scores, query_ref[head])
                dq_ref[rows, :] += dot(key_t_ref[rows, here], grad_scores)
            return carry

        stop = jnp.minimum(tile + 2, tiles)
        lax.fori_loop(0, tile, lambda s, c: chunk(s, c, False), 0)
        lax.fori_loop(tile, stop, lambda s, c: chunk(s, c, True), 0)
        grad_query = turn(
            dq_ref[...] * scale, cos_ref[:, at], sin_ref[:, at], heads, size, back=True
        )
        grad_w_ref[:width, :] += dot(grad_query.astype(BF16), a_ref[at, :])
        da_ref[at, :] = dot(grad_query.T.astype(BF16), wt_ref[:width, :]).astype(BF16)
        return carry

    lax.fori_loop(0, own_tiles, attend, 0)

    def finish(step, carry):
        at = lanes(step)
        key_grad = jnp.concatenate([dk_ref[head, at, :].T for head in range(heads)], axis=0)
        key_grad = turn(key_grad, cos_ref[:, at], sin_ref[:, at], heads, size, back=True)
        value_grad = jnp.concatenate([dv_ref[head, at, :].T for head in range(heads)], axis=0)
        both = jnp.concatenate([key_grad, value_grad], axis=0)
        grad_w_ref[width:, :] += dot(both.astype(BF16), a_ref[at, :])
        total = da_ref[at, :].astype(F32) + dot(both.T.astype(BF16), wt_ref[width:, :])
        da_ref[at, :] = total.astype(BF16)
        return carry

    lax.fori_loop(0, tiles, finish, 0)
    for piece in range(pieces_ref.shape[0]):
        pieces_ref[piece] = grad_w_ref[:, piece * shard : (piece + 1) * shard].astype(BF16)
    for copy in copies:
        copy.wait()
    for far in range(1, owners):
        share_copy(far).wait()
    shares_ref[row] = share_ref[...]
    total = shares_ref[0].astype(F32)
    for giver in range(1, owners):
        total = total + shares_ref[giver].astype(F32)
    output_sum_ref[...] = total

    def settle(step, carry):
        wait_sent(*outgoing(step))
        return carry

    lax.fori_loop(0, owned, settle, 0)


def attn_backward(
    grad_own, a_full, weights_t, cos_t, sin_t, ids, kept,
    grad_wide, outs, grad_output, heads, size, ranks, context, roles, number,
):
    length, model = a_full.shape
    width = heads * size
    owners = outs.shape[0]
    shard = model // context
    shapes = (
        jax.ShapeDtypeStruct(a_full.shape, BF16),
        jax.ShapeDtypeStruct((context, weights_t.shape[0], shard), BF16),
        jax.ShapeDtypeStruct((shard, model), F32),
        jax.ShapeDtypeStruct((context, 2, shard, grad_wide.shape[2]), BF16),
        jax.ShapeDtypeStruct(outs.shape, BF16),
    )
    dims = (heads, size, ranks, size ** (-0.5), context, owners, roles)
    return pl.pallas_call(
        functools.partial(attn_backward_kernel, dims),
        out_shape=shapes,
        in_specs=vmem(12) + hbm(3),
        out_specs=vmem(3) + hbm(2),
        scratch_shapes=[
            pltpu.VMEM((heads, TILE, size), BF16),
            pltpu.VMEM((heads, TILE, size), BF16),
            pltpu.VMEM((width, TILE), F32),
            pltpu.VMEM((heads, length, size), F32),
            pltpu.VMEM((heads, length, size), F32),
            pltpu.VMEM(weights_t.shape, F32),
            pltpu.VMEM(grad_own.shape, BF16),
            pltpu.VMEM((context, shard, model), BF16),
            pltpu.VMEM((shard, model), BF16),
            pltpu.VMEM((owners, shard, model), BF16),
        ]
        + [pltpu.SemaphoreType.DMA((grad_own.shape[0],))] * 2
        + [pltpu.SemaphoreType.DMA((owners,))] * 2
        + [pltpu.SemaphoreType.DMA((context,))] * 4
        + [pltpu.SemaphoreType.DMA((owners,))] * 2
        + [pltpu.SemaphoreType.DMA((3,))],
        compiler_params=params(number, 63),
        cost_estimate=cost(60),
        name="attn_backward",
    )(
        grad_own, a_full, weights_t, cos_t, sin_t, ids, *kept,
        grad_wide, outs, grad_output,
    )


def moe_kernel(
    context, owners, roles, square,
    gates_ref, rows_ref, grads_hbm, wide_hbm, down_hbm,
    dots_back, grad_back, out_back, grad_wide_out, down_in,
    gates_all, rows_all, rows_stage, grads_ref, wide_ref, down_ref,
    rows_t_ref, dye_ref, out_acc, grad_acc, grad_wide_ref, grad_down_ref,
    dots_ref, grad_low, out_low, dots_twin, grad_twin, out_twin,
    dots_sum, grad_sum, out_sum, dots_relay, grad_relay,
    load_sem, local_sem, send_sem, recv_sem, pass_sem, land_sem, twin_sem, come_sem,
    relay_sem, reach_sem, down_send, down_recv, down_on, back_send, back_recv,
    pair_send, pair_recv, home_send, home_recv, lend_send, lend_recv, on_send, on_recv,
    out_send, out_recv, loan_send, loan_recv,
):
    chips = context // 2
    cap, width = rows_all.shape[1:]
    flat = dye_ref.shape
    loads = [
        pltpu.make_async_copy(source, target, load_sem.at[index])
        for index, (source, target) in enumerate(((grads_hbm, grads_ref), (wide_hbm, wide_ref)))
    ]
    for copy in loads:
        copy.start()
    place, row = meet(context, owners)
    chip, core = place // 2, lax.rem(place, 2)
    partner = {"context": place + 1 - 2 * core}
    slot = chip // (chips // roles)
    other = (roles - 1) - slot
    twin = {"context": 2 * lax.rem(chip + chips // 2, chips) + core}

    def block(spot, side, peer):
        return (spot * 2 + side) * owners + peer

    sent, local, passed, lent, relayed = {}, [], [], {}, []
    for far in range(1, owners):
        peer = lax.rem(row + far, owners)
        pairs = [
            (gates_ref.at[peer], gates_all.at[block(slot, core, row)]),
            (rows_ref.at[peer, slot], rows_all.at[block(slot, core, row)]),
        ]
        if roles > 1:
            pairs.append((rows_ref.at[peer, other], rows_stage.at[row]))
        for item, (source, target) in enumerate(pairs):
            sent[item, far] = remote(
                source, target, send_sem.at[item, far], recv_sem.at[item, far], {"expert": peer}
            )
            sent[item, far].start()
    mine = block(slot, core, row)
    for item, (source, target) in enumerate(
        ((gates_ref.at[row], gates_all.at[mine]), (rows_ref.at[row, slot], rows_all.at[mine]))
    ):
        local.append(pltpu.make_async_copy(source, target, local_sem.at[item]))
        local[-1].start()
        passed.append(
            remote(source, target, pass_sem.at[item, 0], land_sem.at[item, 0], partner)
        )
        passed[-1].start()
    if roles > 1:
        for item, (source, everything) in enumerate(
            ((gates_ref.at[row], gates_all), (rows_ref.at[row, other], rows_all))
        ):
            lent[item, 0] = (
                remote(
                    source, everything.at[mine], twin_sem.at[item, 0], come_sem.at[item, 0], twin
                ),
                everything.at[block(other, core, row)],
            )
            lent[item, 0][0].start()

    half = place // chips
    down_rows = down_hbm.shape[1]
    mark = lax.rem(place, chips)
    spot_down = down_ref.at[span(mark, down_rows), :]

    def down_copy(far, here):
        to_chip = chip_at(chip, far, chips, square)
        source = down_hbm.at[to_chip // (chips // roles)]
        if here:
            return pltpu.make_async_copy(source, spot_down, down_recv.at[mark])
        return remote(
            source, spot_down, down_send.at[far], down_recv.at[mark],
            {"context": 2 * to_chip + half},
        )

    @pl.when(half == core)
    def _():
        down_copy(0, True).start()

    @pl.when(half != core)
    def _():
        down_copy(0, False).start()

    fars = [1, 2] if square else list(range(1, chips))
    for far in fars:
        down_copy(far, False).start()

    def arrival(number):
        wait_landed(
            core * chips + number, down_hbm.at[0], down_ref.at[span(number, down_rows), :],
            down_send.at[0], down_recv.at[number],
        )

    def onward(number):
        land = down_ref.at[span(number, down_rows), :]
        return remote(
            land, land, down_on.at[number], down_recv.at[number],
            {"context": 2 * chip_at(chip, 1, chips, square) + core},
        )

    def from_below(number):
        return (core * chips + number) // 2 == chip_at(chip, 2, chips, square)

    for far in range(1, owners):
        peer = lax.rem(row + owners - far, owners)
        for item, everything in enumerate((gates_all, rows_all)):
            sent[item, far].wait_recv()
            landed = everything.at[block(slot, core, peer)]
            passed.append(
                remote(landed, landed, pass_sem.at[item, far], land_sem.at[item, far], partner)
            )
            passed[-1].start()
            if roles > 1:
                if item == 1:
                    sent[2, far].wait_recv()
                lent[item, far] = (
                    remote(
                        landed if item == 0 else rows_stage.at[peer], landed,
                        twin_sem.at[item, far], come_sem.at[item, far], twin,
                    ),
                    everything.at[block(other, core, peer)],
                )
                lent[item, far][0].start()
        if square and far == 1:
            for number in range(chips):

                @pl.when(from_below(number))
                def _():
                    arrival(number)
                    onward(number).start()

    for (item, far), (copy, arriving) in lent.items():
        copy.wait_recv()
        relayed.append(
            remote(
                arriving, arriving, relay_sem.at[item, far], reach_sem.at[item, far], partner
            )
        )
        relayed[-1].start()
    for number in range(chips):
        if square:

            @pl.when(from_below(number))
            def _():
                onward(number).wait_send()

            @pl.when(jnp.logical_not(from_below(number)))
            def _():
                arrival(number)

        else:
            arrival(number)
    for copy in loads + local:
        copy.wait()
    for copy in passed + relayed:
        copy.wait()

    blocks = roles * 2 * owners
    rows_t_ref[...] = rows_all[...].reshape(flat).astype(F32).T.astype(BF16)

    def scale(number, carry):
        columns = gates_all[number].T[:cap]
        column = columns[:, 0:1]
        if roles > 1:
            column = jnp.where(slot == 0, column, columns[:, 1:2])
        dye_ref[span(number, cap), :] = (grads_ref[number].astype(F32) * column).astype(BF16)
        return carry

    lax.fori_loop(0, blocks, scale, 0)
    out_acc[...] = jnp.zeros_like(out_acc)
    grad_acc[...] = jnp.zeros_like(grad_acc)
    back_rows = down_in.shape[1]
    per_step = HIDDEN_TILE // back_rows
    tiles = wide_ref.shape[2] // HIDDEN_TILE

    def leaving(index):
        return (
            core * chips + index, grad_down_ref.at[index], down_in.at[chip],
            back_send.at[index], back_recv.at[chip],
        )

    def hidden_tile(step, carry):
        tile = lax.rem(step + (1 - lax.rem(chip, 2)) * (tiles // 2), tiles)
        at = span(tile, HIDDEN_TILE)
        rows = rows_all[...].reshape(flat)
        dye = dye_ref[...]
        gate, up, down = wide_ref[0, :, at], wide_ref[1, :, at], down_ref[at, :]
        gate_pre = dot(rows, gate)
        up_pre = dot(rows, up)
        sigmoid = jax.nn.sigmoid(gate_pre)
        silu = gate_pre * sigmoid
        hidden = silu * up_pre
        grad_down = dot(hidden.T.astype(BF16), dye).astype(BF16)
        for index in range(per_step):
            grad_down_ref[tile * per_step + index] = grad_down[
                index * back_rows : (index + 1) * back_rows
            ]
        grad_hidden = dot(dye, down, 1, 1).astype(BF16).astype(F32)
        for index in range(per_step):
            here_or_away(*leaving(tile * per_step + index))
        out_acc[...] += dot(hidden.astype(BF16), down).reshape(out_acc.shape)
        grad_gate = (
            grad_hidden * up_pre * sigmoid * (1.0 + gate_pre * (1.0 - sigmoid))
        ).astype(BF16)
        grad_up = (grad_hidden * silu).astype(BF16)
        grad_wide_ref[0, :, at] = dot(rows_t_ref[...], grad_gate).astype(BF16)
        grad_wide_ref[1, :, at] = dot(rows_t_ref[...], grad_up).astype(BF16)
        total = dot(grad_gate, gate, 1, 1) + dot(grad_up, up, 1, 1)
        grad_acc[...] += total.reshape(grad_acc.shape)
        return carry

    lax.fori_loop(0, tiles, hidden_tile, 0)
    store = pltpu.make_async_copy(grad_wide_ref, grad_wide_out, load_sem.at[2])
    store.start()

    order = list(range(1, owners)) + [0]
    turns = (other, slot) if roles > 1 else (slot,)
    pair, gone, loaned, handed, outs, loans = {}, {}, {}, {}, [], []
    items = (
        (dots_ref, dots_twin, dots_sum, dots_relay, dots_back),
        (grad_low, grad_twin, grad_sum, grad_relay, grad_back),
    )

    def share(which, far):
        spot, peer = turns[which], lax.rem(row + far, owners)
        sources = (dots_ref.at[block(spot, 1 - core, peer)], grad_low.at[spot, peer])
        for item, source in enumerate(sources):
            pair[item, which, far] = remote(
                source, items[item][1].at[spot, peer],
                pair_send.at[item, which, far], pair_recv.at[item, which, far], partner,
            )
            pair[item, which, far].start()

    def line(number):
        product = out_acc[number] * grads_ref[number].astype(F32)
        total = product[:, :128]
        for start in range(128, width, 128):
            total = total + product[:, start : start + 128]
        totals = jnp.sum(total.T, axis=0, keepdims=True)
        dots_ref[number, :, :cap] = jnp.broadcast_to(totals, (8, cap))

    def lower(step, carry):
        spot, peer = step // owners, lax.rem(step, owners)
        number = block(spot, 1 - core, peer)
        grad_low[spot, peer] = grad_acc[number].astype(BF16)
        line(number)
        return carry

    def lower_out(step, carry):
        spot, peer = step // owners, lax.rem(step, owners)
        out_low[spot, peer] = out_acc[block(spot, 1 - core, peer)].astype(BF16)
        line(block(spot, core, peer))
        return carry

    lax.fori_loop(0, roles * owners, lower, 0)
    for far in order:
        for which in range(len(turns)):
            share(which, far)
    lax.fori_loop(0, roles * owners, lower_out, 0)
    for which, spot in enumerate(turns):
        outs.append(
            remote(
                out_low.at[spot], out_twin.at[spot], out_send.at[which], out_recv.at[which],
                partner,
            )
        )
        outs[-1].start()

    def leave(which, far):
        peer = lax.rem(row + far, owners)
        spot = turns[which]
        for item, (_, _, total, relay, back) in enumerate(items):
            if roles > 1 and which == 0:
                target = back.at[row, slot] if far == 0 else relay.at[peer]
                loaned[item, far] = remote(
                    total.at[spot, peer], target, lend_send.at[item, far],
                    lend_recv.at[item, far], twin,
                )
                loaned[item, far].start()
            elif far > 0:
                gone[item, far] = remote(
                    total.at[spot, peer], back.at[row, slot], home_send.at[item, far],
                    home_recv.at[item, far], {"expert": peer},
                )
                gone[item, far].start()

    last = None
    for far in order:
        peer = lax.rem(row + far, owners)
        for which, spot in enumerate(turns):
            number = block(spot, core, peer)
            for item in range(2):
                pair[item, which, far].wait_recv()
            dots_sum[spot, peer] = dots_ref[number] + dots_twin[spot, peer]

            def add(part, carry, number=number, spot=spot, peer=peer):
                at = pl.ds(pl.multiple_of(part * (cap // 3), cap // 3), cap // 3)
                grad_sum[spot, peer, at, :] = (
                    grad_acc[number, at, :] + grad_twin[spot, peer, at, :].astype(F32)
                ).astype(BF16)
                return carry

            lax.fori_loop(0, 3, add, 0)
            if last is not None:
                leave(*last)
            last = (which, far)
    dots_back[row, slot] = dots_sum[slot, row]
    grad_back[row, slot] = grad_sum[slot, row]
    leave(*last)
    if roles > 1:
        for far in range(1, owners):
            peer = lax.rem(row + far, owners)
            for item, (_, _, _, relay, back) in enumerate(items):
                loaned[item, far].wait_recv()
                handed[item, far] = remote(
                    relay.at[peer], back.at[row, other], on_send.at[item, far],
                    on_recv.at[item, far], {"expert": peer},
                )
                handed[item, far].start()
    for which, spot in enumerate(turns):
        outs[which].wait_recv()

        def add_out(peer, carry, which=which, spot=spot):
            summed = out_acc[block(spot, core, peer)] + out_twin[spot, peer].astype(F32)
            if roles > 1 and which == 0:
                out_sum[peer] = summed.astype(BF16)
            else:
                out_back[peer, slot] = summed.astype(BF16)
            return carry

        lax.fori_loop(0, owners, add_out, 0)
    if roles > 1:
        loans.append(remote(out_sum, out_back.at[:, slot], loan_send, loan_recv, twin))
        loans[-1].start()
        for item in range(2):
            loaned[item, 0].wait_recv()
    for copy in sent.values():
        copy.wait_send()
    for copy, _ in lent.values():
        copy.wait_send()
    for far in fars:
        down_copy(far, False).wait_send()

    @pl.when(half != core)
    def _():
        down_copy(0, False).wait_send()

    for index in range(chips):
        wait_sent(*leaving(index))
        wait_landed(
            2 * index + place // chips, grad_down_ref.at[0], down_in.at[index],
            back_send.at[index], back_recv.at[index],
        )
    for copy in list(pair.values()) + outs + list(loaned.values()):
        copy.wait_send()
    for copy in list(gone.values()) + list(handed.values()) + loans + [store]:
        copy.wait()


def moe(gates, rows, grads, wide_full, down_weight, context, roles, number):
    owners, _, cap, width = rows.shape
    chips = context // 2
    hidden = wide_full.shape[2]
    blocks = roles * 2 * owners
    slots = blocks * cap
    line = gates.shape[1:]
    square = chips == 4 and roles == 2
    low = (owners, cap, width)
    back = (chips, hidden // chips, width)
    dma = pltpu.SemaphoreType.DMA
    return pl.pallas_call(
        functools.partial(moe_kernel, context, owners, roles, square),
        out_shape=(
            jax.ShapeDtypeStruct((owners, roles) + line, F32),
            jax.ShapeDtypeStruct((owners, roles, cap, width), BF16),
            jax.ShapeDtypeStruct((owners, roles, cap, width), BF16),
            jax.ShapeDtypeStruct(wide_full.shape, BF16),
            jax.ShapeDtypeStruct(back, BF16),
        ),
        in_specs=vmem(2) + hbm(3),
        out_specs=vmem(3) + hbm(2),
        scratch_shapes=[
            pltpu.VMEM((blocks,) + line, F32),
            pltpu.VMEM((blocks, cap, width), BF16),
            pltpu.VMEM(low, BF16),
            pltpu.VMEM((blocks, cap, width), BF16),
            pltpu.VMEM(wide_full.shape, BF16),
            pltpu.VMEM((hidden, width), BF16),
            pltpu.VMEM((width, slots), BF16),
            pltpu.VMEM((slots, width), BF16),
            pltpu.VMEM((blocks, cap, width), F32),
            pltpu.VMEM((blocks, cap, width), F32),
            pltpu.VMEM(wide_full.shape, BF16),
            pltpu.VMEM(back, BF16),
            pltpu.VMEM((blocks,) + line, F32),
            pltpu.VMEM((roles,) + low, BF16),
            pltpu.VMEM((roles,) + low, BF16),
            pltpu.VMEM((roles, owners) + line, F32),
            pltpu.VMEM((roles,) + low, BF16),
            pltpu.VMEM((roles,) + low, BF16),
            pltpu.VMEM((roles, owners) + line, F32),
            pltpu.VMEM((roles,) + low, BF16),
            pltpu.VMEM(low, BF16),
            pltpu.VMEM((owners,) + line, F32),
            pltpu.VMEM(low, BF16),
            dma((3,)),
            dma((2,)),
        ]
        + [dma((3, owners))] * 8
        + [dma((chips,))] * 5
        + [dma((2, roles, owners))] * 2
        + [dma((2, owners))] * 6
        + [dma((roles,))] * 2
        + [dma] * 2,
        compiler_params=params(number, 62),
        cost_estimate=cost(97),
        name="moe",
    )(gates, rows, grads.reshape(blocks, cap, width), wide_full, down_weight)


def finish_kernel(
    chips, owners, groups,
    da_ref, pieces_ref, small_ref, slots_ref, gates_ref, gain_ref, query_w, key_w, value_w,
    base_hbm, returned_hbm, after_hbm, hidden_hbm,
    layer_ref, total_ref, query_ref, key_ref, value_ref, dots_ref, small_all_ref,
    sums_ref, base_ref, returned_ref, after_ref, hidden_ref, columns_ref, load_sem,
    da_twin, da_sum, da_in, w_twin, w_sum, w_in, s_twin, s_sum, s_in, s_total,
    stack_ref, shares, shares_in, block_ref,
    pair_send, pair_recv, chip_send, chip_recv, row_send, row_recv,
):
    loads = [
        pltpu.make_async_copy(source, target, load_sem.at[index])
        for index, (source, target) in enumerate(
            (
                (base_hbm, base_ref), (returned_hbm, returned_ref), (after_hbm, after_ref),
                (hidden_hbm, hidden_ref),
            )
        )
    ]
    for copy in loads:
        copy.start()
    place = lax.axis_index("context")
    row = lax.axis_index("expert")
    chip, core = place // 2, lax.rem(place, 2)
    partner = 2 * chip + 1 - core
    barrier = pltpu.get_barrier_semaphore()

    def greet(device):
        pl.semaphore_signal(
            barrier, inc=1, device_id=device, device_id_type=pl.DeviceIdType.MESH
        )

    greet({"context": partner})
    for far in range(1, chips):
        greet({"context": 2 * lax.rem(chip + far, chips) + core})
    for far in range(1, owners):
        greet({"expert": lax.rem(row + far, owners)})
    pl.semaphore_wait(barrier, chips + owners - 1)

    order = list(range(1, chips)) + [0]
    pair = {}
    for item, (source, target) in enumerate(
        ((small_ref, s_twin), (pieces_ref, w_twin), (da_ref, da_twin))
    ):
        for far in order:
            peer = lax.rem(chip + far, chips)
            pair[item, far] = remote(
                source.at[2 * peer + 1 - core], target.at[peer],
                pair_send.at[item, far], pair_recv.at[item, far], {"context": partner},
            )
            pair[item, far].start()

    def across(item, source, target, far):
        peer = lax.rem(chip + far, chips)
        return remote(
            source.at[peer], target.at[chip], chip_send.at[item, far], chip_recv.at[item, far],
            {"context": 2 * peer + core},
        )

    for far in order:
        peer = lax.rem(chip + far, chips)
        mine = 2 * peer + core
        pair[0, far].wait_recv()
        s_sum[peer] = small_ref[mine] + s_twin[peer]
        pair[1, far].wait_recv()
        w_sum[peer] = (
            pieces_ref[mine].astype(F32) + w_twin[peer].astype(F32)
        ).astype(BF16)
    moved = {}
    for far in range(1, chips):
        moved[0, far] = across(0, s_sum, s_in, far)
        moved[0, far].start()
        moved[1, far] = across(1, w_sum, w_in, far)
        moved[1, far].start()
    last = None
    for far in order:
        peer = lax.rem(chip + far, chips)
        pair[2, far].wait_recv()
        da_sum[peer] = (
            da_ref[2 * peer + core].astype(F32) + da_twin[peer].astype(F32)
        ).astype(BF16)
        if last is not None:
            moved[2, last] = across(2, da_sum, da_in, last)
            moved[2, last].start()
        last = far
    for far in range(1, chips):
        moved[0, far].wait_recv()
        moved[1, far].wait_recv()
    s_in[chip] = s_sum[chip]
    w_in[chip] = w_sum[chip]

    width = w_sum.shape[1] // 3
    shard = w_sum.shape[2]
    per_group = chips // groups
    for group in range(groups):
        total = w_in[group * per_group].astype(F32)
        for other in range(1, per_group):
            total = total + w_in[group * per_group + other].astype(F32)
        for which in range(3):
            stack_ref[which * shard : (which + 1) * shard, group * width : (group + 1) * width] = (
                total[which * width : (which + 1) * width].T
            )
    lines = shares.shape[1]
    for owner in range(owners):
        shares[owner] = stack_ref[owner * lines : (owner + 1) * lines, :].astype(BF16)
    total = s_in[0]
    for other in range(1, chips):
        total = total + s_in[other]
    s_total[...] = total
    rows = {}
    for far in range(1, owners):
        peer = lax.rem(row + far, owners)
        rows[0, far] = remote(
            shares.at[peer], shares_in.at[row], row_send.at[0, far], row_recv.at[0, far],
            {"expert": peer},
        )
        rows[0, far].start()
        rows[1, far] = remote(
            s_total, small_all_ref.at[row], row_send.at[1, far], row_recv.at[1, far],
            {"expert": peer},
        )
        rows[1, far].start()
    shares_in[row] = shares[row]
    small_all_ref[row] = total
    for copy in loads:
        copy.wait()
    count = returned_ref.shape[0]
    chunk = 128
    columns_ref[...] = slots_ref[...].T

    def layer(step, carry):
        at = span(step, chunk)
        places = lax.broadcasted_iota(jnp.int32, (chunk, count), 1).astype(F32)
        total = base_ref[at, :]
        for which in range(2):
            hit = (places == columns_ref[at, which : which + 1]).astype(F32).astype(BF16)
            total = total + gates_ref[at, which : which + 1] * dot(hit, returned_ref[...])
        layer_ref[at, :] = total.astype(BF16)
        return carry

    lax.fori_loop(0, layer_ref.shape[0] // chunk, layer, 0)
    for far in range(1, owners):
        rows[0, far].wait_recv()
    summed = shares_in[0].astype(F32)
    for other in range(1, owners):
        summed = summed + shares_in[other].astype(F32)
    block_ref[...] = summed.astype(BF16)
    for far in range(1, chips):
        moved[2, far].wait_recv()
    for far in range(1, owners):
        peer = lax.rem(row + far, owners)
        rows[2, far] = remote(
            block_ref, sums_ref.at[row], row_send.at[2, far], row_recv.at[2, far],
            {"expert": peer},
        )
        rows[2, far].start()
    sums_ref[row] = summed.astype(BF16)
    da_in[chip] = da_sum[chip]

    def input_rows(step, carry):
        at = span(step, chunk)
        total = da_in[0, at, :].astype(F32)
        for other in range(1, chips):
            total = total + da_in[other, at, :].astype(F32)
        grads = total * gain_ref[...]
        values = hidden_ref[at, :].astype(F32)
        inverse = lax.rsqrt(jnp.mean(values * values, axis=1, keepdims=True) + EPS)
        normed = values * inverse
        mean = jnp.mean(grads * normed, axis=1, keepdims=True)
        total_ref[at, :] = after_ref[at, :] + inverse * (grads - normed * mean)
        return carry

    lax.fori_loop(0, layer_ref.shape[0] // chunk, input_rows, 0)
    for far in range(1, owners):
        rows[1, far].wait_recv()
        rows[2, far].wait_recv()
    for owner in range(owners):
        stack_ref[owner * lines : (owner + 1) * lines, :] = sums_ref[owner].astype(F32)
    dots = jnp.zeros((shard, 1), F32)
    for which, (target, weight) in enumerate(
        ((query_ref, query_w), (key_ref, key_w), (value_ref, value_w))
    ):
        grads = stack_ref[which * shard : (which + 1) * shard, :]
        target[...] = grads
        dots = dots + jnp.sum(grads * weight[...].astype(F32), axis=1, keepdims=True)
    dots_ref[...] = dots
    for copy in list(pair.values()) + list(moved.values()) + list(rows.values()):
        copy.wait_send()


def finish(da, pieces, small, small_inputs, bulk, owners, groups, number):
    context, tokens, width = da.shape
    chips = context // 2
    lines, shard = pieces.shape[1:]
    few = small.shape[1]
    stack = 3 * shard
    block = (stack // owners, width)
    return pl.pallas_call(
        functools.partial(finish_kernel, chips, owners, groups),
        out_shape=(
            jax.ShapeDtypeStruct((tokens, width), BF16),
            jax.ShapeDtypeStruct((tokens, width), F32),
            jax.ShapeDtypeStruct((shard, width), F32),
            jax.ShapeDtypeStruct((shard, width), F32),
            jax.ShapeDtypeStruct((shard, width), F32),
            jax.ShapeDtypeStruct((shard, 1), F32),
            jax.ShapeDtypeStruct((owners, few, shard), F32),
        ),
        in_specs=vmem(9) + hbm(4),
        out_specs=vmem(7),
        scratch_shapes=[pltpu.VMEM((owners,) + block, BF16)]
        + [pltpu.VMEM(array.shape, array.dtype) for array in bulk]
        + [
            pltpu.VMEM((tokens, 8), F32),
            pltpu.SemaphoreType.DMA((4,)),
            pltpu.VMEM((chips, tokens, width), BF16),
            pltpu.VMEM((chips, tokens, width), BF16),
            pltpu.VMEM((chips, tokens, width), BF16),
            pltpu.VMEM((chips, lines, shard), BF16),
            pltpu.VMEM((chips, lines, shard), BF16),
            pltpu.VMEM((chips, lines, shard), BF16),
            pltpu.VMEM((chips, few, shard), F32),
            pltpu.VMEM((chips, few, shard), F32),
            pltpu.VMEM((chips, few, shard), F32),
            pltpu.VMEM((few, shard), F32),
            pltpu.VMEM((stack, width), F32),
            pltpu.VMEM((owners,) + block, BF16),
            pltpu.VMEM((owners,) + block, BF16),
            pltpu.VMEM(block, BF16),
            pltpu.SemaphoreType.DMA((3, chips)),
            pltpu.SemaphoreType.DMA((3, chips)),
            pltpu.SemaphoreType.DMA((3, chips)),
            pltpu.SemaphoreType.DMA((3, chips)),
            pltpu.SemaphoreType.DMA((3, owners)),
            pltpu.SemaphoreType.DMA((3, owners)),
        ],
        compiler_params=pltpu.CompilerParams(
            collective_id=number, has_side_effects=True, vmem_limit_bytes=60 << 20
        ),
        name="finish",
    )(da, pieces, small, *small_inputs, *bulk)


def shards(
    hidden_in,
    prior_logits,
    routes,
    block_ids,
    grad_out,
    attn_gain,
    query_weight,
    key_weight,
    value_weight,
    output_weight,
    moe_gain,
    router_weight,
    prior_weight,
    const_mix,
    const_vector,
    gate_weight,
    up_weight,
    down_weight,
):
    token_rows = hidden_in.shape[1]
    model_width = hidden_in.shape[2]
    head_size = model_width // HEADS
    context = lax.axis_size("context")
    owners = lax.axis_size("expert")
    groups = math.gcd(HEADS, context)
    ranks = context // groups
    heads = HEADS // groups
    width = heads * head_size
    length = context * token_rows
    per_owner = gate_weight.shape[0]
    slot_count = per_owner * owners * CAP
    shard_width = model_width // context
    roles = per_owner
    residual = hidden_in[0].astype(F32)
    prior_rows = prior_logits[0]
    route_rows = routes[0]
    cotangent_low = grad_out[0]
    cotangent = cotangent_low.astype(F32)

    half = head_size // 2
    freq = jnp.power(THETA, -2.0 * jnp.arange(half, dtype=F32) / head_size)
    steps = jnp.concatenate(
        [jnp.arange(token_rows), jnp.arange(context) * token_rows]
    ).astype(F32)
    angle = freq[:, None] * steps[None, :]

    gain_row = attn_gain.reshape(1, model_width)
    (
        out_t, log_total, query_t, ids, weights_t, cos_t, sin_t, slots, key_heads, key_t,
        value_heads, a_full, mix_granules, output_full, wide_full, grad_arrived, _,
    ) = attn_forward(
        hidden_in[0], gain_row, block_ids, jnp.transpose(route_rows), cotangent_low,
        jnp.cos(angle), jnp.sin(angle), query_weight, key_weight, value_weight,
        output_weight, gate_weight, up_weight, heads, head_size, ranks, context, owners, roles, 0,
    )
    kept = (out_t, log_total, query_t, key_heads, key_t, value_heads)
    slot_ids = jnp.arange(slot_count).astype(F32)[:, None]
    hit_first = slot_ids == slots[0:1]
    hit_second = slot_ids == slots[1:2]
    pick_either = hit_first.astype(BF16) + hit_second.astype(BF16)
    blocks = (owners, per_owner, CAP, model_width)

    def pick(rows):
        return jnp.dot(pick_either, rows, preferred_element_type=F32).astype(BF16).reshape(blocks)

    out_blocks = mix_granules.reshape(groups, token_rows, width)
    mix_low = jnp.transpose(out_blocks, (1, 0, 2)).reshape(token_rows, model_width)

    after_attn = residual + jnp.dot(mix_low, output_full, preferred_element_type=F32)
    inv_rms2 = lax.rsqrt(jnp.mean(after_attn * after_attn, axis=1, keepdims=True) + EPS)
    normed_two = after_attn * inv_rms2
    moe_input = normed_two * moe_gain
    narrow = jnp.concatenate(
        [router_weight, jnp.transpose(const_mix.reshape(-1, model_width))], axis=1
    )
    narrow_out = jnp.dot(moe_input, narrow, precision=HIGH, preferred_element_type=F32)
    expert_count = router_weight.shape[1]
    consts = const_mix.shape[0]
    logits = narrow_out[:, :expert_count] + jnp.dot(
        prior_rows, prior_weight, precision=HIGH, preferred_element_type=F32
    )
    probs = jax.nn.softmax(logits, axis=1)
    expert_ids = jnp.arange(expert_count, dtype=jnp.int32)
    first_hot = (route_rows[:, 0:1] == expert_ids[None, :]).astype(F32)
    second_hot = (route_rows[:, 1:2] == expert_ids[None, :]).astype(F32)
    chosen = first_hot + second_hot
    gated = probs * chosen
    first_gate = jnp.sum(probs * first_hot, axis=1, keepdims=True)
    second_gate = jnp.sum(probs * second_hot, axis=1, keepdims=True)
    slot_gate = jnp.sum(
        jnp.where(hit_first, first_gate[None, :, 0], 0.0)
        + jnp.where(hit_second, second_gate[None, :, 0], 0.0),
        axis=1,
    )
    def spread(values):
        values = values.reshape(owners, per_owner, CAP)
        return jnp.pad(values, ((0, 0), (0, 8 - per_owner), (0, 128 - CAP)))

    slot_dot, grad_back, expert_out, grad_wide, down_parts = moe(
        spread(slot_gate), pick(moe_input.astype(BF16)), grad_arrived, wide_full, down_weight,
        context, roles, 2,
    )
    slot_dot = slot_dot[:, :, 0, :CAP].reshape(slot_count)
    grad_back = grad_back.reshape(slot_count, model_width)

    const_soft = jax.nn.softmax(narrow_out[:, expert_count:].reshape(token_rows, consts, 2), axis=2)
    const_gate = gated[:, FFN_E + 2 :]
    copy_gate = gated[:, FFN_E + 1 : FFN_E + 2]
    const_out = [
        const_soft[:, c, 0:1] * moe_input + const_soft[:, c, 1:2] * const_vector[c][None, :]
        for c in range(consts)
    ]
    local_moe = copy_gate * moe_input
    for c in range(consts):
        local_moe = local_moe + const_gate[:, c : c + 1] * const_out[c]
    grad_moe_ffn = lax.dot_general(
        pick_either, grad_back, (((0,), (0,)), ((), ())), preferred_element_type=F32
    )
    first_dot = jnp.sum(jnp.where(hit_first, slot_dot[:, None], 0.0), axis=0)[:, None]
    second_dot = jnp.sum(jnp.where(hit_second, slot_dot[:, None], 0.0), axis=0)[:, None]
    copy_dot = jnp.sum(cotangent * moe_input, axis=1, keepdims=True)
    const_dot = [jnp.sum(cotangent * const_out[c], axis=1, keepdims=True) for c in range(consts)]
    extra = jnp.concatenate(
        [jnp.zeros((token_rows, FFN_E + 1), F32), copy_dot, *const_dot], axis=1
    )
    grad_probs = first_hot * first_dot + second_hot * second_dot + chosen * extra
    grad_logits = probs * (grad_probs - jnp.sum(probs * grad_probs, axis=1, keepdims=True))
    grad_prior_rows = lax.dot_general(
        grad_logits, prior_weight, (((1,), (1,)), ((), ())),
        precision=HIGH, preferred_element_type=F32,
    )
    vector_dot = jnp.dot(
        cotangent, jnp.transpose(const_vector), precision=HIGH, preferred_element_type=F32
    )
    grad_soft = jnp.stack(
        [const_gate * copy_dot, const_gate * vector_dot], axis=2
    )
    grad_mix = const_soft * (grad_soft - jnp.sum(const_soft * grad_soft, axis=2, keepdims=True))
    narrow_grad = jnp.concatenate([grad_logits, grad_mix.reshape(token_rows, -1)], axis=1)
    local_scale = copy_gate + jnp.sum(const_soft[:, :, 0] * const_gate, axis=1, keepdims=True)
    grad_moe_input = (
        grad_moe_ffn
        + lax.dot_general(
            narrow_grad, narrow, (((1,), (1,)), ((), ())),
            precision=HIGH, preferred_element_type=F32,
        )
        + local_scale * cotangent
    )
    small_moe = lax.dot_general(
        narrow_grad, moe_input, (((0,), (0,)), ((), ())),
        precision=HIGH, preferred_element_type=F32,
    )
    small_vector = lax.dot_general(
        const_soft[:, :, 1] * const_gate, cotangent, (((0,), (0,)), ((), ())),
        precision=HIGH, preferred_element_type=F32,
    )
    grad_prior_local = lax.dot_general(
        prior_rows, grad_logits, (((0,), (0,)), ((), ())),
        precision=HIGH, preferred_element_type=F32,
    )
    small_gain = jnp.sum(grad_moe_input * normed_two, axis=0, keepdims=True)
    prior_values = jnp.pad(
        grad_prior_local.reshape(-1), (0, -(expert_count * expert_count) % shard_width)
    ).reshape(-1, 1, shard_width)
    prior_lines = prior_values.shape[0]
    small = jnp.concatenate([small_moe, small_vector, small_gain], axis=0)
    small_lines = small.shape[0]
    small = jnp.concatenate(
        [
            small.reshape(small_lines, context, shard_width),
            jnp.broadcast_to(prior_values, (prior_lines, context, shard_width)),
        ],
        axis=0,
    )
    small = jnp.pad(small, ((0, -small.shape[0] % 8), (0, 0), (0, 0)))
    small = jnp.transpose(small, (1, 0, 2))

    grad_normed_two = grad_moe_input * moe_gain
    grad_after = cotangent + inv_rms2 * (
        grad_normed_two - normed_two * jnp.mean(grad_normed_two * normed_two, axis=1, keepdims=True)
    )
    grad_attn_low = grad_after.astype(BF16)
    grad_mix_low = lax.dot_general(
        grad_attn_low, output_full, (((1,), (1,)), ((), ())), preferred_element_type=F32
    ).astype(BF16)
    grad_pieces = jnp.transpose(grad_mix_low.reshape(token_rows, groups, width), (1, 0, 2))
    grad_own = grad_pieces.reshape(-1, TILE // 2, width)
    grad_output_local = lax.dot_general(
        mix_low, grad_attn_low, (((0,), (0,)), ((), ())), preferred_element_type=F32
    ).astype(BF16)
    da_part, w_pieces, output_sum, wide_parts, returned = attn_backward(
        grad_own, a_full, weights_t, cos_t, sin_t, ids, kept,
        grad_wide, expert_out, grad_output_local,
        heads, head_size, ranks, context, roles, 6,
    )
    returned = returned.reshape(slot_count, model_width)
    same = context // 2 // roles
    wide_parts = wide_parts.reshape(roles, same, 2, 2, shard_width, -1)

    def whole(which):
        total = jnp.sum(wide_parts[:, :, :, which].astype(F32), axis=1)
        return jnp.concatenate([total[:, 0], total[:, 1]], axis=-1)

    down_sum = jnp.sum(
        down_parts.reshape(roles, same, -1, model_width).astype(F32), axis=1
    )
    (
        layer_out, grad_input, grad_query, grad_key, grad_value, gain_dots, small_all,
    ) = finish(
        da_part.reshape(context, token_rows, model_width), w_pieces, small,
        (
            slots, jnp.concatenate([first_gate, second_gate], axis=1), gain_row,
            query_weight, key_weight, value_weight,
        ),
        (after_attn + local_moe, returned, grad_after, hidden_in[0]),
        owners, groups, 5,
    )
    small_own = jnp.sum(small_all, axis=0)
    column = lax.axis_index("context") * shard_width
    grad_attn_gain = gain_dots[:, 0] / lax.dynamic_slice_in_dim(attn_gain, column, shard_width)
    mixes = expert_count + 2 * consts
    grad_prior_weight = small_own[small_lines : small_lines + prior_lines].reshape(-1)
    grad_prior_weight = grad_prior_weight[: expert_count * expert_count].reshape(
        expert_count, expert_count
    )
    return (
        layer_out[None],
        grad_input[None],
        grad_prior_rows[None],
        grad_attn_gain,
        grad_query,
        grad_key,
        grad_value,
        output_sum,
        small_own[small_lines - 1],
        jnp.transpose(small_own[:expert_count]),
        grad_prior_weight,
        small_own[expert_count:mixes].reshape(consts, 2, shard_width),
        small_own[mixes : mixes + consts],
        whole(0),
        whole(1),
        down_sum,
    )


def solution(mesh):
    return jax.shard_map(
        shards,
        mesh=mesh,
        in_specs=(
            P("expert", "context", None),
            P("expert", "context", None),
            P("expert", "context", None),
            P("expert", "context"),
            P("expert", "context", None),
            P(),
            P("context", None),
            P("context", None),
            P("context", None),
            P("context", None),
            P(),
            P(),
            P(),
            P(),
            P(),
            P("expert", "context", None),
            P("expert", "context", None),
            P("expert", "context", None),
        ),
        out_specs=(
            P("expert", "context", None),
            P("expert", "context", None),
            P("expert", "context", None),
            P("context"),
            P("context", None),
            P("context", None),
            P("context", None),
            P("context", None),
            P("context"),
            P("context", None),
            P(),
            P(None, None, "context"),
            P(None, "context"),
            P("expert", "context", None),
            P("expert", "context", None),
            P("expert", "context", None),
        ),
        check_vma=False,
    )
```

```python
import functools
import math

import jax
import jax.numpy as jnp
from jax import lax
from jax.experimental import pallas as pl
from jax.experimental.pallas import tpu as pltpu
from jax.sharding import PartitionSpec as P

HEADS = 12
FFN_E = 8
CAP = 96
TILE = 256
EXTRA = 16
HIDDEN_TILE = 256

EPS = 1e-06
THETA = 10000.0
NEGATIVE = -1e30
HIGH = lax.Precision.HIGHEST
F32 = jnp.float32
BF16 = jnp.bfloat16


def dot(left, right, left_dim=1, right_dim=0):
    return lax.dot_general(
        left, right, (((left_dim,), (right_dim,)), ((), ())), preferred_element_type=F32
    )


def turn(rows, cos_rows, sin_rows, heads, size, back=False):
    half = size // 2
    parts = []
    for head in range(heads):
        first = rows[head * size : head * size + half]
        second = rows[head * size + half : (head + 1) * size]
        if back:
            parts.append(first * cos_rows + second * sin_rows)
            parts.append(second * cos_rows - first * sin_rows)
        else:
            parts.append(first * cos_rows - second * sin_rows)
            parts.append(second * cos_rows + first * sin_rows)
    return jnp.concatenate(parts, axis=0)


def own_tile(index, ranks):
    rank = lax.rem(lax.axis_index("context"), ranks)
    place = lax.rem(index, 2)
    return (index // 2) * (2 * ranks) + jnp.where(place == 0, rank, 2 * ranks - 1 - rank)


def granule_of(slot, ranks):
    return own_tile(slot // 2, ranks) * 2 + lax.rem(slot, 2)


def owner_rank(granule, ranks):
    spot = lax.rem(granule // 2, 2 * ranks)
    return jnp.minimum(spot, 2 * ranks - 1 - spot)


def owner_slot(granule, ranks):
    tile = granule // 2
    upper = jnp.where(lax.rem(tile, 2 * ranks) >= ranks, 1, 0)
    return (tile // (2 * ranks) * 2 + upper) * 2 + lax.rem(granule, 2)


def here_or_away(device, source, target, send, recv):
    place = lax.axis_index("context")

    @pl.when(device == place)
    def _():
        pltpu.make_async_copy(source, target, recv).start()

    @pl.when(device != place)
    def _():
        remote(source, target, send, recv, {"context": device}).start()


def wait_sent(device, source, target, send, recv):
    @pl.when(device != lax.axis_index("context"))
    def _():
        remote(source, target, send, recv, {"context": device}).wait_send()


def wait_landed(device, source, target, send, recv):
    place = lax.axis_index("context")

    @pl.when(device == place)
    def _():
        pltpu.make_async_copy(source, target, recv).wait()

    @pl.when(device != place)
    def _():
        remote(source, target, send, recv, {"context": device}).wait_recv()


def lanes(start):
    return span(start, TILE)


def span(start, size):
    return pl.ds(pl.multiple_of(start * size, size), size)


def cost(micros):
    return pl.CostEstimate(flops=micros * 1_150_000_000, bytes_accessed=0, transcendentals=0)


def vmem(count):
    return [pl.BlockSpec(memory_space=pltpu.VMEM)] * count


def hbm(count):
    return [pl.BlockSpec(memory_space=pl.ANY)] * count


def params(number=None, limit=60):
    if number is None:
        return pltpu.CompilerParams(vmem_limit_bytes=limit << 20)
    return pltpu.CompilerParams(
        collective_id=number, has_side_effects=True, vmem_limit_bytes=limit << 20
    )


def remote(source, target, send, recv, device):
    return pltpu.make_async_remote_copy(
        src_ref=source, dst_ref=target, send_sem=send, recv_sem=recv,
        device_id=device, device_id_type=pl.DeviceIdType.MESH,
    )


def chip_at(chip, far, chips, square, back=False):
    if square:
        x, y = lax.rem(chip, 2), chip // 2
        x = x + (far % 2) * (1 - 2 * x)
        y = y + (far // 2) * (1 - 2 * y)
        return 2 * y + x
    return lax.rem(chip + (chips - far if back else far), chips)


def meet(context, owners):
    place, row = lax.axis_index("context"), lax.axis_index("expert")
    barrier = pltpu.get_barrier_semaphore()
    for far in range(1, context):
        pl.semaphore_signal(
            barrier, inc=1, device_id={"context": lax.rem(place + far, context)},
            device_id_type=pl.DeviceIdType.MESH,
        )
    for far in range(1, owners):
        pl.semaphore_signal(
            barrier, inc=1, device_id={"expert": lax.rem(row + far, owners)},
            device_id_type=pl.DeviceIdType.MESH,
        )
    pl.semaphore_wait(barrier, context + owners - 2)
    return place, row


def attn_forward_kernel(
    dims,
    hidden_ref, gain_ref, own_ids_ref, routes_ref, cotangent_ref, cos_base_ref, sin_base_ref,
    query_w_ref, key_w_ref, value_w_ref, output_ref, gate_ref, up_ref,
    out_t_ref, lse_ref, query_t_ref, ids_all_ref, wt_ref, cos_ref, sin_ref, slots_ref,
    key_out, key_t_out, value_out, a_out, mix_ref,
    output_all_ref, wide_ref, grads_all_ref, stage_ref,
    w_all_ref, value_t_ref, scores_ref, acc_ref, key_ref, key_t_ref, value_ref, a_ref, out_ref,
    ids_ref, pieces_ref, input_ref, grads_ref, keep_sem, granule_send, granule_recv,
    local_sem, send_sem, recv_sem, pass_sem, land_sem, half_send, half_recv,
    row_send, row_recv, hop_send, hop_recv, lend_send, lend_recv, wide_send, wide_recv,
):
    heads, size, ranks, scale, context, owners, roles, square = dims
    length = a_ref.shape[0]
    rows = length // context
    shard = output_ref.shape[0]
    half = wide_ref.shape[2]
    width = heads * size
    tiles = length // TILE
    own_tiles = tiles // ranks
    ext = size + EXTRA
    chips = context // 2
    chunk = 128

    def normalize(step, carry):
        at = span(step, chunk)
        values = hidden_ref[at, :].astype(F32)
        inverse = lax.rsqrt(jnp.mean(values * values, axis=1, keepdims=True) + EPS)
        input_ref[at, :] = (values * inverse * gain_ref[...]).astype(BF16)
        return carry

    lax.fori_loop(0, rows // chunk, normalize, 0)
    ids_ref[...] = jnp.broadcast_to(own_ids_ref[...].astype(F32), ids_ref.shape)
    for which, weight in enumerate((query_w_ref, key_w_ref, value_w_ref)):
        for group in range(context // ranks):
            columns = weight[:, group * width : (group + 1) * width].astype(F32)
            pieces_ref[group, which * width : (which + 1) * width, :] = columns.T.astype(BF16)
    place, row = meet(context, owners)
    chip, core = place // 2, lax.rem(place, 2)
    partner = place + 1 - 2 * core
    slot = chip // (chips // roles)
    other = (roles - 1) - slot
    twin = 2 * lax.rem(chip + chips // 2, chips) + core

    def source(item, device):
        return (ids_ref, pieces_ref.at[device // ranks], input_ref, output_ref)[item]

    def target(item, device):
        return (
            ids_all_ref.at[:, span(device, rows)],
            w_all_ref.at[device],
            a_ref.at[span(device, rows), :],
            output_all_ref.at[span(device, shard), :],
        )[item]

    def from_chip(far):
        return 2 * chip_at(chip, far, chips, square, True) + core

    def sends(item, far):
        if isinstance(far, int) and far == 0:
            peer = partner
        else:
            peer = 2 * chip_at(chip, far, chips, square) + core
        return remote(
            source(item, peer), target(item, place), send_sem.at[item, far],
            recv_sem.at[item, far], {"context": peer},
        )

    def passes(item, far):
        block = target(item, from_chip(far))
        return remote(
            block, block, pass_sem.at[item, far], land_sem.at[item, far], {"context": partner}
        )

    def keeps(item):
        return pltpu.make_async_copy(
            source(item, place), target(item, place), local_sem.at[item]
        )

    def halves(far):
        upper = rows // 2
        start = from_chip(far) * rows + (far - 1) * upper
        block = a_ref.at[pl.ds(pl.multiple_of(start, upper), upper), :]
        return remote(
            block, block, half_send.at[far], half_recv.at[far],
            {"context": 2 * chip_at(chip, 3 - far, chips, square) + core},
        )

    def corner(far):
        upper = rows // 2
        start = from_chip(3) * rows + (far - 1) * upper
        block = a_ref.at[pl.ds(pl.multiple_of(start, upper), upper), :]
        return remote(block, block, half_send.at[far], half_recv.at[far], {"context": partner})

    direct = {item: list(range(1, chips)) for item in range(4)}
    if square:
        direct[2] = [1, 2]
    def begin(item):
        for far in direct[item] + [0]:
            sends(item, far).start()
        keeps(item).start()

    for item in range(3):
        begin(item)

    experts_iota = lax.broadcasted_iota(jnp.int32, (16, rows), 0)
    first_hot = (experts_iota == routes_ref[0:1, :]).astype(F32)
    second_hot = (experts_iota == routes_ref[1:2, :]).astype(F32)
    earlier = lax.broadcasted_iota(jnp.int32, (rows, rows), 0) < lax.broadcasted_iota(
        jnp.int32, (rows, rows), 1
    )
    before = dot((first_hot + second_hot).astype(BF16), earlier.astype(F32).astype(BF16))
    spots = experts_iota.astype(F32) * CAP + before
    slot_lines = []
    for which, hot in enumerate((first_hot, second_hot)):
        found = jnp.sum(hot * spots, axis=0, keepdims=True)
        slot_lines.append(jnp.where(routes_ref[which : which + 1, :] < FFN_E, found, -1.0))
    slots_ref[...] = jnp.concatenate(slot_lines + [jnp.zeros((6, rows), F32)], axis=0)
    per_owner = grads_ref.shape[1] * grads_ref.shape[2]

    def pick_rows(owner, carry):
        places = lax.broadcasted_iota(jnp.int32, (per_owner, rows), 0) + owner * per_owner
        places = places.astype(F32)
        hit = jnp.logical_or(places == slots_ref[0:1, :], places == slots_ref[1:2, :])
        picked = dot(hit.astype(F32).astype(BF16), cotangent_ref[...])
        grads_ref[owner] = picked.astype(BF16).reshape(grads_ref.shape[1:])
        return carry

    lax.fori_loop(0, owners, pick_rows, 0)
    shard_granules = rows // (TILE // 2)
    group = place // ranks
    owned = out_ref.shape[0]

    def outgoing(step):
        granule = granule_of(step, ranks)
        target_slot = group * shard_granules + lax.rem(granule, shard_granules)
        return (
            granule // shard_granules, out_ref.at[step], mix_ref.at[target_slot],
            granule_send.at[step], granule_recv.at[target_slot],
        )

    def part(device, which):
        return grads_ref.at[device, which]

    to_rows, hops, lends = {}, {}, {}
    for far in range(owners):
        peer = lax.rem(row + far, owners)
        spots = [(slot, grads_all_ref.at[slot, core, row])]
        if roles > 1:
            spots.append((other, stage_ref.at[row]))
        for which, (role, spot) in enumerate(spots):
            if far > 0:
                to_rows[which, far] = remote(
                    part(peer, role), spot, row_send.at[which, far], row_recv.at[which, far],
                    {"expert": peer},
                )
            elif which == 0:
                to_rows[which, far] = pltpu.make_async_copy(part(row, role), spot, local_sem.at[4])
            else:
                lends[0] = remote(
                    part(row, role), grads_all_ref.at[slot, core, row], lend_send.at[0],
                    lend_recv.at[0], {"context": twin},
                )
    wide_out, wide_on = [], []
    for which, weight in enumerate((gate_ref, up_ref)):
        spot = wide_ref.at[which, span(place, shard), :]

        def block(device):
            role = device // 2 // (chips // roles)
            return weight.at[role, :, span(lax.rem(device, 2), half)]

        if square:
            peers = [
                (2 * chip_at(chip, far, chips, square) + side, 2 * far + turned)
                for far in (1, 2)
                for turned, side in enumerate((core, 1 - core))
            ] + [(partner, 1)]
        else:
            peers = [(lax.rem(place + far, context), far) for far in range(1, context)]
        for peer, index in peers:
            wide_out.append(
                remote(
                    block(peer), spot, wide_send.at[which, index], wide_recv.at[which, index],
                    {"context": peer},
                )
            )
        wide_out.append(pltpu.make_async_copy(block(place), spot, local_sem.at[5 + which]))
        if square:
            for turned in range(2):
                side = core if turned == 0 else 1 - core
                giver = 2 * chip_at(chip, 2, chips, square) + side
                block_on = wide_ref.at[which, span(giver, shard), :]
                wide_on.append(
                    remote(
                        block_on, block_on, wide_send.at[which, 6 + turned],
                        wide_recv.at[which, 6 + turned],
                        {"context": 2 * chip_at(chip, 1, chips, square) + core},
                    )
                )
    arrives = {}
    if square:
        index = 0
        for which in range(2):
            for far in (1, 2):
                for turned in range(2):
                    arrives[which, far, turned] = wide_out[index]
                    index += 1
            index += 2

    tail = (lax.broadcasted_iota(jnp.int32, (EXTRA, rows), 0) == 0).astype(BF16)
    for item in range(2):
        for far in range(1, chips):
            sends(item, far).wait_recv()
            passes(item, far).start()
        sends(item, 0).wait_recv()
        keeps(item).wait()
        for far in range(1, chips):
            passes(item, far).wait_recv()
    for copy in to_rows.values():
        copy.start()
    for device in range(context):
        wt_ref[:, device * shard : (device + 1) * shard] = w_all_ref[device]

    def project(step, carry):
        far, second = step // 2, lax.rem(step, 2)
        block = 2 * chip_at(chip, far, chips, square, True) + jnp.where(
            second == 0, core, 1 - core
        )

        @pl.when(jnp.logical_and(far == 0, second == 0))
        def _():
            keeps(2).wait()

        @pl.when(jnp.logical_and(far == 0, second == 1))
        def _():
            sends(2, 0).wait_recv()

        if square:

            @pl.when(jnp.logical_and(far == 1, second == 0))
            def _():
                for near in (1, 2):
                    sends(2, near).wait_recv()
                    halves(near).start()
                    passes(2, near).start()
                begin(3)
                for copy in wide_out:
                    copy.start()

            @pl.when(jnp.logical_and(far == 3, second == 0))
            def _():
                for near in (1, 2):
                    corner(near).wait_recv()
                passes(2, 3).start()

        else:

            @pl.when(jnp.logical_and(far > 0, second == 0))
            def _():
                sends(2, far).wait_recv()
                passes(2, far).start()

        @pl.when(jnp.logical_and(far > 0, second == 1))
        def _():
            passes(2, far).wait_recv()

        at = span(block, rows)
        devices = lax.broadcasted_iota(jnp.int32, (size // 2, context), 1) == block
        cos_step = jnp.sum(
            jnp.where(devices, cos_base_ref[:, rows:], 0.0), axis=1, keepdims=True
        )
        sin_step = jnp.sum(
            jnp.where(devices, sin_base_ref[:, rows:], 0.0), axis=1, keepdims=True
        )
        cos_rows, sin_rows = cos_base_ref[:, :rows], sin_base_ref[:, :rows]
        cos_ref[:, at] = cos_step * cos_rows - sin_step * sin_rows
        sin_ref[:, at] = sin_step * cos_rows + cos_step * sin_rows
        both = dot(wt_ref[width:, :], a_ref[at, :], 1, 1)
        key_t = turn(both[:width], cos_ref[:, at], sin_ref[:, at], heads, size)
        key_t_ref[:, at] = key_t.astype(BF16)
        value_t = both[width:]
        for head in range(heads):
            here = slice(head * size, (head + 1) * size)
            key_ref[head, at, :] = key_t[here].T.astype(BF16)
            value_ref[head, at, :] = value_t[here].T.astype(BF16)
            value_t_ref[head * ext : head * ext + size, at] = value_t[here].astype(BF16)
            value_t_ref[head * ext + size : (head + 1) * ext, at] = tail
        return carry

    lax.fori_loop(0, 2 * chips, project, 0)
    if not square:
        begin(3)
        for copy in wide_out:
            copy.start()
    stored = [
        pltpu.make_async_copy(source, target, keep_sem.at[index])
        for index, (source, target) in enumerate(
            ((key_ref, key_out), (key_t_ref, key_t_out), (value_ref, value_out), (a_ref, a_out))
        )
    ]
    for copy in stored:
        copy.start()
    if roles > 1:
        lends[0].start()
    for far in range(owners):
        peer = lax.rem(row + owners - far, owners)
        home = grads_all_ref.at[slot, core, peer]
        if far > 0:
            to_rows[0, far].wait_recv()
        else:
            to_rows[0, far].wait()
        hops[far] = remote(
            home, home, hop_send.at[0, far], hop_recv.at[0, far], {"context": partner}
        )
        hops[far].start()
        if roles > 1 and far > 0:
            to_rows[1, far].wait_recv()
            lends[far] = remote(
                stage_ref.at[peer], home, lend_send.at[far], lend_recv.at[far],
                {"context": twin},
            )
            lends[far].start()

    def relays():
        for far in range(1, chips):
            sends(3, far).wait_recv()
            passes(3, far).start()
        for far in lends:
            lends[far].wait_recv()
            afar(far).start()

    def afar(far):
        away = grads_all_ref.at[other, core, lax.rem(row + owners - far, owners)]
        return remote(
            away, away, hop_send.at[1, far], hop_recv.at[1, far], {"context": partner}
        )

    def attend(index, carry):
        @pl.when(index > 0)
        def _():
            for step in range(2):
                here_or_away(*outgoing(2 * index - 2 + step))

        @pl.when(index == own_tiles - 1)
        def _():
            relays()

        if square:

            @pl.when(index == own_tiles // 2)
            def _():
                for which in range(2):
                    for turned in range(2):
                        arrives[which, 2, turned].wait_recv()
                for copy in wide_on:
                    copy.start()

        tile = own_tile(index, ranks)
        at = lanes(tile)
        query_t = dot(wt_ref[:width, :], a_ref[at, :], 1, 1)
        query_t = turn(query_t, cos_ref[:, at], sin_ref[:, at], heads, size)
        query_t = query_t.astype(BF16) * jnp.asarray(scale, BF16)
        query_t_ref[:, lanes(index)] = query_t
        query_ids = ids_all_ref[0:1, at]

        def score(step, tops, masked):
            here = lanes(step)
            fresh = []
            if masked:
                allowed = ids_all_ref[:, here].T[:, 0:1] <= query_ids
            for head in range(heads):
                part = dot(key_ref[head, here, :], query_t[head * size : (head + 1) * size])
                if masked:
                    part = jnp.where(allowed, part, NEGATIVE)
                scores_ref[head, here, :] = part
                fresh.append(
                    jnp.maximum(tops[head], jnp.max(part.reshape(TILE // 8, 8, TILE), axis=0))
                )
            return tuple(fresh)

        tops = tuple(jnp.full((8, TILE), NEGATIVE, F32) for _ in range(heads))
        stop = jnp.minimum(tile + 2, tiles)
        tops = lax.fori_loop(0, tile, lambda s, c: score(s, c, False), tops)
        tops = lax.fori_loop(tile, stop, lambda s, c: score(s, c, True), tops)
        peaks = [jnp.max(top, axis=0, keepdims=True) for top in tops]
        acc_ref[...] = jnp.zeros_like(acc_ref)

        def combine(step, carry):
            here = lanes(step)
            for head in range(heads):
                weights = jnp.exp(scores_ref[head, here, :] - peaks[head]).astype(BF16)
                acc_ref[head] += dot(value_t_ref[head * ext : (head + 1) * ext, here], weights)
            return carry

        lax.fori_loop(0, stop, combine, 0)
        parts = []
        for head in range(heads):
            total = acc_ref[head, size : size + 1, :]
            part = acc_ref[head, :size, :] * (1.0 / total)
            lse_ref[head : head + 1, lanes(index)] = peaks[head] + jnp.log(total)
            parts.append(part)
        joined = jnp.concatenate(parts, axis=0)
        out_t_ref[:, lanes(index)] = joined
        turned_out = joined.T.astype(BF16)
        out_ref[2 * index] = turned_out[: TILE // 2]
        out_ref[2 * index + 1] = turned_out[TILE // 2 :]
        return carry

    lax.fori_loop(0, own_tiles, attend, 0)
    for step in range(2):
        here_or_away(*outgoing(2 * own_tiles - 2 + step))
    sends(3, 0).wait_recv()
    keeps(3).wait()
    for far in range(1, chips):
        passes(3, far).wait_recv()
    for item in range(4):
        for far in direct[item] + [0]:
            sends(item, far).wait_send()
        for far in range(1, chips):
            passes(item, far).wait_send()
    if square:
        for far in (1, 2):
            halves(far).wait_send()
    forwarded = [arrives[which, 2, turned] for which, _, turned in arrives if _ == 2]
    for copy in wide_out:
        if any(copy is one for one in forwarded):
            copy.wait_send()
        else:
            copy.wait()
    for (which, far), copy in to_rows.items():
        if far > 0:
            copy.wait_send()
    for copy in lends.values():
        copy.wait_send()
    for copy in wide_on + list(hops.values()) + [afar(far) for far in lends] + stored:
        copy.wait()

    def settle(step, carry):
        wait_sent(*outgoing(step))
        giver_group, spot = step // shard_granules, lax.rem(step, shard_granules)
        giver = giver_group * ranks + owner_rank(place * shard_granules + spot, ranks)
        wait_landed(
            giver, out_ref.at[0], mix_ref.at[step], granule_send.at[0], granule_recv.at[step]
        )
        return carry

    lax.fori_loop(0, owned, settle, 0)


def attn_forward(
    hidden, gain, ids, routes, cotangent, cos_base, sin_base,
    query_weight, key_weight, value_weight, output_weight, gate_weight, up_weight,
    heads, size, ranks, context, owners, roles, number,
):
    rows, model = hidden.shape
    length = rows * context
    own = length // ranks
    width = heads * size
    ext = size + EXTRA
    shard = output_weight.shape[0]
    chips = context // 2
    granule = TILE // 2
    head_shape = jax.ShapeDtypeStruct((heads, length, size), BF16)
    turned_shape = jax.ShapeDtypeStruct((width, length), BF16)
    a_shape = jax.ShapeDtypeStruct((length, model), BF16)
    own_shape = jax.ShapeDtypeStruct((own // granule, granule, width), BF16)
    shapes = (
        jax.ShapeDtypeStruct((width, own), F32),
        jax.ShapeDtypeStruct((heads, own), F32),
        jax.ShapeDtypeStruct((width, own), BF16),
        jax.ShapeDtypeStruct((8, length), F32),
        jax.ShapeDtypeStruct((3 * width, model), BF16),
        jax.ShapeDtypeStruct((size // 2, length), F32),
        jax.ShapeDtypeStruct((size // 2, length), F32),
        jax.ShapeDtypeStruct((8, rows), F32),
        head_shape,
        turned_shape,
        head_shape,
        a_shape,
        own_shape,
        jax.ShapeDtypeStruct((model, model), BF16),
        jax.ShapeDtypeStruct((2, model, gate_weight.shape[2] // 2), BF16),
        jax.ShapeDtypeStruct((roles, 2, owners, CAP, model), BF16),
        jax.ShapeDtypeStruct((owners, CAP, model), BF16),
    )
    square = chips == 4 and roles == 2
    dims = (heads, size, ranks, size ** (-0.5), context, owners, roles, square)
    return pl.pallas_call(
        functools.partial(attn_forward_kernel, dims),
        out_shape=shapes,
        in_specs=vmem(10) + hbm(3),
        out_specs=vmem(8) + hbm(9),
        scratch_shapes=[
            pltpu.VMEM((context, 3 * width, shard), BF16),
            pltpu.VMEM((heads * ext, length), BF16),
            pltpu.VMEM((heads, length, TILE), F32),
            pltpu.VMEM((heads, ext, TILE), F32),
        ]
        + [
            pltpu.VMEM(one.shape, one.dtype)
            for one in (head_shape, turned_shape, head_shape, a_shape, own_shape)
        ]
        + [
            pltpu.VMEM((8, rows), F32),
            pltpu.VMEM((context // ranks, 3 * width, shard), BF16),
            pltpu.VMEM((rows, model), BF16),
            pltpu.VMEM((owners, roles, CAP, model), BF16),
        ]
        + [
            pltpu.SemaphoreType.DMA((4,)),
            pltpu.SemaphoreType.DMA((own // granule,)),
            pltpu.SemaphoreType.DMA((own // granule,)),
            pltpu.SemaphoreType.DMA((7,)),
            pltpu.SemaphoreType.DMA((4, chips)),
            pltpu.SemaphoreType.DMA((4, chips)),
            pltpu.SemaphoreType.DMA((4, chips)),
            pltpu.SemaphoreType.DMA((4, chips)),
            pltpu.SemaphoreType.DMA((3,)),
            pltpu.SemaphoreType.DMA((3,)),
        ]
        + [pltpu.SemaphoreType.DMA((2, owners))] * 4
        + [pltpu.SemaphoreType.DMA((owners,))] * 2
        + [pltpu.SemaphoreType.DMA((2, context))] * 2,
        compiler_params=params(number, 62),
        cost_estimate=cost(80),
        name="attn_forward",
    )(
        hidden, gain, ids, routes, cotangent, cos_base, sin_base,
        query_weight, key_weight, value_weight, output_weight, gate_weight, up_weight,
    )


def attn_backward_kernel(
    dims,
    grad_ref, a_hbm, wt_hbm, cos_hbm, sin_hbm, ids_hbm,
    out_t_hbm, lse_hbm, query_t_hbm, key_hbm, key_t_hbm, value_hbm,
    wide_ref, outs_ref, output_ref,
    da_out, pieces_ref, output_sum_ref, wide_in_ref, outs_in_ref,
    a_ref, wt_ref, cos_ref, sin_ref, ids_all_ref,
    out_t_ref, lse_ref, query_t_ref, key_ref, key_t_ref, value_ref, da_ref, load_sem, da_sem,
    query_ref, own_grad_ref, dq_ref, dk_ref, dv_ref, grad_w_ref,
    landed_ref, output_in_ref, share_ref, shares_ref,
    granule_send, granule_recv, share_send, share_recv,
    wide_send, wide_recv, output_send, output_recv,
    row_send, row_recv, local_sem,
):
    heads, size, ranks, scale, context, owners, roles = dims
    length = a_ref.shape[0]
    shard = pieces_ref.shape[2]
    width = heads * size
    tiles = length // TILE
    own_tiles = tiles // ranks
    chips = context // 2
    loads = [
        pltpu.make_async_copy(source, target, load_sem.at[index])
        for index, (source, target) in enumerate(
            (
                (key_hbm, key_ref), (value_hbm, value_ref), (key_t_hbm, key_t_ref),
                (query_t_hbm, query_t_ref), (out_t_hbm, out_t_ref), (lse_hbm, lse_ref),
                (ids_hbm, ids_all_ref), (cos_hbm, cos_ref), (sin_hbm, sin_ref),
                (a_hbm, a_ref), (wt_hbm, wt_ref),
            )
        )
    ]
    for copy in loads:
        copy.start()
    place, row = meet(context, owners)
    chip, core = place // 2, lax.rem(place, 2)
    owned = landed_ref.shape[0]
    shard_granules = owned * ranks // context

    def outgoing(step):
        giver = step // shard_granules
        granule = place * shard_granules + lax.rem(step, shard_granules)
        landing = owner_slot(granule, ranks)
        return (
            giver * ranks + owner_rank(granule, ranks), grad_ref.at[step],
            landed_ref.at[landing], granule_send.at[step], granule_recv.at[landing],
        )

    def launch(step, carry):
        here_or_away(*outgoing(step))
        return carry

    lax.fori_loop(0, owned, launch, 0)
    copies, output_copies = [], []
    for item, (grads, target, send, recv) in enumerate(
        (
            (output_ref, output_in_ref, output_send, output_recv),
            (wide_ref, wide_in_ref, wide_send, wide_recv),
        )
    ):
        for far in range(context):
            peer = lax.rem(place + far, context)
            at = span(peer, shard)
            source = grads.at[:, at, :] if item else grads.at[at, :]
            group_copies = copies if item else output_copies
            if far == 0:
                group_copies.append(
                    pltpu.make_async_copy(source, target.at[place], local_sem.at[item])
                )
            else:
                group_copies.append(
                    remote(
                        source, target.at[place], send.at[far], recv.at[far], {"context": peer}
                    )
                )
    for far in range(owners):
        peer = lax.rem(row + far, owners)
        if far == 0:
            copies.append(
                pltpu.make_async_copy(outs_ref.at[row], outs_in_ref.at[row], local_sem.at[2])
            )
        else:
            copies.append(
                remote(
                    outs_ref.at[peer], outs_in_ref.at[row], row_send.at[far], row_recv.at[far],
                    {"expert": peer},
                )
            )
    dk_ref[...] = jnp.zeros_like(dk_ref)
    dv_ref[...] = jnp.zeros_like(dv_ref)
    da_ref[...] = jnp.zeros_like(da_ref)
    grad_w_ref[...] = jnp.zeros_like(grad_w_ref)
    def landed(step, carry):
        giver = granule_of(step, ranks) // shard_granules
        wait_landed(
            giver, grad_ref.at[0], landed_ref.at[step], granule_send.at[0], granule_recv.at[step]
        )
        return carry

    lax.fori_loop(0, owned, landed, 0)
    for copy in output_copies + copies:
        copy.start()
    for copy in loads:
        copy.wait()

    def share_copy(far):
        return remote(
            share_ref, shares_ref.at[row], share_send.at[far], share_recv.at[far],
            {"expert": lax.rem(row + far, owners)},
        )

    def attend(index, carry):
        tile = own_tile(index, ranks)
        at = lanes(tile)
        query_t = query_t_ref[:, lanes(index)]
        @pl.when(index == own_tiles // 2)
        def _():
            for copy in output_copies:
                copy.wait()
            total = output_in_ref[0].astype(F32)
            for giver in range(1, context):
                total = total + output_in_ref[giver].astype(F32)
            share_ref[...] = total.astype(BF16)

        @pl.when(index == own_tiles // 2 + 1)
        def _():
            for far in range(1, owners):
                share_copy(far).start()

        grad_rows = landed_ref[pl.ds(2 * index, 2)].reshape(TILE, width)
        grad_t = grad_rows.astype(F32).T
        query_rows = query_t.astype(F32).T.astype(BF16)
        query_ids = ids_all_ref[0:1, at]
        deltas, tops, grads_low = [], [], []
        for head in range(heads):
            rows = slice(head * size, (head + 1) * size)
            query_ref[head] = query_rows[:, rows]
            own_grad_ref[head] = grad_rows[:, rows]
            deltas.append(
                jnp.sum(grad_t[rows] * out_t_ref[rows, lanes(index)], axis=0, keepdims=True)
            )
            tops.append(lse_ref[head : head + 1, lanes(index)])
        grad_t_low = grad_t.astype(BF16)
        dq_ref[...] = jnp.zeros_like(dq_ref)

        def chunk(step, carry, masked):
            here = lanes(step)
            if masked:
                allowed = ids_all_ref[:, here].T[:, 0:1] <= query_ids
            for head in range(heads):
                rows = slice(head * size, (head + 1) * size)
                scores = dot(key_ref[head, here, :], query_t[rows]) - tops[head]
                if masked:
                    scores = jnp.where(allowed, scores, NEGATIVE)
                probs = jnp.exp(scores)
                grad_probs = dot(value_ref[head, here, :], grad_t_low[rows])
                grad_scores = (probs * (grad_probs - deltas[head])).astype(BF16)
                dv_ref[head, here, :] += dot(probs.astype(BF16), own_grad_ref[head])
                dk_ref[head, here, :] += dot(grad_scores, query_ref[head])
                dq_ref[rows, :] += dot(key_t_ref[rows, here], grad_scores)
            return carry

        stop = jnp.minimum(tile + 2, tiles)
        lax.fori_loop(0, tile, lambda s, c: chunk(s, c, False), 0)
        lax.fori_loop(tile, stop, lambda s, c: chunk(s, c, True), 0)
        grad_query = turn(
            dq_ref[...] * scale, cos_ref[:, at], sin_ref[:, at], heads, size, back=True
        )
        grad_w_ref[:width, :] += dot(grad_query.astype(BF16), a_ref[at, :])
        da_ref[at, :] = dot(grad_query.T.astype(BF16), wt_ref[:width, :]).astype(BF16)
        return carry

    lax.fori_loop(0, own_tiles, attend, 0)

    def finish(step, carry):
        at = lanes(step)
        key_grad = jnp.concatenate([dk_ref[head, at, :].T for head in range(heads)], axis=0)
        key_grad = turn(key_grad, cos_ref[:, at], sin_ref[:, at], heads, size, back=True)
        value_grad = jnp.concatenate([dv_ref[head, at, :].T for head in range(heads)], axis=0)
        both = jnp.concatenate([key_grad, value_grad], axis=0)
        grad_w_ref[width:, :] += dot(both.astype(BF16), a_ref[at, :])
        total = da_ref[at, :].astype(F32) + dot(both.T.astype(BF16), wt_ref[width:, :])
        da_ref[at, :] = total.astype(BF16)

        @pl.when(step > 0)
        def _():
            keep(step - 1).start()

        return carry

    def keep(step):
        at = lanes(step)
        return pltpu.make_async_copy(da_ref.at[at, :], da_out.at[at, :], da_sem.at[step])

    def kept(step, carry):
        keep(step).wait()
        return carry

    lax.fori_loop(0, tiles, finish, 0)
    for piece in range(pieces_ref.shape[0]):
        pieces_ref[piece] = grad_w_ref[:, piece * shard : (piece + 1) * shard].astype(BF16)
    keep(tiles - 1).start()
    for copy in copies:
        copy.wait()
    lax.fori_loop(0, tiles, kept, 0)
    for far in range(1, owners):
        share_copy(far).wait()
    shares_ref[row] = share_ref[...]
    total = shares_ref[0].astype(F32)
    for giver in range(1, owners):
        total = total + shares_ref[giver].astype(F32)
    output_sum_ref[...] = total

    def settle(step, carry):
        wait_sent(*outgoing(step))
        return carry

    lax.fori_loop(0, owned, settle, 0)


def attn_backward(
    grad_own, a_full, weights_t, cos_t, sin_t, ids, kept,
    grad_wide, outs, grad_output, heads, size, ranks, context, roles, number,
):
    length, model = a_full.shape
    width = heads * size
    owners = outs.shape[0]
    shard = model // context
    shapes = (
        jax.ShapeDtypeStruct(a_full.shape, BF16),
        jax.ShapeDtypeStruct((context, weights_t.shape[0], shard), BF16),
        jax.ShapeDtypeStruct((shard, model), F32),
        jax.ShapeDtypeStruct((context, 2, shard, grad_wide.shape[2]), BF16),
        jax.ShapeDtypeStruct(outs.shape, BF16),
    )
    dims = (heads, size, ranks, size ** (-0.5), context, owners, roles)
    return pl.pallas_call(
        functools.partial(attn_backward_kernel, dims),
        out_shape=shapes,
        in_specs=hbm(15),
        out_specs=hbm(1) + vmem(2) + hbm(2),
        scratch_shapes=[
            pltpu.VMEM(array.shape, array.dtype)
            for array in (a_full, weights_t, cos_t, sin_t, ids) + kept + (a_full,)
        ]
        + [
            pltpu.SemaphoreType.DMA((11,)),
            pltpu.SemaphoreType.DMA((length // TILE,)),
            pltpu.VMEM((heads, TILE, size), BF16),
            pltpu.VMEM((heads, TILE, size), BF16),
            pltpu.VMEM((width, TILE), F32),
            pltpu.VMEM((heads, length, size), F32),
            pltpu.VMEM((heads, length, size), F32),
            pltpu.VMEM(weights_t.shape, F32),
            pltpu.VMEM(grad_own.shape, BF16),
            pltpu.VMEM((context, shard, model), BF16),
            pltpu.VMEM((shard, model), BF16),
            pltpu.VMEM((owners, shard, model), BF16),
        ]
        + [pltpu.SemaphoreType.DMA((grad_own.shape[0],))] * 2
        + [pltpu.SemaphoreType.DMA((owners,))] * 2
        + [pltpu.SemaphoreType.DMA((context,))] * 4
        + [pltpu.SemaphoreType.DMA((owners,))] * 2
        + [pltpu.SemaphoreType.DMA((3,))],
        compiler_params=params(number, 63),
        cost_estimate=cost(60),
        name="attn_backward",
    )(
        grad_own, a_full, weights_t, cos_t, sin_t, ids, *kept,
        grad_wide, outs, grad_output,
    )


def moe_kernel(
    context, owners, roles, square,
    gates_ref, rows_ref, grads_hbm, wide_hbm, down_hbm,
    dots_back, grad_back, out_back, grad_wide_out, down_in,
    gates_all, rows_all, rows_stage, grads_ref, wide_ref, down_ref,
    rows_t_ref, dye_ref, out_acc, grad_acc, grad_wide_ref, grad_down_ref,
    dots_ref, grad_low, out_low, dots_twin, grad_twin, out_twin,
    dots_sum, grad_sum, out_sum, dots_relay, grad_relay,
    load_sem, local_sem, send_sem, recv_sem, pass_sem, land_sem, twin_sem, come_sem,
    relay_sem, reach_sem, down_send, down_recv, down_on, back_send, back_recv,
    pair_send, pair_recv, home_send, home_recv, lend_send, lend_recv, on_send, on_recv,
    out_send, out_recv, loan_send, loan_recv,
):
    chips = context // 2
    cap, width = rows_all.shape[1:]
    flat = dye_ref.shape
    loads = [
        pltpu.make_async_copy(source, target, load_sem.at[index])
        for index, (source, target) in enumerate(((grads_hbm, grads_ref), (wide_hbm, wide_ref)))
    ]
    for copy in loads:
        copy.start()
    place, row = meet(context, owners)
    chip, core = place // 2, lax.rem(place, 2)
    partner = {"context": place + 1 - 2 * core}
    slot = chip // (chips // roles)
    other = (roles - 1) - slot
    twin = {"context": 2 * lax.rem(chip + chips // 2, chips) + core}

    def block(spot, side, peer):
        return (spot * 2 + side) * owners + peer

    sent, local, passed, lent, relayed = {}, [], [], {}, []
    for far in range(1, owners):
        peer = lax.rem(row + far, owners)
        pairs = [
            (gates_ref.at[peer], gates_all.at[block(slot, core, row)]),
            (rows_ref.at[peer, slot], rows_all.at[block(slot, core, row)]),
        ]
        if roles > 1:
            pairs.append((rows_ref.at[peer, other], rows_stage.at[row]))
        for item, (source, target) in enumerate(pairs):
            sent[item, far] = remote(
                source, target, send_sem.at[item, far], recv_sem.at[item, far], {"expert": peer}
            )
            sent[item, far].start()
    mine = block(slot, core, row)
    for item, (source, target) in enumerate(
        ((gates_ref.at[row], gates_all.at[mine]), (rows_ref.at[row, slot], rows_all.at[mine]))
    ):
        local.append(pltpu.make_async_copy(source, target, local_sem.at[item]))
        local[-1].start()
        passed.append(
            remote(source, target, pass_sem.at[item, 0], land_sem.at[item, 0], partner)
        )
        passed[-1].start()
    if roles > 1:
        for item, (source, everything) in enumerate(
            ((gates_ref.at[row], gates_all), (rows_ref.at[row, other], rows_all))
        ):
            lent[item, 0] = (
                remote(
                    source, everything.at[mine], twin_sem.at[item, 0], come_sem.at[item, 0], twin
                ),
                everything.at[block(other, core, row)],
            )
            lent[item, 0][0].start()

    half = place // chips
    down_rows = down_hbm.shape[1]
    mark = lax.rem(place, chips)
    spot_down = down_ref.at[span(mark, down_rows), :]

    def down_copy(far, here):
        to_chip = chip_at(chip, far, chips, square)
        source = down_hbm.at[to_chip // (chips // roles)]
        if here:
            return pltpu.make_async_copy(source, spot_down, down_recv.at[mark])
        return remote(
            source, spot_down, down_send.at[far], down_recv.at[mark],
            {"context": 2 * to_chip + half},
        )

    @pl.when(half == core)
    def _():
        down_copy(0, True).start()

    @pl.when(half != core)
    def _():
        down_copy(0, False).start()

    fars = [1, 2] if square else list(range(1, chips))
    for far in fars:
        down_copy(far, False).start()

    def arrival(number):
        wait_landed(
            core * chips + number, down_hbm.at[0], down_ref.at[span(number, down_rows), :],
            down_send.at[0], down_recv.at[number],
        )

    def onward(number):
        land = down_ref.at[span(number, down_rows), :]
        return remote(
            land, land, down_on.at[number], down_recv.at[number],
            {"context": 2 * chip_at(chip, 1, chips, square) + core},
        )

    def from_below(number):
        return (core * chips + number) // 2 == chip_at(chip, 2, chips, square)

    for far in range(1, owners):
        peer = lax.rem(row + owners - far, owners)
        for item, everything in enumerate((gates_all, rows_all)):
            sent[item, far].wait_recv()
            landed = everything.at[block(slot, core, peer)]
            passed.append(
                remote(landed, landed, pass_sem.at[item, far], land_sem.at[item, far], partner)
            )
            passed[-1].start()
            if roles > 1:
                if item == 1:
                    sent[2, far].wait_recv()
                lent[item, far] = (
                    remote(
                        landed if item == 0 else rows_stage.at[peer], landed,
                        twin_sem.at[item, far], come_sem.at[item, far], twin,
                    ),
                    everything.at[block(other, core, peer)],
                )
                lent[item, far][0].start()
        if square and far == 1:
            for number in range(chips):

                @pl.when(from_below(number))
                def _():
                    arrival(number)
                    onward(number).start()

    for (item, far), (copy, arriving) in lent.items():
        copy.wait_recv()
        relayed.append(
            remote(
                arriving, arriving, relay_sem.at[item, far], reach_sem.at[item, far], partner
            )
        )
        relayed[-1].start()
    for number in range(chips):
        if square:

            @pl.when(from_below(number))
            def _():
                onward(number).wait_send()

            @pl.when(jnp.logical_not(from_below(number)))
            def _():
                arrival(number)

        else:
            arrival(number)
    for copy in loads + local:
        copy.wait()
    for copy in passed + relayed:
        copy.wait()

    blocks = roles * 2 * owners
    rows_t_ref[...] = rows_all[...].reshape(flat).astype(F32).T.astype(BF16)

    def scale(number, carry):
        columns = gates_all[number].T[:cap]
        column = columns[:, 0:1]
        if roles > 1:
            column = jnp.where(slot == 0, column, columns[:, 1:2])
        dye_ref[span(number, cap), :] = (grads_ref[number].astype(F32) * column).astype(BF16)
        return carry

    lax.fori_loop(0, blocks, scale, 0)
    out_acc[...] = jnp.zeros_like(out_acc)
    grad_acc[...] = jnp.zeros_like(grad_acc)
    back_rows = down_in.shape[1]
    per_step = HIDDEN_TILE // back_rows
    tiles = wide_ref.shape[2] // HIDDEN_TILE

    def leaving(index):
        return (
            core * chips + index, grad_down_ref.at[index], down_in.at[chip],
            back_send.at[index], back_recv.at[chip],
        )

    def hidden_tile(step, carry):
        tile = lax.rem(step + (1 - lax.rem(chip, 2)) * (tiles // 2), tiles)
        at = span(tile, HIDDEN_TILE)
        rows = rows_all[...].reshape(flat)
        dye = dye_ref[...]
        gate, up, down = wide_ref[0, :, at], wide_ref[1, :, at], down_ref[at, :]
        gate_pre = dot(rows, gate)
        up_pre = dot(rows, up)
        sigmoid = jax.nn.sigmoid(gate_pre)
        silu = gate_pre * sigmoid
        hidden = silu * up_pre
        grad_down = dot(hidden.T.astype(BF16), dye).astype(BF16)
        for index in range(per_step):
            grad_down_ref[tile * per_step + index] = grad_down[
                index * back_rows : (index + 1) * back_rows
            ]
        grad_hidden = dot(dye, down, 1, 1).astype(BF16).astype(F32)
        for index in range(per_step):
            here_or_away(*leaving(tile * per_step + index))
        out_acc[...] += dot(hidden.astype(BF16), down).reshape(out_acc.shape)
        grad_gate = (
            grad_hidden * up_pre * sigmoid * (1.0 + gate_pre * (1.0 - sigmoid))
        ).astype(BF16)
        grad_up = (grad_hidden * silu).astype(BF16)
        grad_wide_ref[0, :, at] = dot(rows_t_ref[...], grad_gate).astype(BF16)
        grad_wide_ref[1, :, at] = dot(rows_t_ref[...], grad_up).astype(BF16)
        total = dot(grad_gate, gate, 1, 1) + dot(grad_up, up, 1, 1)
        grad_acc[...] += total.reshape(grad_acc.shape)
        return carry

    lax.fori_loop(0, tiles, hidden_tile, 0)
    store = pltpu.make_async_copy(grad_wide_ref, grad_wide_out, load_sem.at[2])
    store.start()

    order = list(range(1, owners)) + [0]
    turns = (other, slot) if roles > 1 else (slot,)
    pair, gone, loaned, handed, outs, loans = {}, {}, {}, {}, [], []
    items = (
        (dots_ref, dots_twin, dots_sum, dots_relay, dots_back),
        (grad_low, grad_twin, grad_sum, grad_relay, grad_back),
    )

    def share(which, far):
        spot, peer = turns[which], lax.rem(row + far, owners)
        sources = (dots_ref.at[block(spot, 1 - core, peer)], grad_low.at[spot, peer])
        for item, source in enumerate(sources):
            pair[item, which, far] = remote(
                source, items[item][1].at[spot, peer],
                pair_send.at[item, which, far], pair_recv.at[item, which, far], partner,
            )
            pair[item, which, far].start()

    def line(number):
        product = out_acc[number] * grads_ref[number].astype(F32)
        total = product[:, :128]
        for start in range(128, width, 128):
            total = total + product[:, start : start + 128]
        totals = jnp.sum(total.T, axis=0, keepdims=True)
        dots_ref[number, :, :cap] = jnp.broadcast_to(totals, (8, cap))

    def lower(step, carry):
        spot, peer = step // owners, lax.rem(step, owners)
        number = block(spot, 1 - core, peer)
        grad_low[spot, peer] = grad_acc[number].astype(BF16)
        line(number)
        return carry

    def lower_out(step, carry):
        spot, peer = step // owners, lax.rem(step, owners)
        out_low[spot, peer] = out_acc[block(spot, 1 - core, peer)].astype(BF16)
        line(block(spot, core, peer))
        return carry

    lax.fori_loop(0, roles * owners, lower, 0)
    for far in order:
        for which in range(len(turns)):
            share(which, far)
    lax.fori_loop(0, roles * owners, lower_out, 0)
    for which, spot in enumerate(turns):
        outs.append(
            remote(
                out_low.at[spot], out_twin.at[spot], out_send.at[which], out_recv.at[which],
                partner,
            )
        )
        outs[-1].start()

    def leave(which, far):
        peer = lax.rem(row + far, owners)
        spot = turns[which]
        for item, (_, _, total, relay, back) in enumerate(items):
            if roles > 1 and which == 0:
                target = back.at[row, slot] if far == 0 else relay.at[peer]
                loaned[item, far] = remote(
                    total.at[spot, peer], target, lend_send.at[item, far],
                    lend_recv.at[item, far], twin,
                )
                loaned[item, far].start()
            elif far > 0:
                gone[item, far] = remote(
                    total.at[spot, peer], back.at[row, slot], home_send.at[item, far],
                    home_recv.at[item, far], {"expert": peer},
                )
                gone[item, far].start()

    last = None
    for far in order:
        peer = lax.rem(row + far, owners)
        for which, spot in enumerate(turns):
            number = block(spot, core, peer)
            for item in range(2):
                pair[item, which, far].wait_recv()
            dots_sum[spot, peer] = dots_ref[number] + dots_twin[spot, peer]

            def add(part, carry, number=number, spot=spot, peer=peer):
                at = pl.ds(pl.multiple_of(part * (cap // 3), cap // 3), cap // 3)
                grad_sum[spot, peer, at, :] = (
                    grad_acc[number, at, :] + grad_twin[spot, peer, at, :].astype(F32)
                ).astype(BF16)
                return carry

            lax.fori_loop(0, 3, add, 0)
            if last is not None:
                leave(*last)
            last = (which, far)
    dots_back[row, slot] = dots_sum[slot, row]
    grad_back[row, slot] = grad_sum[slot, row]
    leave(*last)
    if roles > 1:
        for far in range(1, owners):
            peer = lax.rem(row + far, owners)
            for item, (_, _, _, relay, back) in enumerate(items):
                loaned[item, far].wait_recv()
                handed[item, far] = remote(
                    relay.at[peer], back.at[row, other], on_send.at[item, far],
                    on_recv.at[item, far], {"expert": peer},
                )
                handed[item, far].start()
    for which, spot in enumerate(turns):
        outs[which].wait_recv()

        def add_out(peer, carry, which=which, spot=spot):
            summed = out_acc[block(spot, core, peer)] + out_twin[spot, peer].astype(F32)
            if roles > 1 and which == 0:
                out_sum[peer] = summed.astype(BF16)
            else:
                out_back[peer, slot] = summed.astype(BF16)
            return carry

        lax.fori_loop(0, owners, add_out, 0)
    if roles > 1:
        loans.append(remote(out_sum, out_back.at[:, slot], loan_send, loan_recv, twin))
        loans[-1].start()
        for item in range(2):
            loaned[item, 0].wait_recv()
    for copy in sent.values():
        copy.wait_send()
    for copy, _ in lent.values():
        copy.wait_send()
    for far in fars:
        down_copy(far, False).wait_send()

    @pl.when(half != core)
    def _():
        down_copy(0, False).wait_send()

    for index in range(chips):
        wait_sent(*leaving(index))
        wait_landed(
            2 * index + place // chips, grad_down_ref.at[0], down_in.at[index],
            back_send.at[index], back_recv.at[index],
        )
    for copy in list(pair.values()) + outs + list(loaned.values()):
        copy.wait_send()
    for copy in list(gone.values()) + list(handed.values()) + loans + [store]:
        copy.wait()


def moe(gates, rows, grads, wide_full, down_weight, context, roles, number):
    owners, _, cap, width = rows.shape
    chips = context // 2
    hidden = wide_full.shape[2]
    blocks = roles * 2 * owners
    slots = blocks * cap
    line = gates.shape[1:]
    square = chips == 4 and roles == 2
    low = (owners, cap, width)
    back = (chips, hidden // chips, width)
    dma = pltpu.SemaphoreType.DMA
    return pl.pallas_call(
        functools.partial(moe_kernel, context, owners, roles, square),
        out_shape=(
            jax.ShapeDtypeStruct((owners, roles) + line, F32),
            jax.ShapeDtypeStruct((owners, roles, cap, width), BF16),
            jax.ShapeDtypeStruct((owners, roles, cap, width), BF16),
            jax.ShapeDtypeStruct(wide_full.shape, BF16),
            jax.ShapeDtypeStruct(back, BF16),
        ),
        in_specs=vmem(2) + hbm(3),
        out_specs=vmem(3) + hbm(2),
        scratch_shapes=[
            pltpu.VMEM((blocks,) + line, F32),
            pltpu.VMEM((blocks, cap, width), BF16),
            pltpu.VMEM(low, BF16),
            pltpu.VMEM((blocks, cap, width), BF16),
            pltpu.VMEM(wide_full.shape, BF16),
            pltpu.VMEM((hidden, width), BF16),
            pltpu.VMEM((width, slots), BF16),
            pltpu.VMEM((slots, width), BF16),
            pltpu.VMEM((blocks, cap, width), F32),
            pltpu.VMEM((blocks, cap, width), F32),
            pltpu.VMEM(wide_full.shape, BF16),
            pltpu.VMEM(back, BF16),
            pltpu.VMEM((blocks,) + line, F32),
            pltpu.VMEM((roles,) + low, BF16),
            pltpu.VMEM((roles,) + low, BF16),
            pltpu.VMEM((roles, owners) + line, F32),
            pltpu.VMEM((roles,) + low, BF16),
            pltpu.VMEM((roles,) + low, BF16),
            pltpu.VMEM((roles, owners) + line, F32),
            pltpu.VMEM((roles,) + low, BF16),
            pltpu.VMEM(low, BF16),
            pltpu.VMEM((owners,) + line, F32),
            pltpu.VMEM(low, BF16),
            dma((3,)),
            dma((2,)),
        ]
        + [dma((3, owners))] * 8
        + [dma((chips,))] * 5
        + [dma((2, roles, owners))] * 2
        + [dma((2, owners))] * 6
        + [dma((roles,))] * 2
        + [dma] * 2,
        compiler_params=params(number, 62),
        cost_estimate=cost(97),
        name="moe",
    )(gates, rows, grads.reshape(blocks, cap, width), wide_full, down_weight)


def finish_kernel(
    chips, owners, groups,
    da_ref, pieces_ref, small_ref, slots_ref, gates_ref, gain_ref, query_w, key_w, value_w,
    base_hbm, returned_hbm, after_hbm, hidden_hbm,
    layer_ref, total_ref, query_ref, key_ref, value_ref, dots_ref, small_all_ref,
    sums_ref, base_ref, returned_ref, after_ref, hidden_ref, columns_ref, da_own, load_sem,
    own_sem,
    da_twin, da_sum, da_in, w_twin, w_sum, w_in, s_twin, s_sum, s_in, s_total,
    stack_ref, shares, shares_in, block_ref,
    pair_send, pair_recv, chip_send, chip_recv, row_send, row_recv,
):
    own_core = lax.rem(lax.axis_index("context"), 2)
    owns = [
        pltpu.make_async_copy(da_ref.at[2 * index + own_core], da_own.at[index], own_sem.at[index])
        for index in range(chips)
    ]
    for copy in owns:
        copy.start()
    loads = [
        pltpu.make_async_copy(source, target, load_sem.at[index])
        for index, (source, target) in enumerate(
            (
                (base_hbm, base_ref), (returned_hbm, returned_ref), (after_hbm, after_ref),
                (hidden_hbm, hidden_ref),
            )
        )
    ]
    for copy in loads:
        copy.start()
    place = lax.axis_index("context")
    row = lax.axis_index("expert")
    chip, core = place // 2, lax.rem(place, 2)
    partner = 2 * chip + 1 - core
    barrier = pltpu.get_barrier_semaphore()

    def greet(device):
        pl.semaphore_signal(
            barrier, inc=1, device_id=device, device_id_type=pl.DeviceIdType.MESH
        )

    greet({"context": partner})
    for far in range(1, chips):
        greet({"context": 2 * lax.rem(chip + far, chips) + core})
    for far in range(1, owners):
        greet({"expert": lax.rem(row + far, owners)})
    pl.semaphore_wait(barrier, chips + owners - 1)

    order = list(range(1, chips)) + [0]
    pair = {}
    for item, (source, target) in enumerate(
        ((small_ref, s_twin), (pieces_ref, w_twin), (da_ref, da_twin))
    ):
        for far in order:
            peer = lax.rem(chip + far, chips)
            pair[item, far] = remote(
                source.at[2 * peer + 1 - core], target.at[peer],
                pair_send.at[item, far], pair_recv.at[item, far], {"context": partner},
            )
            pair[item, far].start()

    def across(item, source, target, far):
        peer = lax.rem(chip + far, chips)
        return remote(
            source.at[peer], target.at[chip], chip_send.at[item, far], chip_recv.at[item, far],
            {"context": 2 * peer + core},
        )

    for far in order:
        peer = lax.rem(chip + far, chips)
        mine = 2 * peer + core
        pair[0, far].wait_recv()
        s_sum[peer] = small_ref[mine] + s_twin[peer]
        pair[1, far].wait_recv()
        w_sum[peer] = (
            pieces_ref[mine].astype(F32) + w_twin[peer].astype(F32)
        ).astype(BF16)
    moved = {}
    for far in range(1, chips):
        moved[0, far] = across(0, s_sum, s_in, far)
        moved[0, far].start()
        moved[1, far] = across(1, w_sum, w_in, far)
        moved[1, far].start()
    last = None
    for copy in owns:
        copy.wait()
    for far in order:
        peer = lax.rem(chip + far, chips)
        pair[2, far].wait_recv()
        da_sum[peer] = (
            da_own[peer].astype(F32) + da_twin[peer].astype(F32)
        ).astype(BF16)
        if last is not None:
            moved[2, last] = across(2, da_sum, da_in, last)
            moved[2, last].start()
        last = far
    for far in range(1, chips):
        moved[0, far].wait_recv()
        moved[1, far].wait_recv()
    s_in[chip] = s_sum[chip]
    w_in[chip] = w_sum[chip]

    width = w_sum.shape[1] // 3
    shard = w_sum.shape[2]
    per_group = chips // groups
    for group in range(groups):
        total = w_in[group * per_group].astype(F32)
        for other in range(1, per_group):
            total = total + w_in[group * per_group + other].astype(F32)
        for which in range(3):
            stack_ref[which * shard : (which + 1) * shard, group * width : (group + 1) * width] = (
                total[which * width : (which + 1) * width].T
            )
    lines = shares.shape[1]
    for owner in range(owners):
        shares[owner] = stack_ref[owner * lines : (owner + 1) * lines, :].astype(BF16)
    total = s_in[0]
    for other in range(1, chips):
        total = total + s_in[other]
    s_total[...] = total
    rows = {}
    for far in range(1, owners):
        peer = lax.rem(row + far, owners)
        rows[0, far] = remote(
            shares.at[peer], shares_in.at[row], row_send.at[0, far], row_recv.at[0, far],
            {"expert": peer},
        )
        rows[0, far].start()
        rows[1, far] = remote(
            s_total, small_all_ref.at[row], row_send.at[1, far], row_recv.at[1, far],
            {"expert": peer},
        )
        rows[1, far].start()
    shares_in[row] = shares[row]
    small_all_ref[row] = total
    for copy in loads:
        copy.wait()
    count = returned_ref.shape[0]
    chunk = 128
    columns_ref[...] = slots_ref[...].T

    def layer(step, carry):
        at = span(step, chunk)
        places = lax.broadcasted_iota(jnp.int32, (chunk, count), 1).astype(F32)
        total = base_ref[at, :]
        for which in range(2):
            hit = (places == columns_ref[at, which : which + 1]).astype(F32).astype(BF16)
            total = total + gates_ref[at, which : which + 1] * dot(hit, returned_ref[...])
        layer_ref[at, :] = total.astype(BF16)
        return carry

    lax.fori_loop(0, layer_ref.shape[0] // chunk, layer, 0)
    for far in range(1, owners):
        rows[0, far].wait_recv()
    summed = shares_in[0].astype(F32)
    for other in range(1, owners):
        summed = summed + shares_in[other].astype(F32)
    block_ref[...] = summed.astype(BF16)
    for far in range(1, chips):
        moved[2, far].wait_recv()
    for far in range(1, owners):
        peer = lax.rem(row + far, owners)
        rows[2, far] = remote(
            block_ref, sums_ref.at[row], row_send.at[2, far], row_recv.at[2, far],
            {"expert": peer},
        )
        rows[2, far].start()
    sums_ref[row] = summed.astype(BF16)
    da_in[chip] = da_sum[chip]

    def input_rows(step, carry):
        at = span(step, chunk)
        total = da_in[0, at, :].astype(F32)
        for other in range(1, chips):
            total = total + da_in[other, at, :].astype(F32)
        grads = total * gain_ref[...]
        values = hidden_ref[at, :].astype(F32)
        inverse = lax.rsqrt(jnp.mean(values * values, axis=1, keepdims=True) + EPS)
        normed = values * inverse
        mean = jnp.mean(grads * normed, axis=1, keepdims=True)
        total_ref[at, :] = after_ref[at, :] + inverse * (grads - normed * mean)
        return carry

    lax.fori_loop(0, layer_ref.shape[0] // chunk, input_rows, 0)
    for far in range(1, owners):
        rows[1, far].wait_recv()
        rows[2, far].wait_recv()
    for owner in range(owners):
        stack_ref[owner * lines : (owner + 1) * lines, :] = sums_ref[owner].astype(F32)
    dots = jnp.zeros((shard, 1), F32)
    for which, (target, weight) in enumerate(
        ((query_ref, query_w), (key_ref, key_w), (value_ref, value_w))
    ):
        grads = stack_ref[which * shard : (which + 1) * shard, :]
        target[...] = grads
        dots = dots + jnp.sum(grads * weight[...].astype(F32), axis=1, keepdims=True)
    dots_ref[...] = dots
    for copy in list(pair.values()) + list(moved.values()) + list(rows.values()):
        copy.wait_send()


def finish(da, pieces, small, small_inputs, bulk, owners, groups, number):
    context, tokens, width = da.shape
    chips = context // 2
    lines, shard = pieces.shape[1:]
    few = small.shape[1]
    stack = 3 * shard
    block = (stack // owners, width)
    return pl.pallas_call(
        functools.partial(finish_kernel, chips, owners, groups),
        out_shape=(
            jax.ShapeDtypeStruct((tokens, width), BF16),
            jax.ShapeDtypeStruct((tokens, width), F32),
            jax.ShapeDtypeStruct((shard, width), F32),
            jax.ShapeDtypeStruct((shard, width), F32),
            jax.ShapeDtypeStruct((shard, width), F32),
            jax.ShapeDtypeStruct((shard, 1), F32),
            jax.ShapeDtypeStruct((owners, few, shard), F32),
        ),
        in_specs=hbm(1) + vmem(8) + hbm(4),
        out_specs=vmem(7),
        scratch_shapes=[pltpu.VMEM((owners,) + block, BF16)]
        + [pltpu.VMEM(array.shape, array.dtype) for array in bulk]
        + [
            pltpu.VMEM((tokens, 8), F32),
            pltpu.VMEM((chips, tokens, width), BF16),
            pltpu.SemaphoreType.DMA((4,)),
            pltpu.SemaphoreType.DMA((chips,)),
            pltpu.VMEM((chips, tokens, width), BF16),
            pltpu.VMEM((chips, tokens, width), BF16),
            pltpu.VMEM((chips, tokens, width), BF16),
            pltpu.VMEM((chips, lines, shard), BF16),
            pltpu.VMEM((chips, lines, shard), BF16),
            pltpu.VMEM((chips, lines, shard), BF16),
            pltpu.VMEM((chips, few, shard), F32),
            pltpu.VMEM((chips, few, shard), F32),
            pltpu.VMEM((chips, few, shard), F32),
            pltpu.VMEM((few, shard), F32),
            pltpu.VMEM((stack, width), F32),
            pltpu.VMEM((owners,) + block, BF16),
            pltpu.VMEM((owners,) + block, BF16),
            pltpu.VMEM(block, BF16),
            pltpu.SemaphoreType.DMA((3, chips)),
            pltpu.SemaphoreType.DMA((3, chips)),
            pltpu.SemaphoreType.DMA((3, chips)),
            pltpu.SemaphoreType.DMA((3, chips)),
            pltpu.SemaphoreType.DMA((3, owners)),
            pltpu.SemaphoreType.DMA((3, owners)),
        ],
        compiler_params=pltpu.CompilerParams(
            collective_id=number, has_side_effects=True, vmem_limit_bytes=60 << 20
        ),
        name="finish",
    )(da, pieces, small, *small_inputs, *bulk)


def shards(
    hidden_in,
    prior_logits,
    routes,
    block_ids,
    grad_out,
    attn_gain,
    query_weight,
    key_weight,
    value_weight,
    output_weight,
    moe_gain,
    router_weight,
    prior_weight,
    const_mix,
    const_vector,
    gate_weight,
    up_weight,
    down_weight,
):
    token_rows = hidden_in.shape[1]
    model_width = hidden_in.shape[2]
    head_size = model_width // HEADS
    context = lax.axis_size("context")
    owners = lax.axis_size("expert")
    groups = math.gcd(HEADS, context)
    ranks = context // groups
    heads = HEADS // groups
    width = heads * head_size
    length = context * token_rows
    per_owner = gate_weight.shape[0]
    slot_count = per_owner * owners * CAP
    shard_width = model_width // context
    roles = per_owner
    residual = hidden_in[0].astype(F32)
    prior_rows = prior_logits[0]
    route_rows = routes[0]
    cotangent_low = grad_out[0]
    cotangent = cotangent_low.astype(F32)

    half = head_size // 2
    freq = jnp.power(THETA, -2.0 * jnp.arange(half, dtype=F32) / head_size)
    steps = jnp.concatenate(
        [jnp.arange(token_rows), jnp.arange(context) * token_rows]
    ).astype(F32)
    angle = freq[:, None] * steps[None, :]

    gain_row = attn_gain.reshape(1, model_width)
    (
        out_t, log_total, query_t, ids, weights_t, cos_t, sin_t, slots, key_heads, key_t,
        value_heads, a_full, mix_granules, output_full, wide_full, grad_arrived, _,
    ) = attn_forward(
        hidden_in[0], gain_row, block_ids, jnp.transpose(route_rows), cotangent_low,
        jnp.cos(angle), jnp.sin(angle), query_weight, key_weight, value_weight,
        output_weight, gate_weight, up_weight, heads, head_size, ranks, context, owners, roles, 0,
    )
    kept = (out_t, log_total, query_t, key_heads, key_t, value_heads)
    slot_ids = jnp.arange(slot_count).astype(F32)[:, None]
    hit_first = slot_ids == slots[0:1]
    hit_second = slot_ids == slots[1:2]
    pick_either = hit_first.astype(BF16) + hit_second.astype(BF16)
    blocks = (owners, per_owner, CAP, model_width)

    def pick(rows):
        return jnp.dot(pick_either, rows, preferred_element_type=F32).astype(BF16).reshape(blocks)

    out_blocks = mix_granules.reshape(groups, token_rows, width)
    mix_low = jnp.transpose(out_blocks, (1, 0, 2)).reshape(token_rows, model_width)

    after_attn = residual + jnp.dot(mix_low, output_full, preferred_element_type=F32)
    inv_rms2 = lax.rsqrt(jnp.mean(after_attn * after_attn, axis=1, keepdims=True) + EPS)
    normed_two = after_attn * inv_rms2
    moe_input = normed_two * moe_gain
    narrow = jnp.concatenate(
        [router_weight, jnp.transpose(const_mix.reshape(-1, model_width))], axis=1
    )
    narrow_out = jnp.dot(moe_input, narrow, precision=HIGH, preferred_element_type=F32)
    expert_count = router_weight.shape[1]
    consts = const_mix.shape[0]
    logits = narrow_out[:, :expert_count] + jnp.dot(
        prior_rows, prior_weight, precision=HIGH, preferred_element_type=F32
    )
    probs = jax.nn.softmax(logits, axis=1)
    expert_ids = jnp.arange(expert_count, dtype=jnp.int32)
    first_hot = (route_rows[:, 0:1] == expert_ids[None, :]).astype(F32)
    second_hot = (route_rows[:, 1:2] == expert_ids[None, :]).astype(F32)
    chosen = first_hot + second_hot
    gated = probs * chosen
    first_gate = jnp.sum(probs * first_hot, axis=1, keepdims=True)
    second_gate = jnp.sum(probs * second_hot, axis=1, keepdims=True)
    slot_gate = jnp.sum(
        jnp.where(hit_first, first_gate[None, :, 0], 0.0)
        + jnp.where(hit_second, second_gate[None, :, 0], 0.0),
        axis=1,
    )
    def spread(values):
        values = values.reshape(owners, per_owner, CAP)
        return jnp.pad(values, ((0, 0), (0, 8 - per_owner), (0, 128 - CAP)))

    slot_dot, grad_back, expert_out, grad_wide, down_parts = moe(
        spread(slot_gate), pick(moe_input.astype(BF16)), grad_arrived, wide_full, down_weight,
        context, roles, 2,
    )
    slot_dot = slot_dot[:, :, 0, :CAP].reshape(slot_count)
    grad_back = grad_back.reshape(slot_count, model_width)

    const_soft = jax.nn.softmax(narrow_out[:, expert_count:].reshape(token_rows, consts, 2), axis=2)
    const_gate = gated[:, FFN_E + 2 :]
    copy_gate = gated[:, FFN_E + 1 : FFN_E + 2]
    const_out = [
        const_soft[:, c, 0:1] * moe_input + const_soft[:, c, 1:2] * const_vector[c][None, :]
        for c in range(consts)
    ]
    local_moe = copy_gate * moe_input
    for c in range(consts):
        local_moe = local_moe + const_gate[:, c : c + 1] * const_out[c]
    grad_moe_ffn = lax.dot_general(
        pick_either, grad_back, (((0,), (0,)), ((), ())), preferred_element_type=F32
    )
    first_dot = jnp.sum(jnp.where(hit_first, slot_dot[:, None], 0.0), axis=0)[:, None]
    second_dot = jnp.sum(jnp.where(hit_second, slot_dot[:, None], 0.0), axis=0)[:, None]
    copy_dot = jnp.sum(cotangent * moe_input, axis=1, keepdims=True)
    const_dot = [jnp.sum(cotangent * const_out[c], axis=1, keepdims=True) for c in range(consts)]
    extra = jnp.concatenate(
        [jnp.zeros((token_rows, FFN_E + 1), F32), copy_dot, *const_dot], axis=1
    )
    grad_probs = first_hot * first_dot + second_hot * second_dot + chosen * extra
    grad_logits = probs * (grad_probs - jnp.sum(probs * grad_probs, axis=1, keepdims=True))
    grad_prior_rows = lax.dot_general(
        grad_logits, prior_weight, (((1,), (1,)), ((), ())),
        precision=HIGH, preferred_element_type=F32,
    )
    vector_dot = jnp.dot(
        cotangent, jnp.transpose(const_vector), precision=HIGH, preferred_element_type=F32
    )
    grad_soft = jnp.stack(
        [const_gate * copy_dot, const_gate * vector_dot], axis=2
    )
    grad_mix = const_soft * (grad_soft - jnp.sum(const_soft * grad_soft, axis=2, keepdims=True))
    narrow_grad = jnp.concatenate([grad_logits, grad_mix.reshape(token_rows, -1)], axis=1)
    local_scale = copy_gate + jnp.sum(const_soft[:, :, 0] * const_gate, axis=1, keepdims=True)
    grad_moe_input = (
        grad_moe_ffn
        + lax.dot_general(
            narrow_grad, narrow, (((1,), (1,)), ((), ())),
            precision=HIGH, preferred_element_type=F32,
        )
        + local_scale * cotangent
    )
    small_moe = lax.dot_general(
        narrow_grad, moe_input, (((0,), (0,)), ((), ())),
        precision=HIGH, preferred_element_type=F32,
    )
    small_vector = lax.dot_general(
        const_soft[:, :, 1] * const_gate, cotangent, (((0,), (0,)), ((), ())),
        precision=HIGH, preferred_element_type=F32,
    )
    grad_prior_local = lax.dot_general(
        prior_rows, grad_logits, (((0,), (0,)), ((), ())),
        precision=HIGH, preferred_element_type=F32,
    )
    small_gain = jnp.sum(grad_moe_input * normed_two, axis=0, keepdims=True)
    prior_values = jnp.pad(
        grad_prior_local.reshape(-1), (0, -(expert_count * expert_count) % shard_width)
    ).reshape(-1, 1, shard_width)
    prior_lines = prior_values.shape[0]
    small = jnp.concatenate([small_moe, small_vector, small_gain], axis=0)
    small_lines = small.shape[0]
    small = jnp.concatenate(
        [
            small.reshape(small_lines, context, shard_width),
            jnp.broadcast_to(prior_values, (prior_lines, context, shard_width)),
        ],
        axis=0,
    )
    small = jnp.pad(small, ((0, -small.shape[0] % 8), (0, 0), (0, 0)))
    small = jnp.transpose(small, (1, 0, 2))

    grad_normed_two = grad_moe_input * moe_gain
    grad_after = cotangent + inv_rms2 * (
        grad_normed_two - normed_two * jnp.mean(grad_normed_two * normed_two, axis=1, keepdims=True)
    )
    grad_attn_low = grad_after.astype(BF16)
    grad_mix_low = lax.dot_general(
        grad_attn_low, output_full, (((1,), (1,)), ((), ())), preferred_element_type=F32
    ).astype(BF16)
    grad_pieces = jnp.transpose(grad_mix_low.reshape(token_rows, groups, width), (1, 0, 2))
    grad_own = grad_pieces.reshape(-1, TILE // 2, width)
    grad_output_local = lax.dot_general(
        mix_low, grad_attn_low, (((0,), (0,)), ((), ())), preferred_element_type=F32
    ).astype(BF16)
    da_part, w_pieces, output_sum, wide_parts, returned = attn_backward(
        grad_own, a_full, weights_t, cos_t, sin_t, ids, kept,
        grad_wide, expert_out, grad_output_local,
        heads, head_size, ranks, context, roles, 6,
    )
    returned = returned.reshape(slot_count, model_width)
    same = context // 2 // roles
    wide_parts = wide_parts.reshape(roles, same, 2, 2, shard_width, -1)

    def whole(which):
        total = jnp.sum(wide_parts[:, :, :, which].astype(F32), axis=1)
        return jnp.concatenate([total[:, 0], total[:, 1]], axis=-1)

    down_sum = jnp.sum(
        down_parts.reshape(roles, same, -1, model_width).astype(F32), axis=1
    )
    (
        layer_out, grad_input, grad_query, grad_key, grad_value, gain_dots, small_all,
    ) = finish(
        da_part.reshape(context, token_rows, model_width), w_pieces, small,
        (
            slots, jnp.concatenate([first_gate, second_gate], axis=1), gain_row,
            query_weight, key_weight, value_weight,
        ),
        (after_attn + local_moe, returned, grad_after, hidden_in[0]),
        owners, groups, 5,
    )
    small_own = jnp.sum(small_all, axis=0)
    column = lax.axis_index("context") * shard_width
    grad_attn_gain = gain_dots[:, 0] / lax.dynamic_slice_in_dim(attn_gain, column, shard_width)
    mixes = expert_count + 2 * consts
    grad_prior_weight = small_own[small_lines : small_lines + prior_lines].reshape(-1)
    grad_prior_weight = grad_prior_weight[: expert_count * expert_count].reshape(
        expert_count, expert_count
    )
    return (
        layer_out[None],
        grad_input[None],
        grad_prior_rows[None],
        grad_attn_gain,
        grad_query,
        grad_key,
        grad_value,
        output_sum,
        small_own[small_lines - 1],
        jnp.transpose(small_own[:expert_count]),
        grad_prior_weight,
        small_own[expert_count:mixes].reshape(consts, 2, shard_width),
        small_own[mixes : mixes + consts],
        whole(0),
        whole(1),
        down_sum,
    )


def solution(mesh):
    return jax.shard_map(
        shards,
        mesh=mesh,
        in_specs=(
            P("expert", "context", None),
            P("expert", "context", None),
            P("expert", "context", None),
            P("expert", "context"),
            P("expert", "context", None),
            P(),
            P("context", None),
            P("context", None),
            P("context", None),
            P("context", None),
            P(),
            P(),
            P(),
            P(),
            P(),
            P("expert", "context", None),
            P("expert", "context", None),
            P("expert", "context", None),
        ),
        out_specs=(
            P("expert", "context", None),
            P("expert", "context", None),
            P("expert", "context", None),
            P("context"),
            P("context", None),
            P("context", None),
            P("context", None),
            P("context", None),
            P("context"),
            P("context", None),
            P(),
            P(None, None, "context"),
            P(None, "context"),
            P("expert", "context", None),
            P("expert", "context", None),
            P("expert", "context", None),
        ),
        check_vma=False,
    )
```
